32 devices in a mesh: rep: 4 (over y, x), fsdp: 4 (over z), seq: 2 (over core).
Axes of the slice: x: 2, y: 2, z: 4, core: 2. Of those that a mesh axis runs over, the one named last changes fastest.
Arguments:
- layer_input: bfloat16 [2, 16, 1024, 768], P(None, ('rep', 'fsdp'), 'seq'), may hold values from -6 to 6
- segment: int32 [2, 16, 1024], P(None, ('rep', 'fsdp')), may hold values from 0 to 3, never falling along the last dimension, each value on 1 to 512 neighbouring positions
- rand_blocks: int32 [2, 16, 12, 16, 3], P(None, ('rep', 'fsdp')), may hold values from 0 to 15
- first_gain: bfloat16 [768], P('fsdp'), may hold values from 0.099609375 to 1.8984375
- first_bias: bfloat16 [768], P('fsdp'), may hold values from -1.75 to 1.75
- query_weight: bfloat16 [768, 768], P('fsdp'), may hold values from -0.21875 to 0.21875
- query_bias: bfloat16 [768], P('fsdp'), may hold values from -1.75 to 1.75
- key_weight: bfloat16 [768, 768], P('fsdp'), may hold values from -0.21875 to 0.21875
- value_weight: bfloat16 [768, 768], P('fsdp'), may hold values from -0.21875 to 0.21875
- value_bias: bfloat16 [768], P('fsdp'), may hold values from -1.75 to 1.75
- out_weight: bfloat16 [768, 768], P('fsdp'), may hold values from -1.75 to 1.75
- out_bias: bfloat16 [768], P('fsdp'), may hold values from -1.75 to 1.75
- second_gain: bfloat16 [768], P('fsdp'), may hold values from 0.099609375 to 1.8984375
- second_bias: bfloat16 [768], P('fsdp'), may hold values from -1.75 to 1.75
- up_weight: bfloat16 [768, 3072], P('fsdp'), may hold values from -0.21875 to 0.21875
- up_bias: bfloat16 [3072], P('fsdp'), may hold values from -1.75 to 1.75
- down_weight: bfloat16 [3072, 768], P('fsdp'), may hold values from -0.21875 to 0.21875
- down_bias: bfloat16 [768], P('fsdp'), may hold values from -1.75 to 1.75
- cotangent: bfloat16 [2, 16, 1024, 768], P(None, ('rep', 'fsdp'), 'seq'), may hold values from -6 to 6
Outputs:
- layer_output: bfloat16 [2, 16, 1024, 768], P(None, ('rep', 'fsdp'), 'seq')
- input_grad: bfloat16 [2, 16, 1024, 768], P(None, ('rep', 'fsdp'), 'seq')
- first_gain_grad: float32 [768], P('fsdp')
- first_bias_grad: float32 [768], P('fsdp')
- query_weight_grad: float32 [768, 768], P('fsdp')
- query_bias_grad: float32 [768], P('fsdp')
- key_weight_grad: float32 [768, 768], P('fsdp')
- value_weight_grad: float32 [768, 768], P('fsdp')
- value_bias_grad: float32 [768], P('fsdp')
- out_weight_grad: float32 [768, 768], P('fsdp')
- out_bias_grad: float32 [768], P('fsdp')
- second_gain_grad: float32 [768], P('fsdp')
- second_bias_grad: float32 [768], P('fsdp')
- up_weight_grad: float32 [768, 3072], P('fsdp')
- up_bias_grad: float32 [3072], P('fsdp')
- down_weight_grad: float32 [3072, 768], P('fsdp')
- down_bias_grad: float32 [768], P('fsdp')
The draws below stay inside these ranges and needn't reach their ends.
Inputs may be any that keep to these rules, and one draw needn't show every extreme that they name: segment numbers of a sequence never fall; each document is one run of tokens.
All inputs are finite; a program needn't handle non-finite values.
Results may differ from the reference program's by a relative error of at most 0.02.
Values may be sent and summed in bfloat16 or wider, within the bound.
A program may use at most 192 MiB of HBM per device.

```python
import math
import jax
import jax.numpy as jnp
import numpy as np
from jax import lax

D = 768
HEADS = 12
HDIM = 64
FF = 3072
BLOCK = 64
RAND = 3
LEN = 1024
MB = 2
NBLK = 16
NSEQ = 16


def plant(values, stream_key, smallest, top_value):
    extent = values.shape
    index_at = [jax.random.randint(jax.random.fold_in(stream_key, axis), (), 0, extent[axis]) for axis in range(len(extent))]
    values = values.at[tuple(index_at)].set(smallest)
    longest = extent.index(max(extent))
    index_at[longest] = (index_at[longest] + 1) % extent[longest]
    return values.at[tuple(index_at)].set(top_value)


def shard_levels(key, dims, cuts, least, high):
    factor_of, own = 1.0, jax.random.fold_in(key, 6)
    for axis_at, shards_of in cuts:
        heights = jnp.exp(jax.random.uniform(jax.random.fold_in(own, axis_at), (shards_of,), jnp.float32, least / len(cuts), high / len(cuts)))
        factor_of = factor_of * jnp.repeat(heights, dims[axis_at] // shards_of).reshape([-1 if axis == axis_at else 1 for axis in range(len(dims))])
    return factor_of


def profile(count, total, most, skew):
    loads = [(1 << 20) // math.isqrt(rank ** skew) + 1 for rank in range(2, count + 1)]
    spare, given = total - most - (count - 1), [1] * (count - 1)
    while spare > 0:
        candidates = [i for i in range(count - 1) if given[i] < most]
        whole, budget = sum([loads[i] for i in candidates]), spare
        for i in candidates:
            addition = min(most - given[i], max(1, budget * loads[i] // whole), spare)
            given[i] = given[i] + addition
            spare = spare - addition
    return np.array([most] + given)


def ragged_sizes(key, number_of, total, bound, lean):
    if number_of == 2:
        one = jax.random.randint(key, (), max(1, total - bound), min(bound, total - 1) + 1)
        return jnp.stack([one, total - one])
    tallies = jnp.asarray(profile(number_of, total, bound, lean), jnp.int32)
    couples = (number_of - 1) // 2
    source_of, receiver = tallies[1:1 + 2 * couples:2], tallies[2:2 + 2 * couples:2]
    slack = jnp.minimum(source_of - 1, bound - receiver)
    passed = jax.random.randint(jax.random.fold_in(key, 1), (couples,), 0, 1 << 20) % (slack + 1)
    tallies = tallies.at[1:1 + 2 * couples:2].set(source_of - passed).at[2:2 + 2 * couples:2].set(receiver + passed)
    return tallies[jax.random.permutation(jax.random.fold_in(key, 2), number_of)]


def noise(stream_key, dims, scale, reach, cuts=(), kind=jnp.bfloat16):
    values = jax.random.normal(stream_key, dims, jnp.float32) * scale
    if len(cuts) > 0:
        values = shard_levels(stream_key, dims, cuts, -0.22, 0.18) * values
    return jnp.clip(values, min=-reach, max=reach).astype(kind)


def setup_inputs(seed: int = 0) -> dict:
    arg_keys = jax.random.split(jax.random.key(seed), 20)
    return {
        "layer_input": noise(arg_keys[0], (MB, NSEQ, LEN, D), 1.0, 6.0, ((1, 16), (2, 2))),
        "segment": jax.vmap(lambda own: jnp.searchsorted(jnp.cumsum(ragged_sizes(own, 4, LEN, LEN // 2, 1)), jnp.arange(LEN), side="right"))(jax.random.split(arg_keys[1], MB * NSEQ)).reshape((MB, NSEQ, LEN)).astype(jnp.int32),
        "rand_blocks": plant(jax.random.randint(arg_keys[2], (MB, NSEQ, HEADS, NBLK, RAND), 0, NBLK), jax.random.fold_in(arg_keys[2], 1), 0, NBLK - 1).astype(jnp.int32),
        "first_gain": jnp.clip(1.0 + 0.18 * jax.random.normal(arg_keys[3], (D,), jnp.float32), 0.099609375, 1.8984375).astype(jnp.bfloat16),
        "first_bias": noise(arg_keys[4], (D,), 0.3, 1.75, ((0, 4),)),
        "query_weight": noise(arg_keys[5], (D, D), D ** -0.5, 0.21875, ((0, 4),)),
        "query_bias": noise(arg_keys[6], (D,), 0.3, 1.75, ((0, 4),)),
        "key_weight": noise(arg_keys[7], (D, D), D ** -0.5, 0.21875, ((0, 4),)),
        "value_weight": noise(arg_keys[8], (D, D), D ** -0.5, 0.21875, ((0, 4),)),
        "value_bias": noise(arg_keys[9], (D,), 0.3, 1.75, ((0, 4),)),
        "out_weight": noise(arg_keys[10], (D, D), (D // 64) ** -0.5, 1.75, ((0, 4),)),
        "out_bias": noise(arg_keys[11], (D,), 0.3, 1.75, ((0, 4),)),
        "second_gain": jnp.clip(1.0 + 0.18 * jax.random.normal(arg_keys[12], (D,), jnp.float32), 0.099609375, 1.8984375).astype(jnp.bfloat16),
        "second_bias": noise(arg_keys[13], (D,), 0.3, 1.75, ((0, 4),)),
        "up_weight": noise(arg_keys[14], (D, FF), D ** -0.5, 0.21875, ((0, 4),)),
        "up_bias": noise(arg_keys[15], (FF,), 0.3, 1.75, ((0, 4),)),
        "down_weight": noise(arg_keys[16], (FF, D), (FF // 4) ** -0.5, 0.21875, ((0, 4),)),
        "down_bias": noise(arg_keys[17], (D,), 0.3, 1.75, ((0, 4),)),
        "cotangent": noise(arg_keys[18], (MB, NSEQ, LEN, D), 1.0, 6.0, ((1, 16), (2, 2))),
    }


norm_eps = 1e-05
highest = lax.Precision.HIGHEST

@jax.custom_vjp
def low(v):
    return lax.optimization_barrier(v.astype(jnp.bfloat16)).astype(jnp.float32)

@jax.custom_vjp
def low_back(v):
    return v

def low_keep(v):
    return (low(v), None)

def low_pass(kept, grad):
    return (grad,)

def back_keep(v):
    return (v, None)

def back_low(kept, grad):
    return (low(grad),)
low.defvjp(low_keep, low_pass)
low_back.defvjp(back_keep, back_low)

def layer_norm(values, gain_vec, offset):
    centre = values - lax.optimization_barrier(jnp.mean(values, axis=-1, keepdims=True))
    spread = lax.optimization_barrier(jnp.mean(centre * centre, axis=-1, keepdims=True))
    return centre * lax.rsqrt(spread + norm_eps) * gain_vec + offset

def matmul(left_op, right_op):
    return jnp.dot(left_op, right_op, precision=highest)

def block_allowed(rand_rows, first_block, count_blocks, block_total):
    blocks = jnp.arange(block_total, dtype=jnp.int32)
    query_blocks = first_block + jnp.arange(count_blocks, dtype=jnp.int32)
    chosen = lax.dynamic_slice_in_dim(rand_rows, first_block, count_blocks, axis=1)
    random_hit = jnp.any(chosen[:, :, :, None] == blocks[None, None, None, :], axis=2)
    near_hit = jnp.abs(query_blocks[:, None] - blocks[None, :]) <= 1
    global_hit = (blocks[None, :] == 0) | (blocks[None, :] == block_total - 1) | (query_blocks[:, None] == 0) | (query_blocks[:, None] == block_total - 1)
    return random_hit | (near_hit | global_hit)[None]

def token_allowed(rand_rows, segments, first_row, count_rows, block_size):
    block_total = segments.shape[0] // block_size
    allowed = block_allowed(rand_rows, first_row // block_size, count_rows // block_size, block_total)
    head_count = allowed.shape[0]
    expanded = jnp.broadcast_to(allowed[:, :, None, :, None], (head_count, count_rows // block_size, block_size, block_total, block_size))
    expanded = expanded.reshape(head_count, count_rows, block_total * block_size)
    query_seg = lax.dynamic_slice_in_dim(segments, first_row, count_rows)
    same_doc = query_seg[:, None] == segments[None, :]
    return expanded & same_doc[None]

def layer_seq(tokens, segments, rand_rows, params):
    gain_one, bias_one, w_query, b_query, w_key, w_value, b_value, w_out, b_out, gain_two, bias_two, w_up, b_up, w_down, b_down = params
    length = tokens.shape[0]
    normed = low(layer_norm(tokens, gain_one, bias_one))
    queries = low(low_back(matmul(normed, w_query) + b_query)).reshape(length, HEADS, HDIM)
    keys_all = low(low_back(matmul(normed, w_key))).reshape(length, HEADS, HDIM)
    values_all = low(low_back(matmul(normed, w_value) + b_value)).reshape(length, HEADS, HDIM)
    row_count = min(512, length)

    def attend(row_first):
        query_rows = lax.dynamic_slice_in_dim(queries, row_first, row_count, axis=0)
        raw_scores = low_back(jnp.einsum('qhd,khd->hqk', query_rows, keys_all, precision=highest) * 0.125)
        allowed = token_allowed(rand_rows, segments, row_first, row_count, BLOCK)
        scores = jnp.where(allowed, raw_scores, -1e+30)
        row_peak = lax.optimization_barrier(jnp.max(scores, axis=-1, keepdims=True))
        shifted = jnp.exp(scores - row_peak)
        attn_probs = shifted / lax.optimization_barrier(jnp.sum(shifted, axis=-1, keepdims=True))
        return jnp.einsum('hqk,khd->qhd', low(attn_probs), values_all, precision=highest)
    starts = jnp.arange(length // row_count, dtype=jnp.int32) * row_count
    mixed = lax.map(jax.checkpoint(attend), starts).reshape(length, HEADS * HDIM)
    mixed = low(low_back(mixed))
    middle = tokens + low_back(matmul(mixed, w_out) + b_out)
    normed_two = low(layer_norm(middle, gain_two, bias_two))
    inner_act = low_back(matmul(normed_two, w_up) + b_up)
    hidden = low(jax.nn.gelu(inner_act, approximate=False))
    return middle + low_back(matmul(hidden, w_down) + b_down)

def reference(layer_input, segment, rand_blocks, first_gain, first_bias, query_weight, query_bias, key_weight, value_weight, value_bias, out_weight, out_bias, second_gain, second_bias, up_weight, up_bias, down_weight, down_bias, cotangent):
    params = tuple((element.astype(jnp.float32) for element in (first_gain, first_bias, query_weight, query_bias, key_weight, value_weight, value_bias, out_weight, out_bias, second_gain, second_bias, up_weight, up_bias, down_weight, down_bias)))
    tokens = layer_input.astype(jnp.float32).reshape(-1, LEN, D)
    upstream = cotangent.astype(jnp.float32).reshape(-1, LEN, D)
    seg_all = segment.reshape(-1, LEN)
    rand_all = rand_blocks.reshape(-1, HEADS, NBLK, RAND)

    def scan_step(summed, seq_item):
        seq_tokens, seq_seg, seq_rand, seq_cot = seq_item

        def forward(tok_in, par_in):
            return layer_seq(tok_in, seq_seg, seq_rand, par_in)
        result, backward = jax.vjp(forward, seq_tokens, params)
        grad_tokens, grad_params = backward(seq_cot)
        summed = tuple((first + second for first, second in zip(summed, grad_params)))
        return (summed, (result, grad_tokens))
    zero_grads = tuple((jnp.zeros_like(element) for element in params))
    summed, (results, grad_tokens) = lax.scan(scan_step, zero_grads, (tokens, seg_all, rand_all, upstream))
    layer_output = results.reshape(layer_input.shape).astype(jnp.bfloat16)
    input_grad = grad_tokens.reshape(layer_input.shape).astype(jnp.bfloat16)
    return (layer_output, input_grad, summed[0], summed[1], summed[2], summed[3], summed[4], summed[5], summed[6], summed[7], summed[8], summed[9], summed[10], summed[11], summed[12], summed[13], summed[14])
```

```python
import functools
import jax
import jax.numpy as jnp
from jax import lax
from jax.experimental import pallas as pl
from jax.experimental.pallas import tpu as pltpu
from jax.sharding import PartitionSpec as P

norm_eps = 1e-05

HEADS = 12
HDIM = 64
BLOCK = 64
TQ = 256
TK = 256
NEG = -1e30


def nt(a, b):
    return lax.dot_general(a, b, (((1,), (1,)), ((), ())), preferred_element_type=jnp.float32)


def tn(a, b):
    return lax.dot_general(a, b, (((0,), (0,)), ((), ())), preferred_element_type=jnp.float32)


def nn(a, b):
    return jnp.dot(a, b, preferred_element_type=jnp.float32)


def head_lanes(head):
    lane = lax.broadcasted_iota(jnp.int32, (1, 128), 1)
    return (lane < HDIM) if head == 0 else (lane >= HDIM)


def bias_rows(block_ref, doc_ref, head, tile):
    per = TQ // BLOCK
    rows = [
        jnp.broadcast_to(
            block_ref[0, head, pl.ds(tile * per + b, 1), :], (BLOCK, 128)
        )
        for b in range(per)
    ]
    return (jnp.concatenate(rows, axis=0) + doc_ref[0, pl.ds(tile * TQ, TQ), :]).astype(jnp.bfloat16)


def forward_body(
    span_ref, q_ref, ko_ref, vo_ref, kx_ref, vx_ref, ao_ref, ax_ref, block_ref, doc_ref,
    out_ref, lse_ref, acc_ref, qa_ref,
):
    micro = pl.program_id(0)
    tiles = q_ref.shape[1] // TQ
    group = q_ref.shape[2] // HDIM
    for tile in range(tiles):
        for head in range(group):
            cols = pl.ds(head // 2 * 128, 128)
            q_rows = q_ref[0, pl.ds(tile * TQ, TQ), cols].astype(jnp.float32) * 0.125
            masked = jnp.where(head_lanes(head % 2), q_rows, 0.0).astype(jnp.bfloat16)
            qa_ref[head, :, 0:128] = masked
            qa_ref[head, :, 128:256] = bias_rows(block_ref, doc_ref, head, tile)
        acc_ref[...] = jnp.zeros_like(acc_ref)

        def sweep(k_ref, v_ref, a_ref, base, state):
            def step(j, carry):
                at = pl.ds(pl.multiple_of(j * TK, TK), TK)
                aug = a_ref[0, at, :]
                scores = []
                for head in range(group):
                    cols = pl.ds(head // 2 * 128, 128)
                    k_aug = jnp.concatenate([k_ref[0, at, cols], aug], axis=1)
                    scores.append(nt(k_aug, qa_ref[head]))
                fresh = []
                probs = []
                for head in range(group):
                    top_new = jnp.maximum(carry[head], jnp.max(scores[head], axis=0, keepdims=True))
                    probs.append(jnp.exp(scores[head] - top_new).astype(jnp.bfloat16))
                    fresh.append(top_new)
                for head in range(group):
                    cols = pl.ds(head // 2 * 128, 128)
                    v_rows = jnp.where(head_lanes(head % 2), v_ref[0, at, cols], jnp.bfloat16(1.0))
                    part = tn(v_rows, probs[head])
                    acc_ref[head] = acc_ref[head] * jnp.exp(carry[head] - fresh[head]) + part
                return tuple(fresh)

            return lax.fori_loop(span_ref[micro, tile, base], span_ref[micro, tile, base + 1], step, state)

        state = tuple(jnp.full((1, TQ), -3e38, jnp.float32) for _ in range(group))
        state = sweep(ko_ref, vo_ref, ao_ref, 0, state)
        state = sweep(kx_ref, vx_ref, ax_ref, 2, state)
        for pair in range(group // 2):
            done = []
            for head in range(2):
                at = pair * 2 + head
                mass = acc_ref[at, pl.ds((1 - head) * HDIM, 1), :]
                done.append(acc_ref[at, pl.ds(head * HDIM, HDIM), :] / mass)
                lse_ref[0, pair, pl.ds(head, 1), pl.ds(tile * TQ, TQ)] = state[at] + jnp.log(mass)
            out_ref[0, pl.ds(tile * TQ, TQ), pl.ds(pair * 128, 128)] = (
                jnp.concatenate(done, axis=0).T.astype(out_ref.dtype)
            )


def backward_body(
    span_ref, q_ref, ko_ref, vo_ref, kx_ref, vx_ref, ao_ref, ax_ref, block_ref, doc_ref,
    mixed_ref, grad_ref, lse_ref,
    dq_ref, dko_ref, dvo_ref, dkx_ref, dvx_ref,
    dqt_ref, qa_ref, gm_ref, ko_acc, vo_acc, kx_acc, vx_acc,
):
    micro = pl.program_id(0)
    tiles = q_ref.shape[1] // TQ
    group = q_ref.shape[2] // HDIM
    for ref in (ko_acc, vo_acc, kx_acc, vx_acc):
        ref[...] = jnp.zeros_like(ref)
    for tile in range(tiles):
        rows = pl.ds(tile * TQ, TQ)
        inner = []
        for pair in range(group // 2):
            cols = pl.ds(pair * 128, 128)
            q_rows = q_ref[0, rows, cols].astype(jnp.float32) * 0.125
            grad_rows = grad_ref[0, rows, cols].astype(jnp.float32)
            both = (mixed_ref[0, rows, cols].astype(jnp.float32) * grad_rows).T
            for side in range(2):
                head = pair * 2 + side
                qa_ref[head, :, 0:128] = jnp.where(head_lanes(side), q_rows, 0.0).astype(jnp.bfloat16)
                qa_ref[head, :, 128:256] = bias_rows(block_ref, doc_ref, head, tile)
                gm_ref[head] = jnp.where(head_lanes(side), grad_rows, 0.0).astype(jnp.bfloat16)
                inner.append(jnp.sum(both[side * HDIM:(side + 1) * HDIM, :], axis=0, keepdims=True))
        dqt_ref[...] = jnp.zeros_like(dqt_ref)

        def sweep(k_ref, v_ref, a_ref, k_acc, v_acc, base):
            def step(j, carry):
                at = pl.ds(pl.multiple_of(j * TK, TK), TK)
                aug = a_ref[0, at, :]
                for chunk in range(0, group, CHUNK):
                    heads = range(chunk, min(chunk + CHUNK, group))
                    scores, grads, probs, souls = {}, {}, {}, {}
                    for head in heads:
                        cols = pl.ds(head // 2 * 128, 128)
                        k_aug = jnp.concatenate([k_ref[0, at, cols], aug], axis=1)
                        scores[head] = nt(k_aug, qa_ref[head])
                        grads[head] = nt(v_ref[0, at, cols], gm_ref[head])
                    for head in heads:
                        weight = jnp.exp(scores[head] - lse_ref[0, head // 2, pl.ds(head % 2, 1), rows])
                        souls[head] = (weight * (grads[head] - carry[head])).astype(jnp.bfloat16)
                        probs[head] = weight.astype(jnp.bfloat16)
                    for head in heads:
                        cols = pl.ds(head // 2 * 128, 128)
                        dv = nn(probs[head], gm_ref[head])
                        dk = nn(souls[head], qa_ref[head, :, 0:128])
                        dqt = tn(k_ref[0, at, cols], souls[head])
                        lanes = pl.ds(head * HDIM, HDIM)
                        side = head % 2
                        dqt_ref[lanes, :] += dqt[side * HDIM:(side + 1) * HDIM, :]
                        if side == 0:
                            dv_low, dk_low = dv, dk
                        else:
                            k_acc[at, cols] += dk + dk_low
                            v_acc[at, cols] += dv + dv_low
                return carry

            lax.fori_loop(span_ref[micro, tile, base], span_ref[micro, tile, base + 1], step, tuple(inner))

        sweep(ko_ref, vo_ref, ao_ref, ko_acc, vo_acc, 0)
        sweep(kx_ref, vx_ref, ax_ref, kx_acc, vx_acc, 2)
        for pair in range(group // 2):
            cols = pl.ds(pair * 128, 128)
            dq_ref[0, rows, cols] = (dqt_ref[cols, :] * 0.125).T.astype(dq_ref.dtype)
    dko_ref[0] = ko_acc[...].astype(dko_ref.dtype)
    dvo_ref[0] = vo_acc[...].astype(dvo_ref.dtype)
    dkx_ref[0] = kx_acc[...].astype(dkx_ref.dtype)
    dvx_ref[0] = vx_acc[...].astype(dvx_ref.dtype)


CHUNK = 4


def specs(half, group):
    pair = pl.BlockSpec((1, half, group * HDIM), lambda m, p, s: (m, 0, p))
    aug = pl.BlockSpec((1, half, 128), lambda m, p, s: (m, 0, 0))
    block = pl.BlockSpec((1, group, half // BLOCK, 128), lambda m, p, s: (m, p, 0, 0))
    lse = pl.BlockSpec((1, group // 2, 2, half), lambda m, p, s: (m, p, 0, 0))
    return pair, aug, block, lse


def attend_forward(span, q, ko, vo, kx, vx, ao, ax, block, doc, group=12):
    micro, half, width = q.shape
    pairs = group // 2
    pair = pl.BlockSpec((1, half, group * HDIM), lambda m, p, s: (m, 0, p))
    aug = pl.BlockSpec((1, half, 128), lambda m, p, s: (m, 0, 0))
    blk = pl.BlockSpec((1, group, half // BLOCK, 128), lambda m, p, s: (m, p, 0, 0))
    lse = pl.BlockSpec((1, pairs, 2, half), lambda m, p, s: (m, p, 0, 0))
    return pl.pallas_call(
        forward_body,
        name="attend_forward",
        out_shape=(
            jax.ShapeDtypeStruct((micro, half, width), jnp.bfloat16),
            jax.ShapeDtypeStruct((micro, HEADS // 2, 2, half), jnp.float32),
        ),
        grid_spec=pltpu.PrefetchScalarGridSpec(
            num_scalar_prefetch=1,
            grid=(micro, HEADS // group),
            in_specs=[pair] * 5 + [aug, aug, blk, aug],
            out_specs=(pair, lse),
            scratch_shapes=[
                pltpu.VMEM((group, 128, TQ), jnp.float32),
                pltpu.VMEM((group, TQ, 256), jnp.bfloat16),
            ],
        ),
        cost_estimate=pl.CostEstimate(flops=20_000_000_000, bytes_accessed=20_000_000, transcendentals=0),
    )(span, q, ko, vo, kx, vx, ao, ax, block, doc)


def attend_backward(span, q, ko, vo, kx, vx, ao, ax, block, doc, mixed, grad, lse, group=12):
    micro, half, width = q.shape
    pair, aug, blk, lse_spec = specs(half, group)
    shape = jax.ShapeDtypeStruct((micro, half, width), jnp.bfloat16)
    return pl.pallas_call(
        backward_body,
        name="attend_backward",
        out_shape=(shape,) * 5,
        grid_spec=pltpu.PrefetchScalarGridSpec(
            num_scalar_prefetch=1,
            grid=(micro, HEADS // group),
            in_specs=[pair] * 5 + [aug, aug, blk, aug, pair, pair, lse_spec],
            out_specs=(pair,) * 5,
            scratch_shapes=[
                pltpu.VMEM((group * HDIM, TQ), jnp.float32),
                pltpu.VMEM((group, TQ, 256), jnp.bfloat16),
                pltpu.VMEM((group, TQ, 128), jnp.bfloat16),
            ]
            + [pltpu.VMEM((half, group * HDIM), jnp.float32)] * 4,
        ),
        cost_estimate=pl.CostEstimate(flops=40_000_000_000, bytes_accessed=40_000_000, transcendentals=0),
    )(span, q, ko, vo, kx, vx, ao, ax, block, doc, mixed, grad, lse)


def tables(segment, rand_blocks, side, half):
    micro, length = segment.shape
    blocks = length // BLOCK
    mine = half // BLOCK
    lane = lax.broadcasted_iota(jnp.int32, (1, 1, 128), 2)
    own = lax.dynamic_slice_in_dim(segment, side * half, half, axis=1)
    other = lax.dynamic_slice_in_dim(segment, (1 - side) * half, half, axis=1)

    def aug(seg, which):
        place = (which * half + lax.broadcasted_iota(jnp.int32, (1, half, 1), 1)) // BLOCK
        hit = (lane == place) | (lane == seg[:, :, None] + blocks)
        return hit.astype(jnp.bfloat16)

    doc = jnp.where((lane >= blocks) & (lane < blocks + 4) & (lane != own[:, :, None] + blocks), NEG, 0.0)
    q_block = side * mine + lax.broadcasted_iota(jnp.int32, (1, 1, mine, 1), 2)
    k_block = lax.broadcasted_iota(jnp.int32, (1, 1, 1, 128), 3)
    chosen = lax.dynamic_slice_in_dim(rand_blocks, side * mine, mine, axis=2)
    allowed = (jnp.abs(q_block - k_block) <= 1) | (k_block == 0) | (k_block == blocks - 1)
    allowed = allowed | (q_block == 0) | (q_block == blocks - 1) | (k_block >= blocks)
    for pick in range(rand_blocks.shape[3]):
        allowed = allowed | (chosen[:, :, :, pick:pick + 1] == k_block)
    block = jnp.where(allowed, 0.0, NEG).astype(jnp.float32)
    tiles = half // TQ
    first = own.reshape(micro, tiles, TQ)[:, :, 0]
    last = own.reshape(micro, tiles, TQ)[:, :, TQ - 1]
    begin = jnp.sum((segment[:, None, :] < first[:, :, None]).astype(jnp.int32), axis=-1)
    end = jnp.sum((segment[:, None, :] <= last[:, :, None]).astype(jnp.int32), axis=-1)
    span = []
    for base in (side * half, (1 - side) * half):
        low = jnp.clip((begin - base) // TK, 0, half // TK)
        high = jnp.clip((end - base + TK - 1) // TK, 0, half // TK)
        span += [low, jnp.maximum(high, low)]
    return jnp.stack(span, axis=-1), aug(own, side), aug(other, 1 - side), block, doc.astype(jnp.float32)


MESH = pl.DeviceIdType.MESH
GROUPS = 3


def place():
    rep, shard, side = lax.axis_index("rep"), lax.axis_index("fsdp"), lax.axis_index("seq")
    quad = lax.rem(rep, 4)
    across, along = lax.rem(quad, 2), quad // 2
    near = (1 - 2 * across, 2 - 4 * along)
    return rep, shard, side, quad, near


def chunk(refs, group, shard, quad, side, rows, half=None):
    width = 768 if half is None else 384
    offset = 0 if half is None else half * 384
    low = side * rows
    if group == 0:
        return refs[0].at[quad, pl.ds(pl.multiple_of(shard * (2 * rows) + low, 16), rows), pl.ds(offset, width)]
    if group == 1:
        at = pl.multiple_of(shard * (2 * rows) + low, 16)
        return refs[1].at[pl.ds(at, rows), pl.ds(pl.multiple_of(quad * 768 + offset, 128), width)]
    at = pl.multiple_of(shard * (8 * rows) + quad * (2 * rows) + low, 16)
    return refs[2].at[pl.ds(at, rows), pl.ds(offset, width)]


def greet(peers):
    barrier = pltpu.get_barrier_semaphore()
    for peer in peers:
        pl.semaphore_signal(barrier, inc=1, device_id=peer, device_id_type=MESH)
    pl.semaphore_wait(barrier, len(peers))


def remote(src, dst, send, recv, peer):
    return pltpu.make_async_remote_copy(
        src_ref=src, dst_ref=dst, send_sem=send, recv_sem=recv, device_id=peer, device_id_type=MESH
    )


def gather_body(
    shards, rows, qkvo_in, up_in, down_in, vec_in, qkvo_out, up_out, down_out, vec_out,
    qkvo_stage, up_stage, down_stage, vec_stage,
    in_sem, out_sem, z_send, z_recv, x_send, x_recv, y_send, y_recv, d_send, d_recv, c_send, c_recv,
):
    rep, shard, side, quad, (dx, dy) = place()
    ins, outs = (qkvo_in, up_in, down_in), (qkvo_out, up_out, down_out)
    stages = (qkvo_stage, up_stage, down_stage, vec_stage)
    x_peer, y_peer, partner = (rep + dx, shard, side), (rep + dy, shard, side), (rep, shard, 1 - side)
    z_peers = [(rep, lax.rem(shard + k, shards), side) for k in range(1, shards)]
    for i, src in enumerate((qkvo_in, up_in, down_in, vec_in)):
        pltpu.make_async_copy(src, stages[i], in_sem.at[i]).start()
    greet(z_peers + [x_peer, y_peer, partner])
    sent = []

    def go(copy):
        copy.start()
        sent.append(copy)

    for g in range(GROUPS):
        for k in range(1, shards):
            go(remote(
                chunk(ins, g, 0, quad, side, rows), chunk(outs, g, shard, quad, side, rows),
                z_send.at[g, k - 1], z_recv.at[g, shards - k - 1], z_peers[k - 1],
            ))
        if g == 0:
            for k in range(1, shards):
                go(remote(
                    vec_in, vec_out.at[shard],
                    z_send.at[GROUPS, k - 1], z_recv.at[GROUPS, shards - k - 1], z_peers[k - 1],
                ))
    owned = (
        qkvo_out.at[:, pl.ds(pl.multiple_of(shard * 2 * rows, 16), 2 * rows), :],
        up_out.at[pl.ds(pl.multiple_of(shard * 2 * rows, 16), 2 * rows), :],
        down_out.at[pl.ds(pl.multiple_of(shard * 8 * rows, 16), 8 * rows), :],
        vec_out.at[shard],
    )
    local = []
    for i, src in enumerate((qkvo_in, up_in, down_in, vec_in)):
        pltpu.make_async_copy(src, stages[i], in_sem.at[i]).wait()
        copy = pltpu.make_async_copy(stages[i], owned[i], out_sem.at[i])
        copy.start()
        local.append(copy)

    def piece(g, k, member, core, half=None):
        return chunk(outs, g, lax.rem(shard + k, shards), member, core, rows, half)

    def hop(g, k, member, core, send, recv, peer, half=None):
        ref = piece(g, k, member, core, half)
        return remote(ref, ref, send, recv, peer)

    x_quad, y_quad, d_quad = quad + dx, quad + dy, quad + dx + dy

    def straight(g):
        for k in range(1, shards):
            hop(g, k, quad, side, z_send.at[g, k - 1], z_recv.at[g, k - 1], z_peers[k - 1]).wait_recv()
            go(hop(g, k, quad, side, x_send.at[g, k - 1], x_recv.at[g, k - 1], x_peer))
            go(hop(g, k, quad, side, y_send.at[g, k - 1], y_recv.at[g, k - 1], y_peer))
            go(hop(g, k, quad, side, c_send.at[g, k - 1, 0], c_recv.at[g, k - 1, 0], partner))

    def turn(g):
        for k in range(1, shards):
            hop(g, k, x_quad, side, x_send.at[g, k - 1], x_recv.at[g, k - 1], x_peer).wait_recv()
            go(hop(g, k, x_quad, side, d_send.at[g, k - 1, 1], d_recv.at[g, k - 1, 1], y_peer, 1))
            go(hop(g, k, x_quad, side, c_send.at[g, k - 1, 1], c_recv.at[g, k - 1, 1], partner))
            hop(g, k, y_quad, side, y_send.at[g, k - 1], y_recv.at[g, k - 1], y_peer).wait_recv()
            go(hop(g, k, y_quad, side, d_send.at[g, k - 1, 0], d_recv.at[g, k - 1, 0], x_peer, 0))
            go(hop(g, k, y_quad, side, c_send.at[g, k - 1, 2], c_recv.at[g, k - 1, 2], partner))

    def corner(g):
        for k in range(1, shards):
            hop(g, k, d_quad, side, d_send.at[g, k - 1, 0], d_recv.at[g, k - 1, 0], x_peer, 0).wait_recv()
            hop(g, k, d_quad, side, d_send.at[g, k - 1, 1], d_recv.at[g, k - 1, 1], y_peer, 1).wait_recv()
            go(hop(g, k, d_quad, side, c_send.at[g, k - 1, 3], c_recv.at[g, k - 1, 3], partner))

    straight(0)
    for g in range(GROUPS):
        turn(g)
        if g + 1 < GROUPS:
            straight(g + 1)
        corner(g)
    for g in range(GROUPS):
        for k in range(1, shards):
            for i, member in enumerate((quad, x_quad, y_quad, d_quad)):
                hop(g, k, member, 1 - side, c_send.at[g, k - 1, i], c_recv.at[g, k - 1, i], partner).wait_recv()
    for k in range(1, shards):
        remote(
            vec_in, vec_out.at[lax.rem(shard + k, shards)],
            z_send.at[GROUPS, k - 1], z_recv.at[GROUPS, k - 1], z_peers[k - 1],
        ).wait_recv()
    for copy in sent:
        copy.wait_send()
    for copy in local:
        copy.wait()


def gather_weights(shards, qkvo, up, down, vec):
    rows = qkvo.shape[1] // 2
    model = qkvo.shape[2]
    hidden = up.shape[1]
    any_space = pl.BlockSpec(memory_space=pl.ANY)
    dma = pltpu.SemaphoreType.DMA
    low = jnp.bfloat16
    return pl.pallas_call(
        functools.partial(gather_body, shards, rows),
        name="gather_weights",
        out_shape=(
            jax.ShapeDtypeStruct((4, model, model), low),
            jax.ShapeDtypeStruct((model, hidden), low),
            jax.ShapeDtypeStruct((hidden, model), low),
            jax.ShapeDtypeStruct((shards,) + vec.shape, low),
        ),
        in_specs=[any_space] * 4,
        out_specs=(any_space,) * 4,
        scratch_shapes=[
            pltpu.VMEM(qkvo.shape, low), pltpu.VMEM(up.shape, low),
            pltpu.VMEM(down.shape, low), pltpu.VMEM(vec.shape, low),
            dma((4,)), dma((4,)),
            dma((GROUPS + 1, shards - 1)), dma((GROUPS + 1, shards - 1)),
        ]
        + [dma((GROUPS, shards - 1))] * 4
        + [dma((GROUPS, shards - 1, 2))] * 2
        + [dma((GROUPS, shards - 1, 4))] * 2,
        compiler_params=pltpu.CompilerParams(collective_id=0, has_side_effects=True),
    )(qkvo, up, down, vec)


def add_into(out_ref, refs):
    total = refs[0][...].astype(jnp.float32)
    for ref in refs[1:]:
        total = total + ref[...].astype(jnp.float32)
    out_ref[...] = total.astype(out_ref.dtype)


def reduce_body(
    shards, quads, rows, qkvo_in, up_in, down_in, vec_in, qkvo_out, up_out, down_out, vec_out,
    own, mate, first, second, last, ring, full, vec_sum, vec_mate, vec_last, vec_ring,
    load_sem, c_send, c_recv, f_send, f_recv, s_send, s_recv, z_send, z_recv, q_send, q_recv,
    x_send, x_recv, y_send, y_recv, d_send, d_recv, g_send, g_recv, out_sem, v_send, v_recv,
):
    rep, shard, side, quad, (dx, dy) = place()
    ins, outs = (qkvo_in, up_in, down_in), (qkvo_out, up_out, down_out)
    x_peer, y_peer, partner = (rep + dx, shard, side), (rep + dy, shard, side), (rep, shard, 1 - side)
    x_quad, y_quad, d_quad = quad + dx, quad + dy, quad + dx + dy
    z_peers = [(rep, lax.rem(shard + k, shards), side) for k in range(1, shards)]
    q_peers = [(lax.rem(rep + 4 * k, 4 * quads), shard, side) for k in range(1, quads)]
    greet(z_peers + q_peers + [x_peer, y_peer, partner])

    def c_copy(g, f, m):
        return remote(chunk(ins, g, f, m, 1 - side, rows), mate.at[g, f, m], c_send.at[g, f, m], c_recv.at[g, f, m], partner)

    def load(g, f, m):
        return pltpu.make_async_copy(chunk(ins, g, f, m, side, rows), own.at[g, f, m], load_sem.at[g, f, m])

    def f_copy(g, f, slot, flip):
        peer, to = (y_peer, y_quad) if flip else (x_peer, x_quad)
        member = to if slot == 0 else d_quad
        return remote(own.at[g, f, member], first.at[g, f, slot], f_send.at[g, f, slot], f_recv.at[g, f, slot], peer)

    def s_copy(g, f, flip):
        peer, to = (x_peer, x_quad) if flip else (y_peer, y_quad)
        return remote(own.at[g, f, to], second.at[g, f], s_send.at[g, f], s_recv.at[g, f], peer)

    vec_copies = []

    def vec_go(src, dst, i, peer):
        copy = remote(src, dst, v_send.at[i], v_recv.at[i], peer)
        copy.start()
        vec_copies.append(copy)
        return copy

    swap = vec_go(vec_in, vec_mate.at[0], 0, partner)
    for g in range(GROUPS):
        def begin(f, carry, g=g):
            for m in range(4):
                c_copy(g, f, m).start()
                load(g, f, m).start()
            return carry
        lax.fori_loop(0, shards, begin, 0)

    def merge(g):
        def step(pairs, carry):
            for flip in range(2):
                f = pairs * 2 + flip
                for m in range(4):
                    load(g, f, m).wait()
                    c_copy(g, f, m).wait_recv()
                    add_into(own.at[g, f, m], (own.at[g, f, m], mate.at[g, f, m]))
                for slot in range(2):
                    f_copy(g, f, slot, flip).start()
            return carry
        lax.fori_loop(0, shards // 2, step, 0)

    def fold(g):
        def step(pairs, carry):
            for flip in range(2):
                f = pairs * 2 + flip
                for slot in range(2):
                    f_copy(g, f, slot, flip).wait()
                    member = quad if slot == 0 else (x_quad if flip else y_quad)
                    add_into(own.at[g, f, member], (own.at[g, f, member], first.at[g, f, slot]))
                s_copy(g, f, flip).start()
            return carry
        lax.fori_loop(0, shards // 2, step, 0)

    def settle(g):
        def step(pairs, carry):
            for flip in range(2):
                f = pairs * 2 + flip
                s_copy(g, f, flip).wait()
                add_into(own.at[g, f, quad], (own.at[g, f, quad], second.at[g, f]))
            return carry
        lax.fori_loop(0, shards // 2, step, 0)
        for k in range(1, shards):
            z_copy(g, k).start()

    def z_copy(g, k):
        return remote(
            own.at[g, lax.rem(shard + k, shards), quad], last.at[g, shards - k - 1],
            z_send.at[g, k - 1], z_recv.at[g, shards - k - 1], z_peers[k - 1],
        )

    def z_wait(g, k):
        remote(own.at[g, shard, quad], last.at[g, k - 1], z_send.at[g, k - 1], z_recv.at[g, k - 1], z_peers[k - 1]).wait_recv()

    merge(0)
    swap.wait_recv()
    vec_sum[...] = vec_in[...] + vec_mate[0]
    swap = vec_go(vec_sum, vec_mate.at[1], 1, x_peer)
    merge(1)
    fold(0)
    swap.wait()
    vec_sum[...] = vec_sum[...] + vec_mate[1]
    swap = vec_go(vec_sum, vec_mate.at[2], 2, y_peer)
    merge(2)
    fold(1)
    settle(0)
    swap.wait()
    vec_sum[...] = vec_sum[...] + vec_mate[2]
    for k in range(1, shards):
        copy = remote(
            vec_sum.at[lax.rem(shard + k, shards)], vec_last.at[shards - k - 1],
            v_send.at[2 + k], v_recv.at[2 + shards - k], z_peers[k - 1],
        )
        copy.start()
    fold(2)
    settle(1)
    settle(2)

    def swirl(g):
        for k in range(1, shards):
            z_wait(g, k)
        add_into(full.at[g, quad, side], [own.at[g, shard, quad]] + [last.at[g, k] for k in range(shards - 1)])
        for k in range(1, quads):
            remote(full.at[g, quad, side], ring.at[g, quads - k - 1], q_send.at[g, k - 1], q_recv.at[g, quads - k - 1], q_peers[k - 1]).start()
        for k in range(1, quads):
            remote(full.at[g, quad, side], ring.at[g, k - 1], q_send.at[g, k - 1], q_recv.at[g, k - 1], q_peers[k - 1]).wait()
        if quads > 1:
            add_into(full.at[g, quad, side], [full.at[g, quad, side]] + [ring.at[g, k] for k in range(quads - 1)])
        spread(g, quad, x_send.at[g], x_recv.at[g], x_peer).start()
        spread(g, quad, y_send.at[g], y_recv.at[g], y_peer).start()
        spread(g, quad, g_send.at[g, 0], g_recv.at[g, 0], partner).start()

    def spread(g, member, send, recv, peer, half=None, core=None):
        core = side if core is None else core
        ref = full.at[g, member, core]
        if half is not None:
            ref = full.at[g, member, core, :, pl.ds(half * 384, 384)]
        return remote(ref, ref, send, recv, peer)

    def turn(g):
        spread(g, x_quad, x_send.at[g], x_recv.at[g], x_peer).wait_recv()
        spread(g, x_quad, d_send.at[g, 1], d_recv.at[g, 1], y_peer, 1).start()
        spread(g, x_quad, g_send.at[g, 1], g_recv.at[g, 1], partner).start()
        spread(g, y_quad, y_send.at[g], y_recv.at[g], y_peer).wait_recv()
        spread(g, y_quad, d_send.at[g, 0], d_recv.at[g, 0], x_peer, 0).start()
        spread(g, y_quad, g_send.at[g, 2], g_recv.at[g, 2], partner).start()

    def corner(g):
        spread(g, d_quad, d_send.at[g, 0], d_recv.at[g, 0], x_peer, 0).wait_recv()
        spread(g, d_quad, d_send.at[g, 1], d_recv.at[g, 1], y_peer, 1).wait_recv()
        spread(g, d_quad, g_send.at[g, 3], g_recv.at[g, 3], partner).start()

    def put(g, m, core):
        return pltpu.make_async_copy(full.at[g, m, core], chunk(outs, g, 0, m, core, rows), out_sem.at[g, m, core])

    for g in range(GROUPS):
        swirl(g)
    for g in range(GROUPS):
        turn(g)
    for k in range(1, shards):
        remote(vec_sum.at[shard], vec_last.at[k - 1], v_send.at[2 + k], v_recv.at[2 + k], z_peers[k - 1]).wait()
    total = vec_sum[shard]
    for k in range(shards - 1):
        total = total + vec_last[k]
    vec_ring[0] = total
    for k in range(1, quads):
        remote(vec_ring.at[0], vec_ring.at[quads - k], v_send.at[2 + shards + k], v_recv.at[2 + shards + quads - k], q_peers[k - 1]).start()
    for k in range(1, quads):
        remote(vec_ring.at[0], vec_ring.at[k], v_send.at[2 + shards + k], v_recv.at[2 + shards + k], q_peers[k - 1]).wait()
        total = total + vec_ring[k]
    vec_out[...] = total
    for g in range(GROUPS):
        corner(g)
    for g in range(GROUPS):
        for i, member in enumerate((quad, x_quad, y_quad, d_quad)):
            spread(g, member, g_send.at[g, i], g_recv.at[g, i], partner, core=1 - side).wait_recv()
        for m in range(4):
            for core in range(2):
                put(g, m, core).start()
    for g in range(GROUPS):
        for m in range(4):
            for core in range(2):
                put(g, m, core).wait()

        def drain(f, carry, g=g):
            for m in range(4):
                c_copy(g, f, m).wait_send()
            return carry
        lax.fori_loop(0, shards, drain, 0)
        for k in range(1, shards):
            z_copy(g, k).wait_send()
        spread(g, quad, x_send.at[g], x_recv.at[g], x_peer).wait_send()
        spread(g, quad, y_send.at[g], y_recv.at[g], y_peer).wait_send()
        spread(g, y_quad, d_send.at[g, 0], d_recv.at[g, 0], x_peer, 0).wait_send()
        spread(g, x_quad, d_send.at[g, 1], d_recv.at[g, 1], y_peer, 1).wait_send()
        for i in range(4):
            spread(g, quad, g_send.at[g, i], g_recv.at[g, i], partner).wait_send()
    vec_copies[0].wait_send()


def reduce_grads(shards, quads, qkvo, up, down, vec):
    model, hidden = up.shape
    rows = model // shards // 2
    any_space = pl.BlockSpec(memory_space=pl.ANY)
    vmem_space = pl.BlockSpec(memory_space=pltpu.VMEM)
    dma = pltpu.SemaphoreType.DMA
    low = jnp.bfloat16
    wide = jnp.float32
    piece = (rows, model)
    vec_one = vec.shape[1:]
    spare = max(quads - 1, 1)
    return pl.pallas_call(
        functools.partial(reduce_body, shards, quads, rows),
        name="reduce_grads",
        out_shape=(
            jax.ShapeDtypeStruct((4, 2 * rows, model), low),
            jax.ShapeDtypeStruct((2 * rows, hidden), low),
            jax.ShapeDtypeStruct((8 * rows, model), low),
            jax.ShapeDtypeStruct(vec_one, wide),
        ),
        in_specs=[any_space] * 3 + [vmem_space],
        out_specs=(any_space,) * 3 + (vmem_space,),
        scratch_shapes=[
            pltpu.VMEM((GROUPS, shards, 4) + piece, low),
            pltpu.VMEM((GROUPS, shards, 4) + piece, low),
            pltpu.VMEM((GROUPS, shards, 2) + piece, low),
            pltpu.VMEM((GROUPS, shards) + piece, low),
            pltpu.VMEM((GROUPS, shards - 1) + piece, low),
            pltpu.VMEM((GROUPS, spare) + piece, low),
            pltpu.VMEM((GROUPS, 4, 2) + piece, low),
            pltpu.VMEM(vec.shape, wide),
            pltpu.VMEM((3,) + vec.shape, wide),
            pltpu.VMEM((shards - 1,) + vec_one, wide),
            pltpu.VMEM((quads,) + vec_one, wide),
            dma((GROUPS, shards, 4)),
            dma((GROUPS, shards, 4)), dma((GROUPS, shards, 4)),
            dma((GROUPS, shards, 2)), dma((GROUPS, shards, 2)),
            dma((GROUPS, shards)), dma((GROUPS, shards)),
            dma((GROUPS, shards - 1)), dma((GROUPS, shards - 1)),
            dma((GROUPS, spare)), dma((GROUPS, spare)),
            dma((GROUPS,)), dma((GROUPS,)), dma((GROUPS,)), dma((GROUPS,)),
            dma((GROUPS, 2)), dma((GROUPS, 2)),
            dma((GROUPS, 4)), dma((GROUPS, 4)),
            dma((GROUPS, 4, 2)),
            dma((3 + shards + quads,)), dma((3 + shards + quads,)),
        ],
        compiler_params=pltpu.CompilerParams(
            collective_id=1, has_side_effects=True, vmem_limit_bytes=60_000_000
        ),
    )(qkvo, up, down, vec)


def layer_norm(values, gain, offset):
    centre = values - jnp.mean(values, axis=-1, keepdims=True)
    scale = lax.rsqrt(jnp.mean(centre * centre, axis=-1, keepdims=True) + norm_eps)
    unit = centre * scale
    return unit, scale, (unit * gain + offset).astype(jnp.bfloat16)


def norm_back(upstream, unit, scale, gain):
    scaled = upstream * gain
    mean_one = jnp.mean(scaled, axis=-1, keepdims=True)
    mean_two = jnp.mean(scaled * unit, axis=-1, keepdims=True)
    return (
        scale * (scaled - mean_one - unit * mean_two),
        jnp.sum(upstream * unit, axis=0),
        jnp.sum(upstream, axis=0),
    )


def on_device(
    shards, quads,
    layer_input, segment, rand_blocks, first_gain, first_bias, query_weight, query_bias,
    key_weight, value_weight, value_bias, out_weight, out_bias, second_gain, second_bias,
    up_weight, up_bias, down_weight, down_bias, cotangent,
):
    micro, _, half, model = layer_input.shape
    side = lax.axis_index("seq")
    rows = micro * half
    part = model // shards
    low, wide = jnp.bfloat16, jnp.float32
    vec = jnp.stack(
        [first_gain, first_bias, query_bias, value_bias, out_bias, second_gain, second_bias, down_bias]
        + [up_bias[i * part:(i + 1) * part] for i in range(4)]
    )
    vec = jnp.pad(vec, ((0, 4), (0, 256 - part)))
    w_qkvo, w_up, w_down, vec_all = gather_weights(
        shards, jnp.stack([query_weight, key_weight, value_weight, out_weight]), up_weight, down_weight, vec
    )
    vec_all = vec_all[:, :, :part].astype(wide)
    flat = jnp.moveaxis(vec_all[:, :8], 0, 1).reshape(8, model)
    gain_one, bias_one, b_query, b_value, b_out, gain_two, bias_two, b_down = [flat[i] for i in range(8)]
    b_up = vec_all[:, 8:12].reshape(4 * model)
    span, aug_own, aug_other, block_bias, doc_bias = tables(segment[:, 0], rand_blocks[:, 0], side, half)

    tokens = layer_input.reshape(rows, model).astype(wide)
    unit_one, scale_one, normed = layer_norm(tokens, gain_one, bias_one)
    swap = [(0, 1), (1, 0)]
    keys = nn(normed, w_qkvo[1]).astype(low)
    keys_other = lax.ppermute(keys, "seq", swap)
    values = (nn(normed, w_qkvo[2]) + b_value).astype(low)
    values_other = lax.ppermute(values, "seq", swap)
    queries = (nn(normed, w_qkvo[0]) + b_query).astype(low)
    cut = lambda array: array.reshape(micro, half, model)
    attended = (span, cut(queries), cut(keys), cut(values), cut(keys_other), cut(values_other),
                aug_own, aug_other, block_bias, doc_bias)
    mixed, lse = attend_forward(*attended)
    mixed_rows = mixed.reshape(rows, model)
    middle = tokens + nn(mixed_rows, w_qkvo[3]) + b_out
    unit_two, scale_two, normed_two = layer_norm(middle, gain_two, bias_two)
    inner = nn(normed_two, w_up) + b_up
    phi = 0.5 * (1.0 + lax.erf(inner * 0.7071067811865476))
    hidden = (inner * phi).astype(low)
    slope = phi + inner * (jnp.exp(-0.5 * inner * inner) * 0.3989422804014327)
    result = (middle + nn(hidden, w_down) + b_down).astype(low)

    branch = cotangent.reshape(rows, model)
    upstream = branch.astype(wide)
    d_down = tn(hidden, branch).astype(low)
    grad_inner = (nt(branch, w_down) * slope).astype(low)
    d_up = tn(normed_two, grad_inner).astype(low)
    grad_two, d_gain_two, d_bias_two = norm_back(nt(grad_inner, w_up), unit_two, scale_two, gain_two)
    grad_middle = upstream + grad_two
    grad_attn = grad_middle.astype(low)
    d_out = tn(mixed_rows, grad_attn).astype(low)
    grad_mixed = nt(grad_attn, w_qkvo[3]).astype(low)
    d_query, d_key, d_value, d_key_other, d_value_other = attend_backward(*attended, mixed, cut(grad_mixed), lse)
    join = lambda own, other: (
        own.reshape(rows, model).astype(wide) + lax.ppermute(other.reshape(rows, model), "seq", swap).astype(wide)
    ).astype(low)
    d_query = d_query.reshape(rows, model)
    d_key = join(d_key, d_key_other)
    d_value = join(d_value, d_value_other)
    grad_normed = nt(d_query, w_qkvo[0]) + nt(d_key, w_qkvo[1]) + nt(d_value, w_qkvo[2])
    grad_one, d_gain_one, d_bias_one = norm_back(grad_normed, unit_one, scale_one, gain_one)
    input_grad = (grad_middle + grad_one).astype(low)
    d_qkvo = jnp.stack([tn(normed, d_query), tn(normed, d_key), tn(normed, d_value), d_out.astype(wide)]).astype(low)
    total = lambda array: jnp.sum(array.astype(wide), axis=0)
    small = jnp.stack([d_gain_one, d_bias_one, total(d_query), total(d_value), total(grad_attn),
                       d_gain_two, d_bias_two, total(branch)])
    small = jnp.moveaxis(small.reshape(8, shards, part), 1, 0)
    small = jnp.concatenate([small, total(grad_inner).reshape(shards, 4, part)], axis=1)
    small = jnp.pad(small, ((0, 0), (0, 4), (0, 256 - part)))
    g_qkvo, g_up, g_down, g_vec = reduce_grads(shards, quads, d_qkvo, d_up, d_down, small)
    g_qkvo, g_up, g_down = g_qkvo.astype(wide), g_up.astype(wide), g_down.astype(wide)
    g_vec = g_vec[:, :part]
    shape = layer_input.shape
    return (
        result.reshape(shape), input_grad.reshape(shape), g_vec[0], g_vec[1], g_qkvo[0], g_vec[2],
        g_qkvo[1], g_qkvo[2], g_vec[3], g_qkvo[3], g_vec[4], g_vec[5], g_vec[6], g_up,
        g_vec[8:12].reshape(4 * part), g_down, g_vec[7],
    )


def solution(mesh):
    row = P(None, ("rep", "fsdp"), "seq", None)
    flat, wide = P("fsdp"), P("fsdp", None)
    shards, quads = mesh.shape["fsdp"], mesh.shape["rep"] // 4
    assert mesh.shape["seq"] == 2 and mesh.shape["rep"] % 4 == 0
    return jax.shard_map(
        functools.partial(on_device, shards, quads),
        mesh=mesh,
        in_specs=(
            row, P(None, ("rep", "fsdp"), None), P(None, ("rep", "fsdp"), None, None, None),
            flat, flat, wide, flat, wide, wide, flat, wide, flat, flat, flat, wide, flat, wide, flat, row,
        ),
        out_specs=(row, row, flat, flat, wide, flat, wide, wide, flat, wide, flat, flat, flat, wide, flat, wide, flat),
        check_vma=False,
    )
```

```python
import functools
import jax
import jax.numpy as jnp
from jax import lax
from jax.experimental import pallas as pl
from jax.experimental.pallas import tpu as pltpu
from jax.sharding import PartitionSpec as P

norm_eps = 1e-05

HEADS = 12
HDIM = 64
BLOCK = 64
TQ = 256
TK = 256
NEG = -1e30


def nt(a, b):
    return lax.dot_general(a, b, (((1,), (1,)), ((), ())), preferred_element_type=jnp.float32)


def tn(a, b):
    return lax.dot_general(a, b, (((0,), (0,)), ((), ())), preferred_element_type=jnp.float32)


def nn(a, b):
    return jnp.dot(a, b, preferred_element_type=jnp.float32)


def head_lanes(head):
    lane = lax.broadcasted_iota(jnp.int32, (1, 128), 1)
    return (lane < HDIM) if head == 0 else (lane >= HDIM)


def bias_rows(block_ref, doc_ref, head):
    rows = [
        jnp.broadcast_to(block_ref[0, 0, head, pl.ds(b, 1), :], (BLOCK, 128)) for b in range(TQ // BLOCK)
    ]
    return (jnp.concatenate(rows, axis=0) + doc_ref[0]).astype(jnp.bfloat16)


def unite(whole, own_ref, other_ref, side):
    half = own_ref.shape[1]
    whole[pl.ds(pl.multiple_of(side * half, TK), half), :] = own_ref[0]
    whole[pl.ds(pl.multiple_of((1 - side) * half, TK), half), :] = other_ref[0]


def forward_body(
    span_ref, q_ref, ko_ref, vo_ref, kx_ref, vx_ref, aug_ref, block_ref, doc_ref,
    out_ref, lse_ref, acc_ref, qa_ref, k_all, v_all,
):
    micro, tile = pl.program_id(0), pl.program_id(1)

    @pl.when(tile == 0)
    def _():
        unite(k_all, ko_ref, kx_ref, span_ref[micro, tile, 2])
        unite(v_all, vo_ref, vx_ref, span_ref[micro, tile, 2])

    group = q_ref.shape[2] // HDIM
    for head in range(group):
        cols = pl.ds(head // 2 * 128, 128)
        q_rows = q_ref[0, :, cols].astype(jnp.float32) * 0.125
        masked = jnp.where(head_lanes(head % 2), q_rows, 0.0).astype(jnp.bfloat16)
        qa_ref[head, :, 0:128] = masked
        qa_ref[head, :, 128:256] = bias_rows(block_ref, doc_ref, head)
    acc_ref[...] = jnp.zeros_like(acc_ref)

    def step(j, carry):
        at = pl.ds(pl.multiple_of(j * TK, TK), TK)
        aug = aug_ref[0, at, :]
        scores = []
        for head in range(group):
            cols = pl.ds(head // 2 * 128, 128)
            scores.append(nt(jnp.concatenate([k_all[at, cols], aug], axis=1), qa_ref[head]))
        fresh = []
        probs = []
        for head in range(group):
            top_new = jnp.maximum(carry[head], jnp.max(scores[head], axis=0, keepdims=True))
            probs.append(jnp.exp(scores[head] - top_new).astype(jnp.bfloat16))
            fresh.append(top_new)
        for head in range(group):
            cols = pl.ds(head // 2 * 128, 128)
            v_rows = jnp.where(head_lanes(head % 2), v_all[at, cols], jnp.bfloat16(1.0))
            part = tn(v_rows, probs[head])
            acc_ref[head] = acc_ref[head] * jnp.exp(carry[head] - fresh[head]) + part
        return tuple(fresh)

    state = tuple(jnp.full((1, TQ), -3e38, jnp.float32) for _ in range(group))
    state = lax.fori_loop(span_ref[micro, tile, 0], span_ref[micro, tile, 1], step, state)
    for pair in range(group // 2):
        done = []
        for head in range(2):
            at = pair * 2 + head
            mass = acc_ref[at, pl.ds((1 - head) * HDIM, 1), :]
            done.append(acc_ref[at, pl.ds(head * HDIM, HDIM), :] / mass)
            lse_ref[0, pair, pl.ds(head, 1), :] = state[at] + jnp.log(mass)
        out_ref[0, :, pl.ds(pair * 128, 128)] = jnp.concatenate(done, axis=0).T.astype(out_ref.dtype)


def backward_body(
    micro, carried,
    span_ref, q_ref, ko_ref, vo_ref, kx_ref, vx_ref, aug_ref, block_ref, doc_ref,
    mixed_ref, grad_ref, lse_ref, *rest,
):
    dq_ref, dko_ref, dvo_ref, dkx_ref, dvx_ref = rest[carried:carried + 5]
    dqt_ref, qa_ref, gm_ref, k_acc, v_acc, k_all, v_all = rest[carried + 5:]
    tile = pl.program_id(0)
    side = span_ref[micro, tile, 2]

    @pl.when(tile == 0)
    def _():
        unite(k_all, ko_ref, kx_ref, side)
        unite(v_all, vo_ref, vx_ref, side)
        k_acc[...] = jnp.zeros_like(k_acc)
        v_acc[...] = jnp.zeros_like(v_acc)

    group = q_ref.shape[2] // HDIM
    inner = []
    for pair in range(group // 2):
        cols = pl.ds(pair * 128, 128)
        q_rows = q_ref[0, :, cols].astype(jnp.float32) * 0.125
        grad_rows = grad_ref[0, :, cols].astype(jnp.float32)
        both = (mixed_ref[0, :, cols].astype(jnp.float32) * grad_rows).T
        for half in range(2):
            head = pair * 2 + half
            qa_ref[head, :, 0:128] = jnp.where(head_lanes(half), q_rows, 0.0).astype(jnp.bfloat16)
            qa_ref[head, :, 128:256] = bias_rows(block_ref, doc_ref, head)
            gm_ref[head] = jnp.where(head_lanes(half), grad_rows, 0.0).astype(jnp.bfloat16)
            inner.append(jnp.sum(both[half * HDIM:(half + 1) * HDIM, :], axis=0, keepdims=True))
    dqt_ref[...] = jnp.zeros_like(dqt_ref)

    def step(j, carry):
        at = pl.ds(pl.multiple_of(j * TK, TK), TK)
        aug = aug_ref[0, at, :]
        for chunk in range(0, group, CHUNK):
            heads = range(chunk, min(chunk + CHUNK, group))
            scores, grads, probs, souls = {}, {}, {}, {}
            for head in heads:
                cols = pl.ds(head // 2 * 128, 128)
                scores[head] = nt(jnp.concatenate([k_all[at, cols], aug], axis=1), qa_ref[head])
                grads[head] = nt(v_all[at, cols], gm_ref[head])
            for head in heads:
                weight = jnp.exp(scores[head] - lse_ref[0, head // 2, pl.ds(head % 2, 1), :])
                souls[head] = (weight * (grads[head] - carry[head])).astype(jnp.bfloat16)
                probs[head] = weight.astype(jnp.bfloat16)
            for head in heads:
                cols = pl.ds(head // 2 * 128, 128)
                dv = nn(probs[head], gm_ref[head])
                dk = nn(souls[head], qa_ref[head, :, 0:128])
                dqt = tn(k_all[at, cols], souls[head])
                lanes = pl.ds(head * HDIM, HDIM)
                half = head % 2
                dqt_ref[lanes, :] += dqt[half * HDIM:(half + 1) * HDIM, :]
                if half == 0:
                    dv_low, dk_low = dv, dk
                else:
                    k_acc[at, cols] += dk + dk_low
                    v_acc[at, cols] += dv + dv_low
        return carry

    lax.fori_loop(span_ref[micro, tile, 0], span_ref[micro, tile, 1], step, tuple(inner))
    for pair in range(group // 2):
        cols = pl.ds(pair * 128, 128)
        dq_ref[0, :, cols] = (dqt_ref[cols, :] * 0.125).T.astype(dq_ref.dtype)

    @pl.when(tile == pl.num_programs(0) - 1)
    def _():
        size = dko_ref.shape[1]
        mine = pl.ds(pl.multiple_of(side * size, TK), size)
        theirs = pl.ds(pl.multiple_of((1 - side) * size, TK), size)
        dko_ref[0] = k_acc[mine, :].astype(dko_ref.dtype)
        dvo_ref[0] = v_acc[mine, :].astype(dvo_ref.dtype)
        dkx_ref[0] = k_acc[theirs, :].astype(dkx_ref.dtype)
        dvx_ref[0] = v_acc[theirs, :].astype(dvx_ref.dtype)


CHUNK = 4


def specs(half, length, width, at):
    rows = pl.BlockSpec((1, TQ, width), lambda *i: at(*i) + (0,))
    side = pl.BlockSpec((1, half, width), lambda *i: (at(*i)[0], 0, 0))
    aug = pl.BlockSpec((1, length, 128), lambda *i: (at(*i)[0], 0, 0))
    block = pl.BlockSpec((1, 1, HEADS, TQ // BLOCK, 128), lambda *i: at(*i) + (0, 0, 0))
    doc = pl.BlockSpec((1, TQ, 128), lambda *i: at(*i) + (0,))
    lse = pl.BlockSpec((1, HEADS // 2, 2, TQ), lambda *i: (at(*i)[0], 0, 0, at(*i)[1]))
    return rows, side, aug, block, doc, lse


def attend_forward(span, q, ko, vo, kx, vx, aug, block, doc):
    micro, half, width = q.shape
    length = aug.shape[1]
    rows, side, aug_spec, blk, doc_spec, lse = specs(half, length, width, lambda m, t, s: (m, t))
    return pl.pallas_call(
        forward_body,
        name="attend_forward",
        out_shape=(
            jax.ShapeDtypeStruct((micro, half, width), jnp.bfloat16),
            jax.ShapeDtypeStruct((micro, HEADS // 2, 2, half), jnp.float32),
        ),
        grid_spec=pltpu.PrefetchScalarGridSpec(
            num_scalar_prefetch=1,
            grid=(micro, half // TQ),
            in_specs=[rows] + [side] * 4 + [aug_spec, blk, doc_spec],
            out_specs=(rows, lse),
            scratch_shapes=[
                pltpu.VMEM((HEADS, 128, TQ), jnp.float32),
                pltpu.VMEM((HEADS, TQ, 256), jnp.bfloat16),
                pltpu.VMEM((length, width), jnp.bfloat16),
                pltpu.VMEM((length, width), jnp.bfloat16),
            ],
        ),
        cost_estimate=pl.CostEstimate(flops=20_000_000_000, bytes_accessed=20_000_000, transcendentals=0),
    )(span, q, ko, vo, kx, vx, aug, block, doc)


def attend_backward(step, carried, span, q, ko, vo, kx, vx, aug, block, doc, mixed, grad, lse):
    micro, half, width = q.shape
    length = aug.shape[1]
    rows, side, aug_spec, blk, doc_spec, lse_spec = specs(half, length, width, lambda t, s: (step, t))
    shape = jax.ShapeDtypeStruct((micro, half, width), jnp.bfloat16)
    return pl.pallas_call(
        functools.partial(backward_body, step, len(carried)),
        name="attend_backward",
        out_shape=(shape,) * 5,
        grid_spec=pltpu.PrefetchScalarGridSpec(
            num_scalar_prefetch=1,
            grid=(half // TQ,),
            in_specs=[rows] + [side] * 4 + [aug_spec, blk, doc_spec, rows, rows, lse_spec]
            + [pl.BlockSpec(memory_space=pl.ANY)] * len(carried),
            out_specs=(rows,) + (side,) * 4,
            scratch_shapes=[
                pltpu.VMEM((width, TQ), jnp.float32),
                pltpu.VMEM((HEADS, TQ, 256), jnp.bfloat16),
                pltpu.VMEM((HEADS, TQ, 128), jnp.bfloat16),
                pltpu.VMEM((length, width), jnp.float32),
                pltpu.VMEM((length, width), jnp.float32),
                pltpu.VMEM((length, width), jnp.bfloat16),
                pltpu.VMEM((length, width), jnp.bfloat16),
            ],
        ),
        input_output_aliases={12 + i: i for i in range(len(carried))},
        cost_estimate=pl.CostEstimate(flops=20_000_000_000, bytes_accessed=20_000_000, transcendentals=0),
    )(span, q, ko, vo, kx, vx, aug, block, doc, mixed, grad, lse, *carried)


def tables(segment, rand_blocks, side, half):
    micro, length = segment.shape
    blocks = length // BLOCK
    mine = half // BLOCK
    tiles = half // TQ
    lane = lax.broadcasted_iota(jnp.int32, (1, 1, 128), 2)
    own = lax.dynamic_slice_in_dim(segment, side * half, half, axis=1)
    place = lax.broadcasted_iota(jnp.int32, (1, length, 1), 1) // BLOCK
    aug = ((lane == place) | (lane == segment[:, :, None] + blocks)).astype(jnp.bfloat16)
    doc = jnp.where((lane >= blocks) & (lane < blocks + 4) & (lane != own[:, :, None] + blocks), NEG, 0.0)
    q_block = side * mine + lax.broadcasted_iota(jnp.int32, (1, 1, mine, 1), 2)
    k_block = lax.broadcasted_iota(jnp.int32, (1, 1, 1, 128), 3)
    chosen = lax.dynamic_slice_in_dim(rand_blocks, side * mine, mine, axis=2)
    allowed = (jnp.abs(q_block - k_block) <= 1) | (k_block == 0) | (k_block == blocks - 1)
    allowed = allowed | (q_block == 0) | (q_block == blocks - 1) | (k_block >= blocks)
    for pick in range(rand_blocks.shape[3]):
        allowed = allowed | (chosen[:, :, :, pick:pick + 1] == k_block)
    block = jnp.where(allowed, 0.0, NEG).astype(jnp.float32)
    block = jnp.moveaxis(block.reshape(micro, HEADS, tiles, mine // tiles, 128), 2, 1)
    edges = own.reshape(micro, tiles, TQ)
    first, last = edges[:, :, :1], edges[:, :, TQ - 1:]
    begin = jnp.sum((segment[:, None, :] < first).astype(jnp.int32), axis=-1)
    end = jnp.sum((segment[:, None, :] <= last).astype(jnp.int32), axis=-1)
    span = jnp.stack([begin // TK, (end + TK - 1) // TK, jnp.full_like(begin, side)], axis=-1)
    return span, aug, block, doc.astype(jnp.float32)


MESH = pl.DeviceIdType.MESH
GROUPS = 3


def place():
    rep, shard, side = lax.axis_index("rep"), lax.axis_index("fsdp"), lax.axis_index("seq")
    quad = lax.rem(rep, 4)
    across, along = lax.rem(quad, 2), quad // 2
    near = (1 - 2 * across, 2 - 4 * along)
    return rep, shard, side, quad, near


def chunk(refs, group, shard, quad, side, rows, half=None):
    width = 768 if half is None else 384
    offset = 0 if half is None else half * 384
    low = side * rows
    if group == 0:
        return refs[0].at[quad, pl.ds(pl.multiple_of(shard * (2 * rows) + low, 16), rows), pl.ds(offset, width)]
    if group == 1:
        at = pl.multiple_of(shard * (2 * rows) + low, 16)
        return refs[1].at[pl.ds(at, rows), pl.ds(pl.multiple_of(quad * 768 + offset, 128), width)]
    at = pl.multiple_of(shard * (8 * rows) + quad * (2 * rows) + low, 16)
    return refs[2].at[pl.ds(at, rows), pl.ds(offset, width)]


def greet(peers):
    barrier = pltpu.get_barrier_semaphore()
    for peer in peers:
        pl.semaphore_signal(barrier, inc=1, device_id=peer, device_id_type=MESH)
    pl.semaphore_wait(barrier, len(peers))


def remote(src, dst, send, recv, peer):
    return pltpu.make_async_remote_copy(
        src_ref=src, dst_ref=dst, send_sem=send, recv_sem=recv, device_id=peer, device_id_type=MESH
    )


def gather_body(
    shards, rows, qkvo_in, up_in, down_in, vec_in, x_in,
    qkvo_out, up_out, down_out, vec_out, normed_out, q_out, k_out, v_out, kx_out, vx_out,
    qkvo_stage, up_stage, down_stage, vec_all, weights, normed, results,
    in_sem, out_sem, z_send, z_recv, x_send, x_recv, y_send, y_recv, d_send, d_recv, c_send, c_recv,
    load_sem, save_sem, swap_send, swap_recv,
):
    rep, shard, side, quad, (dx, dy) = place()
    ins, outs = (qkvo_in, up_in, down_in), (qkvo_out, up_out, down_out)
    stages = (qkvo_stage, up_stage, down_stage)
    x_peer, y_peer, partner = (rep + dx, shard, side), (rep + dy, shard, side), (rep, shard, 1 - side)
    z_peers = [(rep, lax.rem(shard + k, shards), side) for k in range(1, shards)]
    for i, src in enumerate(ins):
        pltpu.make_async_copy(src, stages[i], in_sem.at[i]).start()
    greet(z_peers + [x_peer, y_peer, partner])
    sent = []

    def go(copy):
        copy.start()
        sent.append(copy)

    for g in range(GROUPS):
        for k in range(1, shards):
            go(remote(
                chunk(ins, g, 0, quad, side, rows), chunk(outs, g, shard, quad, side, rows),
                z_send.at[g, k - 1], z_recv.at[g, shards - k - 1], z_peers[k - 1],
            ))
        if g == 0:
            for k in range(1, shards):
                go(remote(
                    vec_in, vec_all.at[k - 1],
                    z_send.at[GROUPS, k - 1], z_recv.at[GROUPS, k - 1], z_peers[k - 1],
                ))
    owned = (
        qkvo_out.at[:, pl.ds(pl.multiple_of(shard * 2 * rows, 16), 2 * rows), :],
        up_out.at[pl.ds(pl.multiple_of(shard * 2 * rows, 16), 2 * rows), :],
        down_out.at[pl.ds(pl.multiple_of(shard * 8 * rows, 16), 8 * rows), :],
    )
    local = []
    for i, src in enumerate(ins):
        pltpu.make_async_copy(src, stages[i], in_sem.at[i]).wait()
        copy = pltpu.make_async_copy(stages[i], owned[i], out_sem.at[i])
        copy.start()
        local.append(copy)

    def piece(g, k, member, core, half=None):
        return chunk(outs, g, lax.rem(shard + k, shards), member, core, rows, half)

    def hop(g, k, member, core, send, recv, peer, half=None):
        ref = piece(g, k, member, core, half)
        return remote(ref, ref, send, recv, peer)

    x_quad, y_quad, d_quad = quad + dx, quad + dy, quad + dx + dy

    def straight(g):
        for k in range(1, shards):
            hop(g, k, quad, side, z_send.at[g, k - 1], z_recv.at[g, k - 1], z_peers[k - 1]).wait_recv()
            go(hop(g, k, quad, side, x_send.at[g, k - 1], x_recv.at[g, k - 1], x_peer))
            go(hop(g, k, quad, side, y_send.at[g, k - 1], y_recv.at[g, k - 1], y_peer))
            go(hop(g, k, quad, side, c_send.at[g, k - 1, 0], c_recv.at[g, k - 1, 0], partner))

    def turn(g):
        for k in range(1, shards):
            hop(g, k, x_quad, side, x_send.at[g, k - 1], x_recv.at[g, k - 1], x_peer).wait_recv()
            go(hop(g, k, x_quad, side, d_send.at[g, k - 1, 1], d_recv.at[g, k - 1, 1], y_peer, 1))
            go(hop(g, k, x_quad, side, c_send.at[g, k - 1, 1], c_recv.at[g, k - 1, 1], partner))
            hop(g, k, y_quad, side, y_send.at[g, k - 1], y_recv.at[g, k - 1], y_peer).wait_recv()
            go(hop(g, k, y_quad, side, d_send.at[g, k - 1, 0], d_recv.at[g, k - 1, 0], x_peer, 0))
            go(hop(g, k, y_quad, side, c_send.at[g, k - 1, 2], c_recv.at[g, k - 1, 2], partner))

    def corner(g):
        for k in range(1, shards):
            hop(g, k, d_quad, side, d_send.at[g, k - 1, 0], d_recv.at[g, k - 1, 0], x_peer, 0).wait_recv()
            hop(g, k, d_quad, side, d_send.at[g, k - 1, 1], d_recv.at[g, k - 1, 1], y_peer, 1).wait_recv()
            go(hop(g, k, d_quad, side, c_send.at[g, k - 1, 3], c_recv.at[g, k - 1, 3], partner))

    def gathered(g):
        for k in range(1, shards):
            for i, member in enumerate((quad, x_quad, y_quad, d_quad)):
                hop(g, k, member, 1 - side, c_send.at[g, k - 1, i], c_recv.at[g, k - 1, i], partner).wait_recv()

    def save(i, target):
        copy = pltpu.make_async_copy(normed if i == 3 else results.at[i], target, save_sem.at[i])
        copy.start()
        local.append(copy)

    def norm(step, carry):
        at = pl.ds(pl.multiple_of(step * STEP, STEP), STEP)
        values = x_in[at, :].astype(jnp.float32)
        centre = values - jnp.mean(values, axis=-1, keepdims=True)
        scale = lax.rsqrt(jnp.mean(centre * centre, axis=-1, keepdims=True) + norm_eps)
        normed[at, :] = (centre * scale * vec_out[0:1, :] + vec_out[1:2, :]).astype(normed.dtype)
        return carry

    def project(i, row):
        pltpu.make_async_copy(qkvo_out.at[i], weights.at[i], load_sem.at[i]).wait()

        def step(j, carry):
            at = pl.ds(pl.multiple_of(j * STEP, STEP), STEP)
            product = nn(normed[at, :], weights[i])
            if row is not None:
                product = product + vec_out[row:row + 1, :]
            results[i, at, :] = product.astype(results.dtype)
            return carry
        lax.fori_loop(0, normed.shape[0] // STEP, step, 0)

    def exchange(i, target):
        copy = remote(results.at[i], target, swap_send.at[i - 1], swap_recv.at[i - 1], partner)
        copy.start()
        return copy

    straight(0)
    for k in range(1, shards):
        remote(
            vec_in, vec_all.at[k - 1], z_send.at[GROUPS, k - 1], z_recv.at[GROUPS, k - 1], z_peers[k - 1]
        ).wait_recv()
    total = vec_in[...].astype(jnp.float32)
    for k in range(1, shards):
        total = total + vec_all[k - 1].astype(jnp.float32)
    vec_out[...] = total
    lax.fori_loop(0, normed.shape[0] // STEP // 2, norm, 0)
    turn(0)
    lax.fori_loop(normed.shape[0] // STEP // 2, normed.shape[0] // STEP, norm, 0)
    save(3, normed_out)
    straight(1)
    corner(0)
    turn(1)
    local[0].wait()
    gathered(0)
    for i in (1, 2, 0):
        pltpu.make_async_copy(qkvo_out.at[i], weights.at[i], load_sem.at[i]).start()
    straight(2)
    project(1, None)
    keys = exchange(1, kx_out)
    save(1, k_out)
    corner(1)
    project(2, 3)
    values = exchange(2, vx_out)
    save(2, v_out)
    turn(2)
    project(0, 2)
    save(0, q_out)
    corner(2)
    gathered(1)
    gathered(2)
    keys.wait()
    values.wait()
    for copy in sent:
        copy.wait_send()
    for copy in local[1:]:
        copy.wait()


STEP = 256


def gather_weights(shards, qkvo, up, down, vec, x):
    rows = qkvo.shape[1] // 2
    model = qkvo.shape[2]
    hidden = up.shape[1]
    any_space = pl.BlockSpec(memory_space=pl.ANY)
    vmem_space = pl.BlockSpec(memory_space=pltpu.VMEM)
    dma = pltpu.SemaphoreType.DMA
    low = jnp.bfloat16
    token = jax.ShapeDtypeStruct(x.shape, low)
    return pl.pallas_call(
        functools.partial(gather_body, shards, rows),
        name="gather_weights",
        out_shape=(
            jax.ShapeDtypeStruct((4, model, model), low),
            jax.ShapeDtypeStruct((model, hidden), low),
            jax.ShapeDtypeStruct((hidden, model), low),
            jax.ShapeDtypeStruct(vec.shape, jnp.float32),
        )
        + (token,) * 6,
        in_specs=[any_space] * 3 + [vmem_space] * 2,
        out_specs=(any_space,) * 3 + (vmem_space,) + (any_space,) * 6,
        scratch_shapes=[
            pltpu.VMEM(qkvo.shape, low), pltpu.VMEM(up.shape, low), pltpu.VMEM(down.shape, low),
            pltpu.VMEM((shards - 1,) + vec.shape, low),
            pltpu.VMEM((3, model, model), low),
            pltpu.VMEM(x.shape, low),
            pltpu.VMEM((3,) + x.shape, low),
            dma((3,)), dma((3,)),
            dma((GROUPS + 1, shards - 1)), dma((GROUPS + 1, shards - 1)),
        ]
        + [dma((GROUPS, shards - 1))] * 4
        + [dma((GROUPS, shards - 1, 2))] * 2
        + [dma((GROUPS, shards - 1, 4))] * 2
        + [dma((3,)), dma((4,)), dma((2,)), dma((2,))],
        compiler_params=pltpu.CompilerParams(
            collective_id=0, has_side_effects=True, vmem_limit_bytes=50_000_000
        ),
    )(qkvo, up, down, vec, x)


def add_into(out_ref, refs):
    total = refs[0][...].astype(jnp.float32)
    for ref in refs[1:]:
        total = total + ref[...].astype(jnp.float32)
    out_ref[...] = total.astype(out_ref.dtype)


def reduce_body(
    shards, quads, rows, q_in, k_in, v_in, o_in, up_in, down_in, vec_in, qkvo_out, up_out, down_out, vec_out,
    own, mate, first, second, last, last_up, last_down, ring, ring_up, ring_down,
    full, full_up, full_down, vec_sum, vec_mate, vec_last, vec_ring,
    load_sem, c_send, c_recv, f_send, f_recv, s_send, s_recv, z_send, z_recv, q_send, q_recv,
    x_send, x_recv, y_send, y_recv, d_send, d_recv, g_send, g_recv, out_sem, v_send, v_recv,
):
    rep, shard, side, quad, (dx, dy) = place()
    x_peer, y_peer, partner = (rep + dx, shard, side), (rep + dy, shard, side), (rep, shard, 1 - side)
    x_quad, y_quad, d_quad = quad + dx, quad + dy, quad + dx + dy
    z_peers = [(rep, lax.rem(shard + k, shards), side) for k in range(1, shards)]
    q_peers = [(lax.rem(rep + 4 * k, 4 * quads), shard, side) for k in range(1, quads)]
    greet(z_peers + q_peers + [x_peer, y_peer, partner])
    fulls, lasts, rings = (full, full_up, full_down), (last, last_up, last_down), (ring, ring_up, ring_down)

    def source(g, f):
        return (own.at[f, quad], up_in.at[f], down_in.at[f])[g]

    def block(f, m, core):
        at = pl.multiple_of(f * (2 * rows) + core * rows, 16)
        return (q_in, k_in, v_in, o_in)[m].at[pl.ds(at, rows), :]

    def c_copy(f, m):
        return remote(block(f, m, 1 - side), mate.at[f, m], c_send.at[f, m], c_recv.at[f, m], partner)

    def load(f, m):
        return pltpu.make_async_copy(block(f, m, side), own.at[f, m], load_sem.at[f, m])

    def f_copy(f, slot, flip):
        peer, to = (y_peer, y_quad) if flip else (x_peer, x_quad)
        member = to if slot == 0 else d_quad
        return remote(own.at[f, member], first.at[f, slot], f_send.at[f, slot], f_recv.at[f, slot], peer)

    def s_copy(f, flip):
        peer, to = (x_peer, x_quad) if flip else (y_peer, y_quad)
        return remote(own.at[f, to], second.at[f], s_send.at[f], s_recv.at[f], peer)

    def z_copy(g, k):
        return remote(
            source(g, lax.rem(shard + k, shards)), lasts[g].at[shards - k - 1],
            z_send.at[g, k - 1], z_recv.at[g, shards - k - 1], z_peers[k - 1],
        )

    def z_wait(g, k):
        remote(source(g, shard), lasts[g].at[k - 1], z_send.at[g, k - 1], z_recv.at[g, k - 1], z_peers[k - 1]).wait_recv()

    def vec_go(src, dst, i, peer):
        copy = remote(src, dst, v_send.at[i], v_recv.at[i], peer)
        copy.start()
        return copy

    def spread(g, member, send, recv, peer, half=None, core=None):
        core = side if core is None else core
        ref = fulls[g].at[core, member]
        if half is not None:
            width = ref.shape[-1] // 2
            ref = fulls[g].at[core, member, :, pl.ds(half * width, width)]
        return remote(ref, ref, send, recv, peer)

    def swirl(g):
        mine = fulls[g].at[side, quad]
        for k in range(1, shards):
            z_wait(g, k)
        add_into(mine, [source(g, shard)] + [lasts[g].at[k] for k in range(shards - 1)])
        for k in range(1, quads):
            remote(mine, rings[g].at[quads - k - 1], q_send.at[g, k - 1], q_recv.at[g, quads - k - 1], q_peers[k - 1]).start()
        for k in range(1, quads):
            remote(mine, rings[g].at[k - 1], q_send.at[g, k - 1], q_recv.at[g, k - 1], q_peers[k - 1]).wait()
        if quads > 1:
            add_into(mine, [mine] + [rings[g].at[k] for k in range(quads - 1)])
        spread(g, quad, x_send.at[g], x_recv.at[g], x_peer).start()
        spread(g, quad, y_send.at[g], y_recv.at[g], y_peer).start()
        spread(g, quad, g_send.at[g, 0], g_recv.at[g, 0], partner).start()

    def turn(g):
        spread(g, x_quad, x_send.at[g], x_recv.at[g], x_peer).wait_recv()
        spread(g, x_quad, d_send.at[g, 1], d_recv.at[g, 1], y_peer, 1).start()
        spread(g, x_quad, g_send.at[g, 1], g_recv.at[g, 1], partner).start()
        spread(g, y_quad, y_send.at[g], y_recv.at[g], y_peer).wait_recv()
        spread(g, y_quad, d_send.at[g, 0], d_recv.at[g, 0], x_peer, 0).start()
        spread(g, y_quad, g_send.at[g, 2], g_recv.at[g, 2], partner).start()

    def corner(g):
        spread(g, d_quad, d_send.at[g, 0], d_recv.at[g, 0], x_peer, 0).wait_recv()
        spread(g, d_quad, d_send.at[g, 1], d_recv.at[g, 1], y_peer, 1).wait_recv()
        spread(g, d_quad, g_send.at[g, 3], g_recv.at[g, 3], partner).start()

    def target(g, m, core):
        if g == 0:
            return qkvo_out.at[m, pl.ds(core * rows, rows), :]
        if g == 1:
            return up_out.at[pl.ds(core * rows, rows), pl.ds(m * 768, 768)]
        return down_out.at[pl.ds((core * 4 + m) * rows, rows), :]

    def put(g, m, core):
        return pltpu.make_async_copy(fulls[g].at[core, m], target(g, m, core), out_sem.at[g, m, core])

    def finish(g):
        for i, member in enumerate((quad, x_quad, y_quad, d_quad)):
            spread(g, member, g_send.at[g, i], g_recv.at[g, i], partner, core=1 - side).wait_recv()
        for m in range(4):
            for core in range(2):
                put(g, m, core).start()

    swap_one = vec_go(vec_in, vec_mate.at[0], 0, partner)

    def begin(f, carry):
        for m in range(4):
            c_copy(f, m).start()
            load(f, m).start()
        return carry
    lax.fori_loop(0, shards, begin, 0)
    for g in (2, 1):
        for k in range(1, shards):
            z_copy(g, k).start()

    def merge(step, carry):
        for flip in range(2):
            f = step * 2 + flip
            for m in range(4):
                load(f, m).wait()
                c_copy(f, m).wait_recv()
                add_into(own.at[f, m], (own.at[f, m], mate.at[f, m]))
            for slot in range(2):
                f_copy(f, slot, flip).start()
        return carry
    lax.fori_loop(0, shards // 2, merge, 0)
    swap_one.wait_recv()
    vec_sum[...] = vec_in[...] + vec_mate[0]
    swap = vec_go(vec_sum, vec_mate.at[1], 1, x_peer)

    def fold(step, carry):
        for flip in range(2):
            f = step * 2 + flip
            for slot in range(2):
                f_copy(f, slot, flip).wait()
                member = quad if slot == 0 else (x_quad if flip else y_quad)
                add_into(own.at[f, member], (own.at[f, member], first.at[f, slot]))
            s_copy(f, flip).start()
        return carry
    lax.fori_loop(0, shards // 2, fold, 0)
    swap.wait()
    vec_sum[...] = vec_sum[...] + vec_mate[1]
    swap = vec_go(vec_sum, vec_mate.at[2], 2, y_peer)

    def settle(step, carry):
        for flip in range(2):
            f = step * 2 + flip
            s_copy(f, flip).wait()
            add_into(own.at[f, quad], (own.at[f, quad], second.at[f]))
        return carry
    lax.fori_loop(0, shards // 2, settle, 0)
    for k in range(1, shards):
        z_copy(0, k).start()
    swap.wait()
    vec_sum[...] = vec_sum[...] + vec_mate[2]
    for k in range(1, shards):
        remote(
            vec_sum.at[lax.rem(shard + k, shards)], vec_last.at[shards - k - 1],
            v_send.at[2 + k], v_recv.at[2 + shards - k], z_peers[k - 1],
        ).start()
    swirl(2)
    swirl(1)
    turn(2)
    turn(1)
    corner(2)
    corner(1)
    swirl(0)
    for k in range(1, shards):
        remote(vec_sum.at[shard], vec_last.at[k - 1], v_send.at[2 + k], v_recv.at[2 + k], z_peers[k - 1]).wait()
    total = vec_sum[shard]
    for k in range(shards - 1):
        total = total + vec_last[k]
    vec_ring[0] = total
    for k in range(1, quads):
        remote(vec_ring.at[0], vec_ring.at[quads - k], v_send.at[2 + shards + k], v_recv.at[2 + shards + quads - k], q_peers[k - 1]).start()
    for k in range(1, quads):
        remote(vec_ring.at[0], vec_ring.at[k], v_send.at[2 + shards + k], v_recv.at[2 + shards + k], q_peers[k - 1]).wait()
        total = total + vec_ring[k]
    vec_out[...] = total
    finish(2)
    finish(1)
    turn(0)
    corner(0)
    finish(0)
    for g in range(GROUPS):
        for m in range(4):
            for core in range(2):
                put(g, m, core).wait()
        for k in range(1, shards):
            z_copy(g, k).wait_send()
        spread(g, quad, x_send.at[g], x_recv.at[g], x_peer).wait_send()
        spread(g, quad, y_send.at[g], y_recv.at[g], y_peer).wait_send()
        spread(g, y_quad, d_send.at[g, 0], d_recv.at[g, 0], x_peer, 0).wait_send()
        spread(g, x_quad, d_send.at[g, 1], d_recv.at[g, 1], y_peer, 1).wait_send()
        for i in range(4):
            spread(g, quad, g_send.at[g, i], g_recv.at[g, i], partner).wait_send()

    def drain(f, carry):
        for m in range(4):
            c_copy(f, m).wait_send()
        return carry
    lax.fori_loop(0, shards, drain, 0)
    swap_one.wait_send()


def reduce_grads(shards, quads, qkvo, up, down, vec):
    model = qkvo[0].shape[1]
    rows = model // shards // 2
    any_space = pl.BlockSpec(memory_space=pl.ANY)
    vmem_space = pl.BlockSpec(memory_space=pltpu.VMEM)
    dma = pltpu.SemaphoreType.DMA
    low = jnp.bfloat16
    wide = jnp.float32
    pieces = ((rows, model), up.shape[1:], down.shape[1:])
    vec_one = vec.shape[1:]
    spare = max(quads - 1, 1)
    return pl.pallas_call(
        functools.partial(reduce_body, shards, quads, rows),
        name="reduce_grads",
        out_shape=(
            jax.ShapeDtypeStruct((4, 2 * rows, model), low),
            jax.ShapeDtypeStruct((2 * rows, 4 * model), low),
            jax.ShapeDtypeStruct((8 * rows, model), low),
            jax.ShapeDtypeStruct(vec_one, wide),
        ),
        in_specs=[any_space] * 4 + [vmem_space] * 3,
        out_specs=(any_space,) * 3 + (vmem_space,),
        scratch_shapes=[
            pltpu.VMEM((shards, 4) + pieces[0], low),
            pltpu.VMEM((shards, 4) + pieces[0], low),
            pltpu.VMEM((shards, 2) + pieces[0], low),
            pltpu.VMEM((shards,) + pieces[0], low),
        ]
        + [pltpu.VMEM((shards - 1,) + piece, low) for piece in pieces]
        + [pltpu.VMEM((spare,) + piece, low) for piece in pieces]
        + [pltpu.VMEM((2, 4) + piece, low) for piece in pieces]
        + [
            pltpu.VMEM(vec.shape, wide),
            pltpu.VMEM((3,) + vec.shape, wide),
            pltpu.VMEM((shards - 1,) + vec_one, wide),
            pltpu.VMEM((quads,) + vec_one, wide),
            dma((shards, 4)),
            dma((shards, 4)), dma((shards, 4)),
            dma((shards, 2)), dma((shards, 2)),
            dma((shards,)), dma((shards,)),
            dma((GROUPS, shards - 1)), dma((GROUPS, shards - 1)),
            dma((GROUPS, spare)), dma((GROUPS, spare)),
            dma((GROUPS,)), dma((GROUPS,)), dma((GROUPS,)), dma((GROUPS,)),
            dma((GROUPS, 2)), dma((GROUPS, 2)),
            dma((GROUPS, 4)), dma((GROUPS, 4)),
            dma((GROUPS, 4, 2)),
            dma((3 + shards + quads,)), dma((3 + shards + quads,)),
        ],
        compiler_params=pltpu.CompilerParams(
            collective_id=1, has_side_effects=True, vmem_limit_bytes=60_000_000
        ),
    )(*qkvo, up, down, vec)


def normal_parts(values):
    phi = 0.5 + 0.5 * lax.erf(values * 0.7071067811865476)
    return phi, values * (jnp.exp(-0.5 * values * values) * 0.3989422804014327)


def middle_body(
    shards, rows,
    mixed_in, x_in, grad_in, out_w_in, up_w_in, down_w_in, vec_in, up_b_in,
    result_out, attn_out, mixed_out, d_out_out, up_out, down_out, sums_out, up_sum_out,
    mixed, x, grad, out_w, up_w, down_w, middle, normed, turned, hidden, slope,
    up_grad, down_grad, up_mate, down_mate, up_first, down_first, up_second, down_second,
    load_sem, save_sem, uc_send, uc_recv, dc_send, dc_recv, f_send, f_recv, s_send, s_recv,
):
    rep, shard, side, quad, (dx, dy) = place()
    partner = (rep, shard, 1 - side)
    low, wide = jnp.bfloat16, jnp.float32
    steps = x.shape[0] // STEP
    model = x.shape[1]
    width = 8 * rows
    loads = [
        pltpu.make_async_copy(src, dst, load_sem.at[i])
        for i, (src, dst) in enumerate(((mixed_in, mixed), (x_in, x), (out_w_in, out_w), (grad_in, grad)))
    ]
    for f in range(shards):
        at = pl.ds(f * width, width)
        loads.append(pltpu.make_async_copy(up_w_in.at[:, at], up_w.at[f], load_sem.at[4 + f]))
        loads.append(pltpu.make_async_copy(down_w_in.at[at, :], down_w.at[f], load_sem.at[4 + shards + f]))
    for load in loads:
        load.start()
    greet([(rep + dx, shard, side), (rep + dy, shard, side), partner])
    grads, mates = (up_grad, down_grad), (up_mate, down_mate)
    firsts, seconds = (up_first, down_first), (up_second, down_second)

    def row(i):
        return vec_in[i:i + 1, :]

    def block(j):
        return pl.ds(pl.multiple_of(j * STEP, STEP), STEP)

    def part(g, f, m):
        return up_grad.at[m, f, side] if g == 0 else down_grad.at[f, side, m]

    def mate(g, f, m):
        return up_mate.at[m, f] if g == 0 else down_mate.at[f, m]

    def flip_way(f, second):
        odd = lax.rem(f + second, 2)
        return dx + odd * (dy - dx)

    def up_cross(m):
        return remote(up_grad.at[m, :, 1 - side], up_mate.at[m], uc_send.at[m], uc_recv.at[m], partner)

    def down_cross(f):
        return remote(down_grad.at[f, 1 - side], down_mate.at[f], dc_send.at[f], dc_recv.at[f], partner)

    def f_copy(g, f, slot):
        way = flip_way(f, 0)
        member = quad + way if slot == 0 else quad + dx + dy
        return remote(part(g, f, member), firsts[g].at[f, slot], f_send.at[g, f, slot], f_recv.at[g, f, slot], (rep + way, shard, side))

    def s_copy(g, f):
        way = flip_way(f, 1)
        return remote(part(g, f, quad + way), seconds[g].at[f], s_send.at[g, f], s_recv.at[g, f], (rep + way, shard, side))

    def first_go(g, f):
        for slot in range(2):
            f_copy(g, f, slot).start()

    def down_merge(f):
        down_cross(f).wait_recv()
        for m in range(4):
            add_into(part(1, f, m), (part(1, f, m), mate(1, f, m)))
        first_go(1, f)

    def up_merge(m):
        up_cross(m).wait_recv()

        def step(f, carry):
            add_into(part(0, f, m), (part(0, f, m), mate(0, f, m)))
            return carry
        lax.fori_loop(0, shards, step, 0)

    def each(body):
        def step(f, carry):
            body(f)
            return carry
        lax.fori_loop(0, shards, step, 0)

    def fold(g):
        def body(f):
            for slot in range(2):
                f_copy(g, f, slot).wait()
                member = quad if slot == 0 else quad + flip_way(f, 1)
                add_into(part(g, f, member), (part(g, f, member), firsts[g].at[f, slot]))
            s_copy(g, f).start()
        each(body)

    def settle(g, target):
        def body(f):
            s_copy(g, f).wait()
            add_into(target.at[f], (part(g, f, quad), seconds[g].at[f]))
        each(body)

    saves = []

    def save(src, dst):
        copy = pltpu.make_async_copy(src, dst, save_sem.at[len(saves)])
        copy.start()
        saves.append(copy)

    for load in loads[:3]:
        load.wait()

    def attend_out(j, carry):
        at = block(j)
        values = x[at, :].astype(wide) + nn(mixed[at, :], out_w[...]) + row(4)
        middle[at, :] = values
        centre = values - jnp.mean(values, axis=-1, keepdims=True)
        scale = lax.rsqrt(jnp.mean(centre * centre, axis=-1, keepdims=True) + norm_eps)
        out = centre * scale * row(5) + row(6)
        normed[at, :] = out.astype(low)
        turned[:, at] = out.T.astype(low)
        return carry
    lax.fori_loop(0, steps, attend_out, 0)
    for load in loads[3:]:
        load.wait()

    def expand(f):
        def step(j, carry):
            at = block(j)
            inner = nn(normed[at, :], up_w[f]) + up_b_in[f]
            phi, bump = normal_parts(inner)
            hidden[f, at, :] = (inner * phi).astype(low)
            slope[f, at, :] = (phi + bump).astype(low)
            return carry
        lax.fori_loop(0, steps, step, 0)
        down_grad[f] = tn(hidden[f], grad[...]).astype(low).reshape(2, 4, rows, model)
        down_cross(f).start()

        @pl.when(f > 0)
        def _():
            down_merge(f - 1)
    each(expand)

    def contract(m):
        for h in range(model // width):
            f = m * (model // width) + h

            def step(j, total, f=f):
                at = block(j)
                value = (nt(grad[at, :], down_w[f]) * slope[f, at, :].astype(wide)).astype(low)
                slope[f, at, :] = value
                return total + jnp.sum(value.astype(wide), axis=0, keepdims=True)
            up_sum_out[f] = lax.fori_loop(0, steps, step, jnp.zeros((1, width), wide))
            product = nn(turned[...], slope[f]).astype(low)
            up_grad[m, :, :, :, pl.ds(h * width, width)] = product.reshape(shards, 2, rows, width)
        up_cross(m).start()

        @pl.when(m == 0)
        def _():
            down_merge(shards - 1)

        @pl.when(m > 0)
        def _():
            up_merge(m - 1)

    def contract_step(m, carry):
        contract(m)
        return carry
    lax.fori_loop(0, 4, contract_step, 0)
    fold(1)
    up_merge(3)
    each(lambda f: first_go(0, f))

    def finish(j, carry):
        at = block(j)
        total = middle[at, :] + row(7)
        for f in range(shards):
            total = total + nn(hidden[f, at, :], down_w[f])
        x[at, :] = total.astype(low)
        return carry
    lax.fori_loop(0, steps, finish, 0)
    save(x, result_out)

    def back(j, carry):
        gain_sum, bias_sum, attn_sum, grad_sum = carry
        at = block(j)
        error = nt(slope[0, at, :], up_w[0])
        for f in range(1, shards):
            error = error + nt(slope[f, at, :], up_w[f])
        values = middle[at, :]
        centre = values - jnp.mean(values, axis=-1, keepdims=True)
        scale = lax.rsqrt(jnp.mean(centre * centre, axis=-1, keepdims=True) + norm_eps)
        unit = centre * scale
        scaled = error * row(5)
        mean_one = jnp.mean(scaled, axis=-1, keepdims=True)
        mean_two = jnp.mean(scaled * unit, axis=-1, keepdims=True)
        upstream = grad[at, :].astype(wide)
        attn = (upstream + scale * (scaled - mean_one - unit * mean_two)).astype(low)
        grad[at, :] = attn
        normed[at, :] = nt(attn, out_w[...]).astype(low)
        column = lambda array: jnp.sum(array, axis=0, keepdims=True)
        return (
            gain_sum + column(error * unit), bias_sum + column(error),
            attn_sum + column(attn.astype(wide)), grad_sum + column(upstream),
        )
    zero = jnp.zeros((1, model), wide)
    sums = lax.fori_loop(0, steps // 2, back, (zero,) * 4)
    fold(0)
    sums = lax.fori_loop(steps // 2, steps, back, sums)
    save(normed, mixed_out)
    save(grad, attn_out)
    for i, value in enumerate(sums):
        sums_out[i:i + 1, :] = value
    sums_out[4:8, :] = jnp.zeros((4, model), wide)
    settle(1, down_out)
    out_w[...] = tn(mixed[...], grad[...]).astype(low)
    save(out_w, d_out_out)
    settle(0, up_out)
    for m in range(4):
        up_cross(m).wait_send()
    each(lambda f: down_cross(f).wait_send())
    for copy in saves:
        copy.wait()


def middle_layer(shards, mixed, x, grad, out_w, up_w, down_w, vec, up_b):
    tokens, model = x.shape
    hidden = up_w.shape[1]
    rows = model // shards // 2
    width = 8 * rows
    any_space = pl.BlockSpec(memory_space=pl.ANY)
    vmem_space = pl.BlockSpec(memory_space=pltpu.VMEM)
    dma = pltpu.SemaphoreType.DMA
    low, wide = jnp.bfloat16, jnp.float32
    token = jax.ShapeDtypeStruct((tokens, model), low)
    flat = pltpu.VMEM((tokens, model), low)
    return pl.pallas_call(
        functools.partial(middle_body, shards, rows),
        name="middle_layer",
        out_shape=(
            token, token, token,
            jax.ShapeDtypeStruct((model, model), low),
            jax.ShapeDtypeStruct((shards, rows, model), low),
            jax.ShapeDtypeStruct((shards, rows, model), low),
            jax.ShapeDtypeStruct((8, model), wide),
            jax.ShapeDtypeStruct((shards, 1, width), wide),
        ),
        in_specs=[any_space] * 6 + [vmem_space] * 2,
        out_specs=(any_space,) * 4 + (vmem_space,) * 4,
        scratch_shapes=[
            flat, flat, flat,
            pltpu.VMEM((model, model), low),
            pltpu.VMEM((shards, model, width), low),
            pltpu.VMEM((shards, width, model), low),
            pltpu.VMEM((tokens, model), wide),
            flat,
            pltpu.VMEM((model, tokens), low),
            pltpu.VMEM((shards, tokens, width), low),
            pltpu.VMEM((shards, tokens, width), low),
            pltpu.VMEM((4, shards, 2, rows, model), low),
            pltpu.VMEM((shards, 2, 4, rows, model), low),
            pltpu.VMEM((4, shards, rows, model), low),
            pltpu.VMEM((shards, 4, rows, model), low),
            pltpu.VMEM((shards, 2, rows, model), low),
            pltpu.VMEM((shards, 2, rows, model), low),
            pltpu.VMEM((shards, rows, model), low),
            pltpu.VMEM((shards, rows, model), low),
            dma((4 + 2 * shards,)), dma((4,)),
            dma((4,)), dma((4,)), dma((shards,)), dma((shards,)),
            dma((2, shards, 2)), dma((2, shards, 2)), dma((2, shards)), dma((2, shards)),
        ],
        compiler_params=pltpu.CompilerParams(
            collective_id=2, has_side_effects=True, vmem_limit_bytes=66_000_000
        ),
    )(mixed, x, grad, out_w, up_w, down_w, vec, up_b)


def unit_of(values):
    centre = values - jnp.mean(values, axis=-1, keepdims=True)
    scale = lax.rsqrt(jnp.mean(centre * centre, axis=-1, keepdims=True) + norm_eps)
    return centre * scale, scale


def layer_norm(values, gain, offset):
    unit, scale = unit_of(values)
    return unit, scale, (unit * gain + offset).astype(jnp.bfloat16)


def norm_back(upstream, unit, scale, gain):
    scaled = upstream * gain
    mean_one = jnp.mean(scaled, axis=-1, keepdims=True)
    mean_two = jnp.mean(scaled * unit, axis=-1, keepdims=True)
    return (
        scale * (scaled - mean_one - unit * mean_two),
        jnp.sum(upstream * unit, axis=0),
        jnp.sum(upstream, axis=0),
    )


def on_device(
    shards, quads,
    layer_input, segment, rand_blocks, first_gain, first_bias, query_weight, query_bias,
    key_weight, value_weight, value_bias, out_weight, out_bias, second_gain, second_bias,
    up_weight, up_bias, down_weight, down_bias, cotangent,
):
    micro, _, half, model = layer_input.shape
    side = lax.axis_index("seq")
    rows = micro * half
    part = model // shards
    low, wide = jnp.bfloat16, jnp.float32
    shard = lax.axis_index("fsdp")
    vec = jnp.stack([first_gain, first_bias, query_bias, value_bias, out_bias, second_gain, second_bias, down_bias])
    vec = lax.dynamic_update_slice(jnp.zeros((8, model), low), vec, (0, shard * part))
    wide_bias = lax.dynamic_update_slice(jnp.zeros((4 * model,), low), up_bias, (shard * 4 * part,))
    vec = jnp.concatenate([vec, wide_bias.reshape(4, model), jnp.zeros((4, model), low)])
    w_qkvo, w_up, w_down, vec, normed, queries, keys, values, keys_other, values_other = gather_weights(
        shards, jnp.stack([query_weight, key_weight, value_weight, out_weight]), up_weight, down_weight, vec,
        layer_input.reshape(rows, model),
    )
    gain_one = vec[0]
    span, aug, block_bias, doc_bias = tables(segment[:, 0], rand_blocks[:, 0], side, half)

    tokens = layer_input.reshape(rows, model).astype(wide)
    swap = [(0, 1), (1, 0)]
    cut = lambda array: array.reshape(micro, half, model)
    attended = (span, cut(queries), cut(keys), cut(values), cut(keys_other), cut(values_other),
                aug, block_bias, doc_bias)
    mixed, lse = attend_forward(*attended)
    mixed_rows = mixed.reshape(rows, model)
    result, grad_attn, grad_mixed, d_out, d_up, d_down, sums, d_b_up = middle_layer(
        shards, mixed_rows, layer_input.reshape(rows, model), cotangent.reshape(rows, model),
        w_qkvo[3], w_up, w_down, vec, vec[8:12].reshape(shards, 1, 4 * part),
    )
    grads = attend_backward(0, (), *attended, mixed, cut(grad_mixed), lse)
    d_query, d_key, d_value, d_key_other, d_value_other = attend_backward(
        1, grads, *attended, mixed, cut(grad_mixed), lse
    )
    join = lambda own, other: (
        own.reshape(rows, model).astype(wide) + lax.ppermute(other.reshape(rows, model), "seq", swap).astype(wide)
    ).astype(low)
    d_query = d_query.reshape(rows, model)
    d_key = join(d_key, d_key_other)
    d_value = join(d_value, d_value_other)
    grad_normed = nt(d_query, w_qkvo[0]) + nt(d_key, w_qkvo[1]) + nt(d_value, w_qkvo[2])
    unit_one, scale_one = unit_of(tokens)
    grad_one, d_gain_one, d_bias_one = norm_back(grad_normed, unit_one, scale_one, gain_one)
    input_grad = (grad_attn.astype(wide) + grad_one).astype(low)
    d_qkvo = [tn(normed, d_query).astype(low), tn(normed, d_key).astype(low), tn(normed, d_value).astype(low), d_out]
    total = lambda array: jnp.sum(array.astype(wide), axis=0)
    small = jnp.stack([d_gain_one, d_bias_one, total(d_query), total(d_value), sums[2], sums[0], sums[1], sums[3]])
    small = jnp.moveaxis(small.reshape(8, shards, part), 1, 0)
    small = jnp.concatenate([small, d_b_up.reshape(shards, 4, part)], axis=1)
    small = jnp.pad(small, ((0, 0), (0, 4), (0, 256 - part)))
    g_qkvo, g_up, g_down, g_vec = reduce_grads(shards, quads, d_qkvo, d_up, d_down, small)
    g_qkvo, g_up, g_down = g_qkvo.astype(wide), g_up.astype(wide), g_down.astype(wide)
    g_vec = g_vec[:, :part]
    shape = layer_input.shape
    return (
        result.reshape(shape), input_grad.reshape(shape), g_vec[0], g_vec[1], g_qkvo[0], g_vec[2],
        g_qkvo[1], g_qkvo[2], g_vec[3], g_qkvo[3], g_vec[4], g_vec[5], g_vec[6], g_up,
        g_vec[8:12].reshape(4 * part), g_down, g_vec[7],
    )


def solution(mesh):
    row = P(None, ("rep", "fsdp"), "seq", None)
    flat, wide = P("fsdp"), P("fsdp", None)
    shards, quads = mesh.shape["fsdp"], mesh.shape["rep"] // 4
    assert mesh.shape["seq"] == 2 and mesh.shape["rep"] % 4 == 0
    return jax.shard_map(
        functools.partial(on_device, shards, quads),
        mesh=mesh,
        in_specs=(
            row, P(None, ("rep", "fsdp"), None), P(None, ("rep", "fsdp"), None, None, None),
            flat, flat, wide, flat, wide, wide, flat, wide, flat, flat, flat, wide, flat, wide, flat, row,
        ),
        out_specs=(row, row, flat, flat, wide, flat, wide, wide, flat, wide, flat, flat, flat, wide, flat, wide, flat),
        check_vma=False,
    )
```

```python
import functools
import jax
import jax.numpy as jnp
from jax import lax
from jax.experimental import pallas as pl
from jax.experimental.pallas import tpu as pltpu
from jax.sharding import PartitionSpec as P

norm_eps = 1e-05

HEADS = 12
HDIM = 64
BLOCK = 64
TQ = 256
TK = 256
NEG = -1e30


def nt(a, b):
    return lax.dot_general(a, b, (((1,), (1,)), ((), ())), preferred_element_type=jnp.float32)


def tn(a, b):
    return lax.dot_general(a, b, (((0,), (0,)), ((), ())), preferred_element_type=jnp.float32)


def nn(a, b):
    return jnp.dot(a, b, preferred_element_type=jnp.float32)


def head_lanes(head):
    lane = lax.broadcasted_iota(jnp.int32, (1, 128), 1)
    return (lane < HDIM) if head == 0 else (lane >= HDIM)


def bias_rows(block_ref, doc_ref, head):
    rows = [
        jnp.broadcast_to(block_ref[0, 0, head, pl.ds(b, 1), :], (BLOCK, 128)) for b in range(TQ // BLOCK)
    ]
    return (jnp.concatenate(rows, axis=0) + doc_ref[0]).astype(jnp.bfloat16)


def unite(whole, own_ref, other_ref, side):
    half = own_ref.shape[1]
    whole[pl.ds(pl.multiple_of(side * half, TK), half), :] = own_ref[0]
    whole[pl.ds(pl.multiple_of((1 - side) * half, TK), half), :] = other_ref[0]


def forward_body(
    span_ref, q_ref, ko_ref, vo_ref, kx_ref, vx_ref, aug_ref, block_ref, doc_ref,
    out_ref, lse_ref, acc_ref, qa_ref, k_all, v_all,
):
    micro, tile = pl.program_id(0), pl.program_id(1)

    @pl.when(tile == 0)
    def _():
        unite(k_all, ko_ref, kx_ref, span_ref[micro, tile, 2])
        unite(v_all, vo_ref, vx_ref, span_ref[micro, tile, 2])

    group = q_ref.shape[2] // HDIM
    for head in range(group):
        cols = pl.ds(head // 2 * 128, 128)
        q_rows = q_ref[0, :, cols].astype(jnp.float32) * 0.125
        masked = jnp.where(head_lanes(head % 2), q_rows, 0.0).astype(jnp.bfloat16)
        qa_ref[head, :, 0:128] = masked
        qa_ref[head, :, 128:256] = bias_rows(block_ref, doc_ref, head)
    acc_ref[...] = jnp.zeros_like(acc_ref)

    def step(j, carry):
        at = pl.ds(pl.multiple_of(j * TK, TK), TK)
        aug = aug_ref[0, at, :]
        scores = []
        for head in range(group):
            cols = pl.ds(head // 2 * 128, 128)
            scores.append(nt(jnp.concatenate([k_all[at, cols], aug], axis=1), qa_ref[head]))
        fresh = []
        probs = []
        for head in range(group):
            top_new = jnp.maximum(carry[head], jnp.max(scores[head], axis=0, keepdims=True))
            probs.append(jnp.exp(scores[head] - top_new).astype(jnp.bfloat16))
            fresh.append(top_new)
        for head in range(group):
            cols = pl.ds(head // 2 * 128, 128)
            v_rows = jnp.where(head_lanes(head % 2), v_all[at, cols], jnp.bfloat16(1.0))
            part = tn(v_rows, probs[head])
            acc_ref[head] = acc_ref[head] * jnp.exp(carry[head] - fresh[head]) + part
        return tuple(fresh)

    state = tuple(jnp.full((1, TQ), -3e38, jnp.float32) for _ in range(group))
    state = lax.fori_loop(span_ref[micro, tile, 0], span_ref[micro, tile, 1], step, state)
    for pair in range(group // 2):
        done = []
        for head in range(2):
            at = pair * 2 + head
            mass = acc_ref[at, pl.ds((1 - head) * HDIM, 1), :]
            done.append(acc_ref[at, pl.ds(head * HDIM, HDIM), :] / mass)
            lse_ref[0, pair, pl.ds(head, 1), :] = state[at] + jnp.log(mass)
        out_ref[0, :, pl.ds(pair * 128, 128)] = jnp.concatenate(done, axis=0).T.astype(out_ref.dtype)


def backward_body(
    micro, carried,
    span_ref, q_ref, ko_ref, vo_ref, kx_ref, vx_ref, aug_ref, block_ref, doc_ref,
    mixed_ref, grad_ref, lse_ref, *rest,
):
    dq_ref, dko_ref, dvo_ref, dkx_ref, dvx_ref = rest[carried:carried + 5]
    dqt_ref, qa_ref, gm_ref, k_acc, v_acc, k_all, v_all = rest[carried + 5:]
    tile = pl.program_id(0)
    side = span_ref[micro, tile, 2]

    @pl.when(tile == 0)
    def _():
        unite(k_all, ko_ref, kx_ref, side)
        unite(v_all, vo_ref, vx_ref, side)
        k_acc[...] = jnp.zeros_like(k_acc)
        v_acc[...] = jnp.zeros_like(v_acc)

    group = q_ref.shape[2] // HDIM
    inner = []
    for pair in range(group // 2):
        cols = pl.ds(pair * 128, 128)
        q_rows = q_ref[0, :, cols].astype(jnp.float32) * 0.125
        grad_rows = grad_ref[0, :, cols].astype(jnp.float32)
        both = (mixed_ref[0, :, cols].astype(jnp.float32) * grad_rows).T
        for half in range(2):
            head = pair * 2 + half
            qa_ref[head, :, 0:128] = jnp.where(head_lanes(half), q_rows, 0.0).astype(jnp.bfloat16)
            qa_ref[head, :, 128:256] = bias_rows(block_ref, doc_ref, head)
            gm_ref[head] = jnp.where(head_lanes(half), grad_rows, 0.0).astype(jnp.bfloat16)
            inner.append(jnp.sum(both[half * HDIM:(half + 1) * HDIM, :], axis=0, keepdims=True))
    dqt_ref[...] = jnp.zeros_like(dqt_ref)

    def step(j, carry):
        at = pl.ds(pl.multiple_of(j * TK, TK), TK)
        aug = aug_ref[0, at, :]
        for chunk in range(0, group, CHUNK):
            heads = range(chunk, min(chunk + CHUNK, group))
            scores, grads, probs, souls = {}, {}, {}, {}
            for head in heads:
                cols = pl.ds(head // 2 * 128, 128)
                scores[head] = nt(jnp.concatenate([k_all[at, cols], aug], axis=1), qa_ref[head])
                grads[head] = nt(v_all[at, cols], gm_ref[head])
            for head in heads:
                weight = jnp.exp(scores[head] - lse_ref[0, head // 2, pl.ds(head % 2, 1), :])
                souls[head] = (weight * (grads[head] - carry[head])).astype(jnp.bfloat16)
                probs[head] = weight.astype(jnp.bfloat16)
            for head in heads:
                cols = pl.ds(head // 2 * 128, 128)
                dv = nn(probs[head], gm_ref[head])
                dk = nn(souls[head], qa_ref[head, :, 0:128])
                dqt = tn(k_all[at, cols], souls[head])
                lanes = pl.ds(head * HDIM, HDIM)
                half = head % 2
                dqt_ref[lanes, :] += dqt[half * HDIM:(half + 1) * HDIM, :]
                if half == 0:
                    dv_low, dk_low = dv, dk
                else:
                    k_acc[at, cols] += dk + dk_low
                    v_acc[at, cols] += dv + dv_low
        return carry

    lax.fori_loop(span_ref[micro, tile, 0], span_ref[micro, tile, 1], step, tuple(inner))
    for pair in range(group // 2):
        cols = pl.ds(pair * 128, 128)
        dq_ref[0, :, cols] = (dqt_ref[cols, :] * 0.125).T.astype(dq_ref.dtype)

    @pl.when(tile == pl.num_programs(0) - 1)
    def _():
        size = dko_ref.shape[1]
        mine = pl.ds(pl.multiple_of(side * size, TK), size)
        theirs = pl.ds(pl.multiple_of((1 - side) * size, TK), size)
        dko_ref[0] = k_acc[mine, :].astype(dko_ref.dtype)
        dvo_ref[0] = v_acc[mine, :].astype(dvo_ref.dtype)
        dkx_ref[0] = k_acc[theirs, :].astype(dkx_ref.dtype)
        dvx_ref[0] = v_acc[theirs, :].astype(dvx_ref.dtype)


CHUNK = 4


def specs(half, length, width, at):
    rows = pl.BlockSpec((1, TQ, width), lambda *i: at(*i) + (0,))
    side = pl.BlockSpec((1, half, width), lambda *i: (at(*i)[0], 0, 0))
    aug = pl.BlockSpec((1, length, 128), lambda *i: (at(*i)[0], 0, 0))
    block = pl.BlockSpec((1, 1, HEADS, TQ // BLOCK, 128), lambda *i: at(*i) + (0, 0, 0))
    doc = pl.BlockSpec((1, TQ, 128), lambda *i: at(*i) + (0,))
    lse = pl.BlockSpec((1, HEADS // 2, 2, TQ), lambda *i: (at(*i)[0], 0, 0, at(*i)[1]))
    return rows, side, aug, block, doc, lse


def attend_forward(span, q, ko, vo, kx, vx, aug, block, doc):
    micro, half, width = q.shape
    length = aug.shape[1]
    rows, side, aug_spec, blk, doc_spec, lse = specs(half, length, width, lambda m, t, s: (m, t))
    return pl.pallas_call(
        forward_body,
        name="attend_forward",
        out_shape=(
            jax.ShapeDtypeStruct((micro, half, width), jnp.bfloat16),
            jax.ShapeDtypeStruct((micro, HEADS // 2, 2, half), jnp.float32),
        ),
        grid_spec=pltpu.PrefetchScalarGridSpec(
            num_scalar_prefetch=1,
            grid=(micro, half // TQ),
            in_specs=[rows] + [side] * 4 + [aug_spec, blk, doc_spec],
            out_specs=(rows, lse),
            scratch_shapes=[
                pltpu.VMEM((HEADS, 128, TQ), jnp.float32),
                pltpu.VMEM((HEADS, TQ, 256), jnp.bfloat16),
                pltpu.VMEM((length, width), jnp.bfloat16),
                pltpu.VMEM((length, width), jnp.bfloat16),
            ],
        ),
        cost_estimate=pl.CostEstimate(flops=20_000_000_000, bytes_accessed=20_000_000, transcendentals=0),
    )(span, q, ko, vo, kx, vx, aug, block, doc)


def attend_backward(step, carried, span, q, ko, vo, kx, vx, aug, block, doc, mixed, grad, lse):
    micro, half, width = q.shape
    length = aug.shape[1]
    rows, side, aug_spec, blk, doc_spec, lse_spec = specs(half, length, width, lambda t, s: (step, t))
    shape = jax.ShapeDtypeStruct((micro, half, width), jnp.bfloat16)
    return pl.pallas_call(
        functools.partial(backward_body, step, len(carried)),
        name="attend_backward",
        out_shape=(shape,) * 5,
        grid_spec=pltpu.PrefetchScalarGridSpec(
            num_scalar_prefetch=1,
            grid=(half // TQ,),
            in_specs=[rows] + [side] * 4 + [aug_spec, blk, doc_spec, rows, rows, lse_spec]
            + [pl.BlockSpec(memory_space=pl.ANY)] * len(carried),
            out_specs=(rows,) + (side,) * 4,
            scratch_shapes=[
                pltpu.VMEM((width, TQ), jnp.float32),
                pltpu.VMEM((HEADS, TQ, 256), jnp.bfloat16),
                pltpu.VMEM((HEADS, TQ, 128), jnp.bfloat16),
                pltpu.VMEM((length, width), jnp.float32),
                pltpu.VMEM((length, width), jnp.float32),
                pltpu.VMEM((length, width), jnp.bfloat16),
                pltpu.VMEM((length, width), jnp.bfloat16),
            ],
        ),
        input_output_aliases={12 + i: i for i in range(len(carried))},
        cost_estimate=pl.CostEstimate(flops=20_000_000_000, bytes_accessed=20_000_000, transcendentals=0),
    )(span, q, ko, vo, kx, vx, aug, block, doc, mixed, grad, lse, *carried)


def tables(segment, rand_blocks, side, half):
    micro, length = segment.shape
    blocks = length // BLOCK
    mine = half // BLOCK
    tiles = half // TQ
    lane = lax.broadcasted_iota(jnp.int32, (1, 1, 128), 2)
    own = lax.dynamic_slice_in_dim(segment, side * half, half, axis=1)
    place = lax.broadcasted_iota(jnp.int32, (1, length, 1), 1) // BLOCK
    aug = ((lane == place) | (lane == segment[:, :, None] + blocks)).astype(jnp.bfloat16)
    doc = jnp.where((lane >= blocks) & (lane < blocks + 4) & (lane != own[:, :, None] + blocks), NEG, 0.0)
    q_block = side * mine + lax.broadcasted_iota(jnp.int32, (1, 1, mine, 1), 2)
    k_block = lax.broadcasted_iota(jnp.int32, (1, 1, 1, 128), 3)
    chosen = lax.dynamic_slice_in_dim(rand_blocks, side * mine, mine, axis=2)
    allowed = (jnp.abs(q_block - k_block) <= 1) | (k_block == 0) | (k_block == blocks - 1)
    allowed = allowed | (q_block == 0) | (q_block == blocks - 1) | (k_block >= blocks)
    for pick in range(rand_blocks.shape[3]):
        allowed = allowed | (chosen[:, :, :, pick:pick + 1] == k_block)
    block = jnp.where(allowed, 0.0, NEG).astype(jnp.float32)
    block = jnp.moveaxis(block.reshape(micro, HEADS, tiles, mine // tiles, 128), 2, 1)
    edges = own.reshape(micro, tiles, TQ)
    first, last = edges[:, :, :1], edges[:, :, TQ - 1:]
    begin = jnp.sum((segment[:, None, :] < first).astype(jnp.int32), axis=-1)
    end = jnp.sum((segment[:, None, :] <= last).astype(jnp.int32), axis=-1)
    span = jnp.stack([begin // TK, (end + TK - 1) // TK, jnp.full_like(begin, side)], axis=-1)
    return span, aug, block, doc.astype(jnp.float32)


MESH = pl.DeviceIdType.MESH
GROUPS = 3


def place():
    rep, shard, side = lax.axis_index("rep"), lax.axis_index("fsdp"), lax.axis_index("seq")
    quad = lax.rem(rep, 4)
    across, along = lax.rem(quad, 2), quad // 2
    near = (1 - 2 * across, 2 - 4 * along)
    return rep, shard, side, quad, near


def chunk(refs, group, shard, quad, side, rows, half=None):
    width = 768 if half is None else 384
    offset = 0 if half is None else half * 384
    low = side * rows
    if group == 0:
        return refs[0].at[quad, pl.ds(pl.multiple_of(shard * (2 * rows) + low, 16), rows), pl.ds(offset, width)]
    if group == 1:
        at = pl.multiple_of(shard * (2 * rows) + low, 16)
        return refs[1].at[pl.ds(at, rows), pl.ds(pl.multiple_of(quad * 768 + offset, 128), width)]
    at = pl.multiple_of(shard * (8 * rows) + quad * (2 * rows) + low, 16)
    return refs[2].at[pl.ds(at, rows), pl.ds(offset, width)]


def greet(peers):
    barrier = pltpu.get_barrier_semaphore()
    for peer in peers:
        pl.semaphore_signal(barrier, inc=1, device_id=peer, device_id_type=MESH)
    pl.semaphore_wait(barrier, len(peers))


def remote(src, dst, send, recv, peer):
    return pltpu.make_async_remote_copy(
        src_ref=src, dst_ref=dst, send_sem=send, recv_sem=recv, device_id=peer, device_id_type=MESH
    )


def gather_body(
    shards, rows, qkvo_in, up_in, down_in, vec_in, x_in,
    qkvo_out, up_out, down_out, vec_out, normed_out, q_out, k_out, v_out, kx_out, vx_out,
    qkvo_stage, up_stage, down_stage, vec_all, weights, normed, results,
    in_sem, out_sem, z_send, z_recv, x_send, x_recv, y_send, y_recv, d_send, d_recv, c_send, c_recv,
    load_sem, save_sem, swap_send, swap_recv,
):
    rep, shard, side, quad, (dx, dy) = place()
    ins, outs = (qkvo_in, up_in, down_in), (qkvo_out, up_out, down_out)
    stages = (qkvo_stage, up_stage, down_stage)
    x_peer, y_peer, partner = (rep + dx, shard, side), (rep + dy, shard, side), (rep, shard, 1 - side)
    z_peers = [(rep, lax.rem(shard + k, shards), side) for k in range(1, shards)]
    for i, src in enumerate(ins):
        pltpu.make_async_copy(src, stages[i], in_sem.at[i]).start()
    greet(z_peers + [x_peer, y_peer, partner])
    sent = []

    def go(copy):
        copy.start()
        sent.append(copy)

    for g in range(GROUPS):
        for k in range(1, shards):
            go(remote(
                chunk(ins, g, 0, quad, side, rows), chunk(outs, g, shard, quad, side, rows),
                z_send.at[g, k - 1], z_recv.at[g, shards - k - 1], z_peers[k - 1],
            ))
        if g == 0:
            for k in range(1, shards):
                go(remote(
                    vec_in, vec_all.at[k - 1],
                    z_send.at[GROUPS, k - 1], z_recv.at[GROUPS, k - 1], z_peers[k - 1],
                ))
    owned = (
        qkvo_out.at[:, pl.ds(pl.multiple_of(shard * 2 * rows, 16), 2 * rows), :],
        up_out.at[pl.ds(pl.multiple_of(shard * 2 * rows, 16), 2 * rows), :],
        down_out.at[pl.ds(pl.multiple_of(shard * 8 * rows, 16), 8 * rows), :],
    )
    local = []
    for i, src in enumerate(ins):
        pltpu.make_async_copy(src, stages[i], in_sem.at[i]).wait()
        copy = pltpu.make_async_copy(stages[i], owned[i], out_sem.at[i])
        copy.start()
        local.append(copy)

    def piece(g, k, member, core, half=None):
        return chunk(outs, g, lax.rem(shard + k, shards), member, core, rows, half)

    def hop(g, k, member, core, send, recv, peer, half=None):
        ref = piece(g, k, member, core, half)
        return remote(ref, ref, send, recv, peer)

    x_quad, y_quad, d_quad = quad + dx, quad + dy, quad + dx + dy

    def straight(g):
        for k in range(1, shards):
            hop(g, k, quad, side, z_send.at[g, k - 1], z_recv.at[g, k - 1], z_peers[k - 1]).wait_recv()
            go(hop(g, k, quad, side, x_send.at[g, k - 1], x_recv.at[g, k - 1], x_peer))
            go(hop(g, k, quad, side, y_send.at[g, k - 1], y_recv.at[g, k - 1], y_peer))
            go(hop(g, k, quad, side, c_send.at[g, k - 1, 0], c_recv.at[g, k - 1, 0], partner))

    def turn(g):
        for k in range(1, shards):
            hop(g, k, x_quad, side, x_send.at[g, k - 1], x_recv.at[g, k - 1], x_peer).wait_recv()
            go(hop(g, k, x_quad, side, d_send.at[g, k - 1, 1], d_recv.at[g, k - 1, 1], y_peer, 1))
            go(hop(g, k, x_quad, side, c_send.at[g, k - 1, 1], c_recv.at[g, k - 1, 1], partner))
            hop(g, k, y_quad, side, y_send.at[g, k - 1], y_recv.at[g, k - 1], y_peer).wait_recv()
            go(hop(g, k, y_quad, side, d_send.at[g, k - 1, 0], d_recv.at[g, k - 1, 0], x_peer, 0))
            go(hop(g, k, y_quad, side, c_send.at[g, k - 1, 2], c_recv.at[g, k - 1, 2], partner))

    def corner(g):
        for k in range(1, shards):
            hop(g, k, d_quad, side, d_send.at[g, k - 1, 0], d_recv.at[g, k - 1, 0], x_peer, 0).wait_recv()
            hop(g, k, d_quad, side, d_send.at[g, k - 1, 1], d_recv.at[g, k - 1, 1], y_peer, 1).wait_recv()
            go(hop(g, k, d_quad, side, c_send.at[g, k - 1, 3], c_recv.at[g, k - 1, 3], partner))

    def gathered(g):
        for k in range(1, shards):
            for i, member in enumerate((quad, x_quad, y_quad, d_quad)):
                hop(g, k, member, 1 - side, c_send.at[g, k - 1, i], c_recv.at[g, k - 1, i], partner).wait_recv()

    def save(i, target):
        copy = pltpu.make_async_copy(normed if i == 3 else results.at[i], target, save_sem.at[i])
        copy.start()
        local.append(copy)

    def norm(step, carry):
        at = pl.ds(pl.multiple_of(step * STEP, STEP), STEP)
        values = x_in[at, :].astype(jnp.float32)
        centre = values - jnp.mean(values, axis=-1, keepdims=True)
        scale = lax.rsqrt(jnp.mean(centre * centre, axis=-1, keepdims=True) + norm_eps)
        normed[at, :] = (centre * scale * vec_out[0:1, :] + vec_out[1:2, :]).astype(normed.dtype)
        return carry

    def project(i, row):
        pltpu.make_async_copy(qkvo_out.at[i], weights.at[i], load_sem.at[i]).wait()

        def step(j, carry):
            at = pl.ds(pl.multiple_of(j * STEP, STEP), STEP)
            product = nn(normed[at, :], weights[i])
            if row is not None:
                product = product + vec_out[row:row + 1, :]
            results[i, at, :] = product.astype(results.dtype)
            return carry
        lax.fori_loop(0, normed.shape[0] // STEP, step, 0)

    def exchange(i, target):
        copy = remote(results.at[i], target, swap_send.at[i - 1], swap_recv.at[i - 1], partner)
        copy.start()
        return copy

    straight(0)
    for k in range(1, shards):
        remote(
            vec_in, vec_all.at[k - 1], z_send.at[GROUPS, k - 1], z_recv.at[GROUPS, k - 1], z_peers[k - 1]
        ).wait_recv()
    total = vec_in[...].astype(jnp.float32)
    for k in range(1, shards):
        total = total + vec_all[k - 1].astype(jnp.float32)
    vec_out[...] = total
    lax.fori_loop(0, normed.shape[0] // STEP // 2, norm, 0)
    turn(0)
    lax.fori_loop(normed.shape[0] // STEP // 2, normed.shape[0] // STEP, norm, 0)
    save(3, normed_out)
    straight(1)
    corner(0)
    turn(1)
    local[0].wait()
    gathered(0)
    for i in (1, 2, 0):
        pltpu.make_async_copy(qkvo_out.at[i], weights.at[i], load_sem.at[i]).start()
    straight(2)
    project(1, None)
    keys = exchange(1, kx_out)
    save(1, k_out)
    corner(1)
    project(2, 3)
    values = exchange(2, vx_out)
    save(2, v_out)
    turn(2)
    project(0, 2)
    save(0, q_out)
    corner(2)
    gathered(1)
    gathered(2)
    keys.wait()
    values.wait()
    for copy in sent:
        copy.wait_send()
    for copy in local[1:]:
        copy.wait()


STEP = 256


def gather_weights(shards, qkvo, up, down, vec, x):
    rows = qkvo.shape[1] // 2
    model = qkvo.shape[2]
    hidden = up.shape[1]
    any_space = pl.BlockSpec(memory_space=pl.ANY)
    vmem_space = pl.BlockSpec(memory_space=pltpu.VMEM)
    dma = pltpu.SemaphoreType.DMA
    low = jnp.bfloat16
    token = jax.ShapeDtypeStruct(x.shape, low)
    return pl.pallas_call(
        functools.partial(gather_body, shards, rows),
        name="gather_weights",
        out_shape=(
            jax.ShapeDtypeStruct((4, model, model), low),
            jax.ShapeDtypeStruct((model, hidden), low),
            jax.ShapeDtypeStruct((hidden, model), low),
            jax.ShapeDtypeStruct(vec.shape, jnp.float32),
        )
        + (token,) * 6,
        in_specs=[any_space] * 3 + [vmem_space] * 2,
        out_specs=(any_space,) * 3 + (vmem_space,) + (any_space,) * 6,
        scratch_shapes=[
            pltpu.VMEM(qkvo.shape, low), pltpu.VMEM(up.shape, low), pltpu.VMEM(down.shape, low),
            pltpu.VMEM((shards - 1,) + vec.shape, low),
            pltpu.VMEM((3, model, model), low),
            pltpu.VMEM(x.shape, low),
            pltpu.VMEM((3,) + x.shape, low),
            dma((3,)), dma((3,)),
            dma((GROUPS + 1, shards - 1)), dma((GROUPS + 1, shards - 1)),
        ]
        + [dma((GROUPS, shards - 1))] * 4
        + [dma((GROUPS, shards - 1, 2))] * 2
        + [dma((GROUPS, shards - 1, 4))] * 2
        + [dma((3,)), dma((4,)), dma((2,)), dma((2,))],
        compiler_params=pltpu.CompilerParams(
            collective_id=0, has_side_effects=True, vmem_limit_bytes=50_000_000
        ),
    )(qkvo, up, down, vec, x)


def add_into(out_ref, refs):
    total = refs[0][...].astype(jnp.float32)
    for ref in refs[1:]:
        total = total + ref[...].astype(jnp.float32)
    out_ref[...] = total.astype(out_ref.dtype)


def normal_parts(values):
    phi = 0.5 + 0.5 * lax.erf(values * 0.7071067811865476)
    return phi, values * (jnp.exp(-0.5 * values * values) * 0.3989422804014327)


def middle_body(
    shards, rows,
    mixed_in, x_in, grad_in, qkvo_in, up_w_in, down_w_in, vec_in,
    result_out, attn_out, mixed_out, d_out_out, up_out, down_out, sums_out,
    mixed, x, grad, out_w, up_w, down_w, middle, normed, turned, hidden, slope,
    up_grad, down_grad, up_mate, down_mate, up_first, down_first, up_second, down_second,
    load_sem, save_sem, uc_send, uc_recv, dc_send, dc_recv, f_send, f_recv, s_send, s_recv,
):
    rep, shard, side, quad, (dx, dy) = place()
    partner = (rep, shard, 1 - side)
    low, wide = jnp.bfloat16, jnp.float32
    steps = x.shape[0] // STEP
    model = x.shape[1]
    width = 8 * rows
    loads = [
        pltpu.make_async_copy(src, dst, load_sem.at[i])
        for i, (src, dst) in enumerate(((mixed_in, mixed), (x_in, x), (qkvo_in.at[3], out_w), (grad_in, grad)))
    ]
    for f in range(shards):
        at = pl.ds(f * width, width)
        loads.append(pltpu.make_async_copy(up_w_in.at[:, at], up_w.at[f], load_sem.at[4 + f]))
        loads.append(pltpu.make_async_copy(down_w_in.at[at, :], down_w.at[f], load_sem.at[4 + shards + f]))
    for load in loads:
        load.start()
    greet([(rep + dx, shard, side), (rep + dy, shard, side), partner])
    firsts, seconds = (up_first, down_first), (up_second, down_second)

    def row(i):
        return vec_in[i:i + 1, :]

    def block(j):
        return pl.ds(pl.multiple_of(j * STEP, STEP), STEP)

    def part(g, f, m):
        return up_grad.at[m, f, side] if g == 0 else down_grad.at[f, side, m]

    def mate(g, f, m):
        return up_mate.at[m, f] if g == 0 else down_mate.at[f, m]

    def flip_way(f, second):
        odd = lax.rem(f + second, 2)
        return dx + odd * (dy - dx)

    def up_cross(m):
        return remote(up_grad.at[m, :, 1 - side], up_mate.at[m], uc_send.at[m], uc_recv.at[m], partner)

    def down_cross(f):
        return remote(down_grad.at[f, 1 - side], down_mate.at[f], dc_send.at[f], dc_recv.at[f], partner)

    def f_copy(g, f, slot):
        way = flip_way(f, 0)
        member = quad + way if slot == 0 else quad + dx + dy
        return remote(part(g, f, member), firsts[g].at[f, slot], f_send.at[g, f, slot], f_recv.at[g, f, slot], (rep + way, shard, side))

    def s_copy(g, f):
        way = flip_way(f, 1)
        return remote(part(g, f, quad + way), seconds[g].at[f], s_send.at[g, f], s_recv.at[g, f], (rep + way, shard, side))

    def first_go(g, f):
        for slot in range(2):
            f_copy(g, f, slot).start()

    def down_merge(f):
        down_cross(f).wait_recv()
        for m in range(4):
            add_into(part(1, f, m), (part(1, f, m), mate(1, f, m)))
        first_go(1, f)

    def up_merge(m):
        up_cross(m).wait_recv()

        def step(f, carry):
            add_into(part(0, f, m), (part(0, f, m), mate(0, f, m)))
            return carry
        lax.fori_loop(0, shards, step, 0)

    def each(body):
        def step(f, carry):
            body(f)
            return carry
        lax.fori_loop(0, shards, step, 0)

    def fold(g):
        def body(f):
            for slot in range(2):
                f_copy(g, f, slot).wait()
                member = quad if slot == 0 else quad + flip_way(f, 1)
                add_into(part(g, f, member), (part(g, f, member), firsts[g].at[f, slot]))
            s_copy(g, f).start()
        each(body)

    def settle(g, target):
        def body(f):
            s_copy(g, f).wait()
            add_into(target.at[f], (part(g, f, quad), seconds[g].at[f]))
        each(body)

    saves = []

    def save(src, dst):
        copy = pltpu.make_async_copy(src, dst, save_sem.at[len(saves)])
        copy.start()
        saves.append(copy)

    for load in loads[:3]:
        load.wait()

    def attend_out(j, carry):
        at = block(j)
        values = x[at, :].astype(wide) + nn(mixed[at, :], out_w[...]) + row(4)
        middle[at, :] = values
        centre = values - jnp.mean(values, axis=-1, keepdims=True)
        scale = lax.rsqrt(jnp.mean(centre * centre, axis=-1, keepdims=True) + norm_eps)
        out = centre * scale * row(5) + row(6)
        normed[at, :] = out.astype(low)
        turned[:, at] = out.T.astype(low)
        return carry
    lax.fori_loop(0, steps, attend_out, 0)
    for load in loads[3:]:
        load.wait()

    def bias_at(f):
        first = f * width
        return pl.ds(8 + first // model, 1), pl.ds(pl.multiple_of(lax.rem(first, model), 128), width)

    def expand(f):
        bias = vec_in[bias_at(f)]

        def step(j, carry):
            at = block(j)
            inner = nn(normed[at, :], up_w[f]) + bias
            phi, bump = normal_parts(inner)
            hidden[f, at, :] = (inner * phi).astype(low)
            slope[f, at, :] = (phi + bump).astype(low)
            return carry
        lax.fori_loop(0, steps, step, 0)
        down_grad[f] = tn(hidden[f], grad[...]).astype(low).reshape(2, 4, rows, model)
        down_cross(f).start()

        @pl.when(f > 0)
        def _():
            down_merge(f - 1)
    each(expand)

    def contract(m):
        for h in range(model // width):
            f = m * (model // width) + h

            def step(j, total, f=f):
                at = block(j)
                value = (nt(grad[at, :], down_w[f]) * slope[f, at, :].astype(wide)).astype(low)
                slope[f, at, :] = value
                return total + jnp.sum(value.astype(wide), axis=0, keepdims=True)
            sums_out[bias_at(f)] = lax.fori_loop(0, steps, step, jnp.zeros((1, width), wide))
            product = nn(turned[...], slope[f]).astype(low)
            up_grad[m, :, :, :, pl.ds(h * width, width)] = product.reshape(shards, 2, rows, width)
        up_cross(m).start()

        @pl.when(m == 0)
        def _():
            down_merge(shards - 1)

        @pl.when(m > 0)
        def _():
            up_merge(m - 1)

    def contract_step(m, carry):
        contract(m)
        return carry
    lax.fori_loop(0, 4, contract_step, 0)
    fold(1)
    up_merge(3)
    each(lambda f: first_go(0, f))

    def finish(j, carry):
        at = block(j)
        total = middle[at, :] + row(7)
        for f in range(shards):
            total = total + nn(hidden[f, at, :], down_w[f])
        x[at, :] = total.astype(low)
        return carry
    lax.fori_loop(0, steps, finish, 0)
    save(x, result_out)

    def back(j, carry):
        gain_sum, bias_sum, attn_sum, grad_sum = carry
        at = block(j)
        error = nt(slope[0, at, :], up_w[0])
        for f in range(1, shards):
            error = error + nt(slope[f, at, :], up_w[f])
        values = middle[at, :]
        centre = values - jnp.mean(values, axis=-1, keepdims=True)
        scale = lax.rsqrt(jnp.mean(centre * centre, axis=-1, keepdims=True) + norm_eps)
        unit = centre * scale
        scaled = error * row(5)
        mean_one = jnp.mean(scaled, axis=-1, keepdims=True)
        mean_two = jnp.mean(scaled * unit, axis=-1, keepdims=True)
        upstream = grad[at, :].astype(wide)
        attn = (upstream + scale * (scaled - mean_one - unit * mean_two)).astype(low)
        grad[at, :] = attn
        normed[at, :] = nt(attn, out_w[...]).astype(low)
        column = lambda array: jnp.sum(array, axis=0, keepdims=True)
        return (
            gain_sum + column(error * unit), bias_sum + column(error),
            attn_sum + column(attn.astype(wide)), grad_sum + column(upstream),
        )
    zero = jnp.zeros((1, model), wide)
    sums = lax.fori_loop(0, steps // 2, back, (zero,) * 4)
    fold(0)
    sums = lax.fori_loop(steps // 2, steps, back, sums)
    save(normed, mixed_out)
    save(grad, attn_out)
    for i, value in enumerate(sums):
        sums_out[i:i + 1, :] = value
    sums_out[4:8, :] = jnp.zeros((4, model), wide)
    sums_out[12:16, :] = jnp.zeros((4, model), wide)
    settle(1, down_out)
    out_w[...] = tn(mixed[...], grad[...]).astype(low)
    save(out_w, d_out_out)
    settle(0, up_out)
    for m in range(4):
        up_cross(m).wait_send()
    each(lambda f: down_cross(f).wait_send())
    for copy in saves:
        copy.wait()


def middle_layer(shards, mixed, x, grad, qkvo, up_w, down_w, vec):
    tokens, model = x.shape
    hidden = up_w.shape[1]
    rows = model // shards // 2
    width = 8 * rows
    any_space = pl.BlockSpec(memory_space=pl.ANY)
    vmem_space = pl.BlockSpec(memory_space=pltpu.VMEM)
    dma = pltpu.SemaphoreType.DMA
    low, wide = jnp.bfloat16, jnp.float32
    token = jax.ShapeDtypeStruct((tokens, model), low)
    flat = pltpu.VMEM((tokens, model), low)
    return pl.pallas_call(
        functools.partial(middle_body, shards, rows),
        name="middle_layer",
        out_shape=(
            token, token, token,
            jax.ShapeDtypeStruct((model, model), low),
            jax.ShapeDtypeStruct((shards, rows, model), low),
            jax.ShapeDtypeStruct((shards, rows, model), low),
            jax.ShapeDtypeStruct((16, model), wide),
        ),
        in_specs=[any_space] * 6 + [vmem_space],
        out_specs=(any_space,) * 4 + (vmem_space,) * 3,
        scratch_shapes=[
            flat, flat, flat,
            pltpu.VMEM((model, model), low),
            pltpu.VMEM((shards, model, width), low),
            pltpu.VMEM((shards, width, model), low),
            pltpu.VMEM((tokens, model), wide),
            flat,
            pltpu.VMEM((model, tokens), low),
            pltpu.VMEM((shards, tokens, width), low),
            pltpu.VMEM((shards, tokens, width), low),
            pltpu.VMEM((4, shards, 2, rows, model), low),
            pltpu.VMEM((shards, 2, 4, rows, model), low),
            pltpu.VMEM((4, shards, rows, model), low),
            pltpu.VMEM((shards, 4, rows, model), low),
            pltpu.VMEM((shards, 2, rows, model), low),
            pltpu.VMEM((shards, 2, rows, model), low),
            pltpu.VMEM((shards, rows, model), low),
            pltpu.VMEM((shards, rows, model), low),
            dma((4 + 2 * shards,)), dma((4,)),
            dma((4,)), dma((4,)), dma((shards,)), dma((shards,)),
            dma((2, shards, 2)), dma((2, shards, 2)), dma((2, shards)), dma((2, shards)),
        ],
        compiler_params=pltpu.CompilerParams(
            collective_id=2, has_side_effects=True, vmem_limit_bytes=66_000_000
        ),
    )(mixed, x, grad, qkvo, up_w, down_w, vec)


def final_body(
    shards, quads, rows,
    dq_in, dk_in, dv_in, dkx_in, dvx_in, normed_in, x_in, attn_in, w_in, d_out_in, up_in, down_in, vec_in, small_in,
    qkvo_out, up_out, down_out, vec_out, input_out,
    dq, dk, dv, dkx, dvx, normed, turned, x, attn, weights, grads, mate, first, second,
    last, last_up, last_down, ring, ring_up, ring_down, full, full_up, full_down, vec_sum, vec_mate, vec_ring,
    load_sem, save_sem, w_send, w_recv, c_send, c_recv, f_send, f_recv, s_send, s_recv, z_send, z_recv, q_send, q_recv,
    x_send, x_recv, y_send, y_recv, d_send, d_recv, g_send, g_recv, out_sem, v_send, v_recv,
):
    rep, shard, side, quad, (dx, dy) = place()
    low, wide = jnp.bfloat16, jnp.float32
    steps = x.shape[0] // STEP
    model = x.shape[1]
    x_peer, y_peer, partner = (rep + dx, shard, side), (rep + dy, shard, side), (rep, shard, 1 - side)
    x_quad, y_quad, d_quad = quad + dx, quad + dy, quad + dx + dy
    z_peers = [(rep, lax.rem(shard + k, shards), side) for k in range(1, shards)]
    q_peers = [(lax.rem(rep + 4 * k, 4 * quads), shard, side) for k in range(1, quads)]
    loads = [
        pltpu.make_async_copy(src, dst, load_sem.at[i])
        for i, (src, dst) in enumerate((
            (normed_in, normed), (dq_in, dq), (d_out_in, grads.at[3]), (dk_in, dk), (dv_in, dv),
            (w_in.at[0], weights.at[0]), (w_in.at[1], weights.at[1]), (w_in.at[2], weights.at[2]),
            (x_in, x), (attn_in, attn),
        ))
    ]
    for load in loads:
        load.start()
    greet(z_peers + q_peers + [x_peer, y_peer, partner])
    swaps = [
        remote(src, dst, w_send.at[i], w_recv.at[i], partner)
        for i, (src, dst) in enumerate(((dkx_in, dkx), (dvx_in, dvx)))
    ]
    for swap in swaps:
        swap.start()
    fulls, lasts, rings = (full, full_up, full_down), (last, last_up, last_down), (ring, ring_up, ring_down)

    def block(j):
        return pl.ds(pl.multiple_of(j * STEP, STEP), STEP)

    def part(f, m):
        return grads.at[m, f, side]

    def source(g, f):
        return (part(f, quad), up_in.at[f], down_in.at[f])[g]

    def flip_way(f, after):
        odd = lax.rem(f + after, 2)
        return dx + odd * (dy - dx)

    def cross(m):
        return remote(grads.at[m, :, 1 - side], mate.at[m], c_send.at[m], c_recv.at[m], partner)

    def f_copy(f, slot):
        way = flip_way(f, 0)
        member = quad + way if slot == 0 else d_quad
        return remote(part(f, member), first.at[f, slot], f_send.at[f, slot], f_recv.at[f, slot], (rep + way, shard, side))

    def s_copy(f):
        way = flip_way(f, 1)
        return remote(part(f, quad + way), second.at[f], s_send.at[f], s_recv.at[f], (rep + way, shard, side))

    def z_copy(g, k):
        return remote(
            source(g, lax.rem(shard + k, shards)), lasts[g].at[shards - k - 1],
            z_send.at[g, k - 1], z_recv.at[g, shards - k - 1], z_peers[k - 1],
        )

    def z_wait(g, k):
        remote(source(g, shard), lasts[g].at[k - 1], z_send.at[g, k - 1], z_recv.at[g, k - 1], z_peers[k - 1]).wait_recv()

    def vec_copy(src, i, peer, slot=None):
        return remote(src, vec_mate.at[i if slot is None else slot], v_send.at[i], v_recv.at[i if slot is None else slot], peer)

    def spread(g, member, send, recv, peer, half=None, core=None):
        core = side if core is None else core
        ref = fulls[g].at[core, member]
        if half is not None:
            width = ref.shape[-1] // 2
            ref = fulls[g].at[core, member, :, pl.ds(half * width, width)]
        return remote(ref, ref, send, recv, peer)

    def swirl(g):
        mine = fulls[g].at[side, quad]
        for k in range(1, shards):
            z_wait(g, k)
        add_into(mine, [source(g, shard)] + [lasts[g].at[k] for k in range(shards - 1)])
        for k in range(1, quads):
            remote(mine, rings[g].at[quads - k - 1], q_send.at[g, k - 1], q_recv.at[g, quads - k - 1], q_peers[k - 1]).start()
        for k in range(1, quads):
            remote(mine, rings[g].at[k - 1], q_send.at[g, k - 1], q_recv.at[g, k - 1], q_peers[k - 1]).wait()
        if quads > 1:
            add_into(mine, [mine] + [rings[g].at[k] for k in range(quads - 1)])
        spread(g, quad, x_send.at[g], x_recv.at[g], x_peer).start()
        spread(g, quad, y_send.at[g], y_recv.at[g], y_peer).start()
        spread(g, quad, g_send.at[g, 0], g_recv.at[g, 0], partner).start()

    def turn(g):
        spread(g, x_quad, x_send.at[g], x_recv.at[g], x_peer).wait_recv()
        spread(g, x_quad, d_send.at[g, 1], d_recv.at[g, 1], y_peer, 1).start()
        spread(g, x_quad, g_send.at[g, 1], g_recv.at[g, 1], partner).start()
        spread(g, y_quad, y_send.at[g], y_recv.at[g], y_peer).wait_recv()
        spread(g, y_quad, d_send.at[g, 0], d_recv.at[g, 0], x_peer, 0).start()
        spread(g, y_quad, g_send.at[g, 2], g_recv.at[g, 2], partner).start()

    def corner(g):
        spread(g, d_quad, d_send.at[g, 0], d_recv.at[g, 0], x_peer, 0).wait_recv()
        spread(g, d_quad, d_send.at[g, 1], d_recv.at[g, 1], y_peer, 1).wait_recv()
        spread(g, d_quad, g_send.at[g, 3], g_recv.at[g, 3], partner).start()

    def target(g, m, core):
        if g == 0:
            return qkvo_out.at[m, pl.ds(core * rows, rows), :]
        if g == 1:
            return up_out.at[pl.ds(core * rows, rows), pl.ds(m * model, model)]
        return down_out.at[pl.ds((core * 4 + m) * rows, rows), :]

    def put(g, m, core):
        return pltpu.make_async_copy(fulls[g].at[core, m], target(g, m, core), out_sem.at[g, m, core])

    def finish(g):
        for i, member in enumerate((quad, x_quad, y_quad, d_quad)):
            spread(g, member, g_send.at[g, i], g_recv.at[g, i], partner, core=1 - side).wait_recv()
        for m in range(4):
            for core in range(2):
                put(g, m, core).start()

    def each(body):
        def step(f, carry):
            body(f)
            return carry
        lax.fori_loop(0, shards, step, 0)

    def column(array):
        return jnp.sum(array.astype(wide), axis=0, keepdims=True)

    def weight_grad(m, errors):
        grads[m] = nn(turned[...], errors[...]).astype(low).reshape(shards, 2, rows, model)
        cross(m).start()

    def merge(m):
        cross(m).wait_recv()

        def step(f, carry):
            add_into(part(f, m), (part(f, m), mate.at[m, f]))
            return carry
        lax.fori_loop(0, shards, step, 0)

    for g in (2, 1):
        for k in range(1, shards):
            z_copy(g, k).start()
    loads[2].wait()
    cross(3).start()
    loads[0].wait()

    def flip(j, carry):
        turned[:, block(j)] = normed[block(j), :].astype(wide).T.astype(low)
        return carry
    lax.fori_loop(0, steps, flip, 0)
    loads[1].wait()
    weight_grad(0, dq)
    merge(3)
    for i, (mine, theirs) in enumerate(((dk, dkx), (dv, dvx))):
        loads[3 + i].wait()
        swaps[i].wait_recv()

        def join(j, carry, mine=mine, theirs=theirs):
            mine[block(j), :] = (mine[block(j), :].astype(wide) + theirs[block(j), :].astype(wide)).astype(low)
            return carry
        lax.fori_loop(0, steps, join, 0)
        weight_grad(1 + i, mine)
        merge(i)
    merge(2)

    def begin(f):
        for slot in range(2):
            f_copy(f, slot).start()
    each(begin)
    for load in loads[5:]:
        load.wait()

    def back(j, carry):
        at = block(j)
        error = nt(dq[at, :], weights[0]) + nt(dk[at, :], weights[1]) + nt(dv[at, :], weights[2])
        values = x[at, :].astype(wide)
        centre = values - jnp.mean(values, axis=-1, keepdims=True)
        scale = lax.rsqrt(jnp.mean(centre * centre, axis=-1, keepdims=True) + norm_eps)
        unit = centre * scale
        scaled = error * vec_in[0:1, :]
        mean_one = jnp.mean(scaled, axis=-1, keepdims=True)
        mean_two = jnp.mean(scaled * unit, axis=-1, keepdims=True)
        x[at, :] = (attn[at, :].astype(wide) + scale * (scaled - mean_one - unit * mean_two)).astype(low)
        gain, bias, query, value = carry
        return gain + column(error * unit), bias + column(error), query + column(dq[at, :]), value + column(dv[at, :])
    zero = jnp.zeros((1, model), wide)
    sums = lax.fori_loop(0, steps, back, (zero,) * 4)
    save = pltpu.make_async_copy(x, input_out, save_sem.at[0])
    save.start()
    vec_sum[...] = small_in[...]
    for i, value in enumerate(sums):
        vec_sum[4 + i:5 + i, :] = value
    vec_copy(vec_sum, 0, partner).start()

    def fold(f):
        for slot in range(2):
            f_copy(f, slot).wait()
            member = quad if slot == 0 else quad + flip_way(f, 1)
            add_into(part(f, member), (part(f, member), first.at[f, slot]))
        s_copy(f).start()
    each(fold)
    vec_copy(vec_sum, 0, partner).wait()
    vec_sum[...] = vec_sum[...] + vec_mate[0]
    vec_copy(vec_sum, 1, x_peer).start()
    swirl(2)
    swirl(1)

    def settle(f):
        s_copy(f).wait()
        add_into(part(f, quad), (part(f, quad), second.at[f]))
    each(settle)
    for k in range(1, shards):
        z_copy(0, k).start()
    vec_copy(vec_sum, 1, x_peer).wait()
    vec_sum[...] = vec_sum[...] + vec_mate[1]
    vec_copy(vec_sum, 2, y_peer).start()
    turn(2)
    turn(1)
    vec_copy(vec_sum, 2, y_peer).wait()
    vec_sum[...] = vec_sum[...] + vec_mate[2]
    for k in range(1, shards):
        vec_copy(vec_sum, 2 + k, z_peers[k - 1], 2 + shards - k).start()
    corner(2)
    corner(1)
    swirl(0)
    finish(2)
    finish(1)
    total = vec_sum[...]
    for k in range(1, shards):
        vec_copy(vec_sum, 2 + k, z_peers[k - 1]).wait()
        total = total + vec_mate[2 + k]
    vec_ring[0] = total
    base = 2 + shards
    for k in range(1, quads):
        remote(vec_ring.at[0], vec_ring.at[quads - k], v_send.at[base + k], v_recv.at[base + quads - k], q_peers[k - 1]).start()
    for k in range(1, quads):
        remote(vec_ring.at[0], vec_ring.at[k], v_send.at[base + k], v_recv.at[base + k], q_peers[k - 1]).wait()
        total = total + vec_ring[k]
    vec_out[...] = total
    turn(0)
    corner(0)
    finish(0)
    for g in range(GROUPS):
        for m in range(4):
            for core in range(2):
                put(g, m, core).wait()
        for k in range(1, shards):
            z_copy(g, k).wait_send()
        spread(g, quad, x_send.at[g], x_recv.at[g], x_peer).wait_send()
        spread(g, quad, y_send.at[g], y_recv.at[g], y_peer).wait_send()
        spread(g, y_quad, d_send.at[g, 0], d_recv.at[g, 0], x_peer, 0).wait_send()
        spread(g, x_quad, d_send.at[g, 1], d_recv.at[g, 1], y_peer, 1).wait_send()
        for i in range(4):
            spread(g, quad, g_send.at[g, i], g_recv.at[g, i], partner).wait_send()
    for m in range(4):
        cross(m).wait_send()
    for swap in swaps:
        swap.wait_send()
    save.wait()


def final_layer(shards, quads, dq, dk, dv, dkx, dvx, normed, x, attn, w_qkvo, d_out, up, down, vec, small):
    tokens, model = x.shape
    rows = model // shards // 2
    any_space = pl.BlockSpec(memory_space=pl.ANY)
    vmem_space = pl.BlockSpec(memory_space=pltpu.VMEM)
    dma = pltpu.SemaphoreType.DMA
    low, wide = jnp.bfloat16, jnp.float32
    piece = (rows, model)
    spare = max(quads - 1, 1)
    flat = pltpu.VMEM((tokens, model), low)
    return pl.pallas_call(
        functools.partial(final_body, shards, quads, rows),
        name="final_layer",
        out_shape=(
            jax.ShapeDtypeStruct((4, 2 * rows, model), low),
            jax.ShapeDtypeStruct((2 * rows, 4 * model), low),
            jax.ShapeDtypeStruct((8 * rows, model), low),
            jax.ShapeDtypeStruct(small.shape, wide),
            jax.ShapeDtypeStruct((tokens, model), low),
        ),
        in_specs=[any_space] * 10 + [vmem_space] * 4,
        out_specs=(any_space,) * 3 + (vmem_space, any_space),
        scratch_shapes=[flat] * 6
        + [pltpu.VMEM((model, tokens), low), flat, flat, pltpu.VMEM((3, model, model), low)]
        + [
            pltpu.VMEM((4, shards, 2) + piece, low),
            pltpu.VMEM((4, shards) + piece, low),
            pltpu.VMEM((shards, 2) + piece, low),
            pltpu.VMEM((shards,) + piece, low),
        ]
        + [pltpu.VMEM((shards - 1,) + piece, low)] * 3
        + [pltpu.VMEM((spare,) + piece, low)] * 3
        + [pltpu.VMEM((2, 4) + piece, low)] * 3
        + [
            pltpu.VMEM(small.shape, wide),
            pltpu.VMEM((2 + shards,) + small.shape, wide),
            pltpu.VMEM((quads,) + small.shape, wide),
            dma((10,)), dma((1,)), dma((2,)), dma((2,)),
            dma((4,)), dma((4,)),
            dma((shards, 2)), dma((shards, 2)),
            dma((shards,)), dma((shards,)),
            dma((GROUPS, shards - 1)), dma((GROUPS, shards - 1)),
            dma((GROUPS, spare)), dma((GROUPS, spare)),
            dma((GROUPS,)), dma((GROUPS,)), dma((GROUPS,)), dma((GROUPS,)),
            dma((GROUPS, 2)), dma((GROUPS, 2)),
            dma((GROUPS, 4)), dma((GROUPS, 4)),
            dma((GROUPS, 4, 2)),
            dma((3 + shards + quads,)), dma((3 + shards + quads,)),
        ],
        compiler_params=pltpu.CompilerParams(
            collective_id=1, has_side_effects=True, vmem_limit_bytes=62_000_000
        ),
    )(dq, dk, dv, dkx, dvx, normed, x, attn, w_qkvo, d_out, up, down, vec, small)


def on_device(
    shards, quads,
    layer_input, segment, rand_blocks, first_gain, first_bias, query_weight, query_bias,
    key_weight, value_weight, value_bias, out_weight, out_bias, second_gain, second_bias,
    up_weight, up_bias, down_weight, down_bias, cotangent,
):
    micro, _, half, model = layer_input.shape
    side = lax.axis_index("seq")
    rows = micro * half
    part = model // shards
    low, wide = jnp.bfloat16, jnp.float32
    shard = lax.axis_index("fsdp")
    vec = jnp.concatenate([
        first_gain, first_bias, query_bias, value_bias, out_bias, second_gain, second_bias, down_bias
    ]).reshape(8, part)
    vec = lax.dynamic_update_slice(jnp.zeros((16, model), low), vec, (0, shard * part))
    inside = lax.rem(shard * 4 * part, model)
    vec = lax.dynamic_update_slice(
        vec, up_bias.reshape(1, 4 * part), (8 + shard * 4 * part // model, inside)
    )
    w_qkvo, w_up, w_down, vec, normed, queries, keys, values, keys_other, values_other = gather_weights(
        shards, jnp.stack([query_weight, key_weight, value_weight, out_weight]), up_weight, down_weight, vec,
        layer_input.reshape(rows, model),
    )
    span, aug, block_bias, doc_bias = tables(segment[:, 0], rand_blocks[:, 0], side, half)

    cut = lambda array: array.reshape(micro, half, model)
    attended = (span, cut(queries), cut(keys), cut(values), cut(keys_other), cut(values_other),
                aug, block_bias, doc_bias)
    mixed, lse = attend_forward(*attended)
    mixed_rows = mixed.reshape(rows, model)
    tokens = layer_input.reshape(rows, model)
    result, grad_attn, grad_mixed, d_out, d_up, d_down, small = middle_layer(
        shards, mixed_rows, tokens, cotangent.reshape(rows, model), w_qkvo, w_up, w_down, vec
    )
    grads = attend_backward(0, (), *attended, mixed, cut(grad_mixed), lse)
    grads = attend_backward(1, grads, *attended, mixed, cut(grad_mixed), lse)
    grads = [array.reshape(rows, model) for array in (grads[0], grads[1], grads[2], grads[3], grads[4])]
    g_qkvo, g_up, g_down, small, input_grad = final_layer(
        shards, quads, *grads, normed, tokens, grad_attn, w_qkvo,
        d_out.reshape(shards, 2, part // 2, model), d_up, d_down, vec, small,
    )
    g_qkvo, g_up, g_down = g_qkvo.astype(wide), g_up.astype(wide), g_down.astype(wide)
    flat = lax.dynamic_slice(small, (0, shard * part), (8, part))
    d_b_up = lax.dynamic_slice(small, (8 + shard * 4 * part // model, inside), (1, 4 * part)).reshape(4 * part)
    shape = layer_input.shape
    return (
        result.reshape(shape), input_grad.reshape(shape), flat[4], flat[5], g_qkvo[0], flat[6],
        g_qkvo[1], g_qkvo[2], flat[7], g_qkvo[3], flat[2], flat[0], flat[1], g_up, d_b_up, g_down, flat[3],
    )


def solution(mesh):
    row = P(None, ("rep", "fsdp"), "seq", None)
    flat, wide = P("fsdp"), P("fsdp", None)
    shards, quads = mesh.shape["fsdp"], mesh.shape["rep"] // 4
    assert mesh.shape["seq"] == 2 and mesh.shape["rep"] % 4 == 0
    return jax.shard_map(
        functools.partial(on_device, shards, quads),
        mesh=mesh,
        in_specs=(
            row, P(None, ("rep", "fsdp"), None), P(None, ("rep", "fsdp"), None, None, None),
            flat, flat, wide, flat, wide, wide, flat, wide, flat, flat, flat, wide, flat, wide, flat, row,
        ),
        out_specs=(row, row, flat, flat, wide, flat, wide, wide, flat, wide, flat, flat, flat, wide, flat, wide, flat),
        check_vma=False,
    )
```

```python
import functools
import jax
import jax.numpy as jnp
from jax import lax
from jax.experimental import pallas as pl
from jax.experimental.pallas import tpu as pltpu
from jax.sharding import PartitionSpec as P

norm_eps = 1e-05

HEADS = 12
HDIM = 64
BLOCK = 64
TQ = 256
TK = 256
NEG = -1e30


def nt(a, b):
    return lax.dot_general(a, b, (((1,), (1,)), ((), ())), preferred_element_type=jnp.float32)


def tn(a, b):
    return lax.dot_general(a, b, (((0,), (0,)), ((), ())), preferred_element_type=jnp.float32)


def nn(a, b):
    return jnp.dot(a, b, preferred_element_type=jnp.float32)


def head_lanes(head):
    lane = lax.broadcasted_iota(jnp.int32, (1, 128), 1)
    return (lane < HDIM) if head == 0 else (lane >= HDIM)


def bias_rows(block_ref, doc_ref, head):
    rows = [
        jnp.broadcast_to(block_ref[0, 0, head, pl.ds(b, 1), :], (BLOCK, 128)) for b in range(TQ // BLOCK)
    ]
    return (jnp.concatenate(rows, axis=0) + doc_ref[0]).astype(jnp.bfloat16)


def unite(whole, own_ref, other_ref, side):
    half = own_ref.shape[1]
    whole[pl.ds(pl.multiple_of(side * half, TK), half), :] = own_ref[0]
    whole[pl.ds(pl.multiple_of((1 - side) * half, TK), half), :] = other_ref[0]


def forward_body(
    span_ref, q_ref, ko_ref, vo_ref, kx_ref, vx_ref, aug_ref, block_ref, doc_ref,
    out_ref, lse_ref, acc_ref, qa_ref, k_all, v_all,
):
    micro, tile = pl.program_id(0), pl.program_id(1)

    @pl.when(tile == 0)
    def _():
        unite(k_all, ko_ref, kx_ref, span_ref[micro, tile, 2])
        unite(v_all, vo_ref, vx_ref, span_ref[micro, tile, 2])

    group = q_ref.shape[2] // HDIM
    for head in range(group):
        cols = pl.ds(head // 2 * 128, 128)
        q_rows = q_ref[0, :, cols].astype(jnp.float32) * 0.125
        masked = jnp.where(head_lanes(head % 2), q_rows, 0.0).astype(jnp.bfloat16)
        qa_ref[head, :, 0:128] = masked
        qa_ref[head, :, 128:256] = bias_rows(block_ref, doc_ref, head)
    acc_ref[...] = jnp.zeros_like(acc_ref)

    def step(j, carry):
        at = pl.ds(pl.multiple_of(j * TK, TK), TK)
        aug = aug_ref[0, at, :]
        scores = []
        for head in range(group):
            cols = pl.ds(head // 2 * 128, 128)
            scores.append(nt(jnp.concatenate([k_all[at, cols], aug], axis=1), qa_ref[head]))
        fresh = []
        probs = []
        for head in range(group):
            top_new = jnp.maximum(carry[head], jnp.max(scores[head], axis=0, keepdims=True))
            probs.append(jnp.exp(scores[head] - top_new).astype(jnp.bfloat16))
            fresh.append(top_new)
        for head in range(group):
            cols = pl.ds(head // 2 * 128, 128)
            v_rows = jnp.where(head_lanes(head % 2), v_all[at, cols], jnp.bfloat16(1.0))
            part = tn(v_rows, probs[head])
            acc_ref[head] = acc_ref[head] * jnp.exp(carry[head] - fresh[head]) + part
        return tuple(fresh)

    state = tuple(jnp.full((1, TQ), -3e38, jnp.float32) for _ in range(group))
    state = lax.fori_loop(span_ref[micro, tile, 0], span_ref[micro, tile, 1], step, state)
    for pair in range(group // 2):
        done = []
        for head in range(2):
            at = pair * 2 + head
            mass = acc_ref[at, pl.ds((1 - head) * HDIM, 1), :]
            done.append(acc_ref[at, pl.ds(head * HDIM, HDIM), :] / mass)
            lse_ref[0, pair, pl.ds(head, 1), :] = state[at] + jnp.log(mass)
        out_ref[0, :, pl.ds(pair * 128, 128)] = jnp.concatenate(done, axis=0).T.astype(out_ref.dtype)


def backward_body(
    micro, carried,
    span_ref, q_ref, ko_ref, vo_ref, kx_ref, vx_ref, aug_ref, block_ref, doc_ref,
    mixed_ref, grad_ref, lse_ref, *rest,
):
    dq_ref, dko_ref, dvo_ref, dkx_ref, dvx_ref = rest[carried:carried + 5]
    dqt_ref, qa_ref, gm_ref, k_acc, v_acc, k_all, v_all = rest[carried + 5:]
    tile = pl.program_id(0)
    side = span_ref[micro, tile, 2]

    @pl.when(tile == 0)
    def _():
        unite(k_all, ko_ref, kx_ref, side)
        unite(v_all, vo_ref, vx_ref, side)
        k_acc[...] = jnp.zeros_like(k_acc)
        v_acc[...] = jnp.zeros_like(v_acc)

    group = q_ref.shape[2] // HDIM
    inner = []
    for pair in range(group // 2):
        cols = pl.ds(pair * 128, 128)
        q_rows = q_ref[0, :, cols].astype(jnp.float32) * 0.125
        grad_rows = grad_ref[0, :, cols].astype(jnp.float32)
        both = (mixed_ref[0, :, cols].astype(jnp.float32) * grad_rows).T
        for half in range(2):
            head = pair * 2 + half
            qa_ref[head, :, 0:128] = jnp.where(head_lanes(half), q_rows, 0.0).astype(jnp.bfloat16)
            qa_ref[head, :, 128:256] = bias_rows(block_ref, doc_ref, head)
            gm_ref[head] = jnp.where(head_lanes(half), grad_rows, 0.0).astype(jnp.bfloat16)
            inner.append(jnp.sum(both[half * HDIM:(half + 1) * HDIM, :], axis=0, keepdims=True))
    dqt_ref[...] = jnp.zeros_like(dqt_ref)

    def step(j, carry):
        at = pl.ds(pl.multiple_of(j * TK, TK), TK)
        aug = aug_ref[0, at, :]
        for chunk in range(0, group, CHUNK):
            heads = range(chunk, min(chunk + CHUNK, group))
            scores, grads, probs, souls = {}, {}, {}, {}
            for head in heads:
                cols = pl.ds(head // 2 * 128, 128)
                scores[head] = nt(jnp.concatenate([k_all[at, cols], aug], axis=1), qa_ref[head])
                grads[head] = nt(v_all[at, cols], gm_ref[head])
            for head in heads:
                weight = jnp.exp(scores[head] - lse_ref[0, head // 2, pl.ds(head % 2, 1), :])
                souls[head] = (weight * (grads[head] - carry[head])).astype(jnp.bfloat16)
                probs[head] = weight.astype(jnp.bfloat16)
            for head in heads:
                cols = pl.ds(head // 2 * 128, 128)
                dv = nn(probs[head], gm_ref[head])
                dk = nn(souls[head], qa_ref[head, :, 0:128])
                dqt = tn(k_all[at, cols], souls[head])
                lanes = pl.ds(head * HDIM, HDIM)
                half = head % 2
                dqt_ref[lanes, :] += dqt[half * HDIM:(half + 1) * HDIM, :]
                if half == 0:
                    dv_low, dk_low = dv, dk
                else:
                    k_acc[at, cols] += dk + dk_low
                    v_acc[at, cols] += dv + dv_low
        return carry

    lax.fori_loop(span_ref[micro, tile, 0], span_ref[micro, tile, 1], step, tuple(inner))
    for pair in range(group // 2):
        cols = pl.ds(pair * 128, 128)
        dq_ref[0, :, cols] = (dqt_ref[cols, :] * 0.125).T.astype(dq_ref.dtype)

    @pl.when(tile == pl.num_programs(0) - 1)
    def _():
        size = dko_ref.shape[1]
        mine = pl.ds(pl.multiple_of(side * size, TK), size)
        theirs = pl.ds(pl.multiple_of((1 - side) * size, TK), size)
        dko_ref[0] = k_acc[mine, :].astype(dko_ref.dtype)
        dvo_ref[0] = v_acc[mine, :].astype(dvo_ref.dtype)
        dkx_ref[0] = k_acc[theirs, :].astype(dkx_ref.dtype)
        dvx_ref[0] = v_acc[theirs, :].astype(dvx_ref.dtype)


CHUNK = 4


def specs(half, length, width, at):
    rows = pl.BlockSpec((1, TQ, width), lambda *i: at(*i) + (0,))
    side = pl.BlockSpec((1, half, width), lambda *i: (at(*i)[0], 0, 0))
    aug = pl.BlockSpec((1, length, 128), lambda *i: (at(*i)[0], 0, 0))
    block = pl.BlockSpec((1, 1, HEADS, TQ // BLOCK, 128), lambda *i: at(*i) + (0, 0, 0))
    doc = pl.BlockSpec((1, TQ, 128), lambda *i: at(*i) + (0,))
    lse = pl.BlockSpec((1, HEADS // 2, 2, TQ), lambda *i: (at(*i)[0], 0, 0, at(*i)[1]))
    return rows, side, aug, block, doc, lse


def attend_forward(span, q, ko, vo, kx, vx, aug, block, doc):
    micro, half, width = q.shape
    length = aug.shape[1]
    rows, side, aug_spec, blk, doc_spec, lse = specs(half, length, width, lambda m, t, s: (m, t))
    return pl.pallas_call(
        forward_body,
        name="attend_forward",
        out_shape=(
            jax.ShapeDtypeStruct((micro, half, width), jnp.bfloat16),
            jax.ShapeDtypeStruct((micro, HEADS // 2, 2, half), jnp.float32),
        ),
        grid_spec=pltpu.PrefetchScalarGridSpec(
            num_scalar_prefetch=1,
            grid=(micro, half // TQ),
            in_specs=[rows] + [side] * 4 + [aug_spec, blk, doc_spec],
            out_specs=(rows, lse),
            scratch_shapes=[
                pltpu.VMEM((HEADS, 128, TQ), jnp.float32),
                pltpu.VMEM((HEADS, TQ, 256), jnp.bfloat16),
                pltpu.VMEM((length, width), jnp.bfloat16),
                pltpu.VMEM((length, width), jnp.bfloat16),
            ],
        ),
        cost_estimate=pl.CostEstimate(flops=20_000_000_000, bytes_accessed=20_000_000, transcendentals=0),
    )(span, q, ko, vo, kx, vx, aug, block, doc)


def attend_backward(step, carried, span, q, ko, vo, kx, vx, aug, block, doc, mixed, grad, lse):
    micro, half, width = q.shape
    length = aug.shape[1]
    rows, side, aug_spec, blk, doc_spec, lse_spec = specs(half, length, width, lambda t, s: (step, t))
    shape = jax.ShapeDtypeStruct((micro, half, width), jnp.bfloat16)
    return pl.pallas_call(
        functools.partial(backward_body, step, len(carried)),
        name="attend_backward",
        out_shape=(shape,) * 5,
        grid_spec=pltpu.PrefetchScalarGridSpec(
            num_scalar_prefetch=1,
            grid=(half // TQ,),
            in_specs=[rows] + [side] * 4 + [aug_spec, blk, doc_spec, rows, rows, lse_spec]
            + [pl.BlockSpec(memory_space=pl.ANY)] * len(carried),
            out_specs=(rows,) + (side,) * 4,
            scratch_shapes=[
                pltpu.VMEM((width, TQ), jnp.float32),
                pltpu.VMEM((HEADS, TQ, 256), jnp.bfloat16),
                pltpu.VMEM((HEADS, TQ, 128), jnp.bfloat16),
                pltpu.VMEM((length, width), jnp.float32),
                pltpu.VMEM((length, width), jnp.float32),
                pltpu.VMEM((length, width), jnp.bfloat16),
                pltpu.VMEM((length, width), jnp.bfloat16),
            ],
        ),
        input_output_aliases={12 + i: i for i in range(len(carried))},
        cost_estimate=pl.CostEstimate(flops=20_000_000_000, bytes_accessed=20_000_000, transcendentals=0),
    )(span, q, ko, vo, kx, vx, aug, block, doc, mixed, grad, lse, *carried)


def tables(segment, rand_blocks, side, half):
    micro, length = segment.shape
    blocks = length // BLOCK
    mine = half // BLOCK
    tiles = half // TQ
    lane = lax.broadcasted_iota(jnp.int32, (1, 1, 128), 2)
    own = lax.dynamic_slice_in_dim(segment, side * half, half, axis=1)
    place = lax.broadcasted_iota(jnp.int32, (1, length, 1), 1) // BLOCK
    aug = ((lane == place) | (lane == segment[:, :, None] + blocks)).astype(jnp.bfloat16)
    doc = jnp.where((lane >= blocks) & (lane < blocks + 4) & (lane != own[:, :, None] + blocks), NEG, 0.0)
    q_block = side * mine + lax.broadcasted_iota(jnp.int32, (1, 1, mine, 1), 2)
    k_block = lax.broadcasted_iota(jnp.int32, (1, 1, 1, 128), 3)
    chosen = lax.dynamic_slice_in_dim(rand_blocks, side * mine, mine, axis=2)
    allowed = (jnp.abs(q_block - k_block) <= 1) | (k_block == 0) | (k_block == blocks - 1)
    allowed = allowed | (q_block == 0) | (q_block == blocks - 1) | (k_block >= blocks)
    for pick in range(rand_blocks.shape[3]):
        allowed = allowed | (chosen[:, :, :, pick:pick + 1] == k_block)
    block = jnp.where(allowed, 0.0, NEG).astype(jnp.float32)
    block = jnp.moveaxis(block.reshape(micro, HEADS, tiles, mine // tiles, 128), 2, 1)
    edges = own.reshape(micro, tiles, TQ)
    first, last = edges[:, :, :1], edges[:, :, TQ - 1:]
    begin = jnp.sum((segment[:, None, :] < first).astype(jnp.int32), axis=-1)
    end = jnp.sum((segment[:, None, :] <= last).astype(jnp.int32), axis=-1)
    span = jnp.stack([begin // TK, (end + TK - 1) // TK, jnp.full_like(begin, side)], axis=-1)
    return span, aug, block, doc.astype(jnp.float32)


MESH = pl.DeviceIdType.MESH
GROUPS = 3


def place():
    rep, shard, side = lax.axis_index("rep"), lax.axis_index("fsdp"), lax.axis_index("seq")
    quad = lax.rem(rep, 4)
    across, along = lax.rem(quad, 2), quad // 2
    near = (1 - 2 * across, 2 - 4 * along)
    return rep, shard, side, quad, near


def chunk(refs, group, shard, quad, side, rows, half=None):
    width = 768 if half is None else 384
    offset = 0 if half is None else half * 384
    low = side * rows
    if group == 0:
        return refs[0].at[quad, pl.ds(pl.multiple_of(shard * (2 * rows) + low, 16), rows), pl.ds(offset, width)]
    if group == 1:
        at = pl.multiple_of(shard * (2 * rows) + low, 16)
        return refs[1].at[pl.ds(at, rows), pl.ds(pl.multiple_of(quad * 768 + offset, 128), width)]
    at = pl.multiple_of(shard * (8 * rows) + quad * (2 * rows) + low, 16)
    return refs[2].at[pl.ds(at, rows), pl.ds(offset, width)]


def greet(peers):
    barrier = pltpu.get_barrier_semaphore()
    for peer in peers:
        pl.semaphore_signal(barrier, inc=1, device_id=peer, device_id_type=MESH)
    pl.semaphore_wait(barrier, len(peers))


def remote(src, dst, send, recv, peer):
    return pltpu.make_async_remote_copy(
        src_ref=src, dst_ref=dst, send_sem=send, recv_sem=recv, device_id=peer, device_id_type=MESH
    )


def gather_body(
    shards, rows, qkvo_in, up_in, down_in, vec_in, x_in,
    qkvo_out, up_out, down_out, vec_out, normed_out, q_out, k_out, v_out, kx_out, vx_out,
    qkvo_stage, up_stage, down_stage, vec_all, weights, normed, results,
    in_sem, out_sem, z_send, z_recv, x_send, x_recv, y_send, y_recv, d_send, d_recv, c_send, c_recv,
    load_sem, save_sem, swap_send, swap_recv,
):
    rep, shard, side, quad, (dx, dy) = place()
    ins, outs = (qkvo_in, up_in, down_in), (qkvo_out, up_out, down_out)
    stages = (qkvo_stage, up_stage, down_stage)
    x_peer, y_peer, partner = (rep + dx, shard, side), (rep + dy, shard, side), (rep, shard, 1 - side)
    z_peers = [(rep, lax.rem(shard + k, shards), side) for k in range(1, shards)]
    for i, src in enumerate(ins):
        pltpu.make_async_copy(src, stages[i], in_sem.at[i]).start()
    greet(z_peers + [x_peer, y_peer, partner])
    sent = []

    def go(copy):
        copy.start()
        sent.append(copy)

    for g in range(GROUPS):
        for k in range(1, shards):
            go(remote(
                chunk(ins, g, 0, quad, side, rows), chunk(outs, g, shard, quad, side, rows),
                z_send.at[g, k - 1], z_recv.at[g, shards - k - 1], z_peers[k - 1],
            ))
        if g == 0:
            for k in range(1, shards):
                go(remote(
                    vec_in, vec_all.at[k - 1],
                    z_send.at[GROUPS, k - 1], z_recv.at[GROUPS, k - 1], z_peers[k - 1],
                ))
    owned = (
        qkvo_out.at[:, pl.ds(pl.multiple_of(shard * 2 * rows, 16), 2 * rows), :],
        up_out.at[pl.ds(pl.multiple_of(shard * 2 * rows, 16), 2 * rows), :],
        down_out.at[pl.ds(pl.multiple_of(shard * 8 * rows, 16), 8 * rows), :],
    )
    local = []
    for i, src in enumerate(ins):
        pltpu.make_async_copy(src, stages[i], in_sem.at[i]).wait()
        copy = pltpu.make_async_copy(stages[i], owned[i], out_sem.at[i])
        copy.start()
        local.append(copy)

    def piece(g, k, member, core, half=None):
        return chunk(outs, g, lax.rem(shard + k, shards), member, core, rows, half)

    def hop(g, k, member, core, send, recv, peer, half=None):
        ref = piece(g, k, member, core, half)
        return remote(ref, ref, send, recv, peer)

    x_quad, y_quad, d_quad = quad + dx, quad + dy, quad + dx + dy

    def straight(g):
        for k in range(1, shards):
            hop(g, k, quad, side, z_send.at[g, k - 1], z_recv.at[g, k - 1], z_peers[k - 1]).wait_recv()
            go(hop(g, k, quad, side, x_send.at[g, k - 1], x_recv.at[g, k - 1], x_peer))
            go(hop(g, k, quad, side, y_send.at[g, k - 1], y_recv.at[g, k - 1], y_peer))
            go(hop(g, k, quad, side, c_send.at[g, k - 1, 0], c_recv.at[g, k - 1, 0], partner))

    def turn(g):
        for k in range(1, shards):
            hop(g, k, x_quad, side, x_send.at[g, k - 1], x_recv.at[g, k - 1], x_peer).wait_recv()
            go(hop(g, k, x_quad, side, d_send.at[g, k - 1, 1], d_recv.at[g, k - 1, 1], y_peer, 1))
            go(hop(g, k, x_quad, side, c_send.at[g, k - 1, 1], c_recv.at[g, k - 1, 1], partner))
            hop(g, k, y_quad, side, y_send.at[g, k - 1], y_recv.at[g, k - 1], y_peer).wait_recv()
            go(hop(g, k, y_quad, side, d_send.at[g, k - 1, 0], d_recv.at[g, k - 1, 0], x_peer, 0))
            go(hop(g, k, y_quad, side, c_send.at[g, k - 1, 2], c_recv.at[g, k - 1, 2], partner))

    def corner(g):
        for k in range(1, shards):
            hop(g, k, d_quad, side, d_send.at[g, k - 1, 0], d_recv.at[g, k - 1, 0], x_peer, 0).wait_recv()
            hop(g, k, d_quad, side, d_send.at[g, k - 1, 1], d_recv.at[g, k - 1, 1], y_peer, 1).wait_recv()
            go(hop(g, k, d_quad, side, c_send.at[g, k - 1, 3], c_recv.at[g, k - 1, 3], partner))

    def gathered(g):
        for k in range(1, shards):
            for i, member in enumerate((quad, x_quad, y_quad, d_quad)):
                hop(g, k, member, 1 - side, c_send.at[g, k - 1, i], c_recv.at[g, k - 1, i], partner).wait_recv()

    def save(i, target):
        copy = pltpu.make_async_copy(normed if i == 3 else results.at[i], target, save_sem.at[i])
        copy.start()
        local.append(copy)

    def norm(step, carry):
        at = pl.ds(pl.multiple_of(step * STEP, STEP), STEP)
        values = x_in[at, :].astype(jnp.float32)
        centre = values - jnp.mean(values, axis=-1, keepdims=True)
        scale = lax.rsqrt(jnp.mean(centre * centre, axis=-1, keepdims=True) + norm_eps)
        normed[at, :] = (centre * scale * vec_out[0:1, :] + vec_out[1:2, :]).astype(normed.dtype)
        return carry

    def project(i, row):
        pltpu.make_async_copy(qkvo_out.at[i], weights.at[i], load_sem.at[i]).wait()

        def step(j, carry):
            at = pl.ds(pl.multiple_of(j * STEP, STEP), STEP)
            product = nn(normed[at, :], weights[i])
            if row is not None:
                product = product + vec_out[row:row + 1, :]
            results[i, at, :] = product.astype(results.dtype)
            return carry
        lax.fori_loop(0, normed.shape[0] // STEP, step, 0)

    def exchange(i, target):
        copy = remote(results.at[i], target, swap_send.at[i - 1], swap_recv.at[i - 1], partner)
        copy.start()
        return copy

    straight(0)
    for k in range(1, shards):
        remote(
            vec_in, vec_all.at[k - 1], z_send.at[GROUPS, k - 1], z_recv.at[GROUPS, k - 1], z_peers[k - 1]
        ).wait_recv()
    total = vec_in[...].astype(jnp.float32)
    for k in range(1, shards):
        total = total + vec_all[k - 1].astype(jnp.float32)
    vec_out[...] = total
    lax.fori_loop(0, normed.shape[0] // STEP // 2, norm, 0)
    turn(0)
    lax.fori_loop(normed.shape[0] // STEP // 2, normed.shape[0] // STEP, norm, 0)
    save(3, normed_out)
    straight(1)
    corner(0)
    turn(1)
    local[0].wait()
    gathered(0)
    for i in (1, 2, 0):
        pltpu.make_async_copy(qkvo_out.at[i], weights.at[i], load_sem.at[i]).start()
    straight(2)
    project(1, None)
    keys = exchange(1, kx_out)
    save(1, k_out)
    corner(1)
    project(2, 3)
    values = exchange(2, vx_out)
    save(2, v_out)
    turn(2)
    project(0, 2)
    save(0, q_out)
    corner(2)
    gathered(1)
    gathered(2)
    keys.wait()
    values.wait()
    for copy in sent:
        copy.wait_send()
    for copy in local[1:]:
        copy.wait()


STEP = 256


def gather_weights(shards, qkvo, up, down, vec, x):
    rows = qkvo.shape[1] // 2
    model = qkvo.shape[2]
    hidden = up.shape[1]
    any_space = pl.BlockSpec(memory_space=pl.ANY)
    vmem_space = pl.BlockSpec(memory_space=pltpu.VMEM)
    dma = pltpu.SemaphoreType.DMA
    low = jnp.bfloat16
    token = jax.ShapeDtypeStruct(x.shape, low)
    return pl.pallas_call(
        functools.partial(gather_body, shards, rows),
        name="gather_weights",
        out_shape=(
            jax.ShapeDtypeStruct((4, model, model), low),
            jax.ShapeDtypeStruct((model, hidden), low),
            jax.ShapeDtypeStruct((hidden, model), low),
            jax.ShapeDtypeStruct(vec.shape, jnp.float32),
        )
        + (token,) * 6,
        in_specs=[any_space] * 3 + [vmem_space] * 2,
        out_specs=(any_space,) * 3 + (vmem_space,) + (any_space,) * 6,
        scratch_shapes=[
            pltpu.VMEM(qkvo.shape, low), pltpu.VMEM(up.shape, low), pltpu.VMEM(down.shape, low),
            pltpu.VMEM((shards - 1,) + vec.shape, low),
            pltpu.VMEM((3, model, model), low),
            pltpu.VMEM(x.shape, low),
            pltpu.VMEM((3,) + x.shape, low),
            dma((3,)), dma((3,)),
            dma((GROUPS + 1, shards - 1)), dma((GROUPS + 1, shards - 1)),
        ]
        + [dma((GROUPS, shards - 1))] * 4
        + [dma((GROUPS, shards - 1, 2))] * 2
        + [dma((GROUPS, shards - 1, 4))] * 2
        + [dma((3,)), dma((4,)), dma((2,)), dma((2,))],
        compiler_params=pltpu.CompilerParams(
            collective_id=0, has_side_effects=True, vmem_limit_bytes=50_000_000
        ),
    )(qkvo, up, down, vec, x)


def add_into(out_ref, refs):
    total = refs[0][...].astype(jnp.float32)
    for ref in refs[1:]:
        total = total + ref[...].astype(jnp.float32)
    out_ref[...] = total.astype(out_ref.dtype)


def normal_parts(values):
    phi = 0.5 + 0.5 * lax.erf(values * 0.7071067811865476)
    return phi, values * (jnp.exp(-0.5 * values * values) * 0.3989422804014327)


def middle_body(
    shards, rows,
    mixed_in, x_in, grad_in, qkvo_in, up_w_in, down_w_in, vec_in,
    result_out, attn_out, mixed_out, d_out_out, up_out, down_out, sums_out,
    mixed, x, grad, out_w, up_w, down_w, middle, normed, turned, hidden, slope,
    up_grad, down_grad, up_mate, down_mate, up_first, down_first, down_second,
    load_sem, save_sem, uc_send, uc_recv, dc_send, dc_recv, f_send, f_recv, s_send, s_recv,
):
    rep, shard, side, quad, (dx, dy) = place()
    partner = (rep, shard, 1 - side)
    low, wide = jnp.bfloat16, jnp.float32
    steps = x.shape[0] // STEP
    model = x.shape[1]
    width = 8 * rows
    loads = [
        pltpu.make_async_copy(src, dst, load_sem.at[i])
        for i, (src, dst) in enumerate(((mixed_in, mixed), (x_in, x), (qkvo_in.at[3], out_w), (grad_in, grad)))
    ]
    for f in range(shards):
        at = pl.ds(f * width, width)
        loads.append(pltpu.make_async_copy(up_w_in.at[:, at], up_w.at[f], load_sem.at[4 + f]))
        loads.append(pltpu.make_async_copy(down_w_in.at[at, :], down_w.at[f], load_sem.at[4 + shards + f]))
    for load in loads:
        load.start()
    greet([(rep + dx, shard, side), (rep + dy, shard, side), partner])
    firsts = (up_first, down_first)

    def row(i):
        return vec_in[i:i + 1, :]

    def block(j):
        return pl.ds(pl.multiple_of(j * STEP, STEP), STEP)

    def part(g, f, m):
        return up_grad.at[m, f, side] if g == 0 else down_grad.at[f, side, m]

    def mate(g, f, m):
        return up_mate.at[m, f] if g == 0 else down_mate.at[f, m]

    def flip_way(f, second):
        odd = lax.rem(f + second, 2)
        return dx + odd * (dy - dx)

    def up_cross(m):
        return remote(up_grad.at[m, :, 1 - side], up_mate.at[m], uc_send.at[m], uc_recv.at[m], partner)

    def down_cross(f):
        return remote(down_grad.at[f, 1 - side], down_mate.at[f], dc_send.at[f], dc_recv.at[f], partner)

    def f_copy(g, f, slot):
        way = flip_way(f, 0)
        member = quad + way if slot == 0 else quad + dx + dy
        return remote(part(g, f, member), firsts[g].at[f, slot], f_send.at[g, f, slot], f_recv.at[g, f, slot], (rep + way, shard, side))

    def s_copy(f):
        way = flip_way(f, 1)
        return remote(part(1, f, quad + way), down_second.at[f], s_send.at[f], s_recv.at[f], (rep + way, shard, side))

    def first_go(g, f, m):
        @pl.when(m == quad + dx + dy)
        def _():
            f_copy(g, f, 1).start()

        @pl.when(m == quad + flip_way(f, 0))
        def _():
            f_copy(g, f, 0).start()

    def down_merge(f):
        down_cross(f).wait_recv()
        for m in range(4):
            add_into(part(1, f, m), (part(1, f, m), mate(1, f, m)))
            first_go(1, f, m)

    def up_merge(m):
        up_cross(m).wait_recv()

        def step(f, carry):
            add_into(part(0, f, m), (part(0, f, m), mate(0, f, m)))
            first_go(0, f, m)
            return carry
        lax.fori_loop(0, shards, step, 0)

    def each(body):
        def step(f, carry):
            body(f)
            return carry
        lax.fori_loop(0, shards, step, 0)

    def down_fold(f):
        for slot in range(2):
            f_copy(1, f, slot).wait()
            member = quad if slot == 0 else quad + flip_way(f, 1)
            add_into(part(1, f, member), (part(1, f, member), down_first.at[f, slot]))
        s_copy(f).start()

    def down_settle(f):
        s_copy(f).wait()
        add_into(down_out.at[f], (part(1, f, quad), down_second.at[f]))

    def up_fold(f):
        for slot in range(2):
            f_copy(0, f, slot).wait()
            member = quad if slot == 0 else quad + flip_way(f, 1)
            add_into(up_out.at[slot, f], (part(0, f, member), up_first.at[f, slot]))

    saves = []

    def save(src, dst):
        copy = pltpu.make_async_copy(src, dst, save_sem.at[len(saves)])
        copy.start()
        saves.append(copy)

    for load in loads[:3]:
        load.wait()

    def attend_out(j, carry):
        at = block(j)
        values = x[at, :].astype(wide) + nn(mixed[at, :], out_w[...]) + row(4)
        middle[at, :] = values
        centre = values - jnp.mean(values, axis=-1, keepdims=True)
        scale = lax.rsqrt(jnp.mean(centre * centre, axis=-1, keepdims=True) + norm_eps)
        out = centre * scale * row(5) + row(6)
        normed[at, :] = out.astype(low)
        turned[:, at] = out.T.astype(low)
        return carry
    lax.fori_loop(0, steps, attend_out, 0)
    for load in loads[3:]:
        load.wait()

    def bias_at(f):
        first = f * width
        return pl.ds(8 + first // model, 1), pl.ds(pl.multiple_of(lax.rem(first, model), 128), width)

    def expand(f):
        bias = vec_in[bias_at(f)]

        def step(j, carry):
            at = block(j)
            inner = nn(normed[at, :], up_w[f]) + bias
            phi, bump = normal_parts(inner)
            hidden[f, at, :] = (inner * phi).astype(low)
            slope[f, at, :] = (phi + bump).astype(low)
            return carry
        lax.fori_loop(0, steps, step, 0)
        down_grad[f] = tn(hidden[f], grad[...]).astype(low).reshape(2, 4, rows, model)
        down_cross(f).start()

        @pl.when(f > 0)
        def _():
            down_merge(f - 1)
    each(expand)

    def contract(m):
        for h in range(model // width):
            f = m * (model // width) + h

            def step(j, total, f=f):
                at = block(j)
                value = (nt(grad[at, :], down_w[f]) * slope[f, at, :].astype(wide)).astype(low)
                slope[f, at, :] = value
                return total + jnp.sum(value.astype(wide), axis=0, keepdims=True)
            sums_out[bias_at(f)] = lax.fori_loop(0, steps, step, jnp.zeros((1, width), wide))
            product = nn(turned[...], slope[f]).astype(low)
            up_grad[m, :, :, :, pl.ds(h * width, width)] = product.reshape(shards, 2, rows, width)
        up_cross(m).start()

        @pl.when(m == 0)
        def _():
            down_merge(shards - 1)

        @pl.when(m > 0)
        def _():
            up_merge(m - 1)

    def contract_step(m, carry):
        contract(m)
        return carry
    lax.fori_loop(0, 4, contract_step, 0)
    up_merge(3)
    each(down_fold)

    def finish(j, carry):
        at = block(j)
        total = middle[at, :] + row(7)
        for f in range(shards):
            total = total + nn(hidden[f, at, :], down_w[f])
        x[at, :] = total.astype(low)
        return carry
    lax.fori_loop(0, steps, finish, 0)
    save(x, result_out)

    def back(j, carry):
        gain_sum, bias_sum, attn_sum, grad_sum = carry
        at = block(j)
        error = nt(slope[0, at, :], up_w[0])
        for f in range(1, shards):
            error = error + nt(slope[f, at, :], up_w[f])
        values = middle[at, :]
        centre = values - jnp.mean(values, axis=-1, keepdims=True)
        scale = lax.rsqrt(jnp.mean(centre * centre, axis=-1, keepdims=True) + norm_eps)
        unit = centre * scale
        scaled = error * row(5)
        mean_one = jnp.mean(scaled, axis=-1, keepdims=True)
        mean_two = jnp.mean(scaled * unit, axis=-1, keepdims=True)
        upstream = grad[at, :].astype(wide)
        attn = (upstream + scale * (scaled - mean_one - unit * mean_two)).astype(low)
        grad[at, :] = attn
        normed[at, :] = nt(attn, out_w[...]).astype(low)
        column = lambda array: jnp.sum(array, axis=0, keepdims=True)
        return (
            gain_sum + column(error * unit), bias_sum + column(error),
            attn_sum + column(attn.astype(wide)), grad_sum + column(upstream),
        )
    zero = jnp.zeros((1, model), wide)
    sums = lax.fori_loop(0, steps, back, (zero,) * 4)
    save(normed, mixed_out)
    save(grad, attn_out)
    for i, value in enumerate(sums):
        sums_out[i:i + 1, :] = value
    sums_out[4:8, :] = jnp.zeros((4, model), wide)
    sums_out[12:16, :] = jnp.zeros((4, model), wide)
    each(down_settle)
    out_w[...] = tn(mixed[...], grad[...]).astype(low)
    save(out_w, d_out_out)
    each(up_fold)
    for m in range(4):
        up_cross(m).wait_send()
    each(lambda f: down_cross(f).wait_send())
    for copy in saves:
        copy.wait()


def middle_layer(shards, mixed, x, grad, qkvo, up_w, down_w, vec):
    tokens, model = x.shape
    hidden = up_w.shape[1]
    rows = model // shards // 2
    width = 8 * rows
    any_space = pl.BlockSpec(memory_space=pl.ANY)
    vmem_space = pl.BlockSpec(memory_space=pltpu.VMEM)
    dma = pltpu.SemaphoreType.DMA
    low, wide = jnp.bfloat16, jnp.float32
    token = jax.ShapeDtypeStruct((tokens, model), low)
    flat = pltpu.VMEM((tokens, model), low)
    return pl.pallas_call(
        functools.partial(middle_body, shards, rows),
        name="middle_layer",
        out_shape=(
            token, token, token,
            jax.ShapeDtypeStruct((model, model), low),
            jax.ShapeDtypeStruct((2, shards, rows, model), low),
            jax.ShapeDtypeStruct((shards, rows, model), low),
            jax.ShapeDtypeStruct((16, model), wide),
        ),
        in_specs=[any_space] * 6 + [vmem_space],
        out_specs=(any_space,) * 4 + (vmem_space,) * 3,
        scratch_shapes=[
            flat, flat, flat,
            pltpu.VMEM((model, model), low),
            pltpu.VMEM((shards, model, width), low),
            pltpu.VMEM((shards, width, model), low),
            pltpu.VMEM((tokens, model), wide),
            flat,
            pltpu.VMEM((model, tokens), low),
            pltpu.VMEM((shards, tokens, width), low),
            pltpu.VMEM((shards, tokens, width), low),
            pltpu.VMEM((4, shards, 2, rows, model), low),
            pltpu.VMEM((shards, 2, 4, rows, model), low),
            pltpu.VMEM((4, shards, rows, model), low),
            pltpu.VMEM((shards, 4, rows, model), low),
            pltpu.VMEM((shards, 2, rows, model), low),
            pltpu.VMEM((shards, 2, rows, model), low),
            pltpu.VMEM((shards, rows, model), low),
            dma((4 + 2 * shards,)), dma((4,)),
            dma((4,)), dma((4,)), dma((shards,)), dma((shards,)),
            dma((2, shards, 2)), dma((2, shards, 2)), dma((shards,)), dma((shards,)),
        ],
        compiler_params=pltpu.CompilerParams(
            collective_id=2, has_side_effects=True, vmem_limit_bytes=66_000_000
        ),
    )(mixed, x, grad, qkvo, up_w, down_w, vec)


def final_body(
    shards, quads, rows,
    dq_in, dk_in, dv_in, dkx_in, dvx_in, normed_in, x_in, attn_in, w_in, d_out_in, up_in, down_in, vec_in, small_in,
    qkvo_out, up_out, down_out, vec_out, input_out,
    dq, dk, dv, dkx, dvx, normed, turned, x, attn, weights, grads, mate, first, second, up_sum, up_second,
    last, last_up, last_down, ring, ring_up, ring_down, full, full_up, full_down, vec_sum, vec_mate, vec_ring,
    load_sem, save_sem, w_send, w_recv, c_send, c_recv, f_send, f_recv, s_send, s_recv, z_send, z_recv, q_send, q_recv, u_send, u_recv,
    x_send, x_recv, y_send, y_recv, d_send, d_recv, g_send, g_recv, out_sem, v_send, v_recv,
):
    rep, shard, side, quad, (dx, dy) = place()
    low, wide = jnp.bfloat16, jnp.float32
    steps = x.shape[0] // STEP
    model = x.shape[1]
    x_peer, y_peer, partner = (rep + dx, shard, side), (rep + dy, shard, side), (rep, shard, 1 - side)
    x_quad, y_quad, d_quad = quad + dx, quad + dy, quad + dx + dy
    z_peers = [(rep, lax.rem(shard + k, shards), side) for k in range(1, shards)]
    q_peers = [(lax.rem(rep + 4 * k, 4 * quads), shard, side) for k in range(1, quads)]
    loads = [
        pltpu.make_async_copy(src, dst, load_sem.at[i])
        for i, (src, dst) in enumerate((
            (normed_in, normed), (dq_in, dq), (d_out_in, grads.at[3]), (dk_in, dk), (dv_in, dv),
            (w_in.at[0], weights.at[0]), (w_in.at[1], weights.at[1]), (w_in.at[2], weights.at[2]),
            (x_in, x), (attn_in, attn),
        ))
    ]
    for load in loads:
        load.start()
    greet(z_peers + q_peers + [x_peer, y_peer, partner])
    swaps = [
        remote(src, dst, w_send.at[i], w_recv.at[i], partner)
        for i, (src, dst) in enumerate(((dkx_in, dkx), (dvx_in, dvx)))
    ]
    for swap in swaps:
        swap.start()
    fulls, lasts, rings = (full, full_up, full_down), (last, last_up, last_down), (ring, ring_up, ring_down)

    def block(j):
        return pl.ds(pl.multiple_of(j * STEP, STEP), STEP)

    def part(f, m):
        return grads.at[m, f, side]

    def source(g, f):
        return (part(f, quad), up_sum.at[f], down_in.at[f])[g]

    def flip_way(f, after):
        odd = lax.rem(f + after, 2)
        return dx + odd * (dy - dx)

    def cross(m):
        return remote(grads.at[m, :, 1 - side], mate.at[m], c_send.at[m], c_recv.at[m], partner)

    def f_copy(f, slot):
        way = flip_way(f, 0)
        member = quad + way if slot == 0 else d_quad
        return remote(part(f, member), first.at[f, slot], f_send.at[f, slot], f_recv.at[f, slot], (rep + way, shard, side))

    def s_copy(f):
        way = flip_way(f, 1)
        return remote(part(f, quad + way), second.at[f], s_send.at[f], s_recv.at[f], (rep + way, shard, side))

    def z_copy(g, k):
        return remote(
            source(g, lax.rem(shard + k, shards)), lasts[g].at[shards - k - 1],
            z_send.at[g, k - 1], z_recv.at[g, shards - k - 1], z_peers[k - 1],
        )

    def z_wait(g, k):
        remote(source(g, shard), lasts[g].at[k - 1], z_send.at[g, k - 1], z_recv.at[g, k - 1], z_peers[k - 1]).wait_recv()

    def vec_copy(src, i, peer, slot=None):
        return remote(src, vec_mate.at[i if slot is None else slot], v_send.at[i], v_recv.at[i if slot is None else slot], peer)

    def spread(g, member, send, recv, peer, half=None, core=None):
        core = side if core is None else core
        ref = fulls[g].at[core, member]
        if half is not None:
            width = ref.shape[-1] // 2
            ref = fulls[g].at[core, member, :, pl.ds(half * width, width)]
        return remote(ref, ref, send, recv, peer)

    def swirl(g):
        mine = fulls[g].at[side, quad]
        for k in range(1, shards):
            z_wait(g, k)
        add_into(mine, [source(g, shard)] + [lasts[g].at[k] for k in range(shards - 1)])
        for k in range(1, quads):
            remote(mine, rings[g].at[quads - k - 1], q_send.at[g, k - 1], q_recv.at[g, quads - k - 1], q_peers[k - 1]).start()
        for k in range(1, quads):
            remote(mine, rings[g].at[k - 1], q_send.at[g, k - 1], q_recv.at[g, k - 1], q_peers[k - 1]).wait()
        if quads > 1:
            add_into(mine, [mine] + [rings[g].at[k] for k in range(quads - 1)])
        spread(g, quad, x_send.at[g], x_recv.at[g], x_peer).start()
        spread(g, quad, y_send.at[g], y_recv.at[g], y_peer).start()
        spread(g, quad, g_send.at[g, 0], g_recv.at[g, 0], partner).start()

    def turn(g):
        spread(g, x_quad, x_send.at[g], x_recv.at[g], x_peer).wait_recv()
        spread(g, x_quad, d_send.at[g, 1], d_recv.at[g, 1], y_peer, 1).start()
        spread(g, x_quad, g_send.at[g, 1], g_recv.at[g, 1], partner).start()
        spread(g, y_quad, y_send.at[g], y_recv.at[g], y_peer).wait_recv()
        spread(g, y_quad, d_send.at[g, 0], d_recv.at[g, 0], x_peer, 0).start()
        spread(g, y_quad, g_send.at[g, 2], g_recv.at[g, 2], partner).start()

    def corner(g):
        spread(g, d_quad, d_send.at[g, 0], d_recv.at[g, 0], x_peer, 0).wait_recv()
        spread(g, d_quad, d_send.at[g, 1], d_recv.at[g, 1], y_peer, 1).wait_recv()
        spread(g, d_quad, g_send.at[g, 3], g_recv.at[g, 3], partner).start()

    def target(g, m, core):
        if g == 0:
            return qkvo_out.at[m, pl.ds(core * rows, rows), :]
        if g == 1:
            return up_out.at[pl.ds(core * rows, rows), pl.ds(m * model, model)]
        return down_out.at[pl.ds((core * 4 + m) * rows, rows), :]

    def put(g, m, core):
        return pltpu.make_async_copy(fulls[g].at[core, m], target(g, m, core), out_sem.at[g, m, core])

    def finish(g):
        for i, member in enumerate((quad, x_quad, y_quad, d_quad)):
            spread(g, member, g_send.at[g, i], g_recv.at[g, i], partner, core=1 - side).wait_recv()
        for m in range(4):
            for core in range(2):
                put(g, m, core).start()

    def each(body):
        def step(f, carry):
            body(f)
            return carry
        lax.fori_loop(0, shards, step, 0)

    def column(array):
        return jnp.sum(array.astype(wide), axis=0, keepdims=True)

    def weight_grad(m, errors):
        grads[m] = nn(turned[...], errors[...]).astype(low).reshape(shards, 2, rows, model)
        cross(m).start()

    def merge(m):
        cross(m).wait_recv()

        def step(f, carry):
            add_into(part(f, m), (part(f, m), mate.at[m, f]))

            @pl.when(m == d_quad)
            def _():
                f_copy(f, 1).start()

            @pl.when(m == quad + flip_way(f, 0))
            def _():
                f_copy(f, 0).start()
            return carry
        lax.fori_loop(0, shards, step, 0)

    def u_copy(f):
        return remote(up_in.at[1, f], up_second.at[f], u_send.at[f], u_recv.at[f], (rep + flip_way(f, 1), shard, side))
    each(lambda f: u_copy(f).start())
    for k in range(1, shards):
        z_copy(2, k).start()
    loads[2].wait()
    cross(3).start()
    loads[0].wait()

    def flip(j, carry):
        turned[:, block(j)] = normed[block(j), :].astype(wide).T.astype(low)
        return carry
    lax.fori_loop(0, steps, flip, 0)
    loads[1].wait()
    weight_grad(0, dq)
    merge(3)
    for i, (mine, theirs) in enumerate(((dk, dkx), (dv, dvx))):
        loads[3 + i].wait()
        swaps[i].wait_recv()

        def join(j, carry, mine=mine, theirs=theirs):
            mine[block(j), :] = (mine[block(j), :].astype(wide) + theirs[block(j), :].astype(wide)).astype(low)
            return carry
        lax.fori_loop(0, steps, join, 0)
        weight_grad(1 + i, mine)
        merge(i)
    merge(2)

    def up_settle(f):
        u_copy(f).wait()
        add_into(up_sum.at[f], (up_in.at[0, f], up_second.at[f]))
    each(up_settle)
    for k in range(1, shards):
        z_copy(1, k).start()
    for load in loads[5:]:
        load.wait()

    def back(j, carry):
        at = block(j)
        error = nt(dq[at, :], weights[0]) + nt(dk[at, :], weights[1]) + nt(dv[at, :], weights[2])
        values = x[at, :].astype(wide)
        centre = values - jnp.mean(values, axis=-1, keepdims=True)
        scale = lax.rsqrt(jnp.mean(centre * centre, axis=-1, keepdims=True) + norm_eps)
        unit = centre * scale
        scaled = error * vec_in[0:1, :]
        mean_one = jnp.mean(scaled, axis=-1, keepdims=True)
        mean_two = jnp.mean(scaled * unit, axis=-1, keepdims=True)
        x[at, :] = (attn[at, :].astype(wide) + scale * (scaled - mean_one - unit * mean_two)).astype(low)
        gain, bias, query, value = carry
        return gain + column(error * unit), bias + column(error), query + column(dq[at, :]), value + column(dv[at, :])
    zero = jnp.zeros((1, model), wide)
    sums = lax.fori_loop(0, steps // 2, back, (zero,) * 4)

    def fold(f):
        for slot in range(2):
            f_copy(f, slot).wait()
            member = quad if slot == 0 else quad + flip_way(f, 1)
            add_into(part(f, member), (part(f, member), first.at[f, slot]))
        s_copy(f).start()
    each(fold)
    sums = lax.fori_loop(steps // 2, steps, back, sums)
    save = pltpu.make_async_copy(x, input_out, save_sem.at[0])
    save.start()
    vec_sum[...] = small_in[...]
    for i, value in enumerate(sums):
        vec_sum[4 + i:5 + i, :] = value
    vec_copy(vec_sum, 0, partner).start()

    def settle(f):
        s_copy(f).wait()
        add_into(part(f, quad), (part(f, quad), second.at[f]))
    each(settle)
    for k in range(1, shards):
        z_copy(0, k).start()
    vec_copy(vec_sum, 0, partner).wait()
    vec_sum[...] = vec_sum[...] + vec_mate[0]
    vec_copy(vec_sum, 1, x_peer).start()
    swirl(2)
    swirl(1)
    vec_copy(vec_sum, 1, x_peer).wait()
    vec_sum[...] = vec_sum[...] + vec_mate[1]
    vec_copy(vec_sum, 2, y_peer).start()
    turn(2)
    turn(1)
    vec_copy(vec_sum, 2, y_peer).wait()
    vec_sum[...] = vec_sum[...] + vec_mate[2]
    for k in range(1, shards):
        vec_copy(vec_sum, 2 + k, z_peers[k - 1], 2 + shards - k).start()
    corner(2)
    corner(1)
    swirl(0)
    finish(2)
    finish(1)
    total = vec_sum[...]
    for k in range(1, shards):
        vec_copy(vec_sum, 2 + k, z_peers[k - 1]).wait()
        total = total + vec_mate[2 + k]
    vec_ring[0] = total
    base = 2 + shards
    for k in range(1, quads):
        remote(vec_ring.at[0], vec_ring.at[quads - k], v_send.at[base + k], v_recv.at[base + quads - k], q_peers[k - 1]).start()
    for k in range(1, quads):
        remote(vec_ring.at[0], vec_ring.at[k], v_send.at[base + k], v_recv.at[base + k], q_peers[k - 1]).wait()
        total = total + vec_ring[k]
    vec_out[...] = total
    turn(0)
    corner(0)
    finish(0)
    for g in range(GROUPS):
        for m in range(4):
            for core in range(2):
                put(g, m, core).wait()
        for k in range(1, shards):
            z_copy(g, k).wait_send()
        spread(g, quad, x_send.at[g], x_recv.at[g], x_peer).wait_send()
        spread(g, quad, y_send.at[g], y_recv.at[g], y_peer).wait_send()
        spread(g, y_quad, d_send.at[g, 0], d_recv.at[g, 0], x_peer, 0).wait_send()
        spread(g, x_quad, d_send.at[g, 1], d_recv.at[g, 1], y_peer, 1).wait_send()
        for i in range(4):
            spread(g, quad, g_send.at[g, i], g_recv.at[g, i], partner).wait_send()
    for m in range(4):
        cross(m).wait_send()
    for swap in swaps:
        swap.wait_send()
    save.wait()


def final_layer(shards, quads, dq, dk, dv, dkx, dvx, normed, x, attn, w_qkvo, d_out, up, down, vec, small):
    tokens, model = x.shape
    rows = model // shards // 2
    any_space = pl.BlockSpec(memory_space=pl.ANY)
    vmem_space = pl.BlockSpec(memory_space=pltpu.VMEM)
    dma = pltpu.SemaphoreType.DMA
    low, wide = jnp.bfloat16, jnp.float32
    piece = (rows, model)
    spare = max(quads - 1, 1)
    flat = pltpu.VMEM((tokens, model), low)
    return pl.pallas_call(
        functools.partial(final_body, shards, quads, rows),
        name="final_layer",
        out_shape=(
            jax.ShapeDtypeStruct((4, 2 * rows, model), low),
            jax.ShapeDtypeStruct((2 * rows, 4 * model), low),
            jax.ShapeDtypeStruct((8 * rows, model), low),
            jax.ShapeDtypeStruct(small.shape, wide),
            jax.ShapeDtypeStruct((tokens, model), low),
        ),
        in_specs=[any_space] * 10 + [vmem_space] * 4,
        out_specs=(any_space,) * 3 + (vmem_space, any_space),
        scratch_shapes=[flat] * 6
        + [pltpu.VMEM((model, tokens), low), flat, flat, pltpu.VMEM((3, model, model), low)]
        + [
            pltpu.VMEM((4, shards, 2) + piece, low),
            pltpu.VMEM((4, shards) + piece, low),
            pltpu.VMEM((shards, 2) + piece, low),
            pltpu.VMEM((shards,) + piece, low),
            pltpu.VMEM((shards,) + piece, low),
            pltpu.VMEM((shards,) + piece, low),
        ]
        + [pltpu.VMEM((shards - 1,) + piece, low)] * 3
        + [pltpu.VMEM((spare,) + piece, low)] * 3
        + [pltpu.VMEM((2, 4) + piece, low)] * 3
        + [
            pltpu.VMEM(small.shape, wide),
            pltpu.VMEM((2 + shards,) + small.shape, wide),
            pltpu.VMEM((quads,) + small.shape, wide),
            dma((10,)), dma((1,)), dma((2,)), dma((2,)),
            dma((4,)), dma((4,)),
            dma((shards, 2)), dma((shards, 2)),
            dma((shards,)), dma((shards,)),
            dma((GROUPS, shards - 1)), dma((GROUPS, shards - 1)),
            dma((GROUPS, spare)), dma((GROUPS, spare)), dma((shards,)), dma((shards,)),
            dma((GROUPS,)), dma((GROUPS,)), dma((GROUPS,)), dma((GROUPS,)),
            dma((GROUPS, 2)), dma((GROUPS, 2)),
            dma((GROUPS, 4)), dma((GROUPS, 4)),
            dma((GROUPS, 4, 2)),
            dma((3 + shards + quads,)), dma((3 + shards + quads,)),
        ],
        compiler_params=pltpu.CompilerParams(
            collective_id=1, has_side_effects=True, vmem_limit_bytes=62_000_000
        ),
    )(dq, dk, dv, dkx, dvx, normed, x, attn, w_qkvo, d_out, up, down, vec, small)


def on_device(
    shards, quads,
    layer_input, segment, rand_blocks, first_gain, first_bias, query_weight, query_bias,
    key_weight, value_weight, value_bias, out_weight, out_bias, second_gain, second_bias,
    up_weight, up_bias, down_weight, down_bias, cotangent,
):
    micro, _, half, model = layer_input.shape
    side = lax.axis_index("seq")
    rows = micro * half
    part = model // shards
    low, wide = jnp.bfloat16, jnp.float32
    shard = lax.axis_index("fsdp")
    rank = lax.broadcasted_iota(jnp.int32, (16, 1), 0)
    vec = jnp.zeros((16, part), low)
    for i, bias in enumerate((first_gain, first_bias, query_bias, value_bias, out_bias, second_gain, second_bias, down_bias)):
        vec = jnp.where(rank == i, bias[None, :], vec)
    vec = lax.dynamic_update_slice(jnp.zeros((16, model), low), vec, (0, shard * part))
    inside = lax.rem(shard * 4 * part, model)
    line = 8 + shard * 4 * part // model
    if 4 * part == model:
        vec = jnp.where(rank == line, up_bias[None, :], vec)
    else:
        vec = lax.dynamic_update_slice(vec, up_bias.reshape(1, 4 * part), (line, inside))
    w_qkvo, w_up, w_down, vec, normed, queries, keys, values, keys_other, values_other = gather_weights(
        shards, jnp.stack([query_weight, key_weight, value_weight, out_weight]), up_weight, down_weight, vec,
        layer_input.reshape(rows, model),
    )
    span, aug, block_bias, doc_bias = tables(segment[:, 0], rand_blocks[:, 0], side, half)

    cut = lambda array: array.reshape(micro, half, model)
    attended = (span, cut(queries), cut(keys), cut(values), cut(keys_other), cut(values_other),
                aug, block_bias, doc_bias)
    mixed, lse = attend_forward(*attended)
    mixed_rows = mixed.reshape(rows, model)
    tokens = layer_input.reshape(rows, model)
    result, grad_attn, grad_mixed, d_out, d_up, d_down, small = middle_layer(
        shards, mixed_rows, tokens, cotangent.reshape(rows, model), w_qkvo, w_up, w_down, vec
    )
    grads = attend_backward(0, (), *attended, mixed, cut(grad_mixed), lse)
    grads = attend_backward(1, grads, *attended, mixed, cut(grad_mixed), lse)
    grads = [array.reshape(rows, model) for array in (grads[0], grads[1], grads[2], grads[3], grads[4])]
    g_qkvo, g_up, g_down, small, input_grad = final_layer(
        shards, quads, *grads, normed, tokens, grad_attn, w_qkvo,
        d_out.reshape(shards, 2, part // 2, model), d_up, d_down, vec, small,
    )
    g_qkvo, g_up, g_down = g_qkvo.astype(wide), g_up.astype(wide), g_down.astype(wide)
    flat = lax.dynamic_slice(small, (0, shard * part), (8, part))
    d_b_up = lax.dynamic_slice(small, (line, inside), (1, 4 * part)).reshape(4 * part)
    shape = layer_input.shape
    return (
        result.reshape(shape), input_grad.reshape(shape), flat[4], flat[5], g_qkvo[0], flat[6],
        g_qkvo[1], g_qkvo[2], flat[7], g_qkvo[3], flat[2], flat[0], flat[1], g_up, d_b_up, g_down, flat[3],
    )


def solution(mesh):
    row = P(None, ("rep", "fsdp"), "seq", None)
    flat, wide = P("fsdp"), P("fsdp", None)
    shards, quads = mesh.shape["fsdp"], mesh.shape["rep"] // 4
    assert mesh.shape["seq"] == 2 and mesh.shape["rep"] % 4 == 0
    return jax.shard_map(
        functools.partial(on_device, shards, quads),
        mesh=mesh,
        in_specs=(
            row, P(None, ("rep", "fsdp"), None), P(None, ("rep", "fsdp"), None, None, None),
            flat, flat, wide, flat, wide, wide, flat, wide, flat, flat, flat, wide, flat, wide, flat, row,
        ),
        out_specs=(row, row, flat, flat, wide, flat, wide, wide, flat, wide, flat, flat, flat, wide, flat, wide, flat),
        check_vma=False,
    )
```

```python
import functools
import jax
import jax.numpy as jnp
from jax import lax
from jax.experimental import pallas as pl
from jax.experimental.pallas import tpu as pltpu
from jax.sharding import PartitionSpec as P

norm_eps = 1e-05

HEADS = 12
HDIM = 64
BLOCK = 64
TQ = 256
TK = 256
NEG = -1e30


def nt(a, b):
    return lax.dot_general(a, b, (((1,), (1,)), ((), ())), preferred_element_type=jnp.float32)


def tn(a, b):
    return lax.dot_general(a, b, (((0,), (0,)), ((), ())), preferred_element_type=jnp.float32)


def nn(a, b):
    return jnp.dot(a, b, preferred_element_type=jnp.float32)


def head_lanes(head):
    lane = lax.broadcasted_iota(jnp.int32, (1, 128), 1)
    return (lane < HDIM) if head == 0 else (lane >= HDIM)


def bias_rows(block_ref, doc_ref, head):
    rows = [
        jnp.broadcast_to(block_ref[0, 0, head, pl.ds(b, 1), :], (BLOCK, 128)) for b in range(TQ // BLOCK)
    ]
    return (jnp.concatenate(rows, axis=0) + doc_ref[0]).astype(jnp.bfloat16)


def unite(whole, own_ref, other_ref, side):
    half = own_ref.shape[1]
    whole[pl.ds(pl.multiple_of(side * half, TK), half), :] = own_ref[0]
    whole[pl.ds(pl.multiple_of((1 - side) * half, TK), half), :] = other_ref[0]


def forward_body(
    span_ref, q_ref, ko_ref, vo_ref, kx_ref, vx_ref, aug_ref, block_ref, doc_ref,
    out_ref, lse_ref, acc_ref, qa_ref, k_all, v_all,
):
    micro, tile = pl.program_id(0), pl.program_id(1)

    @pl.when(tile == 0)
    def _():
        unite(k_all, ko_ref, kx_ref, span_ref[micro, tile, 2])
        unite(v_all, vo_ref, vx_ref, span_ref[micro, tile, 2])

    group = q_ref.shape[2] // HDIM
    for head in range(group):
        cols = pl.ds(head // 2 * 128, 128)
        q_rows = q_ref[0, :, cols].astype(jnp.float32) * 0.125
        masked = jnp.where(head_lanes(head % 2), q_rows, 0.0).astype(jnp.bfloat16)
        qa_ref[head, :, 0:128] = masked
        qa_ref[head, :, 128:256] = bias_rows(block_ref, doc_ref, head)
    acc_ref[...] = jnp.zeros_like(acc_ref)

    def step(j, carry):
        at = pl.ds(pl.multiple_of(j * TK, TK), TK)
        aug = aug_ref[0, at, :]
        scores = []
        for head in range(group):
            cols = pl.ds(head // 2 * 128, 128)
            scores.append(nt(jnp.concatenate([k_all[at, cols], aug], axis=1), qa_ref[head]))
        fresh = []
        probs = []
        for head in range(group):
            top_new = jnp.maximum(carry[head], jnp.max(scores[head], axis=0, keepdims=True))
            probs.append(jnp.exp(scores[head] - top_new).astype(jnp.bfloat16))
            fresh.append(top_new)
        for head in range(group):
            cols = pl.ds(head // 2 * 128, 128)
            v_rows = jnp.where(head_lanes(head % 2), v_all[at, cols], jnp.bfloat16(1.0))
            part = tn(v_rows, probs[head])
            acc_ref[head] = acc_ref[head] * jnp.exp(carry[head] - fresh[head]) + part
        return tuple(fresh)

    state = tuple(jnp.full((1, TQ), -3e38, jnp.float32) for _ in range(group))
    state = lax.fori_loop(span_ref[micro, tile, 0], span_ref[micro, tile, 1], step, state)
    for pair in range(group // 2):
        done = []
        for head in range(2):
            at = pair * 2 + head
            mass = acc_ref[at, pl.ds((1 - head) * HDIM, 1), :]
            done.append(acc_ref[at, pl.ds(head * HDIM, HDIM), :] / mass)
            lse_ref[0, pair, pl.ds(head, 1), :] = state[at] + jnp.log(mass)
        out_ref[0, :, pl.ds(pair * 128, 128)] = jnp.concatenate(done, axis=0).T.astype(out_ref.dtype)


def backward_body(
    micro, carried,
    span_ref, q_ref, ko_ref, vo_ref, kx_ref, vx_ref, aug_ref, block_ref, doc_ref,
    mixed_ref, grad_ref, lse_ref, *rest,
):
    dq_ref, dko_ref, dvo_ref, dkx_ref, dvx_ref = rest[carried:carried + 5]
    dqt_ref, qa_ref, gm_ref, k_acc, v_acc, k_all, v_all = rest[carried + 5:]
    tile = pl.program_id(0)
    side = span_ref[micro, tile, 2]

    @pl.when(tile == 0)
    def _():
        unite(k_all, ko_ref, kx_ref, side)
        unite(v_all, vo_ref, vx_ref, side)
        k_acc[...] = jnp.zeros_like(k_acc)
        v_acc[...] = jnp.zeros_like(v_acc)

    group = q_ref.shape[2] // HDIM
    inner = []
    for pair in range(group // 2):
        cols = pl.ds(pair * 128, 128)
        q_rows = q_ref[0, :, cols].astype(jnp.float32) * 0.125
        grad_rows = grad_ref[0, :, cols].astype(jnp.float32)
        both = (mixed_ref[0, :, cols].astype(jnp.float32) * grad_rows).T
        for half in range(2):
            head = pair * 2 + half
            qa_ref[head, :, 0:128] = jnp.where(head_lanes(half), q_rows, 0.0).astype(jnp.bfloat16)
            qa_ref[head, :, 128:256] = bias_rows(block_ref, doc_ref, head)
            gm_ref[head] = jnp.where(head_lanes(half), grad_rows, 0.0).astype(jnp.bfloat16)
            inner.append(jnp.sum(both[half * HDIM:(half + 1) * HDIM, :], axis=0, keepdims=True))
    dqt_ref[...] = jnp.zeros_like(dqt_ref)

    def step(j, carry):
        at = pl.ds(pl.multiple_of(j * TK, TK), TK)
        aug = aug_ref[0, at, :]
        for chunk in range(0, group, CHUNK):
            heads = range(chunk, min(chunk + CHUNK, group))
            scores, grads, probs, souls = {}, {}, {}, {}
            for head in heads:
                cols = pl.ds(head // 2 * 128, 128)
                scores[head] = nt(jnp.concatenate([k_all[at, cols], aug], axis=1), qa_ref[head])
                grads[head] = nt(v_all[at, cols], gm_ref[head])
            for head in heads:
                weight = jnp.exp(scores[head] - lse_ref[0, head // 2, pl.ds(head % 2, 1), :])
                souls[head] = (weight * (grads[head] - carry[head])).astype(jnp.bfloat16)
                probs[head] = weight.astype(jnp.bfloat16)
            for head in heads:
                cols = pl.ds(head // 2 * 128, 128)
                dv = nn(probs[head], gm_ref[head])
                dk = nn(souls[head], qa_ref[head, :, 0:128])
                dqt = tn(k_all[at, cols], souls[head])
                lanes = pl.ds(head * HDIM, HDIM)
                half = head % 2
                dqt_ref[lanes, :] += dqt[half * HDIM:(half + 1) * HDIM, :]
                if half == 0:
                    dv_low, dk_low = dv, dk
                else:
                    k_acc[at, cols] += dk + dk_low
                    v_acc[at, cols] += dv + dv_low
        return carry

    lax.fori_loop(span_ref[micro, tile, 0], span_ref[micro, tile, 1], step, tuple(inner))
    for pair in range(group // 2):
        cols = pl.ds(pair * 128, 128)
        dq_ref[0, :, cols] = (dqt_ref[cols, :] * 0.125).T.astype(dq_ref.dtype)

    @pl.when(tile == pl.num_programs(0) - 1)
    def _():
        size = dko_ref.shape[1]
        mine = pl.ds(pl.multiple_of(side * size, TK), size)
        theirs = pl.ds(pl.multiple_of((1 - side) * size, TK), size)
        dko_ref[0] = k_acc[mine, :].astype(dko_ref.dtype)
        dvo_ref[0] = v_acc[mine, :].astype(dvo_ref.dtype)
        dkx_ref[0] = k_acc[theirs, :].astype(dkx_ref.dtype)
        dvx_ref[0] = v_acc[theirs, :].astype(dvx_ref.dtype)


CHUNK = 4


def specs(half, length, width, at):
    rows = pl.BlockSpec((1, TQ, width), lambda *i: at(*i) + (0,))
    side = pl.BlockSpec((1, half, width), lambda *i: (at(*i)[0], 0, 0))
    aug = pl.BlockSpec((1, length, 128), lambda *i: (at(*i)[0], 0, 0))
    block = pl.BlockSpec((1, 1, HEADS, TQ // BLOCK, 128), lambda *i: at(*i) + (0, 0, 0))
    doc = pl.BlockSpec((1, TQ, 128), lambda *i: at(*i) + (0,))
    lse = pl.BlockSpec((1, HEADS // 2, 2, TQ), lambda *i: (at(*i)[0], 0, 0, at(*i)[1]))
    return rows, side, aug, block, doc, lse


def attend_forward(span, q, ko, vo, kx, vx, aug, block, doc):
    micro, half, width = q.shape
    length = aug.shape[1]
    rows, side, aug_spec, blk, doc_spec, lse = specs(half, length, width, lambda m, t, s: (m, t))
    return pl.pallas_call(
        forward_body,
        name="attend_forward",
        out_shape=(
            jax.ShapeDtypeStruct((micro, half, width), jnp.bfloat16),
            jax.ShapeDtypeStruct((micro, HEADS // 2, 2, half), jnp.float32),
        ),
        grid_spec=pltpu.PrefetchScalarGridSpec(
            num_scalar_prefetch=1,
            grid=(micro, half // TQ),
            in_specs=[rows] + [side] * 4 + [aug_spec, blk, doc_spec],
            out_specs=(rows, lse),
            scratch_shapes=[
                pltpu.VMEM((HEADS, 128, TQ), jnp.float32),
                pltpu.VMEM((HEADS, TQ, 256), jnp.bfloat16),
                pltpu.VMEM((length, width), jnp.bfloat16),
                pltpu.VMEM((length, width), jnp.bfloat16),
            ],
        ),
        cost_estimate=pl.CostEstimate(flops=20_000_000_000, bytes_accessed=20_000_000, transcendentals=0),
    )(span, q, ko, vo, kx, vx, aug, block, doc)


def attend_backward(step, carried, span, q, ko, vo, kx, vx, aug, block, doc, mixed, grad, lse):
    micro, half, width = q.shape
    length = aug.shape[1]
    rows, side, aug_spec, blk, doc_spec, lse_spec = specs(half, length, width, lambda t, s: (step, t))
    shape = jax.ShapeDtypeStruct((micro, half, width), jnp.bfloat16)
    return pl.pallas_call(
        functools.partial(backward_body, step, len(carried)),
        name="attend_backward",
        out_shape=(shape,) * 5,
        grid_spec=pltpu.PrefetchScalarGridSpec(
            num_scalar_prefetch=1,
            grid=(half // TQ,),
            in_specs=[rows] + [side] * 4 + [aug_spec, blk, doc_spec, rows, rows, lse_spec]
            + [pl.BlockSpec(memory_space=pl.ANY)] * len(carried),
            out_specs=(rows,) + (side,) * 4,
            scratch_shapes=[
                pltpu.VMEM((width, TQ), jnp.float32),
                pltpu.VMEM((HEADS, TQ, 256), jnp.bfloat16),
                pltpu.VMEM((HEADS, TQ, 128), jnp.bfloat16),
                pltpu.VMEM((length, width), jnp.float32),
                pltpu.VMEM((length, width), jnp.float32),
                pltpu.VMEM((length, width), jnp.bfloat16),
                pltpu.VMEM((length, width), jnp.bfloat16),
            ],
        ),
        input_output_aliases={12 + i: i for i in range(len(carried))},
        cost_estimate=pl.CostEstimate(flops=20_000_000_000, bytes_accessed=20_000_000, transcendentals=0),
    )(span, q, ko, vo, kx, vx, aug, block, doc, mixed, grad, lse, *carried)


def tables(segment, rand_blocks, side, half):
    micro, length = segment.shape
    blocks = length // BLOCK
    mine = half // BLOCK
    tiles = half // TQ
    lane = lax.broadcasted_iota(jnp.int32, (1, 1, 128), 2)
    own = lax.dynamic_slice_in_dim(segment, side * half, half, axis=1)
    place = lax.broadcasted_iota(jnp.int32, (1, length, 1), 1) // BLOCK
    aug = ((lane == place) | (lane == segment[:, :, None] + blocks)).astype(jnp.bfloat16)
    doc = jnp.where((lane >= blocks) & (lane < blocks + 4) & (lane != own[:, :, None] + blocks), NEG, 0.0)
    q_block = side * mine + lax.broadcasted_iota(jnp.int32, (1, 1, mine, 1), 2)
    k_block = lax.broadcasted_iota(jnp.int32, (1, 1, 1, 128), 3)
    chosen = lax.dynamic_slice_in_dim(rand_blocks, side * mine, mine, axis=2)
    allowed = (jnp.abs(q_block - k_block) <= 1) | (k_block == 0) | (k_block == blocks - 1)
    allowed = allowed | (q_block == 0) | (q_block == blocks - 1) | (k_block >= blocks)
    for pick in range(rand_blocks.shape[3]):
        allowed = allowed | (chosen[:, :, :, pick:pick + 1] == k_block)
    block = jnp.where(allowed, 0.0, NEG).astype(jnp.float32)
    block = jnp.moveaxis(block.reshape(micro, HEADS, tiles, mine // tiles, 128), 2, 1)
    edges = own.reshape(micro, tiles, TQ)
    first, last = edges[:, :, :1], edges[:, :, TQ - 1:]
    begin = jnp.sum((segment[:, None, :] < first).astype(jnp.int32), axis=-1)
    end = jnp.sum((segment[:, None, :] <= last).astype(jnp.int32), axis=-1)
    span = jnp.stack([begin // TK, (end + TK - 1) // TK, jnp.full_like(begin, side)], axis=-1)
    return span, aug, block, doc.astype(jnp.float32)


MESH = pl.DeviceIdType.MESH
GROUPS = 3


def place():
    rep, shard, side = lax.axis_index("rep"), lax.axis_index("fsdp"), lax.axis_index("seq")
    quad = lax.rem(rep, 4)
    across, along = lax.rem(quad, 2), quad // 2
    near = (1 - 2 * across, 2 - 4 * along)
    return rep, shard, side, quad, near


def chunk(refs, group, shard, quad, side, rows, half=None):
    width = 768 if half is None else 384
    offset = 0 if half is None else half * 384
    low = side * rows
    if group == 0:
        return refs[0].at[quad, pl.ds(pl.multiple_of(shard * (2 * rows) + low, 16), rows), pl.ds(offset, width)]
    at = pl.multiple_of(shard * (2 * rows) + low, 16)
    return refs[1].at[pl.ds(at, rows), pl.ds(pl.multiple_of(quad * 768 + offset, 128), width)]


def greet(peers):
    barrier = pltpu.get_barrier_semaphore()
    for peer in peers:
        pl.semaphore_signal(barrier, inc=1, device_id=peer, device_id_type=MESH)
    pl.semaphore_wait(barrier, len(peers))


def remote(src, dst, send, recv, peer):
    return pltpu.make_async_remote_copy(
        src_ref=src, dst_ref=dst, send_sem=send, recv_sem=recv, device_id=peer, device_id_type=MESH
    )


def gather_body(
    shards, rows, qkvo_in, up_in, down_in, vec_in, x_in,
    qkvo_out, up_out, down_out, vec_out, normed_out, q_out, k_out, v_out, kx_out, vx_out,
    qkvo_stage, up_stage, vec_all, weights, normed, results,
    in_sem, out_sem, z_send, z_recv, x_send, x_recv, y_send, y_recv, d_send, d_recv, c_send, c_recv,
    load_sem, save_sem, swap_send, swap_recv,
):
    rep, shard, side, quad, (dx, dy) = place()
    ins, outs = (qkvo_in, up_in), (qkvo_out, up_out)
    stages = (qkvo_stage, up_stage)
    x_peer, y_peer, partner = (rep + dx, shard, side), (rep + dy, shard, side), (rep, shard, 1 - side)
    z_peers = [(rep, lax.rem(shard + k, shards), side) for k in range(1, shards)]
    for i, src in enumerate(ins):
        pltpu.make_async_copy(src, stages[i], in_sem.at[i]).start()
    greet(z_peers + [x_peer, y_peer, partner])
    sent = []

    def go(copy):
        copy.start()
        sent.append(copy)

    for g in range(EARLY):
        for k in range(1, shards):
            go(remote(
                chunk(ins, g, 0, quad, side, rows), chunk(outs, g, shard, quad, side, rows),
                z_send.at[g, k - 1], z_recv.at[g, shards - k - 1], z_peers[k - 1],
            ))
        if g == 0:
            for k in range(1, shards):
                go(remote(
                    vec_in, vec_all.at[k - 1],
                    z_send.at[EARLY, k - 1], z_recv.at[EARLY, k - 1], z_peers[k - 1],
                ))
    for k in range(1, shards):
        go(remote(
            down_in.at[pl.ds(pl.multiple_of((quad * 2 + side) * rows, 16), rows), :], down_out.at[shard],
            z_send.at[EARLY + 1, k - 1], z_recv.at[EARLY + 1, shards - k - 1], z_peers[k - 1],
        ))
    owned = (
        qkvo_out.at[:, pl.ds(pl.multiple_of(shard * 2 * rows, 16), 2 * rows), :],
        up_out.at[pl.ds(pl.multiple_of(shard * 2 * rows, 16), 2 * rows), :],
    )
    local = []
    for i, src in enumerate(ins):
        pltpu.make_async_copy(src, stages[i], in_sem.at[i]).wait()
        copy = pltpu.make_async_copy(stages[i], owned[i], out_sem.at[i])
        copy.start()
        local.append(copy)

    def piece(g, k, member, core, half=None):
        return chunk(outs, g, lax.rem(shard + k, shards), member, core, rows, half)

    def hop(g, k, member, core, send, recv, peer, half=None):
        ref = piece(g, k, member, core, half)
        return remote(ref, ref, send, recv, peer)

    x_quad, y_quad, d_quad = quad + dx, quad + dy, quad + dx + dy

    def straight(g):
        for k in range(1, shards):
            hop(g, k, quad, side, z_send.at[g, k - 1], z_recv.at[g, k - 1], z_peers[k - 1]).wait_recv()
            go(hop(g, k, quad, side, x_send.at[g, k - 1], x_recv.at[g, k - 1], x_peer))
            go(hop(g, k, quad, side, y_send.at[g, k - 1], y_recv.at[g, k - 1], y_peer))
            go(hop(g, k, quad, side, c_send.at[g, k - 1, 0], c_recv.at[g, k - 1, 0], partner))

    def turn(g):
        for k in range(1, shards):
            hop(g, k, x_quad, side, x_send.at[g, k - 1], x_recv.at[g, k - 1], x_peer).wait_recv()
            go(hop(g, k, x_quad, side, d_send.at[g, k - 1, 1], d_recv.at[g, k - 1, 1], y_peer, 1))
            go(hop(g, k, x_quad, side, c_send.at[g, k - 1, 1], c_recv.at[g, k - 1, 1], partner))
            hop(g, k, y_quad, side, y_send.at[g, k - 1], y_recv.at[g, k - 1], y_peer).wait_recv()
            go(hop(g, k, y_quad, side, d_send.at[g, k - 1, 0], d_recv.at[g, k - 1, 0], x_peer, 0))
            go(hop(g, k, y_quad, side, c_send.at[g, k - 1, 2], c_recv.at[g, k - 1, 2], partner))

    def corner(g):
        for k in range(1, shards):
            hop(g, k, d_quad, side, d_send.at[g, k - 1, 0], d_recv.at[g, k - 1, 0], x_peer, 0).wait_recv()
            hop(g, k, d_quad, side, d_send.at[g, k - 1, 1], d_recv.at[g, k - 1, 1], y_peer, 1).wait_recv()
            go(hop(g, k, d_quad, side, c_send.at[g, k - 1, 3], c_recv.at[g, k - 1, 3], partner))

    def gathered(g):
        for k in range(1, shards):
            for i, member in enumerate((quad, x_quad, y_quad, d_quad)):
                hop(g, k, member, 1 - side, c_send.at[g, k - 1, i], c_recv.at[g, k - 1, i], partner).wait_recv()

    def save(i, target):
        copy = pltpu.make_async_copy(normed if i == 3 else results.at[i], target, save_sem.at[i])
        copy.start()
        local.append(copy)

    def norm(step, carry):
        at = pl.ds(pl.multiple_of(step * STEP, STEP), STEP)
        values = x_in[at, :].astype(jnp.float32)
        centre = values - jnp.mean(values, axis=-1, keepdims=True)
        scale = lax.rsqrt(jnp.mean(centre * centre, axis=-1, keepdims=True) + norm_eps)
        normed[at, :] = (centre * scale * vec_out[0:1, :] + vec_out[1:2, :]).astype(normed.dtype)
        return carry

    def project(i, row):
        pltpu.make_async_copy(qkvo_out.at[i], weights.at[i], load_sem.at[i]).wait()

        def step(j, carry):
            at = pl.ds(pl.multiple_of(j * STEP, STEP), STEP)
            product = nn(normed[at, :], weights[i])
            if row is not None:
                product = product + vec_out[row:row + 1, :]
            results[i, at, :] = product.astype(results.dtype)
            return carry
        lax.fori_loop(0, normed.shape[0] // STEP, step, 0)

    def exchange(i, target):
        copy = remote(results.at[i], target, swap_send.at[i - 1], swap_recv.at[i - 1], partner)
        copy.start()
        return copy

    straight(0)
    for k in range(1, shards):
        remote(
            vec_in, vec_all.at[k - 1], z_send.at[EARLY, k - 1], z_recv.at[EARLY, k - 1], z_peers[k - 1]
        ).wait_recv()
    total = vec_in[...].astype(jnp.float32)
    for k in range(1, shards):
        total = total + vec_all[k - 1].astype(jnp.float32)
    vec_out[...] = total
    lax.fori_loop(0, normed.shape[0] // STEP // 2, norm, 0)
    turn(0)
    lax.fori_loop(normed.shape[0] // STEP // 2, normed.shape[0] // STEP, norm, 0)
    save(3, normed_out)
    straight(1)
    corner(0)
    local[0].wait()
    gathered(0)
    for i in (1, 2, 0):
        pltpu.make_async_copy(qkvo_out.at[i], weights.at[i], load_sem.at[i]).start()
    project(1, None)
    keys = exchange(1, kx_out)
    save(1, k_out)
    turn(1)
    project(2, 3)
    values = exchange(2, vx_out)
    save(2, v_out)
    corner(1)
    project(0, 2)
    save(0, q_out)
    gathered(1)
    for k in range(1, shards):
        remote(
            down_out.at[shard], down_out.at[lax.rem(shard + k, shards)],
            z_send.at[EARLY + 1, k - 1], z_recv.at[EARLY + 1, k - 1], z_peers[k - 1],
        ).wait_recv()
    keys.wait()
    values.wait()
    for copy in sent:
        copy.wait_send()
    for copy in local[1:]:
        copy.wait()


STEP = 256
EARLY = 2


def gather_weights(shards, qkvo, up, down, vec, x):
    rows = qkvo.shape[1] // 2
    model = qkvo.shape[2]
    hidden = up.shape[1]
    any_space = pl.BlockSpec(memory_space=pl.ANY)
    vmem_space = pl.BlockSpec(memory_space=pltpu.VMEM)
    dma = pltpu.SemaphoreType.DMA
    low = jnp.bfloat16
    token = jax.ShapeDtypeStruct(x.shape, low)
    return pl.pallas_call(
        functools.partial(gather_body, shards, rows),
        name="gather_weights",
        out_shape=(
            jax.ShapeDtypeStruct((4, model, model), low),
            jax.ShapeDtypeStruct((model, hidden), low),
            jax.ShapeDtypeStruct((shards, rows, model), low),
            jax.ShapeDtypeStruct(vec.shape, jnp.float32),
        )
        + (token,) * 6,
        in_specs=[any_space] * 3 + [vmem_space] * 2,
        out_specs=(any_space,) * 3 + (vmem_space,) + (any_space,) * 6,
        scratch_shapes=[
            pltpu.VMEM(qkvo.shape, low), pltpu.VMEM(up.shape, low),
            pltpu.VMEM((shards - 1,) + vec.shape, low),
            pltpu.VMEM((3, model, model), low),
            pltpu.VMEM(x.shape, low),
            pltpu.VMEM((3,) + x.shape, low),
            dma((2,)), dma((2,)),
            dma((EARLY + 2, shards - 1)), dma((EARLY + 2, shards - 1)),
        ]
        + [dma((EARLY, shards - 1))] * 4
        + [dma((EARLY, shards - 1, 2))] * 2
        + [dma((EARLY, shards - 1, 4))] * 2
        + [dma((3,)), dma((4,)), dma((2,)), dma((2,))],
        compiler_params=pltpu.CompilerParams(
            collective_id=0, has_side_effects=True, vmem_limit_bytes=50_000_000
        ),
    )(qkvo, up, down, vec, x)


def add_into(out_ref, refs):
    total = refs[0][...].astype(jnp.float32)
    for ref in refs[1:]:
        total = total + ref[...].astype(jnp.float32)
    out_ref[...] = total.astype(out_ref.dtype)


def normal_parts(values):
    phi = 0.5 + 0.5 * lax.erf(values * 0.7071067811865476)
    return phi, values * (jnp.exp(-0.5 * values * values) * 0.3989422804014327)


def middle_body(
    shards, rows,
    mixed_in, x_in, grad_in, qkvo_in, up_w_in, down_w_in, down_z_in, vec_in,
    result_out, attn_out, mixed_out, d_out_out, up_out, down_out, sums_out,
    mixed, x, grad, out_w, up_w, down_w, middle, normed, turned, hidden, slope,
    up_grad, down_grad, up_mate, down_mate, up_first, down_first, down_second,
    load_sem, save_sem, uc_send, uc_recv, dc_send, dc_recv, f_send, f_recv, s_send, s_recv,
    x_send, x_recv, y_send, y_recv, d_send, d_recv, g_send, g_recv,
):
    rep, shard, side, quad, (dx, dy) = place()
    partner = (rep, shard, 1 - side)
    low, wide = jnp.bfloat16, jnp.float32
    steps = x.shape[0] // STEP
    model = x.shape[1]
    width = 8 * rows
    loads = [
        pltpu.make_async_copy(src, dst, load_sem.at[i])
        for i, (src, dst) in enumerate(((mixed_in, mixed), (x_in, x), (qkvo_in.at[3], out_w), (grad_in, grad)))
    ]
    for f in range(shards):
        at = pl.ds(f * width, width)
        loads.append(pltpu.make_async_copy(up_w_in.at[:, at], up_w.at[f], load_sem.at[4 + f]))
    loads.append(pltpu.make_async_copy(down_w_in, down_w.at[shard], load_sem.at[4 + shards]))
    for k in range(1, shards):
        f = lax.rem(shard + k, shards)
        at = pl.ds(pl.multiple_of((quad * 2 + side) * rows, 16), rows)
        loads.append(pltpu.make_async_copy(down_z_in.at[f], down_w.at[f, at, :], load_sem.at[4 + shards + k]))
    for load in loads:
        load.start()
    x_peer, y_peer = (rep + dx, shard, side), (rep + dy, shard, side)
    x_quad, y_quad, d_quad = quad + dx, quad + dy, quad + dx + dy
    greet([x_peer, y_peer, partner])

    def piece(f, member, core, half=None):
        at = pl.ds(pl.multiple_of((member * 2 + core) * rows, 16), rows)
        if half is None:
            return down_w.at[f, at, :]
        return down_w.at[f, at, pl.ds(half * (model // 2), model // 2)]

    def hop(k, member, core, send, recv, peer, half=None):
        ref = piece(lax.rem(shard + k, shards), member, core, half)
        return remote(ref, ref, send, recv, peer)

    def own_piece(k, send, recv, peer):
        f = lax.rem(shard + k, shards)
        return remote(down_z_in.at[f], piece(f, quad, side), send, recv, peer)

    def straight(k):
        return (
            own_piece(k, x_send.at[k - 1], x_recv.at[k - 1], x_peer),
            own_piece(k, y_send.at[k - 1], y_recv.at[k - 1], y_peer),
            own_piece(k, g_send.at[k - 1, 0], g_recv.at[k - 1, 0], partner),
        )

    def turn():
        for k in range(1, shards):
            hop(k, x_quad, side, x_send.at[k - 1], x_recv.at[k - 1], x_peer).wait_recv()
            hop(k, x_quad, side, d_send.at[k - 1, 1], d_recv.at[k - 1, 1], y_peer, 1).start()
            hop(k, x_quad, side, g_send.at[k - 1, 1], g_recv.at[k - 1, 1], partner).start()
            hop(k, y_quad, side, y_send.at[k - 1], y_recv.at[k - 1], y_peer).wait_recv()
            hop(k, y_quad, side, d_send.at[k - 1, 0], d_recv.at[k - 1, 0], x_peer, 0).start()
            hop(k, y_quad, side, g_send.at[k - 1, 2], g_recv.at[k - 1, 2], partner).start()

    def corner():
        for k in range(1, shards):
            hop(k, d_quad, side, d_send.at[k - 1, 0], d_recv.at[k - 1, 0], x_peer, 0).wait_recv()
            hop(k, d_quad, side, d_send.at[k - 1, 1], d_recv.at[k - 1, 1], y_peer, 1).wait_recv()
            hop(k, d_quad, side, g_send.at[k - 1, 3], g_recv.at[k - 1, 3], partner).start()

    def gathered():
        for k in range(1, shards):
            for i, member in enumerate((quad, x_quad, y_quad, d_quad)):
                hop(k, member, 1 - side, g_send.at[k - 1, i], g_recv.at[k - 1, i], partner).wait_recv()

    def flushed():
        for k in range(1, shards):
            for copy in straight(k):
                copy.wait_send()
            hop(k, y_quad, side, d_send.at[k - 1, 0], d_recv.at[k - 1, 0], x_peer, 0).wait_send()
            hop(k, x_quad, side, d_send.at[k - 1, 1], d_recv.at[k - 1, 1], y_peer, 1).wait_send()
            for i in range(1, 4):
                hop(k, quad, side, g_send.at[k - 1, i], g_recv.at[k - 1, i], partner).wait_send()

    for k in range(1, shards):
        for copy in straight(k):
            copy.start()
    firsts = (up_first, down_first)

    def row(i):
        return vec_in[i:i + 1, :]

    def block(j):
        return pl.ds(pl.multiple_of(j * STEP, STEP), STEP)

    def part(g, f, m):
        return up_grad.at[m, f, side] if g == 0 else down_grad.at[f, side, m]

    def mate(g, f, m):
        return up_mate.at[m, f] if g == 0 else down_mate.at[f, m]

    def flip_way(f, second):
        odd = lax.rem(f + second, 2)
        return dx + odd * (dy - dx)

    def up_cross(m):
        return remote(up_grad.at[m, :, 1 - side], up_mate.at[m], uc_send.at[m], uc_recv.at[m], partner)

    def down_cross(f):
        return remote(down_grad.at[f, 1 - side], down_mate.at[f], dc_send.at[f], dc_recv.at[f], partner)

    def f_copy(g, f, slot):
        way = flip_way(f, 0)
        member = quad + way if slot == 0 else quad + dx + dy
        return remote(part(g, f, member), firsts[g].at[f, slot], f_send.at[g, f, slot], f_recv.at[g, f, slot], (rep + way, shard, side))

    def s_copy(f):
        way = flip_way(f, 1)
        return remote(part(1, f, quad + way), down_second.at[f], s_send.at[f], s_recv.at[f], (rep + way, shard, side))

    def first_go(g, f, m):
        @pl.when(m == quad + dx + dy)
        def _():
            f_copy(g, f, 1).start()

        @pl.when(m == quad + flip_way(f, 0))
        def _():
            f_copy(g, f, 0).start()

    def down_merge(f):
        down_cross(f).wait_recv()
        for m in range(4):
            add_into(part(1, f, m), (part(1, f, m), mate(1, f, m)))
            first_go(1, f, m)

    def up_merge(m):
        up_cross(m).wait_recv()

        def step(f, carry):
            add_into(part(0, f, m), (part(0, f, m), mate(0, f, m)))
            first_go(0, f, m)
            return carry
        lax.fori_loop(0, shards, step, 0)

    def each(body):
        def step(f, carry):
            body(f)
            return carry
        lax.fori_loop(0, shards, step, 0)

    def down_fold(f):
        for slot in range(2):
            f_copy(1, f, slot).wait()
            member = quad if slot == 0 else quad + flip_way(f, 1)
            add_into(part(1, f, member), (part(1, f, member), down_first.at[f, slot]))
        s_copy(f).start()

    def down_settle(f):
        s_copy(f).wait()
        add_into(down_out.at[f], (part(1, f, quad), down_second.at[f]))

    def up_fold(f):
        for slot in range(2):
            f_copy(0, f, slot).wait()
            member = quad if slot == 0 else quad + flip_way(f, 1)
            add_into(up_out.at[slot, f], (part(0, f, member), up_first.at[f, slot]))

    saves = []

    def save(src, dst):
        copy = pltpu.make_async_copy(src, dst, save_sem.at[len(saves)])
        copy.start()
        saves.append(copy)

    for load in loads[:3]:
        load.wait()

    def attend_out(j, carry):
        at = block(j)
        values = x[at, :].astype(wide) + nn(mixed[at, :], out_w[...]) + row(4)
        middle[at, :] = values
        centre = values - jnp.mean(values, axis=-1, keepdims=True)
        scale = lax.rsqrt(jnp.mean(centre * centre, axis=-1, keepdims=True) + norm_eps)
        out = centre * scale * row(5) + row(6)
        normed[at, :] = out.astype(low)
        turned[:, at] = out.T.astype(low)
        return carry
    lax.fori_loop(0, steps, attend_out, 0)
    for load in loads[3:]:
        load.wait()

    def bias_at(f):
        first = f * width
        return pl.ds(8 + first // model, 1), pl.ds(pl.multiple_of(lax.rem(first, model), 128), width)

    def expand(f):
        bias = vec_in[bias_at(f)]

        def step(j, carry):
            at = block(j)
            inner = nn(normed[at, :], up_w[f]) + bias
            phi, bump = normal_parts(inner)
            hidden[f, at, :] = (inner * phi).astype(low)
            slope[f, at, :] = (phi + bump).astype(low)
            return carry
        lax.fori_loop(0, steps, step, 0)
        down_grad[f] = tn(hidden[f], grad[...]).astype(low).reshape(2, 4, rows, model)
        down_cross(f).start()

        @pl.when(f > 0)
        def _():
            down_merge(f - 1)

        @pl.when(f == 0)
        def _():
            turn()

        @pl.when(f == 1)
        def _():
            corner()
    each(expand)
    gathered()

    def contract(m):
        for h in range(model // width):
            f = m * (model // width) + h

            def step(j, total, f=f):
                at = block(j)
                value = (nt(grad[at, :], down_w[f]) * slope[f, at, :].astype(wide)).astype(low)
                slope[f, at, :] = value
                return total + jnp.sum(value.astype(wide), axis=0, keepdims=True)
            sums_out[bias_at(f)] = lax.fori_loop(0, steps, step, jnp.zeros((1, width), wide))
            product = nn(turned[...], slope[f]).astype(low)
            up_grad[m, :, :, :, pl.ds(h * width, width)] = product.reshape(shards, 2, rows, width)
        up_cross(m).start()

        @pl.when(m == 0)
        def _():
            down_merge(shards - 1)

        @pl.when(m > 0)
        def _():
            up_merge(m - 1)

    def contract_step(m, carry):
        contract(m)
        return carry
    lax.fori_loop(0, 4, contract_step, 0)
    up_merge(3)
    each(down_fold)

    def finish(j, carry):
        at = block(j)
        total = middle[at, :] + row(7)
        for f in range(shards):
            total = total + nn(hidden[f, at, :], down_w[f])
        x[at, :] = total.astype(low)
        return carry
    lax.fori_loop(0, steps, finish, 0)
    save(x, result_out)

    def back(j, carry):
        gain_sum, bias_sum, attn_sum, grad_sum = carry
        at = block(j)
        error = nt(slope[0, at, :], up_w[0])
        for f in range(1, shards):
            error = error + nt(slope[f, at, :], up_w[f])
        values = middle[at, :]
        centre = values - jnp.mean(values, axis=-1, keepdims=True)
        scale = lax.rsqrt(jnp.mean(centre * centre, axis=-1, keepdims=True) + norm_eps)
        unit = centre * scale
        scaled = error * row(5)
        mean_one = jnp.mean(scaled, axis=-1, keepdims=True)
        mean_two = jnp.mean(scaled * unit, axis=-1, keepdims=True)
        upstream = grad[at, :].astype(wide)
        attn = (upstream + scale * (scaled - mean_one - unit * mean_two)).astype(low)
        grad[at, :] = attn
        normed[at, :] = nt(attn, out_w[...]).astype(low)
        column = lambda array: jnp.sum(array, axis=0, keepdims=True)
        return (
            gain_sum + column(error * unit), bias_sum + column(error),
            attn_sum + column(attn.astype(wide)), grad_sum + column(upstream),
        )
    zero = jnp.zeros((1, model), wide)
    sums = lax.fori_loop(0, steps, back, (zero,) * 4)
    save(normed, mixed_out)
    save(grad, attn_out)
    for i, value in enumerate(sums):
        sums_out[i:i + 1, :] = value
    sums_out[4:8, :] = jnp.zeros((4, model), wide)
    sums_out[12:16, :] = jnp.zeros((4, model), wide)
    each(down_settle)
    out_w[...] = tn(mixed[...], grad[...]).astype(low)
    save(out_w, d_out_out)
    each(up_fold)
    for m in range(4):
        up_cross(m).wait_send()
    each(lambda f: down_cross(f).wait_send())
    flushed()
    for copy in saves:
        copy.wait()


def middle_layer(shards, mixed, x, grad, qkvo, up_w, down_w, down_z, vec):
    tokens, model = x.shape
    hidden = up_w.shape[1]
    rows = model // shards // 2
    width = 8 * rows
    any_space = pl.BlockSpec(memory_space=pl.ANY)
    vmem_space = pl.BlockSpec(memory_space=pltpu.VMEM)
    dma = pltpu.SemaphoreType.DMA
    low, wide = jnp.bfloat16, jnp.float32
    token = jax.ShapeDtypeStruct((tokens, model), low)
    flat = pltpu.VMEM((tokens, model), low)
    return pl.pallas_call(
        functools.partial(middle_body, shards, rows),
        name="middle_layer",
        out_shape=(
            token, token, token,
            jax.ShapeDtypeStruct((model, model), low),
            jax.ShapeDtypeStruct((2, shards, rows, model), low),
            jax.ShapeDtypeStruct((shards, rows, model), low),
            jax.ShapeDtypeStruct((16, model), wide),
        ),
        in_specs=[any_space] * 7 + [vmem_space],
        out_specs=(any_space,) * 4 + (vmem_space,) * 3,
        scratch_shapes=[
            flat, flat, flat,
            pltpu.VMEM((model, model), low),
            pltpu.VMEM((shards, model, width), low),
            pltpu.VMEM((shards, width, model), low),
            pltpu.VMEM((tokens, model), wide),
            flat,
            pltpu.VMEM((model, tokens), low),
            pltpu.VMEM((shards, tokens, width), low),
            pltpu.VMEM((shards, tokens, width), low),
            pltpu.VMEM((4, shards, 2, rows, model), low),
            pltpu.VMEM((shards, 2, 4, rows, model), low),
            pltpu.VMEM((4, shards, rows, model), low),
            pltpu.VMEM((shards, 4, rows, model), low),
            pltpu.VMEM((shards, 2, rows, model), low),
            pltpu.VMEM((shards, 2, rows, model), low),
            pltpu.VMEM((shards, rows, model), low),
            dma((4 + 2 * shards,)), dma((4,)),
            dma((4,)), dma((4,)), dma((shards,)), dma((shards,)),
            dma((2, shards, 2)), dma((2, shards, 2)), dma((shards,)), dma((shards,)),
        ]
        + [dma((shards - 1,))] * 4
        + [dma((shards - 1, 2))] * 2
        + [dma((shards - 1, 4))] * 2,
        compiler_params=pltpu.CompilerParams(
            collective_id=2, has_side_effects=True, vmem_limit_bytes=66_000_000
        ),
    )(mixed, x, grad, qkvo, up_w, down_w, down_z, vec)


def final_body(
    shards, quads, rows,
    dq_in, dk_in, dv_in, dkx_in, dvx_in, normed_in, x_in, attn_in, w_in, d_out_in, up_in, down_in, vec_in, small_in,
    qkvo_out, up_out, down_out, vec_out, input_out,
    dq, dk, dv, dkx, dvx, normed, turned, x, attn, weights, grads, mate, first, second, up_sum, up_second,
    last, last_up, last_down, ring, ring_up, ring_down, full, full_up, full_down, vec_sum, vec_mate, vec_ring,
    load_sem, save_sem, w_send, w_recv, c_send, c_recv, f_send, f_recv, s_send, s_recv, z_send, z_recv, q_send, q_recv, u_send, u_recv,
    x_send, x_recv, y_send, y_recv, d_send, d_recv, g_send, g_recv, out_sem, v_send, v_recv,
):
    rep, shard, side, quad, (dx, dy) = place()
    low, wide = jnp.bfloat16, jnp.float32
    steps = x.shape[0] // STEP
    model = x.shape[1]
    x_peer, y_peer, partner = (rep + dx, shard, side), (rep + dy, shard, side), (rep, shard, 1 - side)
    x_quad, y_quad, d_quad = quad + dx, quad + dy, quad + dx + dy
    z_peers = [(rep, lax.rem(shard + k, shards), side) for k in range(1, shards)]
    q_peers = [(lax.rem(rep + 4 * k, 4 * quads), shard, side) for k in range(1, quads)]
    loads = [
        pltpu.make_async_copy(src, dst, load_sem.at[i])
        for i, (src, dst) in enumerate((
            (normed_in, normed), (dq_in, dq), (d_out_in, grads.at[3]), (dk_in, dk), (dv_in, dv),
            (w_in.at[0], weights.at[0]), (w_in.at[1], weights.at[1]), (w_in.at[2], weights.at[2]),
            (x_in, x), (attn_in, attn),
        ))
    ]
    for load in loads:
        load.start()
    greet(z_peers + q_peers + [x_peer, y_peer, partner])
    swaps = [
        remote(src, dst, w_send.at[i], w_recv.at[i], partner)
        for i, (src, dst) in enumerate(((dkx_in, dkx), (dvx_in, dvx)))
    ]
    for swap in swaps:
        swap.start()
    fulls, lasts, rings = (full, full_up, full_down), (last, last_up, last_down), (ring, ring_up, ring_down)

    def block(j):
        return pl.ds(pl.multiple_of(j * STEP, STEP), STEP)

    def part(f, m):
        return grads.at[m, f, side]

    def source(g, f):
        return (part(f, quad), up_sum.at[f], down_in.at[f])[g]

    def flip_way(f, after):
        odd = lax.rem(f + after, 2)
        return dx + odd * (dy - dx)

    def cross(m):
        return remote(grads.at[m, :, 1 - side], mate.at[m], c_send.at[m], c_recv.at[m], partner)

    def f_copy(f, slot):
        way = flip_way(f, 0)
        member = quad + way if slot == 0 else d_quad
        return remote(part(f, member), first.at[f, slot], f_send.at[f, slot], f_recv.at[f, slot], (rep + way, shard, side))

    def s_copy(f):
        way = flip_way(f, 1)
        return remote(part(f, quad + way), second.at[f], s_send.at[f], s_recv.at[f], (rep + way, shard, side))

    def z_copy(g, k):
        return remote(
            source(g, lax.rem(shard + k, shards)), lasts[g].at[shards - k - 1],
            z_send.at[g, k - 1], z_recv.at[g, shards - k - 1], z_peers[k - 1],
        )

    def z_wait(g, k):
        remote(source(g, shard), lasts[g].at[k - 1], z_send.at[g, k - 1], z_recv.at[g, k - 1], z_peers[k - 1]).wait_recv()

    def vec_copy(src, i, peer, slot=None):
        return remote(src, vec_mate.at[i if slot is None else slot], v_send.at[i], v_recv.at[i if slot is None else slot], peer)

    def spread(g, member, send, recv, peer, half=None, core=None):
        core = side if core is None else core
        ref = fulls[g].at[core, member]
        if half is not None:
            width = ref.shape[-1] // 2
            ref = fulls[g].at[core, member, :, pl.ds(half * width, width)]
        return remote(ref, ref, send, recv, peer)

    def swirl(g):
        mine = fulls[g].at[side, quad]
        for k in range(1, shards):
            z_wait(g, k)
        add_into(mine, [source(g, shard)] + [lasts[g].at[k] for k in range(shards - 1)])
        for k in range(1, quads):
            remote(mine, rings[g].at[quads - k - 1], q_send.at[g, k - 1], q_recv.at[g, quads - k - 1], q_peers[k - 1]).start()
        for k in range(1, quads):
            remote(mine, rings[g].at[k - 1], q_send.at[g, k - 1], q_recv.at[g, k - 1], q_peers[k - 1]).wait()
        if quads > 1:
            add_into(mine, [mine] + [rings[g].at[k] for k in range(quads - 1)])
        spread(g, quad, x_send.at[g], x_recv.at[g], x_peer).start()
        spread(g, quad, y_send.at[g], y_recv.at[g], y_peer).start()
        spread(g, quad, g_send.at[g, 0], g_recv.at[g, 0], partner).start()

    def turn(g):
        spread(g, x_quad, x_send.at[g], x_recv.at[g], x_peer).wait_recv()
        spread(g, x_quad, d_send.at[g, 1], d_recv.at[g, 1], y_peer, 1).start()
        spread(g, x_quad, g_send.at[g, 1], g_recv.at[g, 1], partner).start()
        spread(g, y_quad, y_send.at[g], y_recv.at[g], y_peer).wait_recv()
        spread(g, y_quad, d_send.at[g, 0], d_recv.at[g, 0], x_peer, 0).start()
        spread(g, y_quad, g_send.at[g, 2], g_recv.at[g, 2], partner).start()

    def corner(g):
        spread(g, d_quad, d_send.at[g, 0], d_recv.at[g, 0], x_peer, 0).wait_recv()
        spread(g, d_quad, d_send.at[g, 1], d_recv.at[g, 1], y_peer, 1).wait_recv()
        spread(g, d_quad, g_send.at[g, 3], g_recv.at[g, 3], partner).start()

    def target(g, m, core):
        if g == 0:
            return qkvo_out.at[m, pl.ds(core * rows, rows), :]
        if g == 1:
            return up_out.at[pl.ds(core * rows, rows), pl.ds(m * model, model)]
        return down_out.at[pl.ds((core * 4 + m) * rows, rows), :]

    def put(g, m, core):
        return pltpu.make_async_copy(fulls[g].at[core, m], target(g, m, core), out_sem.at[g, m, core])

    def finish(g):
        for i, member in enumerate((quad, x_quad, y_quad, d_quad)):
            spread(g, member, g_send.at[g, i], g_recv.at[g, i], partner, core=1 - side).wait_recv()
        for m in range(4):
            for core in range(2):
                put(g, m, core).start()

    def each(body):
        def step(f, carry):
            body(f)
            return carry
        lax.fori_loop(0, shards, step, 0)

    def column(array):
        return jnp.sum(array.astype(wide), axis=0, keepdims=True)

    def weight_grad(m, errors):
        grads[m] = nn(turned[...], errors[...]).astype(low).reshape(shards, 2, rows, model)
        cross(m).start()

    def merge(m):
        cross(m).wait_recv()

        def step(f, carry):
            add_into(part(f, m), (part(f, m), mate.at[m, f]))

            @pl.when(m == d_quad)
            def _():
                f_copy(f, 1).start()

            @pl.when(m == quad + flip_way(f, 0))
            def _():
                f_copy(f, 0).start()
            return carry
        lax.fori_loop(0, shards, step, 0)

    def u_copy(f):
        return remote(up_in.at[1, f], up_second.at[f], u_send.at[f], u_recv.at[f], (rep + flip_way(f, 1), shard, side))
    each(lambda f: u_copy(f).start())
    for k in range(1, shards):
        z_copy(2, k).start()
    loads[2].wait()
    cross(3).start()
    loads[0].wait()

    def flip(j, carry):
        turned[:, block(j)] = normed[block(j), :].astype(wide).T.astype(low)
        return carry
    lax.fori_loop(0, steps, flip, 0)
    loads[1].wait()
    weight_grad(0, dq)
    merge(3)
    for i, (mine, theirs) in enumerate(((dk, dkx), (dv, dvx))):
        loads[3 + i].wait()
        swaps[i].wait_recv()

        def join(j, carry, mine=mine, theirs=theirs):
            mine[block(j), :] = (mine[block(j), :].astype(wide) + theirs[block(j), :].astype(wide)).astype(low)
            return carry
        lax.fori_loop(0, steps, join, 0)
        weight_grad(1 + i, mine)
        merge(i)
    merge(2)

    def up_settle(f):
        u_copy(f).wait()
        add_into(up_sum.at[f], (up_in.at[0, f], up_second.at[f]))
    each(up_settle)
    for k in range(1, shards):
        z_copy(1, k).start()
    for load in loads[5:]:
        load.wait()

    def back(j, carry):
        at = block(j)
        error = nt(dq[at, :], weights[0]) + nt(dk[at, :], weights[1]) + nt(dv[at, :], weights[2])
        values = x[at, :].astype(wide)
        centre = values - jnp.mean(values, axis=-1, keepdims=True)
        scale = lax.rsqrt(jnp.mean(centre * centre, axis=-1, keepdims=True) + norm_eps)
        unit = centre * scale
        scaled = error * vec_in[0:1, :]
        mean_one = jnp.mean(scaled, axis=-1, keepdims=True)
        mean_two = jnp.mean(scaled * unit, axis=-1, keepdims=True)
        x[at, :] = (attn[at, :].astype(wide) + scale * (scaled - mean_one - unit * mean_two)).astype(low)
        gain, bias, query, value = carry
        return gain + column(error * unit), bias + column(error), query + column(dq[at, :]), value + column(dv[at, :])
    zero = jnp.zeros((1, model), wide)
    sums = lax.fori_loop(0, steps // 2, back, (zero,) * 4)

    def fold(f):
        for slot in range(2):
            f_copy(f, slot).wait()
            member = quad if slot == 0 else quad + flip_way(f, 1)
            add_into(part(f, member), (part(f, member), first.at[f, slot]))
        s_copy(f).start()
    each(fold)
    sums = lax.fori_loop(steps // 2, steps, back, sums)
    save = pltpu.make_async_copy(x, input_out, save_sem.at[0])
    save.start()
    vec_sum[...] = small_in[...]
    for i, value in enumerate(sums):
        vec_sum[4 + i:5 + i, :] = value
    vec_copy(vec_sum, 0, partner).start()

    def settle(f):
        s_copy(f).wait()
        add_into(part(f, quad), (part(f, quad), second.at[f]))
    each(settle)
    for k in range(1, shards):
        z_copy(0, k).start()
    vec_copy(vec_sum, 0, partner).wait()
    vec_sum[...] = vec_sum[...] + vec_mate[0]
    vec_copy(vec_sum, 1, x_peer).start()
    swirl(2)
    swirl(1)
    vec_copy(vec_sum, 1, x_peer).wait()
    vec_sum[...] = vec_sum[...] + vec_mate[1]
    vec_copy(vec_sum, 2, y_peer).start()
    turn(2)
    turn(1)
    vec_copy(vec_sum, 2, y_peer).wait()
    vec_sum[...] = vec_sum[...] + vec_mate[2]
    for k in range(1, shards):
        vec_copy(vec_sum, 2 + k, z_peers[k - 1], 2 + shards - k).start()
    corner(2)
    corner(1)
    swirl(0)
    finish(2)
    finish(1)
    total = vec_sum[...]
    for k in range(1, shards):
        vec_copy(vec_sum, 2 + k, z_peers[k - 1]).wait()
        total = total + vec_mate[2 + k]
    vec_ring[0] = total
    base = 2 + shards
    for k in range(1, quads):
        remote(vec_ring.at[0], vec_ring.at[quads - k], v_send.at[base + k], v_recv.at[base + quads - k], q_peers[k - 1]).start()
    for k in range(1, quads):
        remote(vec_ring.at[0], vec_ring.at[k], v_send.at[base + k], v_recv.at[base + k], q_peers[k - 1]).wait()
        total = total + vec_ring[k]
    vec_out[...] = total
    turn(0)
    corner(0)
    finish(0)
    for g in range(GROUPS):
        for m in range(4):
            for core in range(2):
                put(g, m, core).wait()
        for k in range(1, shards):
            z_copy(g, k).wait_send()
        spread(g, quad, x_send.at[g], x_recv.at[g], x_peer).wait_send()
        spread(g, quad, y_send.at[g], y_recv.at[g], y_peer).wait_send()
        spread(g, y_quad, d_send.at[g, 0], d_recv.at[g, 0], x_peer, 0).wait_send()
        spread(g, x_quad, d_send.at[g, 1], d_recv.at[g, 1], y_peer, 1).wait_send()
        for i in range(4):
            spread(g, quad, g_send.at[g, i], g_recv.at[g, i], partner).wait_send()
    for m in range(4):
        cross(m).wait_send()
    for swap in swaps:
        swap.wait_send()
    save.wait()


def final_layer(shards, quads, dq, dk, dv, dkx, dvx, normed, x, attn, w_qkvo, d_out, up, down, vec, small):
    tokens, model = x.shape
    rows = model // shards // 2
    any_space = pl.BlockSpec(memory_space=pl.ANY)
    vmem_space = pl.BlockSpec(memory_space=pltpu.VMEM)
    dma = pltpu.SemaphoreType.DMA
    low, wide = jnp.bfloat16, jnp.float32
    piece = (rows, model)
    spare = max(quads - 1, 1)
    flat = pltpu.VMEM((tokens, model), low)
    return pl.pallas_call(
        functools.partial(final_body, shards, quads, rows),
        name="final_layer",
        out_shape=(
            jax.ShapeDtypeStruct((4, 2 * rows, model), low),
            jax.ShapeDtypeStruct((2 * rows, 4 * model), low),
            jax.ShapeDtypeStruct((8 * rows, model), low),
            jax.ShapeDtypeStruct(small.shape, wide),
            jax.ShapeDtypeStruct((tokens, model), low),
        ),
        in_specs=[any_space] * 10 + [vmem_space] * 4,
        out_specs=(any_space,) * 3 + (vmem_space, any_space),
        scratch_shapes=[flat] * 6
        + [pltpu.VMEM((model, tokens), low), flat, flat, pltpu.VMEM((3, model, model), low)]
        + [
            pltpu.VMEM((4, shards, 2) + piece, low),
            pltpu.VMEM((4, shards) + piece, low),
            pltpu.VMEM((shards, 2) + piece, low),
            pltpu.VMEM((shards,) + piece, low),
            pltpu.VMEM((shards,) + piece, low),
            pltpu.VMEM((shards,) + piece, low),
        ]
        + [pltpu.VMEM((shards - 1,) + piece, low)] * 3
        + [pltpu.VMEM((spare,) + piece, low)] * 3
        + [pltpu.VMEM((2, 4) + piece, low)] * 3
        + [
            pltpu.VMEM(small.shape, wide),
            pltpu.VMEM((2 + shards,) + small.shape, wide),
            pltpu.VMEM((quads,) + small.shape, wide),
            dma((10,)), dma((1,)), dma((2,)), dma((2,)),
            dma((4,)), dma((4,)),
            dma((shards, 2)), dma((shards, 2)),
            dma((shards,)), dma((shards,)),
            dma((GROUPS, shards - 1)), dma((GROUPS, shards - 1)),
            dma((GROUPS, spare)), dma((GROUPS, spare)), dma((shards,)), dma((shards,)),
            dma((GROUPS,)), dma((GROUPS,)), dma((GROUPS,)), dma((GROUPS,)),
            dma((GROUPS, 2)), dma((GROUPS, 2)),
            dma((GROUPS, 4)), dma((GROUPS, 4)),
            dma((GROUPS, 4, 2)),
            dma((3 + shards + quads,)), dma((3 + shards + quads,)),
        ],
        compiler_params=pltpu.CompilerParams(
            collective_id=1, has_side_effects=True, vmem_limit_bytes=62_000_000
        ),
    )(dq, dk, dv, dkx, dvx, normed, x, attn, w_qkvo, d_out, up, down, vec, small)


def on_device(
    shards, quads,
    layer_input, segment, rand_blocks, first_gain, first_bias, query_weight, query_bias,
    key_weight, value_weight, value_bias, out_weight, out_bias, second_gain, second_bias,
    up_weight, up_bias, down_weight, down_bias, cotangent,
):
    micro, _, half, model = layer_input.shape
    side = lax.axis_index("seq")
    rows = micro * half
    part = model // shards
    low, wide = jnp.bfloat16, jnp.float32
    shard = lax.axis_index("fsdp")
    rank = lax.broadcasted_iota(jnp.int32, (16, 1), 0)
    vec = jnp.zeros((16, part), low)
    for i, bias in enumerate((first_gain, first_bias, query_bias, value_bias, out_bias, second_gain, second_bias, down_bias)):
        vec = jnp.where(rank == i, bias[None, :], vec)
    vec = lax.dynamic_update_slice(jnp.zeros((16, model), low), vec, (0, shard * part))
    inside = lax.rem(shard * 4 * part, model)
    line = 8 + shard * 4 * part // model
    if 4 * part == model:
        vec = jnp.where(rank == line, up_bias[None, :], vec)
    else:
        vec = lax.dynamic_update_slice(vec, up_bias.reshape(1, 4 * part), (line, inside))
    w_qkvo, w_up, down_z, vec, normed, queries, keys, values, keys_other, values_other = gather_weights(
        shards, jnp.stack([query_weight, key_weight, value_weight, out_weight]), up_weight, down_weight, vec,
        layer_input.reshape(rows, model),
    )
    span, aug, block_bias, doc_bias = tables(segment[:, 0], rand_blocks[:, 0], side, half)

    cut = lambda array: array.reshape(micro, half, model)
    attended = (span, cut(queries), cut(keys), cut(values), cut(keys_other), cut(values_other),
                aug, block_bias, doc_bias)
    mixed, lse = attend_forward(*attended)
    mixed_rows = mixed.reshape(rows, model)
    tokens = layer_input.reshape(rows, model)
    result, grad_attn, grad_mixed, d_out, d_up, d_down, small = middle_layer(
        shards, mixed_rows, tokens, cotangent.reshape(rows, model), w_qkvo, w_up, down_weight, down_z, vec
    )
    grads = attend_backward(0, (), *attended, mixed, cut(grad_mixed), lse)
    grads = attend_backward(1, grads, *attended, mixed, cut(grad_mixed), lse)
    grads = [array.reshape(rows, model) for array in (grads[0], grads[1], grads[2], grads[3], grads[4])]
    g_qkvo, g_up, g_down, small, input_grad = final_layer(
        shards, quads, *grads, normed, tokens, grad_attn, w_qkvo,
        d_out.reshape(shards, 2, part // 2, model), d_up, d_down, vec, small,
    )
    g_qkvo, g_up, g_down = g_qkvo.astype(wide), g_up.astype(wide), g_down.astype(wide)
    flat = lax.dynamic_slice(small, (0, shard * part), (8, part))
    d_b_up = lax.dynamic_slice(small, (line, inside), (1, 4 * part)).reshape(4 * part)
    shape = layer_input.shape
    return (
        result.reshape(shape), input_grad.reshape(shape), flat[4], flat[5], g_qkvo[0], flat[6],
        g_qkvo[1], g_qkvo[2], flat[7], g_qkvo[3], flat[2], flat[0], flat[1], g_up, d_b_up, g_down, flat[3],
    )


def solution(mesh):
    row = P(None, ("rep", "fsdp"), "seq", None)
    flat, wide = P("fsdp"), P("fsdp", None)
    shards, quads = mesh.shape["fsdp"], mesh.shape["rep"] // 4
    assert mesh.shape["seq"] == 2 and mesh.shape["rep"] % 4 == 0
    return jax.shard_map(
        functools.partial(on_device, shards, quads),
        mesh=mesh,
        in_specs=(
            row, P(None, ("rep", "fsdp"), None), P(None, ("rep", "fsdp"), None, None, None),
            flat, flat, wide, flat, wide, wide, flat, wide, flat, flat, flat, wide, flat, wide, flat, row,
        ),
        out_specs=(row, row, flat, flat, wide, flat, wide, wide, flat, wide, flat, flat, flat, wide, flat, wide, flat),
        check_vma=False,
    )
```

```python
import functools
import jax
import jax.numpy as jnp
from jax import lax
from jax.experimental import pallas as pl
from jax.experimental.pallas import tpu as pltpu
from jax.sharding import PartitionSpec as P

norm_eps = 1e-05

HEADS = 12
HDIM = 64
BLOCK = 64
TQ = 256
TK = 256
NEG = -1e30


def nt(a, b):
    return lax.dot_general(a, b, (((1,), (1,)), ((), ())), preferred_element_type=jnp.float32)


def tn(a, b):
    return lax.dot_general(a, b, (((0,), (0,)), ((), ())), preferred_element_type=jnp.float32)


def nn(a, b):
    return jnp.dot(a, b, preferred_element_type=jnp.float32)


def head_lanes(head):
    lane = lax.broadcasted_iota(jnp.int32, (1, 128), 1)
    return (lane < HDIM) if head == 0 else (lane >= HDIM)


def bias_rows(block_ref, doc_ref, head):
    rows = [
        jnp.broadcast_to(block_ref[0, 0, head, pl.ds(b, 1), :], (BLOCK, 128)) for b in range(TQ // BLOCK)
    ]
    return (jnp.concatenate(rows, axis=0) + doc_ref[0]).astype(jnp.bfloat16)


def unite(whole, own_ref, other_ref, side):
    half = own_ref.shape[1]
    whole[pl.ds(pl.multiple_of(side * half, TK), half), :] = own_ref[0]
    whole[pl.ds(pl.multiple_of((1 - side) * half, TK), half), :] = other_ref[0]


def forward_body(
    span_ref, q_ref, ko_ref, vo_ref, kx_ref, vx_ref, aug_ref, block_ref, doc_ref,
    out_ref, lse_ref, acc_ref, qa_ref, k_all, v_all,
):
    micro, tile = pl.program_id(0), pl.program_id(1)

    @pl.when(tile == 0)
    def _():
        unite(k_all, ko_ref, kx_ref, span_ref[micro, tile, 2])
        unite(v_all, vo_ref, vx_ref, span_ref[micro, tile, 2])

    group = q_ref.shape[2] // HDIM
    for head in range(group):
        cols = pl.ds(head // 2 * 128, 128)
        q_rows = q_ref[0, :, cols].astype(jnp.float32) * 0.125
        masked = jnp.where(head_lanes(head % 2), q_rows, 0.0).astype(jnp.bfloat16)
        qa_ref[head, :, 0:128] = masked
        qa_ref[head, :, 128:256] = bias_rows(block_ref, doc_ref, head)
    acc_ref[...] = jnp.zeros_like(acc_ref)

    def step(j, carry):
        at = pl.ds(pl.multiple_of(j * TK, TK), TK)
        aug = aug_ref[0, at, :]
        scores = []
        for head in range(group):
            cols = pl.ds(head // 2 * 128, 128)
            scores.append(nt(jnp.concatenate([k_all[at, cols], aug], axis=1), qa_ref[head]))
        fresh = []
        probs = []
        for head in range(group):
            top_new = jnp.maximum(carry[head], jnp.max(scores[head], axis=0, keepdims=True))
            probs.append(jnp.exp(scores[head] - top_new).astype(jnp.bfloat16))
            fresh.append(top_new)
        for head in range(group):
            cols = pl.ds(head // 2 * 128, 128)
            v_rows = jnp.where(head_lanes(head % 2), v_all[at, cols], jnp.bfloat16(1.0))
            part = tn(v_rows, probs[head])
            acc_ref[head] = acc_ref[head] * jnp.exp(carry[head] - fresh[head]) + part
        return tuple(fresh)

    state = tuple(jnp.full((1, TQ), -3e38, jnp.float32) for _ in range(group))
    state = lax.fori_loop(span_ref[micro, tile, 0], span_ref[micro, tile, 1], step, state)
    for pair in range(group // 2):
        done = []
        for head in range(2):
            at = pair * 2 + head
            mass = acc_ref[at, pl.ds((1 - head) * HDIM, 1), :]
            done.append(acc_ref[at, pl.ds(head * HDIM, HDIM), :] / mass)
            lse_ref[0, pair, pl.ds(head, 1), :] = state[at] + jnp.log(mass)
        out_ref[0, :, pl.ds(pair * 128, 128)] = jnp.concatenate(done, axis=0).T.astype(out_ref.dtype)


def backward_body(
    span_ref, q_ref, ko_ref, vo_ref, kx_ref, vx_ref, aug_ref, block_ref, doc_ref,
    mixed_ref, grad_ref, lse_ref,
    dq_ref, dko_ref, dvo_ref, dkx_ref, dvx_ref,
    dqt_ref, qa_ref, gm_ref, k_acc, v_acc, k_all, v_all,
):
    micro, tile = pl.program_id(0), pl.program_id(1)
    side = span_ref[micro, tile, 2]

    @pl.when(tile == 0)
    def _():
        unite(k_all, ko_ref, kx_ref, side)
        unite(v_all, vo_ref, vx_ref, side)
        k_acc[...] = jnp.zeros_like(k_acc)
        v_acc[...] = jnp.zeros_like(v_acc)

    group = q_ref.shape[2] // HDIM
    inner = []
    for pair in range(group // 2):
        cols = pl.ds(pair * 128, 128)
        q_rows = q_ref[0, :, cols].astype(jnp.float32) * 0.125
        grad_rows = grad_ref[0, :, cols].astype(jnp.float32)
        both = (mixed_ref[0, :, cols].astype(jnp.float32) * grad_rows).T
        for half in range(2):
            head = pair * 2 + half
            qa_ref[head, :, 0:128] = jnp.where(head_lanes(half), q_rows, 0.0).astype(jnp.bfloat16)
            qa_ref[head, :, 128:256] = bias_rows(block_ref, doc_ref, head)
            gm_ref[head] = jnp.where(head_lanes(half), grad_rows, 0.0).astype(jnp.bfloat16)
            inner.append(jnp.sum(both[half * HDIM:(half + 1) * HDIM, :], axis=0, keepdims=True))
    dqt_ref[...] = jnp.zeros_like(dqt_ref)

    def step(j, carry):
        at = pl.ds(pl.multiple_of(j * TK, TK), TK)
        aug = aug_ref[0, at, :]
        for chunk in range(0, group, CHUNK):
            heads = range(chunk, min(chunk + CHUNK, group))
            scores, grads, probs, souls = {}, {}, {}, {}
            for head in heads:
                cols = pl.ds(head // 2 * 128, 128)
                scores[head] = nt(jnp.concatenate([k_all[at, cols], aug], axis=1), qa_ref[head])
                grads[head] = nt(v_all[at, cols], gm_ref[head])
            for head in heads:
                weight = jnp.exp(scores[head] - lse_ref[0, head // 2, pl.ds(head % 2, 1), :])
                souls[head] = (weight * (grads[head] - carry[head])).astype(jnp.bfloat16)
                probs[head] = weight.astype(jnp.bfloat16)
            for head in heads:
                cols = pl.ds(head // 2 * 128, 128)
                dv = nn(probs[head], gm_ref[head])
                dk = nn(souls[head], qa_ref[head, :, 0:128])
                dqt = tn(k_all[at, cols], souls[head])
                lanes = pl.ds(head * HDIM, HDIM)
                half = head % 2
                dqt_ref[lanes, :] += dqt[half * HDIM:(half + 1) * HDIM, :]
                if half == 0:
                    dv_low, dk_low = dv, dk
                else:
                    k_acc[at, cols] += dk + dk_low
                    v_acc[at, cols] += dv + dv_low
        return carry

    lax.fori_loop(span_ref[micro, tile, 0], span_ref[micro, tile, 1], step, tuple(inner))
    for pair in range(group // 2):
        cols = pl.ds(pair * 128, 128)
        dq_ref[0, :, cols] = (dqt_ref[cols, :] * 0.125).T.astype(dq_ref.dtype)

    @pl.when(tile == pl.num_programs(1) - 1)
    def _():
        size = dko_ref.shape[1]
        mine = pl.ds(pl.multiple_of(side * size, TK), size)
        theirs = pl.ds(pl.multiple_of((1 - side) * size, TK), size)
        dko_ref[0] = k_acc[mine, :].astype(dko_ref.dtype)
        dvo_ref[0] = v_acc[mine, :].astype(dvo_ref.dtype)
        dkx_ref[0] = k_acc[theirs, :].astype(dkx_ref.dtype)
        dvx_ref[0] = v_acc[theirs, :].astype(dvx_ref.dtype)


CHUNK = 4


def specs(half, length, width, at):
    rows = pl.BlockSpec((1, TQ, width), lambda *i: at(*i) + (0,))
    side = pl.BlockSpec((1, half, width), lambda *i: (at(*i)[0], 0, 0))
    aug = pl.BlockSpec((1, length, 128), lambda *i: (at(*i)[0], 0, 0))
    block = pl.BlockSpec((1, 1, HEADS, TQ // BLOCK, 128), lambda *i: at(*i) + (0, 0, 0))
    doc = pl.BlockSpec((1, TQ, 128), lambda *i: at(*i) + (0,))
    lse = pl.BlockSpec((1, HEADS // 2, 2, TQ), lambda *i: (at(*i)[0], 0, 0, at(*i)[1]))
    return rows, side, aug, block, doc, lse


def attend_forward(span, q, ko, vo, kx, vx, aug, block, doc):
    micro, half, width = q.shape
    length = aug.shape[1]
    rows, side, aug_spec, blk, doc_spec, lse = specs(half, length, width, lambda m, t, s: (m, t))
    return pl.pallas_call(
        forward_body,
        name="attend_forward",
        out_shape=(
            jax.ShapeDtypeStruct((micro, half, width), jnp.bfloat16),
            jax.ShapeDtypeStruct((micro, HEADS // 2, 2, half), jnp.float32),
        ),
        grid_spec=pltpu.PrefetchScalarGridSpec(
            num_scalar_prefetch=1,
            grid=(micro, half // TQ),
            in_specs=[rows] + [side] * 4 + [aug_spec, blk, doc_spec],
            out_specs=(rows, lse),
            scratch_shapes=[
                pltpu.VMEM((HEADS, 128, TQ), jnp.float32),
                pltpu.VMEM((HEADS, TQ, 256), jnp.bfloat16),
                pltpu.VMEM((length, width), jnp.bfloat16),
                pltpu.VMEM((length, width), jnp.bfloat16),
            ],
        ),
        cost_estimate=pl.CostEstimate(flops=20_000_000_000, bytes_accessed=20_000_000, transcendentals=0),
    )(span, q, ko, vo, kx, vx, aug, block, doc)


def attend_backward(span, q, ko, vo, kx, vx, aug, block, doc, mixed, grad, lse):
    micro, half, width = q.shape
    length = aug.shape[1]
    rows, side, aug_spec, blk, doc_spec, lse_spec = specs(half, length, width, lambda m, t, s: (m, t))
    shape = jax.ShapeDtypeStruct((micro, half, width), jnp.bfloat16)
    return pl.pallas_call(
        backward_body,
        name="attend_backward",
        out_shape=(shape,) * 5,
        grid_spec=pltpu.PrefetchScalarGridSpec(
            num_scalar_prefetch=1,
            grid=(micro, half // TQ),
            in_specs=[rows] + [side] * 4 + [aug_spec, blk, doc_spec, rows, rows, lse_spec],
            out_specs=(rows,) + (side,) * 4,
            scratch_shapes=[
                pltpu.VMEM((width, TQ), jnp.float32),
                pltpu.VMEM((HEADS, TQ, 256), jnp.bfloat16),
                pltpu.VMEM((HEADS, TQ, 128), jnp.bfloat16),
                pltpu.VMEM((length, width), jnp.float32),
                pltpu.VMEM((length, width), jnp.float32),
                pltpu.VMEM((length, width), jnp.bfloat16),
                pltpu.VMEM((length, width), jnp.bfloat16),
            ],
        ),
        cost_estimate=pl.CostEstimate(flops=20_000_000_000, bytes_accessed=20_000_000, transcendentals=0),
    )(span, q, ko, vo, kx, vx, aug, block, doc, mixed, grad, lse)


def tables(segment, rand_blocks, side, half):
    micro, length = segment.shape
    blocks = length // BLOCK
    mine = half // BLOCK
    tiles = half // TQ
    lane = lax.broadcasted_iota(jnp.int32, (1, 1, 128), 2)
    own = lax.dynamic_slice_in_dim(segment, side * half, half, axis=1)
    place = lax.broadcasted_iota(jnp.int32, (1, length, 1), 1) // BLOCK
    aug = ((lane == place) | (lane == segment[:, :, None] + blocks)).astype(jnp.bfloat16)
    doc = jnp.where((lane >= blocks) & (lane < blocks + 4) & (lane != own[:, :, None] + blocks), NEG, 0.0)
    q_block = side * mine + lax.broadcasted_iota(jnp.int32, (1, 1, mine, 1), 2)
    k_block = lax.broadcasted_iota(jnp.int32, (1, 1, 1, 128), 3)
    chosen = lax.dynamic_slice_in_dim(rand_blocks, side * mine, mine, axis=2)
    allowed = (jnp.abs(q_block - k_block) <= 1) | (k_block == 0) | (k_block == blocks - 1)
    allowed = allowed | (q_block == 0) | (q_block == blocks - 1) | (k_block >= blocks)
    for pick in range(rand_blocks.shape[3]):
        allowed = allowed | (chosen[:, :, :, pick:pick + 1] == k_block)
    block = jnp.where(allowed, 0.0, NEG).astype(jnp.float32)
    block = jnp.moveaxis(block.reshape(micro, HEADS, tiles, mine // tiles, 128), 2, 1)
    edges = own.reshape(micro, tiles, TQ)
    first, last = edges[:, :, :1], edges[:, :, TQ - 1:]
    begin = jnp.sum((segment[:, None, :] < first).astype(jnp.int32), axis=-1)
    end = jnp.sum((segment[:, None, :] <= last).astype(jnp.int32), axis=-1)
    span = jnp.stack([begin // TK, (end + TK - 1) // TK, jnp.full_like(begin, side)], axis=-1)
    return span, aug, block, doc.astype(jnp.float32)


MESH = pl.DeviceIdType.MESH
GROUPS = 3


def place():
    rep, shard, side = lax.axis_index("rep"), lax.axis_index("fsdp"), lax.axis_index("seq")
    quad = lax.rem(rep, 4)
    across, along = lax.rem(quad, 2), quad // 2
    near = (1 - 2 * across, 2 - 4 * along)
    return rep, shard, side, quad, near


def chunk(refs, group, shard, quad, side, rows, half=None):
    width = 768 if half is None else 384
    offset = 0 if half is None else half * 384
    low = side * rows
    if group == 0:
        return refs[0].at[quad, pl.ds(pl.multiple_of(shard * (2 * rows) + low, 16), rows), pl.ds(offset, width)]
    at = pl.multiple_of(shard * (2 * rows) + low, 16)
    return refs[1].at[pl.ds(at, rows), pl.ds(pl.multiple_of(quad * 768 + offset, 128), width)]


def greet(peers):
    barrier = pltpu.get_barrier_semaphore()
    for peer in peers:
        pl.semaphore_signal(barrier, inc=1, device_id=peer, device_id_type=MESH)
    pl.semaphore_wait(barrier, len(peers))


def remote(src, dst, send, recv, peer):
    return pltpu.make_async_remote_copy(
        src_ref=src, dst_ref=dst, send_sem=send, recv_sem=recv, device_id=peer, device_id_type=MESH
    )


def gather_body(
    shards, rows, qkvo_in, up_in, down_in, vec_in, x_in,
    qkvo_out, up_out, down_out, vec_out, normed_out, q_out, k_out, v_out, kx_out, vx_out,
    qkvo_stage, up_stage, vec_all, weights, normed, results,
    in_sem, out_sem, z_send, z_recv, x_send, x_recv, y_send, y_recv, d_send, d_recv, c_send, c_recv,
    load_sem, save_sem, swap_send, swap_recv,
):
    rep, shard, side, quad, (dx, dy) = place()
    ins, outs = (qkvo_in, up_in), (qkvo_out, up_out)
    stages = (qkvo_stage, up_stage)
    x_peer, y_peer, partner = (rep + dx, shard, side), (rep + dy, shard, side), (rep, shard, 1 - side)
    z_peers = [(rep, lax.rem(shard + k, shards), side) for k in range(1, shards)]
    for i, src in enumerate(ins):
        pltpu.make_async_copy(src, stages[i], in_sem.at[i]).start()
    greet(z_peers + [x_peer, y_peer, partner])
    sent = []

    def go(copy):
        copy.start()
        sent.append(copy)

    for g in range(EARLY):
        for k in range(1, shards):
            go(remote(
                chunk(ins, g, 0, quad, side, rows), chunk(outs, g, shard, quad, side, rows),
                z_send.at[g, k - 1], z_recv.at[g, shards - k - 1], z_peers[k - 1],
            ))
        if g == 0:
            for k in range(1, shards):
                go(remote(
                    vec_in, vec_all.at[k - 1],
                    z_send.at[EARLY, k - 1], z_recv.at[EARLY, k - 1], z_peers[k - 1],
                ))
    for k in range(1, shards):
        go(remote(
            down_in.at[pl.ds(pl.multiple_of((quad * 2 + side) * rows, 16), rows), :], down_out.at[shard],
            z_send.at[EARLY + 1, k - 1], z_recv.at[EARLY + 1, shards - k - 1], z_peers[k - 1],
        ))
    owned = (
        qkvo_out.at[:, pl.ds(pl.multiple_of(shard * 2 * rows, 16), 2 * rows), :],
        up_out.at[pl.ds(pl.multiple_of(shard * 2 * rows, 16), 2 * rows), :],
    )
    local = []
    for i, src in enumerate(ins):
        pltpu.make_async_copy(src, stages[i], in_sem.at[i]).wait()
        copy = pltpu.make_async_copy(stages[i], owned[i], out_sem.at[i])
        copy.start()
        local.append(copy)

    def piece(g, k, member, core, half=None):
        return chunk(outs, g, lax.rem(shard + k, shards), member, core, rows, half)

    def hop(g, k, member, core, send, recv, peer, half=None):
        ref = piece(g, k, member, core, half)
        return remote(ref, ref, send, recv, peer)

    x_quad, y_quad, d_quad = quad + dx, quad + dy, quad + dx + dy

    def straight(g):
        for k in range(1, shards):
            hop(g, k, quad, side, z_send.at[g, k - 1], z_recv.at[g, k - 1], z_peers[k - 1]).wait_recv()
            go(hop(g, k, quad, side, x_send.at[g, k - 1], x_recv.at[g, k - 1], x_peer))
            go(hop(g, k, quad, side, y_send.at[g, k - 1], y_recv.at[g, k - 1], y_peer))
            go(hop(g, k, quad, side, c_send.at[g, k - 1, 0], c_recv.at[g, k - 1, 0], partner))

    def turn(g):
        for k in range(1, shards):
            hop(g, k, x_quad, side, x_send.at[g, k - 1], x_recv.at[g, k - 1], x_peer).wait_recv()
            go(hop(g, k, x_quad, side, d_send.at[g, k - 1, 1], d_recv.at[g, k - 1, 1], y_peer, 1))
            go(hop(g, k, x_quad, side, c_send.at[g, k - 1, 1], c_recv.at[g, k - 1, 1], partner))
            hop(g, k, y_quad, side, y_send.at[g, k - 1], y_recv.at[g, k - 1], y_peer).wait_recv()
            go(hop(g, k, y_quad, side, d_send.at[g, k - 1, 0], d_recv.at[g, k - 1, 0], x_peer, 0))
            go(hop(g, k, y_quad, side, c_send.at[g, k - 1, 2], c_recv.at[g, k - 1, 2], partner))

    def corner(g):
        for k in range(1, shards):
            hop(g, k, d_quad, side, d_send.at[g, k - 1, 0], d_recv.at[g, k - 1, 0], x_peer, 0).wait_recv()
            hop(g, k, d_quad, side, d_send.at[g, k - 1, 1], d_recv.at[g, k - 1, 1], y_peer, 1).wait_recv()
            go(hop(g, k, d_quad, side, c_send.at[g, k - 1, 3], c_recv.at[g, k - 1, 3], partner))

    def gathered(g):
        for k in range(1, shards):
            for i, member in enumerate((quad, x_quad, y_quad, d_quad)):
                hop(g, k, member, 1 - side, c_send.at[g, k - 1, i], c_recv.at[g, k - 1, i], partner).wait_recv()

    def save(i, target):
        copy = pltpu.make_async_copy(normed if i == 3 else results.at[i], target, save_sem.at[i])
        copy.start()
        local.append(copy)

    def norm(step, carry):
        at = pl.ds(pl.multiple_of(step * STEP, STEP), STEP)
        values = x_in[at, :].astype(jnp.float32)
        centre = values - jnp.mean(values, axis=-1, keepdims=True)
        scale = lax.rsqrt(jnp.mean(centre * centre, axis=-1, keepdims=True) + norm_eps)
        normed[at, :] = (centre * scale * vec_out[0:1, :] + vec_out[1:2, :]).astype(normed.dtype)
        return carry

    def project(i, row):
        pltpu.make_async_copy(qkvo_out.at[i], weights.at[i], load_sem.at[i]).wait()

        def step(j, carry):
            at = pl.ds(pl.multiple_of(j * STEP, STEP), STEP)
            product = nn(normed[at, :], weights[i])
            if row is not None:
                product = product + vec_out[row:row + 1, :]
            results[i, at, :] = product.astype(results.dtype)
            return carry
        lax.fori_loop(0, normed.shape[0] // STEP, step, 0)

    def exchange(i, target):
        copy = remote(results.at[i], target, swap_send.at[i - 1], swap_recv.at[i - 1], partner)
        copy.start()
        return copy

    straight(0)
    for k in range(1, shards):
        remote(
            vec_in, vec_all.at[k - 1], z_send.at[EARLY, k - 1], z_recv.at[EARLY, k - 1], z_peers[k - 1]
        ).wait_recv()
    total = vec_in[...].astype(jnp.float32)
    for k in range(1, shards):
        total = total + vec_all[k - 1].astype(jnp.float32)
    vec_out[...] = total
    lax.fori_loop(0, normed.shape[0] // STEP // 2, norm, 0)
    turn(0)
    lax.fori_loop(normed.shape[0] // STEP // 2, normed.shape[0] // STEP, norm, 0)
    save(3, normed_out)
    straight(1)
    corner(0)
    local[0].wait()
    gathered(0)
    for i in (1, 2, 0):
        pltpu.make_async_copy(qkvo_out.at[i], weights.at[i], load_sem.at[i]).start()
    project(1, None)
    keys = exchange(1, kx_out)
    save(1, k_out)
    turn(1)
    project(2, 3)
    values = exchange(2, vx_out)
    save(2, v_out)
    corner(1)
    project(0, 2)
    save(0, q_out)
    gathered(1)
    for k in range(1, shards):
        remote(
            down_out.at[shard], down_out.at[lax.rem(shard + k, shards)],
            z_send.at[EARLY + 1, k - 1], z_recv.at[EARLY + 1, k - 1], z_peers[k - 1],
        ).wait_recv()
    keys.wait()
    values.wait()
    for copy in sent:
        copy.wait_send()
    for copy in local[1:]:
        copy.wait()


STEP = 256
EARLY = 2
WIDE = 512


def gather_weights(shards, qkvo, up, down, vec, x):
    rows = qkvo.shape[1] // 2
    model = qkvo.shape[2]
    hidden = up.shape[1]
    any_space = pl.BlockSpec(memory_space=pl.ANY)
    vmem_space = pl.BlockSpec(memory_space=pltpu.VMEM)
    dma = pltpu.SemaphoreType.DMA
    low = jnp.bfloat16
    token = jax.ShapeDtypeStruct(x.shape, low)
    return pl.pallas_call(
        functools.partial(gather_body, shards, rows),
        name="gather_weights",
        out_shape=(
            jax.ShapeDtypeStruct((4, model, model), low),
            jax.ShapeDtypeStruct((model, hidden), low),
            jax.ShapeDtypeStruct((shards, rows, model), low),
            jax.ShapeDtypeStruct(vec.shape, jnp.float32),
        )
        + (token,) * 6,
        in_specs=[any_space] * 3 + [vmem_space] * 2,
        out_specs=(any_space,) * 3 + (vmem_space,) + (any_space,) * 6,
        scratch_shapes=[
            pltpu.VMEM(qkvo.shape, low), pltpu.VMEM(up.shape, low),
            pltpu.VMEM((shards - 1,) + vec.shape, low),
            pltpu.VMEM((3, model, model), low),
            pltpu.VMEM(x.shape, low),
            pltpu.VMEM((3,) + x.shape, low),
            dma((2,)), dma((2,)),
            dma((EARLY + 2, shards - 1)), dma((EARLY + 2, shards - 1)),
        ]
        + [dma((EARLY, shards - 1))] * 4
        + [dma((EARLY, shards - 1, 2))] * 2
        + [dma((EARLY, shards - 1, 4))] * 2
        + [dma((3,)), dma((4,)), dma((2,)), dma((2,))],
        compiler_params=pltpu.CompilerParams(
            collective_id=0, has_side_effects=True, vmem_limit_bytes=50_000_000
        ),
    )(qkvo, up, down, vec, x)


def add_into(out_ref, refs):
    total = refs[0][...].astype(jnp.float32)
    for ref in refs[1:]:
        total = total + ref[...].astype(jnp.float32)
    out_ref[...] = total.astype(out_ref.dtype)


def normal_parts(values):
    phi = 0.5 + 0.5 * lax.erf(values * 0.7071067811865476)
    return phi, values * (jnp.exp(-0.5 * values * values) * 0.3989422804014327)


def middle_body(
    shards, rows,
    mixed_in, x_in, grad_in, qkvo_in, up_w_in, down_w_in, down_z_in, vec_in,
    result_out, attn_out, mixed_out, d_out_out, up_out, down_out, sums_out,
    mixed, x, grad, out_w, up_w, down_w, middle, normed, turned, hidden, slope,
    up_grad, down_grad, up_mate, down_mate, up_first, down_first, down_second,
    load_sem, save_sem, uc_send, uc_recv, dc_send, dc_recv, f_send, f_recv, s_send, s_recv,
    x_send, x_recv, y_send, y_recv, d_send, d_recv, g_send, g_recv,
):
    rep, shard, side, quad, (dx, dy) = place()
    partner = (rep, shard, 1 - side)
    low, wide = jnp.bfloat16, jnp.float32
    steps = x.shape[0] // WIDE
    model = x.shape[1]
    width = 8 * rows
    loads = [
        pltpu.make_async_copy(src, dst, load_sem.at[i])
        for i, (src, dst) in enumerate(((mixed_in, mixed), (x_in, x), (qkvo_in.at[3], out_w), (grad_in, grad)))
    ]
    for f in range(shards):
        at = pl.ds(f * width, width)
        loads.append(pltpu.make_async_copy(up_w_in.at[:, at], up_w.at[f], load_sem.at[4 + f]))
    loads.append(pltpu.make_async_copy(down_w_in, down_w.at[shard], load_sem.at[4 + shards]))
    for k in range(1, shards):
        f = lax.rem(shard + k, shards)
        at = pl.ds(pl.multiple_of((quad * 2 + side) * rows, 16), rows)
        loads.append(pltpu.make_async_copy(down_z_in.at[f], down_w.at[f, at, :], load_sem.at[4 + shards + k]))
    for load in loads:
        load.start()
    x_peer, y_peer = (rep + dx, shard, side), (rep + dy, shard, side)
    x_quad, y_quad, d_quad = quad + dx, quad + dy, quad + dx + dy
    greet([x_peer, y_peer, partner])

    def piece(f, member, core, half=None):
        at = pl.ds(pl.multiple_of((member * 2 + core) * rows, 16), rows)
        if half is None:
            return down_w.at[f, at, :]
        return down_w.at[f, at, pl.ds(half * (model // 2), model // 2)]

    def hop(k, member, core, send, recv, peer, half=None):
        ref = piece(lax.rem(shard + k, shards), member, core, half)
        return remote(ref, ref, send, recv, peer)

    def own_piece(k, send, recv, peer):
        f = lax.rem(shard + k, shards)
        return remote(down_z_in.at[f], piece(f, quad, side), send, recv, peer)

    def straight(k):
        return (
            own_piece(k, x_send.at[k - 1], x_recv.at[k - 1], x_peer),
            own_piece(k, y_send.at[k - 1], y_recv.at[k - 1], y_peer),
            own_piece(k, g_send.at[k - 1, 0], g_recv.at[k - 1, 0], partner),
        )

    def turn():
        for k in range(1, shards):
            hop(k, x_quad, side, x_send.at[k - 1], x_recv.at[k - 1], x_peer).wait_recv()
            hop(k, x_quad, side, d_send.at[k - 1, 1], d_recv.at[k - 1, 1], y_peer, 1).start()
            hop(k, x_quad, side, g_send.at[k - 1, 1], g_recv.at[k - 1, 1], partner).start()
            hop(k, y_quad, side, y_send.at[k - 1], y_recv.at[k - 1], y_peer).wait_recv()
            hop(k, y_quad, side, d_send.at[k - 1, 0], d_recv.at[k - 1, 0], x_peer, 0).start()
            hop(k, y_quad, side, g_send.at[k - 1, 2], g_recv.at[k - 1, 2], partner).start()

    def corner():
        for k in range(1, shards):
            hop(k, d_quad, side, d_send.at[k - 1, 0], d_recv.at[k - 1, 0], x_peer, 0).wait_recv()
            hop(k, d_quad, side, d_send.at[k - 1, 1], d_recv.at[k - 1, 1], y_peer, 1).wait_recv()
            hop(k, d_quad, side, g_send.at[k - 1, 3], g_recv.at[k - 1, 3], partner).start()

    def gathered():
        for k in range(1, shards):
            for i, member in enumerate((quad, x_quad, y_quad, d_quad)):
                hop(k, member, 1 - side, g_send.at[k - 1, i], g_recv.at[k - 1, i], partner).wait_recv()

    def flushed():
        for k in range(1, shards):
            for copy in straight(k):
                copy.wait_send()
            hop(k, y_quad, side, d_send.at[k - 1, 0], d_recv.at[k - 1, 0], x_peer, 0).wait_send()
            hop(k, x_quad, side, d_send.at[k - 1, 1], d_recv.at[k - 1, 1], y_peer, 1).wait_send()
            for i in range(1, 4):
                hop(k, quad, side, g_send.at[k - 1, i], g_recv.at[k - 1, i], partner).wait_send()

    for k in range(1, shards):
        for copy in straight(k):
            copy.start()
    firsts = (up_first, down_first)

    def row(i):
        return vec_in[i:i + 1, :]

    def block(j):
        return pl.ds(pl.multiple_of(j * WIDE, WIDE), WIDE)

    def part(g, f, m):
        return up_grad.at[m, f, side] if g == 0 else down_grad.at[f, side, m]

    def mate(g, f, m):
        return up_mate.at[m, f] if g == 0 else down_mate.at[f, m]

    def flip_way(f, second):
        odd = lax.rem(f + second, 2)
        return dx + odd * (dy - dx)

    def up_cross(m):
        return remote(up_grad.at[m, :, 1 - side], up_mate.at[m], uc_send.at[m], uc_recv.at[m], partner)

    def down_cross(f):
        return remote(down_grad.at[f, 1 - side], down_mate.at[f], dc_send.at[f], dc_recv.at[f], partner)

    def f_copy(g, f, slot):
        way = flip_way(f, 0)
        member = quad + way if slot == 0 else quad + dx + dy
        return remote(part(g, f, member), firsts[g].at[f, slot], f_send.at[g, f, slot], f_recv.at[g, f, slot], (rep + way, shard, side))

    def s_copy(f):
        way = flip_way(f, 1)
        return remote(part(1, f, quad + way), down_second.at[f], s_send.at[f], s_recv.at[f], (rep + way, shard, side))

    def first_go(g, f, m):
        @pl.when(m == quad + dx + dy)
        def _():
            f_copy(g, f, 1).start()

        @pl.when(m == quad + flip_way(f, 0))
        def _():
            f_copy(g, f, 0).start()

    def down_merge(f):
        down_cross(f).wait_recv()
        for m in range(4):
            add_into(part(1, f, m), (part(1, f, m), mate(1, f, m)))
            first_go(1, f, m)

    def up_merge(m):
        up_cross(m).wait_recv()

        def step(f, carry):
            add_into(part(0, f, m), (part(0, f, m), mate(0, f, m)))
            first_go(0, f, m)
            return carry
        lax.fori_loop(0, shards, step, 0)

    def each(body):
        def step(f, carry):
            body(f)
            return carry
        lax.fori_loop(0, shards, step, 0)

    def down_fold(f):
        for slot in range(2):
            f_copy(1, f, slot).wait()
            member = quad if slot == 0 else quad + flip_way(f, 1)
            add_into(part(1, f, member), (part(1, f, member), down_first.at[f, slot]))
        s_copy(f).start()

    def down_settle(f):
        s_copy(f).wait()
        add_into(down_out.at[f], (part(1, f, quad), down_second.at[f]))

    def up_fold(f):
        for slot in range(2):
            f_copy(0, f, slot).wait()
            member = quad if slot == 0 else quad + flip_way(f, 1)
            add_into(up_out.at[slot, f], (part(0, f, member), up_first.at[f, slot]))

    saves = []

    def save(src, dst):
        copy = pltpu.make_async_copy(src, dst, save_sem.at[len(saves)])
        copy.start()
        saves.append(copy)

    for load in loads[:3]:
        load.wait()

    def attend_out(j, carry):
        at = block(j)
        values = x[at, :].astype(wide) + nn(mixed[at, :], out_w[...]) + row(4)
        middle[at, :] = values
        centre = values - jnp.mean(values, axis=-1, keepdims=True)
        scale = lax.rsqrt(jnp.mean(centre * centre, axis=-1, keepdims=True) + norm_eps)
        out = centre * scale * row(5) + row(6)
        normed[at, :] = out.astype(low)
        turned[:, at] = out.T.astype(low)
        return carry
    lax.fori_loop(0, steps, attend_out, 0)
    for load in loads[3:]:
        load.wait()

    def bias_at(f):
        first = f * width
        return pl.ds(8 + first // model, 1), pl.ds(pl.multiple_of(lax.rem(first, model), 128), width)

    def expand(f):
        bias = vec_in[bias_at(f)]

        def step(j, carry):
            at = block(j)
            inner = nn(normed[at, :], up_w[f]) + bias
            phi, bump = normal_parts(inner)
            hidden[f, at, :] = (inner * phi).astype(low)
            slope[f, at, :] = (phi + bump).astype(low)
            return carry
        lax.fori_loop(0, steps, step, 0)
        down_grad[f] = tn(hidden[f], grad[...]).astype(low).reshape(2, 4, rows, model)
        down_cross(f).start()

        @pl.when(f > 0)
        def _():
            down_merge(f - 1)

        @pl.when(f == 0)
        def _():
            turn()

        @pl.when(f == 1)
        def _():
            corner()
    each(expand)
    gathered()

    def contract(m):
        for h in range(model // width):
            f = m * (model // width) + h

            def step(j, total, f=f):
                at = block(j)
                value = (nt(grad[at, :], down_w[f]) * slope[f, at, :].astype(wide)).astype(low)
                slope[f, at, :] = value
                return total + jnp.sum(value.astype(wide), axis=0, keepdims=True)
            sums_out[bias_at(f)] = lax.fori_loop(0, steps, step, jnp.zeros((1, width), wide))
            product = nn(turned[...], slope[f]).astype(low)
            up_grad[m, :, :, :, pl.ds(h * width, width)] = product.reshape(shards, 2, rows, width)
        up_cross(m).start()

        @pl.when(m == 0)
        def _():
            down_merge(shards - 1)

        @pl.when(m > 0)
        def _():
            up_merge(m - 1)

    def contract_step(m, carry):
        contract(m)
        return carry
    lax.fori_loop(0, 4, contract_step, 0)
    up_merge(3)
    each(down_fold)

    def finish(j, carry):
        at = block(j)
        total = middle[at, :] + row(7)
        for f in range(shards):
            total = total + nn(hidden[f, at, :], down_w[f])
        x[at, :] = total.astype(low)
        return carry
    lax.fori_loop(0, steps, finish, 0)
    save(x, result_out)

    def back(j, carry):
        gain_sum, bias_sum, attn_sum, grad_sum = carry
        at = block(j)
        error = nt(slope[0, at, :], up_w[0])
        for f in range(1, shards):
            error = error + nt(slope[f, at, :], up_w[f])
        values = middle[at, :]
        centre = values - jnp.mean(values, axis=-1, keepdims=True)
        scale = lax.rsqrt(jnp.mean(centre * centre, axis=-1, keepdims=True) + norm_eps)
        unit = centre * scale
        scaled = error * row(5)
        mean_one = jnp.mean(scaled, axis=-1, keepdims=True)
        mean_two = jnp.mean(scaled * unit, axis=-1, keepdims=True)
        upstream = grad[at, :].astype(wide)
        attn = (upstream + scale * (scaled - mean_one - unit * mean_two)).astype(low)
        grad[at, :] = attn
        normed[at, :] = nt(attn, out_w[...]).astype(low)
        column = lambda array: jnp.sum(array, axis=0, keepdims=True)
        return (
            gain_sum + column(error * unit), bias_sum + column(error),
            attn_sum + column(attn.astype(wide)), grad_sum + column(upstream),
        )
    zero = jnp.zeros((1, model), wide)
    sums = lax.fori_loop(0, steps, back, (zero,) * 4)
    save(normed, mixed_out)
    save(grad, attn_out)
    for i, value in enumerate(sums):
        sums_out[i:i + 1, :] = value
    sums_out[4:8, :] = jnp.zeros((4, model), wide)
    sums_out[12:16, :] = jnp.zeros((4, model), wide)
    each(down_settle)
    out_w[...] = tn(mixed[...], grad[...]).astype(low)
    save(out_w, d_out_out)
    each(up_fold)
    for m in range(4):
        up_cross(m).wait_send()
    each(lambda f: down_cross(f).wait_send())
    flushed()
    for copy in saves:
        copy.wait()


def middle_layer(shards, mixed, x, grad, qkvo, up_w, down_w, down_z, vec):
    tokens, model = x.shape
    hidden = up_w.shape[1]
    rows = model // shards // 2
    width = 8 * rows
    any_space = pl.BlockSpec(memory_space=pl.ANY)
    vmem_space = pl.BlockSpec(memory_space=pltpu.VMEM)
    dma = pltpu.SemaphoreType.DMA
    low, wide = jnp.bfloat16, jnp.float32
    token = jax.ShapeDtypeStruct((tokens, model), low)
    flat = pltpu.VMEM((tokens, model), low)
    return pl.pallas_call(
        functools.partial(middle_body, shards, rows),
        name="middle_layer",
        out_shape=(
            token, token, token,
            jax.ShapeDtypeStruct((model, model), low),
            jax.ShapeDtypeStruct((2, shards, rows, model), low),
            jax.ShapeDtypeStruct((shards, rows, model), low),
            jax.ShapeDtypeStruct((16, model), wide),
        ),
        in_specs=[any_space] * 7 + [vmem_space],
        out_specs=(any_space,) * 4 + (vmem_space,) * 3,
        scratch_shapes=[
            flat, flat, flat,
            pltpu.VMEM((model, model), low),
            pltpu.VMEM((shards, model, width), low),
            pltpu.VMEM((shards, width, model), low),
            pltpu.VMEM((tokens, model), wide),
            flat,
            pltpu.VMEM((model, tokens), low),
            pltpu.VMEM((shards, tokens, width), low),
            pltpu.VMEM((shards, tokens, width), low),
            pltpu.VMEM((4, shards, 2, rows, model), low),
            pltpu.VMEM((shards, 2, 4, rows, model), low),
            pltpu.VMEM((4, shards, rows, model), low),
            pltpu.VMEM((shards, 4, rows, model), low),
            pltpu.VMEM((shards, 2, rows, model), low),
            pltpu.VMEM((shards, 2, rows, model), low),
            pltpu.VMEM((shards, rows, model), low),
            dma((4 + 2 * shards,)), dma((4,)),
            dma((4,)), dma((4,)), dma((shards,)), dma((shards,)),
            dma((2, shards, 2)), dma((2, shards, 2)), dma((shards,)), dma((shards,)),
        ]
        + [dma((shards - 1,))] * 4
        + [dma((shards - 1, 2))] * 2
        + [dma((shards - 1, 4))] * 2,
        compiler_params=pltpu.CompilerParams(
            collective_id=2, has_side_effects=True, vmem_limit_bytes=66_000_000
        ),
    )(mixed, x, grad, qkvo, up_w, down_w, down_z, vec)


def final_body(
    shards, quads, rows,
    dq_in, dk_in, dv_in, dkx_in, dvx_in, normed_in, x_in, attn_in, w_in, d_out_in, up_in, down_in, vec_in, small_in,
    qkvo_out, up_out, down_out, vec_out, input_out,
    dq, dk, dv, dkx, dvx, normed, turned, x, attn, weights, grads, mate, first, second, up_sum, up_second,
    last, last_up, last_down, ring, ring_up, ring_down, full, full_up, full_down, vec_sum, vec_mate, vec_ring,
    load_sem, save_sem, w_send, w_recv, c_send, c_recv, f_send, f_recv, s_send, s_recv, z_send, z_recv, q_send, q_recv, u_send, u_recv,
    x_send, x_recv, y_send, y_recv, d_send, d_recv, g_send, g_recv, out_sem, v_send, v_recv,
):
    rep, shard, side, quad, (dx, dy) = place()
    low, wide = jnp.bfloat16, jnp.float32
    steps = x.shape[0] // STEP
    model = x.shape[1]
    x_peer, y_peer, partner = (rep + dx, shard, side), (rep + dy, shard, side), (rep, shard, 1 - side)
    x_quad, y_quad, d_quad = quad + dx, quad + dy, quad + dx + dy
    z_peers = [(rep, lax.rem(shard + k, shards), side) for k in range(1, shards)]
    q_peers = [(lax.rem(rep + 4 * k, 4 * quads), shard, side) for k in range(1, quads)]
    loads = [
        pltpu.make_async_copy(src, dst, load_sem.at[i])
        for i, (src, dst) in enumerate((
            (normed_in, normed), (dq_in, dq), (d_out_in, grads.at[3]), (dk_in, dk), (dv_in, dv),
            (w_in.at[0], weights.at[0]), (w_in.at[1], weights.at[1]), (w_in.at[2], weights.at[2]),
            (x_in, x), (attn_in, attn),
        ))
    ]
    for load in loads:
        load.start()
    greet(z_peers + q_peers + [x_peer, y_peer, partner])
    swaps = [
        remote(src, dst, w_send.at[i], w_recv.at[i], partner)
        for i, (src, dst) in enumerate(((dkx_in, dkx), (dvx_in, dvx)))
    ]
    for swap in swaps:
        swap.start()
    fulls, lasts, rings = (full, full_up, full_down), (last, last_up, last_down), (ring, ring_up, ring_down)

    def block(j):
        return pl.ds(pl.multiple_of(j * STEP, STEP), STEP)

    def part(f, m):
        return grads.at[m, f, side]

    def source(g, f):
        return (part(f, quad), up_sum.at[f], down_in.at[f])[g]

    def flip_way(f, after):
        odd = lax.rem(f + after, 2)
        return dx + odd * (dy - dx)

    def cross(m):
        return remote(grads.at[m, :, 1 - side], mate.at[m], c_send.at[m], c_recv.at[m], partner)

    def f_copy(f, slot):
        way = flip_way(f, 0)
        member = quad + way if slot == 0 else d_quad
        return remote(part(f, member), first.at[f, slot], f_send.at[f, slot], f_recv.at[f, slot], (rep + way, shard, side))

    def s_copy(f):
        way = flip_way(f, 1)
        return remote(part(f, quad + way), second.at[f], s_send.at[f], s_recv.at[f], (rep + way, shard, side))

    def z_copy(g, k):
        return remote(
            source(g, lax.rem(shard + k, shards)), lasts[g].at[shards - k - 1],
            z_send.at[g, k - 1], z_recv.at[g, shards - k - 1], z_peers[k - 1],
        )

    def z_wait(g, k):
        remote(source(g, shard), lasts[g].at[k - 1], z_send.at[g, k - 1], z_recv.at[g, k - 1], z_peers[k - 1]).wait_recv()

    def vec_copy(src, i, peer, slot=None):
        return remote(src, vec_mate.at[i if slot is None else slot], v_send.at[i], v_recv.at[i if slot is None else slot], peer)

    def spread(g, member, send, recv, peer, half=None, core=None):
        core = side if core is None else core
        ref = fulls[g].at[core, member]
        if half is not None:
            width = ref.shape[-1] // 2
            ref = fulls[g].at[core, member, :, pl.ds(half * width, width)]
        return remote(ref, ref, send, recv, peer)

    def swirl(g):
        mine = fulls[g].at[side, quad]
        for k in range(1, shards):
            z_wait(g, k)
        add_into(mine, [source(g, shard)] + [lasts[g].at[k] for k in range(shards - 1)])
        for k in range(1, quads):
            remote(mine, rings[g].at[quads - k - 1], q_send.at[g, k - 1], q_recv.at[g, quads - k - 1], q_peers[k - 1]).start()
        for k in range(1, quads):
            remote(mine, rings[g].at[k - 1], q_send.at[g, k - 1], q_recv.at[g, k - 1], q_peers[k - 1]).wait()
        if quads > 1:
            add_into(mine, [mine] + [rings[g].at[k] for k in range(quads - 1)])
        spread(g, quad, x_send.at[g], x_recv.at[g], x_peer).start()
        spread(g, quad, y_send.at[g], y_recv.at[g], y_peer).start()
        spread(g, quad, g_send.at[g, 0], g_recv.at[g, 0], partner).start()

    def turn(g):
        spread(g, x_quad, x_send.at[g], x_recv.at[g], x_peer).wait_recv()
        spread(g, x_quad, d_send.at[g, 1], d_recv.at[g, 1], y_peer, 1).start()
        spread(g, x_quad, g_send.at[g, 1], g_recv.at[g, 1], partner).start()
        spread(g, y_quad, y_send.at[g], y_recv.at[g], y_peer).wait_recv()
        spread(g, y_quad, d_send.at[g, 0], d_recv.at[g, 0], x_peer, 0).start()
        spread(g, y_quad, g_send.at[g, 2], g_recv.at[g, 2], partner).start()

    def corner(g):
        spread(g, d_quad, d_send.at[g, 0], d_recv.at[g, 0], x_peer, 0).wait_recv()
        spread(g, d_quad, d_send.at[g, 1], d_recv.at[g, 1], y_peer, 1).wait_recv()
        spread(g, d_quad, g_send.at[g, 3], g_recv.at[g, 3], partner).start()

    def target(g, m, core):
        if g == 0:
            return qkvo_out.at[m, pl.ds(core * rows, rows), :]
        if g == 1:
            return up_out.at[pl.ds(core * rows, rows), pl.ds(m * model, model)]
        return down_out.at[pl.ds((core * 4 + m) * rows, rows), :]

    def put(g, m, core):
        return pltpu.make_async_copy(fulls[g].at[core, m], target(g, m, core), out_sem.at[g, m, core])

    def finish(g):
        for i, member in enumerate((quad, x_quad, y_quad, d_quad)):
            spread(g, member, g_send.at[g, i], g_recv.at[g, i], partner, core=1 - side).wait_recv()
        for m in range(4):
            for core in range(2):
                put(g, m, core).start()

    def each(body):
        def step(f, carry):
            body(f)
            return carry
        lax.fori_loop(0, shards, step, 0)

    def column(array):
        return jnp.sum(array.astype(wide), axis=0, keepdims=True)

    def weight_grad(m, errors):
        grads[m] = nn(turned[...], errors[...]).astype(low).reshape(shards, 2, rows, model)
        cross(m).start()

    def merge(m):
        cross(m).wait_recv()

        def step(f, carry):
            add_into(part(f, m), (part(f, m), mate.at[m, f]))

            @pl.when(m == d_quad)
            def _():
                f_copy(f, 1).start()

            @pl.when(m == quad + flip_way(f, 0))
            def _():
                f_copy(f, 0).start()
            return carry
        lax.fori_loop(0, shards, step, 0)

    def u_copy(f):
        return remote(up_in.at[1, f], up_second.at[f], u_send.at[f], u_recv.at[f], (rep + flip_way(f, 1), shard, side))
    each(lambda f: u_copy(f).start())
    for k in range(1, shards):
        z_copy(2, k).start()
    loads[2].wait()
    cross(3).start()
    loads[0].wait()

    def flip(j, carry):
        turned[:, block(j)] = normed[block(j), :].astype(wide).T.astype(low)
        return carry
    lax.fori_loop(0, steps, flip, 0)
    loads[1].wait()
    weight_grad(0, dq)
    merge(3)
    for i, (mine, theirs) in enumerate(((dk, dkx), (dv, dvx))):
        loads[3 + i].wait()
        swaps[i].wait_recv()

        def join(j, carry, mine=mine, theirs=theirs):
            mine[block(j), :] = (mine[block(j), :].astype(wide) + theirs[block(j), :].astype(wide)).astype(low)
            return carry
        lax.fori_loop(0, steps, join, 0)
        weight_grad(1 + i, mine)
        merge(i)
    merge(2)

    def up_settle(f):
        u_copy(f).wait()
        add_into(up_sum.at[f], (up_in.at[0, f], up_second.at[f]))
    each(up_settle)
    for k in range(1, shards):
        z_copy(1, k).start()
    for load in loads[5:]:
        load.wait()

    def back(j, carry):
        at = block(j)
        error = nt(dq[at, :], weights[0]) + nt(dk[at, :], weights[1]) + nt(dv[at, :], weights[2])
        values = x[at, :].astype(wide)
        centre = values - jnp.mean(values, axis=-1, keepdims=True)
        scale = lax.rsqrt(jnp.mean(centre * centre, axis=-1, keepdims=True) + norm_eps)
        unit = centre * scale
        scaled = error * vec_in[0:1, :]
        mean_one = jnp.mean(scaled, axis=-1, keepdims=True)
        mean_two = jnp.mean(scaled * unit, axis=-1, keepdims=True)
        x[at, :] = (attn[at, :].astype(wide) + scale * (scaled - mean_one - unit * mean_two)).astype(low)
        gain, bias, query, value = carry
        return gain + column(error * unit), bias + column(error), query + column(dq[at, :]), value + column(dv[at, :])
    zero = jnp.zeros((1, model), wide)
    sums = lax.fori_loop(0, steps // 2, back, (zero,) * 4)

    def fold(f):
        for slot in range(2):
            f_copy(f, slot).wait()
            member = quad if slot == 0 else quad + flip_way(f, 1)
            add_into(part(f, member), (part(f, member), first.at[f, slot]))
        s_copy(f).start()
    each(fold)
    sums = lax.fori_loop(steps // 2, steps, back, sums)
    save = pltpu.make_async_copy(x, input_out, save_sem.at[0])
    save.start()
    vec_sum[...] = small_in[...]
    for i, value in enumerate(sums):
        vec_sum[4 + i:5 + i, :] = value
    vec_copy(vec_sum, 0, partner).start()

    def settle(f):
        s_copy(f).wait()
        add_into(part(f, quad), (part(f, quad), second.at[f]))
    each(settle)
    for k in range(1, shards):
        z_copy(0, k).start()
    vec_copy(vec_sum, 0, partner).wait()
    vec_sum[...] = vec_sum[...] + vec_mate[0]
    vec_copy(vec_sum, 1, x_peer).start()
    swirl(2)
    swirl(1)
    vec_copy(vec_sum, 1, x_peer).wait()
    vec_sum[...] = vec_sum[...] + vec_mate[1]
    vec_copy(vec_sum, 2, y_peer).start()
    turn(2)
    turn(1)
    vec_copy(vec_sum, 2, y_peer).wait()
    vec_sum[...] = vec_sum[...] + vec_mate[2]
    for k in range(1, shards):
        vec_copy(vec_sum, 2 + k, z_peers[k - 1], 2 + shards - k).start()
    corner(2)
    corner(1)
    swirl(0)
    finish(2)
    finish(1)
    total = vec_sum[...]
    for k in range(1, shards):
        vec_copy(vec_sum, 2 + k, z_peers[k - 1]).wait()
        total = total + vec_mate[2 + k]
    vec_ring[0] = total
    base = 2 + shards
    for k in range(1, quads):
        remote(vec_ring.at[0], vec_ring.at[quads - k], v_send.at[base + k], v_recv.at[base + quads - k], q_peers[k - 1]).start()
    for k in range(1, quads):
        remote(vec_ring.at[0], vec_ring.at[k], v_send.at[base + k], v_recv.at[base + k], q_peers[k - 1]).wait()
        total = total + vec_ring[k]
    vec_out[...] = total
    turn(0)
    corner(0)
    finish(0)
    for g in range(GROUPS):
        for m in range(4):
            for core in range(2):
                put(g, m, core).wait()
        for k in range(1, shards):
            z_copy(g, k).wait_send()
        spread(g, quad, x_send.at[g], x_recv.at[g], x_peer).wait_send()
        spread(g, quad, y_send.at[g], y_recv.at[g], y_peer).wait_send()
        spread(g, y_quad, d_send.at[g, 0], d_recv.at[g, 0], x_peer, 0).wait_send()
        spread(g, x_quad, d_send.at[g, 1], d_recv.at[g, 1], y_peer, 1).wait_send()
        for i in range(4):
            spread(g, quad, g_send.at[g, i], g_recv.at[g, i], partner).wait_send()
    for m in range(4):
        cross(m).wait_send()
    for swap in swaps:
        swap.wait_send()
    save.wait()


def final_layer(shards, quads, dq, dk, dv, dkx, dvx, normed, x, attn, w_qkvo, d_out, up, down, vec, small):
    tokens, model = x.shape
    rows = model // shards // 2
    any_space = pl.BlockSpec(memory_space=pl.ANY)
    vmem_space = pl.BlockSpec(memory_space=pltpu.VMEM)
    dma = pltpu.SemaphoreType.DMA
    low, wide = jnp.bfloat16, jnp.float32
    piece = (rows, model)
    spare = max(quads - 1, 1)
    flat = pltpu.VMEM((tokens, model), low)
    return pl.pallas_call(
        functools.partial(final_body, shards, quads, rows),
        name="final_layer",
        out_shape=(
            jax.ShapeDtypeStruct((4, 2 * rows, model), low),
            jax.ShapeDtypeStruct((2 * rows, 4 * model), low),
            jax.ShapeDtypeStruct((8 * rows, model), low),
            jax.ShapeDtypeStruct(small.shape, wide),
            jax.ShapeDtypeStruct((tokens, model), low),
        ),
        in_specs=[any_space] * 10 + [vmem_space] * 4,
        out_specs=(any_space,) * 3 + (vmem_space, any_space),
        scratch_shapes=[flat] * 6
        + [pltpu.VMEM((model, tokens), low), flat, flat, pltpu.VMEM((3, model, model), low)]
        + [
            pltpu.VMEM((4, shards, 2) + piece, low),
            pltpu.VMEM((4, shards) + piece, low),
            pltpu.VMEM((shards, 2) + piece, low),
            pltpu.VMEM((shards,) + piece, low),
            pltpu.VMEM((shards,) + piece, low),
            pltpu.VMEM((shards,) + piece, low),
        ]
        + [pltpu.VMEM((shards - 1,) + piece, low)] * 3
        + [pltpu.VMEM((spare,) + piece, low)] * 3
        + [pltpu.VMEM((2, 4) + piece, low)] * 3
        + [
            pltpu.VMEM(small.shape, wide),
            pltpu.VMEM((2 + shards,) + small.shape, wide),
            pltpu.VMEM((quads,) + small.shape, wide),
            dma((10,)), dma((1,)), dma((2,)), dma((2,)),
            dma((4,)), dma((4,)),
            dma((shards, 2)), dma((shards, 2)),
            dma((shards,)), dma((shards,)),
            dma((GROUPS, shards - 1)), dma((GROUPS, shards - 1)),
            dma((GROUPS, spare)), dma((GROUPS, spare)), dma((shards,)), dma((shards,)),
            dma((GROUPS,)), dma((GROUPS,)), dma((GROUPS,)), dma((GROUPS,)),
            dma((GROUPS, 2)), dma((GROUPS, 2)),
            dma((GROUPS, 4)), dma((GROUPS, 4)),
            dma((GROUPS, 4, 2)),
            dma((3 + shards + quads,)), dma((3 + shards + quads,)),
        ],
        compiler_params=pltpu.CompilerParams(
            collective_id=1, has_side_effects=True, vmem_limit_bytes=62_000_000
        ),
    )(dq, dk, dv, dkx, dvx, normed, x, attn, w_qkvo, d_out, up, down, vec, small)


def on_device(
    shards, quads,
    layer_input, segment, rand_blocks, first_gain, first_bias, query_weight, query_bias,
    key_weight, value_weight, value_bias, out_weight, out_bias, second_gain, second_bias,
    up_weight, up_bias, down_weight, down_bias, cotangent,
):
    micro, _, half, model = layer_input.shape
    side = lax.axis_index("seq")
    rows = micro * half
    part = model // shards
    low, wide = jnp.bfloat16, jnp.float32
    shard = lax.axis_index("fsdp")
    rank = lax.broadcasted_iota(jnp.int32, (16, 1), 0)
    vec = jnp.zeros((16, part), low)
    for i, bias in enumerate((first_gain, first_bias, query_bias, value_bias, out_bias, second_gain, second_bias, down_bias)):
        vec = jnp.where(rank == i, bias[None, :], vec)
    vec = lax.dynamic_update_slice(jnp.zeros((16, model), low), vec, (0, shard * part))
    inside = lax.rem(shard * 4 * part, model)
    line = 8 + shard * 4 * part // model
    if 4 * part == model:
        vec = jnp.where(rank == line, up_bias[None, :], vec)
    else:
        vec = lax.dynamic_update_slice(vec, up_bias.reshape(1, 4 * part), (line, inside))
    w_qkvo, w_up, down_z, vec, normed, queries, keys, values, keys_other, values_other = gather_weights(
        shards, jnp.stack([query_weight, key_weight, value_weight, out_weight]), up_weight, down_weight, vec,
        layer_input.reshape(rows, model),
    )
    span, aug, block_bias, doc_bias = tables(segment[:, 0], rand_blocks[:, 0], side, half)

    cut = lambda array: array.reshape(micro, half, model)
    attended = (span, cut(queries), cut(keys), cut(values), cut(keys_other), cut(values_other),
                aug, block_bias, doc_bias)
    mixed, lse = attend_forward(*attended)
    mixed_rows = mixed.reshape(rows, model)
    tokens = layer_input.reshape(rows, model)
    result, grad_attn, grad_mixed, d_out, d_up, d_down, small = middle_layer(
        shards, mixed_rows, tokens, cotangent.reshape(rows, model), w_qkvo, w_up, down_weight, down_z, vec
    )
    grads = [array.reshape(rows, model) for array in attend_backward(*attended, mixed, cut(grad_mixed), lse)]
    g_qkvo, g_up, g_down, small, input_grad = final_layer(
        shards, quads, *grads, normed, tokens, grad_attn, w_qkvo,
        d_out.reshape(shards, 2, part // 2, model), d_up, d_down, vec, small,
    )
    g_qkvo, g_up, g_down = g_qkvo.astype(wide), g_up.astype(wide), g_down.astype(wide)
    flat = lax.dynamic_slice(small, (0, shard * part), (8, part))
    d_b_up = lax.dynamic_slice(small, (line, inside), (1, 4 * part)).reshape(4 * part)
    shape = layer_input.shape
    return (
        result.reshape(shape), input_grad.reshape(shape), flat[4], flat[5], g_qkvo[0], flat[6],
        g_qkvo[1], g_qkvo[2], flat[7], g_qkvo[3], flat[2], flat[0], flat[1], g_up, d_b_up, g_down, flat[3],
    )


def solution(mesh):
    row = P(None, ("rep", "fsdp"), "seq", None)
    flat, wide = P("fsdp"), P("fsdp", None)
    shards, quads = mesh.shape["fsdp"], mesh.shape["rep"] // 4
    assert mesh.shape["seq"] == 2 and mesh.shape["rep"] % 4 == 0
    return jax.shard_map(
        functools.partial(on_device, shards, quads),
        mesh=mesh,
        in_specs=(
            row, P(None, ("rep", "fsdp"), None), P(None, ("rep", "fsdp"), None, None, None),
            flat, flat, wide, flat, wide, wide, flat, wide, flat, flat, flat, wide, flat, wide, flat, row,
        ),
        out_specs=(row, row, flat, flat, wide, flat, wide, wide, flat, wide, flat, flat, flat, wide, flat, wide, flat),
        check_vma=False,
    )
```

```python
import functools
import jax
import jax.numpy as jnp
from jax import lax
from jax.experimental import pallas as pl
from jax.experimental.pallas import tpu as pltpu
from jax.sharding import PartitionSpec as P

norm_eps = 1e-05

HEADS = 12
HDIM = 64
BLOCK = 64
TQ = 256
TK = 256
NEG = -1e30


def nt(a, b):
    return lax.dot_general(a, b, (((1,), (1,)), ((), ())), preferred_element_type=jnp.float32)


def tn(a, b):
    return lax.dot_general(a, b, (((0,), (0,)), ((), ())), preferred_element_type=jnp.float32)


def nn(a, b):
    return jnp.dot(a, b, preferred_element_type=jnp.float32)


def head_lanes(head):
    lane = lax.broadcasted_iota(jnp.int32, (1, 128), 1)
    return (lane < HDIM) if head == 0 else (lane >= HDIM)


def bias_rows(block_ref, doc_ref, head):
    rows = [
        jnp.broadcast_to(block_ref[0, 0, head, pl.ds(b, 1), :], (BLOCK, 128)) for b in range(TQ // BLOCK)
    ]
    return (jnp.concatenate(rows, axis=0) + doc_ref[0]).astype(jnp.bfloat16)


def unite(whole, own_ref, other_ref, side):
    half = own_ref.shape[1]
    whole[pl.ds(pl.multiple_of(side * half, TK), half), :] = own_ref[0]
    whole[pl.ds(pl.multiple_of((1 - side) * half, TK), half), :] = other_ref[0]


def forward_body(
    span_ref, q_ref, ko_ref, vo_ref, kx_ref, vx_ref, aug_ref, block_ref, doc_ref,
    out_ref, lse_ref, acc_ref, qa_ref, k_all, v_all,
):
    micro, tile = pl.program_id(0), pl.program_id(1)

    @pl.when(tile == 0)
    def _():
        unite(k_all, ko_ref, kx_ref, span_ref[micro, tile, 2])
        unite(v_all, vo_ref, vx_ref, span_ref[micro, tile, 2])

    group = q_ref.shape[2] // HDIM
    for head in range(group):
        cols = pl.ds(head // 2 * 128, 128)
        q_rows = q_ref[0, :, cols].astype(jnp.float32) * 0.125
        masked = jnp.where(head_lanes(head % 2), q_rows, 0.0).astype(jnp.bfloat16)
        qa_ref[head, :, 0:128] = masked
        qa_ref[head, :, 128:256] = bias_rows(block_ref, doc_ref, head)
    acc_ref[...] = jnp.zeros_like(acc_ref)

    def step(j, carry):
        at = pl.ds(pl.multiple_of(j * TK, TK), TK)
        aug = aug_ref[0, at, :]
        scores = []
        for head in range(group):
            cols = pl.ds(head // 2 * 128, 128)
            scores.append(nt(jnp.concatenate([k_all[at, cols], aug], axis=1), qa_ref[head]))
        fresh = []
        probs = []
        for head in range(group):
            top_new = jnp.maximum(carry[head], jnp.max(scores[head], axis=0, keepdims=True))
            probs.append(jnp.exp(scores[head] - top_new).astype(jnp.bfloat16))
            fresh.append(top_new)
        for head in range(group):
            cols = pl.ds(head // 2 * 128, 128)
            v_rows = jnp.where(head_lanes(head % 2), v_all[at, cols], jnp.bfloat16(1.0))
            part = tn(v_rows, probs[head])
            acc_ref[head] = acc_ref[head] * jnp.exp(carry[head] - fresh[head]) + part
        return tuple(fresh)

    state = tuple(jnp.full((1, TQ), -3e38, jnp.float32) for _ in range(group))
    state = lax.fori_loop(span_ref[micro, tile, 0], span_ref[micro, tile, 1], step, state)
    for pair in range(group // 2):
        done = []
        for head in range(2):
            at = pair * 2 + head
            mass = acc_ref[at, pl.ds((1 - head) * HDIM, 1), :]
            done.append(acc_ref[at, pl.ds(head * HDIM, HDIM), :] / mass)
            lse_ref[0, pair, pl.ds(head, 1), :] = state[at] + jnp.log(mass)
        out_ref[0, :, pl.ds(pair * 128, 128)] = jnp.concatenate(done, axis=0).T.astype(out_ref.dtype)


def backward_body(
    span_ref, q_ref, ko_ref, vo_ref, kx_ref, vx_ref, aug_ref, block_ref, doc_ref,
    mixed_ref, grad_ref, lse_ref,
    dq_ref, dko_ref, dvo_ref, dkx_ref, dvx_ref,
    dqt_ref, qa_ref, gm_ref, k_acc, v_acc, k_all, v_all,
):
    micro, tile = pl.program_id(0), pl.program_id(1)
    side = span_ref[micro, tile, 2]

    @pl.when(tile == 0)
    def _():
        unite(k_all, ko_ref, kx_ref, side)
        unite(v_all, vo_ref, vx_ref, side)
        k_acc[...] = jnp.zeros_like(k_acc)
        v_acc[...] = jnp.zeros_like(v_acc)

    group = q_ref.shape[2] // HDIM
    inner = []
    for pair in range(group // 2):
        cols = pl.ds(pair * 128, 128)
        q_rows = q_ref[0, :, cols].astype(jnp.float32) * 0.125
        grad_rows = grad_ref[0, :, cols].astype(jnp.float32)
        both = (mixed_ref[0, :, cols].astype(jnp.float32) * grad_rows).T
        for half in range(2):
            head = pair * 2 + half
            qa_ref[head, :, 0:128] = jnp.where(head_lanes(half), q_rows, 0.0).astype(jnp.bfloat16)
            qa_ref[head, :, 128:256] = bias_rows(block_ref, doc_ref, head)
            gm_ref[head] = jnp.where(head_lanes(half), grad_rows, 0.0).astype(jnp.bfloat16)
            inner.append(jnp.sum(both[half * HDIM:(half + 1) * HDIM, :], axis=0, keepdims=True))
    dqt_ref[...] = jnp.zeros_like(dqt_ref)

    def step(j, carry):
        at = pl.ds(pl.multiple_of(j * TK, TK), TK)
        aug = aug_ref[0, at, :]
        for chunk in range(0, group, CHUNK):
            heads = range(chunk, min(chunk + CHUNK, group))
            scores, grads, probs, souls = {}, {}, {}, {}
            for head in heads:
                cols = pl.ds(head // 2 * 128, 128)
                scores[head] = nt(jnp.concatenate([k_all[at, cols], aug], axis=1), qa_ref[head])
                grads[head] = nt(v_all[at, cols], gm_ref[head])
            for head in heads:
                weight = jnp.exp(scores[head] - lse_ref[0, head // 2, pl.ds(head % 2, 1), :])
                souls[head] = (weight * (grads[head] - carry[head])).astype(jnp.bfloat16)
                probs[head] = weight.astype(jnp.bfloat16)
            for head in heads:
                cols = pl.ds(head // 2 * 128, 128)
                dv = nn(probs[head], gm_ref[head])
                dk = nn(souls[head], qa_ref[head, :, 0:128])
                dqt = tn(k_all[at, cols], souls[head])
                lanes = pl.ds(head * HDIM, HDIM)
                half = head % 2
                dqt_ref[lanes, :] += dqt[half * HDIM:(half + 1) * HDIM, :]
                if half == 0:
                    dv_low, dk_low = dv, dk
                else:
                    k_acc[at, cols] += dk + dk_low
                    v_acc[at, cols] += dv + dv_low
        return carry

    lax.fori_loop(span_ref[micro, tile, 0], span_ref[micro, tile, 1], step, tuple(inner))
    for pair in range(group // 2):
        cols = pl.ds(pair * 128, 128)
        dq_ref[0, :, cols] = (dqt_ref[cols, :] * 0.125).T.astype(dq_ref.dtype)

    @pl.when(tile == pl.num_programs(1) - 1)
    def _():
        size = dko_ref.shape[1]
        mine = pl.ds(pl.multiple_of(side * size, TK), size)
        theirs = pl.ds(pl.multiple_of((1 - side) * size, TK), size)
        dko_ref[0] = k_acc[mine, :].astype(dko_ref.dtype)
        dvo_ref[0] = v_acc[mine, :].astype(dvo_ref.dtype)
        dkx_ref[0] = k_acc[theirs, :].astype(dkx_ref.dtype)
        dvx_ref[0] = v_acc[theirs, :].astype(dvx_ref.dtype)


CHUNK = 4


def specs(half, length, width, at):
    rows = pl.BlockSpec((1, TQ, width), lambda *i: at(*i) + (0,))
    side = pl.BlockSpec((1, half, width), lambda *i: (at(*i)[0], 0, 0))
    aug = pl.BlockSpec((1, length, 128), lambda *i: (at(*i)[0], 0, 0))
    block = pl.BlockSpec((1, 1, HEADS, TQ // BLOCK, 128), lambda *i: at(*i) + (0, 0, 0))
    doc = pl.BlockSpec((1, TQ, 128), lambda *i: at(*i) + (0,))
    lse = pl.BlockSpec((1, HEADS // 2, 2, TQ), lambda *i: (at(*i)[0], 0, 0, at(*i)[1]))
    return rows, side, aug, block, doc, lse


def attend_forward(span, q, ko, vo, kx, vx, aug, block, doc):
    micro, half, width = q.shape
    length = aug.shape[1]
    rows, side, aug_spec, blk, doc_spec, lse = specs(half, length, width, lambda m, t, s: (m, t))
    return pl.pallas_call(
        forward_body,
        name="attend_forward",
        out_shape=(
            jax.ShapeDtypeStruct((micro, half, width), jnp.bfloat16),
            jax.ShapeDtypeStruct((micro, HEADS // 2, 2, half), jnp.float32),
        ),
        grid_spec=pltpu.PrefetchScalarGridSpec(
            num_scalar_prefetch=1,
            grid=(micro, half // TQ),
            in_specs=[rows] + [side] * 4 + [aug_spec, blk, doc_spec],
            out_specs=(rows, lse),
            scratch_shapes=[
                pltpu.VMEM((HEADS, 128, TQ), jnp.float32),
                pltpu.VMEM((HEADS, TQ, 256), jnp.bfloat16),
                pltpu.VMEM((length, width), jnp.bfloat16),
                pltpu.VMEM((length, width), jnp.bfloat16),
            ],
        ),
        cost_estimate=pl.CostEstimate(flops=20_000_000_000, bytes_accessed=20_000_000, transcendentals=0),
    )(span, q, ko, vo, kx, vx, aug, block, doc)


def attend_backward(span, q, ko, vo, kx, vx, aug, block, doc, mixed, grad, lse):
    micro, half, width = q.shape
    length = aug.shape[1]
    rows, side, aug_spec, blk, doc_spec, lse_spec = specs(half, length, width, lambda m, t, s: (m, t))
    shape = jax.ShapeDtypeStruct((micro, half, width), jnp.bfloat16)
    return pl.pallas_call(
        backward_body,
        name="attend_backward",
        out_shape=(shape,) * 5,
        grid_spec=pltpu.PrefetchScalarGridSpec(
            num_scalar_prefetch=1,
            grid=(micro, half // TQ),
            in_specs=[rows] + [side] * 4 + [aug_spec, blk, doc_spec, rows, rows, lse_spec],
            out_specs=(rows,) + (side,) * 4,
            scratch_shapes=[
                pltpu.VMEM((width, TQ), jnp.float32),
                pltpu.VMEM((HEADS, TQ, 256), jnp.bfloat16),
                pltpu.VMEM((HEADS, TQ, 128), jnp.bfloat16),
                pltpu.VMEM((length, width), jnp.float32),
                pltpu.VMEM((length, width), jnp.float32),
                pltpu.VMEM((length, width), jnp.bfloat16),
                pltpu.VMEM((length, width), jnp.bfloat16),
            ],
        ),
        cost_estimate=pl.CostEstimate(flops=20_000_000_000, bytes_accessed=20_000_000, transcendentals=0),
    )(span, q, ko, vo, kx, vx, aug, block, doc, mixed, grad, lse)


def tables(segment, rand_blocks, side, half):
    micro, length = segment.shape
    blocks = length // BLOCK
    mine = half // BLOCK
    tiles = half // TQ
    own = lax.dynamic_slice_in_dim(segment, side * half, half, axis=1)
    q_block = side * mine + lax.broadcasted_iota(jnp.int32, (1, 1, mine, 1), 2)
    k_block = lax.broadcasted_iota(jnp.int32, (1, 1, 1, 128), 3)
    chosen = lax.dynamic_slice_in_dim(rand_blocks, side * mine, mine, axis=2)
    allowed = (jnp.abs(q_block - k_block) <= 1) | (k_block == 0) | (k_block == blocks - 1)
    allowed = allowed | (q_block == 0) | (q_block == blocks - 1) | (k_block >= blocks)
    for pick in range(rand_blocks.shape[3]):
        allowed = allowed | (chosen[:, :, :, pick:pick + 1] == k_block)
    block = jnp.where(allowed, 0.0, NEG).astype(jnp.float32)
    block = jnp.moveaxis(block.reshape(micro, HEADS, tiles, mine // tiles, 128), 2, 1)
    edges = own.reshape(micro, tiles, TQ)
    first, last = edges[:, :, :1], edges[:, :, TQ - 1:]
    begin = jnp.sum((segment[:, None, :] < first).astype(jnp.int32), axis=-1)
    end = jnp.sum((segment[:, None, :] <= last).astype(jnp.int32), axis=-1)
    span = jnp.stack([begin // TK, (end + TK - 1) // TK, jnp.full_like(begin, side)], axis=-1)
    return span, block


MESH = pl.DeviceIdType.MESH
GROUPS = 3


def place():
    rep, shard, side = lax.axis_index("rep"), lax.axis_index("fsdp"), lax.axis_index("seq")
    quad = lax.rem(rep, 4)
    across, along = lax.rem(quad, 2), quad // 2
    near = (1 - 2 * across, 2 - 4 * along)
    return rep, shard, side, quad, near


def chunk(refs, group, shard, quad, side, rows, half=None):
    width = 768 if half is None else 384
    offset = 0 if half is None else half * 384
    low = side * rows
    if group == 0:
        return refs[0].at[quad, pl.ds(pl.multiple_of(shard * (2 * rows) + low, 16), rows), pl.ds(offset, width)]
    at = pl.multiple_of(shard * (2 * rows) + low, 16)
    return refs[1].at[pl.ds(at, rows), pl.ds(pl.multiple_of(quad * 768 + offset, 128), width)]


def greet(peers):
    barrier = pltpu.get_barrier_semaphore()
    for peer in peers:
        pl.semaphore_signal(barrier, inc=1, device_id=peer, device_id_type=MESH)
    pl.semaphore_wait(barrier, len(peers))


def remote(src, dst, send, recv, peer):
    return pltpu.make_async_remote_copy(
        src_ref=src, dst_ref=dst, send_sem=send, recv_sem=recv, device_id=peer, device_id_type=MESH
    )


def gather_body(
    shards, rows, q_in, k_in, v_in, o_in, up_in, down_in, vec_in, x_in, segment_in,
    qkvo_out, up_out, down_out, vec_out, aug_out, doc_out, normed_out, q_out, k_out, v_out, kx_out, vx_out,
    qkvo_stage, up_stage, vec_all, weights, normed, results, columns,
    in_sem, out_sem, z_send, z_recv, x_send, x_recv, y_send, y_recv, d_send, d_recv, c_send, c_recv,
    load_sem, save_sem, swap_send, swap_recv,
):
    rep, shard, side, quad, (dx, dy) = place()
    squares, outs = (q_in, k_in, v_in, o_in), (qkvo_out, up_out)
    x_peer, y_peer, partner = (rep + dx, shard, side), (rep + dy, shard, side), (rep, shard, 1 - side)
    z_peers = [(rep, lax.rem(shard + k, shards), side) for k in range(1, shards)]
    staged = [pltpu.make_async_copy(src, qkvo_stage.at[i], in_sem.at[i]) for i, src in enumerate(squares)]
    staged.append(pltpu.make_async_copy(up_in, up_stage, in_sem.at[4]))
    for copy in staged:
        copy.start()
    greet(z_peers + [x_peer, y_peer, partner])
    sent = []

    def go(copy):
        copy.start()
        sent.append(copy)

    def mine(g, k, src):
        return remote(
            src, chunk(outs, g, shard, quad, side, rows),
            z_send.at[g, k - 1], z_recv.at[g, shards - k - 1], z_peers[k - 1],
        )

    own_rows = pl.ds(pl.multiple_of(side * rows, 16), rows)
    for g in range(EARLY):
        for k in range(1, shards):
            if g == 1:
                go(mine(g, k, up_in.at[own_rows, pl.ds(pl.multiple_of(quad * 768, 128), 768)]))
                continue
            for member, square in enumerate(squares):
                copy = mine(g, k, square.at[own_rows, :])
                pl.when(quad == member)(copy.start)
            sent.append(copy)
        if g == 0:
            for k in range(1, shards):
                go(remote(
                    vec_in, vec_all.at[k - 1],
                    z_send.at[EARLY, k - 1], z_recv.at[EARLY, k - 1], z_peers[k - 1],
                ))
    for k in range(1, shards):
        go(remote(
            down_in.at[pl.ds(pl.multiple_of((quad * 2 + side) * rows, 16), rows), :], down_out.at[shard],
            z_send.at[EARLY + 1, k - 1], z_recv.at[EARLY + 1, shards - k - 1], z_peers[k - 1],
        ))
    owned = (
        qkvo_out.at[:, pl.ds(pl.multiple_of(shard * 2 * rows, 16), 2 * rows), :],
        up_out.at[pl.ds(pl.multiple_of(shard * 2 * rows, 16), 2 * rows), :],
    )
    local = []
    for i, stage in enumerate((qkvo_stage, up_stage)):
        for copy in (staged[:4], staged[4:])[i]:
            copy.wait()
        copy = pltpu.make_async_copy(stage, owned[i], out_sem.at[i])
        copy.start()
        local.append(copy)
    length = segment_in.shape[1]
    half = doc_out.shape[1]
    blocks = length // BLOCK
    lane = lax.broadcasted_iota(jnp.int32, (1, 128), 1)
    place_of = lax.broadcasted_iota(jnp.int32, (length, 1), 0) // BLOCK
    for m in range(segment_in.shape[0]):
        numbers = jnp.broadcast_to(segment_in[m:m + 1, :].astype(jnp.float32), (128, length))
        columns[...] = numbers.T.astype(jnp.int32)
        hit = (lane == place_of) | (lane == columns[...] + blocks)
        aug_out[m] = jnp.where(hit, 1.0, 0.0).astype(aug_out.dtype)
        own = columns[pl.ds(pl.multiple_of(side * half, TQ), half), :]
        other = (lane >= blocks) & (lane < blocks + 4) & (lane != own + blocks)
        doc_out[m] = jnp.where(other, NEG, 0.0)

    def piece(g, k, member, core, half=None):
        return chunk(outs, g, lax.rem(shard + k, shards), member, core, rows, half)

    def hop(g, k, member, core, send, recv, peer, half=None):
        ref = piece(g, k, member, core, half)
        return remote(ref, ref, send, recv, peer)

    x_quad, y_quad, d_quad = quad + dx, quad + dy, quad + dx + dy

    def straight(g):
        for k in range(1, shards):
            hop(g, k, quad, side, z_send.at[g, k - 1], z_recv.at[g, k - 1], z_peers[k - 1]).wait_recv()
            go(hop(g, k, quad, side, x_send.at[g, k - 1], x_recv.at[g, k - 1], x_peer))
            go(hop(g, k, quad, side, y_send.at[g, k - 1], y_recv.at[g, k - 1], y_peer))
            go(hop(g, k, quad, side, c_send.at[g, k - 1, 0], c_recv.at[g, k - 1, 0], partner))

    def turn(g):
        for k in range(1, shards):
            hop(g, k, x_quad, side, x_send.at[g, k - 1], x_recv.at[g, k - 1], x_peer).wait_recv()
            go(hop(g, k, x_quad, side, d_send.at[g, k - 1, 1], d_recv.at[g, k - 1, 1], y_peer, 1))
            go(hop(g, k, x_quad, side, c_send.at[g, k - 1, 1], c_recv.at[g, k - 1, 1], partner))
            hop(g, k, y_quad, side, y_send.at[g, k - 1], y_recv.at[g, k - 1], y_peer).wait_recv()
            go(hop(g, k, y_quad, side, d_send.at[g, k - 1, 0], d_recv.at[g, k - 1, 0], x_peer, 0))
            go(hop(g, k, y_quad, side, c_send.at[g, k - 1, 2], c_recv.at[g, k - 1, 2], partner))

    def corner(g):
        for k in range(1, shards):
            hop(g, k, d_quad, side, d_send.at[g, k - 1, 0], d_recv.at[g, k - 1, 0], x_peer, 0).wait_recv()
            hop(g, k, d_quad, side, d_send.at[g, k - 1, 1], d_recv.at[g, k - 1, 1], y_peer, 1).wait_recv()
            go(hop(g, k, d_quad, side, c_send.at[g, k - 1, 3], c_recv.at[g, k - 1, 3], partner))

    def gathered(g):
        for k in range(1, shards):
            for i, member in enumerate((quad, x_quad, y_quad, d_quad)):
                hop(g, k, member, 1 - side, c_send.at[g, k - 1, i], c_recv.at[g, k - 1, i], partner).wait_recv()

    def save(i, target):
        copy = pltpu.make_async_copy(normed if i == 3 else results.at[i], target, save_sem.at[i])
        copy.start()
        local.append(copy)

    def norm(step, carry):
        at = pl.ds(pl.multiple_of(step * STEP, STEP), STEP)
        values = x_in[at, :].astype(jnp.float32)
        centre = values - jnp.mean(values, axis=-1, keepdims=True)
        scale = lax.rsqrt(jnp.mean(centre * centre, axis=-1, keepdims=True) + norm_eps)
        normed[at, :] = (centre * scale * vec_out[0:1, :] + vec_out[1:2, :]).astype(normed.dtype)
        return carry

    def project(i, row):
        pltpu.make_async_copy(qkvo_out.at[i], weights.at[i], load_sem.at[i]).wait()

        def step(j, carry):
            at = pl.ds(pl.multiple_of(j * STEP, STEP), STEP)
            product = nn(normed[at, :], weights[i])
            if row is not None:
                product = product + vec_out[row:row + 1, :]
            results[i, at, :] = product.astype(results.dtype)
            return carry
        lax.fori_loop(0, normed.shape[0] // STEP, step, 0)

    def exchange(i, target):
        copy = remote(results.at[i], target, swap_send.at[i - 1], swap_recv.at[i - 1], partner)
        copy.start()
        return copy

    straight(0)
    for k in range(1, shards):
        remote(
            vec_in, vec_all.at[k - 1], z_send.at[EARLY, k - 1], z_recv.at[EARLY, k - 1], z_peers[k - 1]
        ).wait_recv()
    total = vec_in[...].astype(jnp.float32)
    for k in range(1, shards):
        total = total + vec_all[k - 1].astype(jnp.float32)
    vec_out[...] = total
    lax.fori_loop(0, normed.shape[0] // STEP // 2, norm, 0)
    turn(0)
    lax.fori_loop(normed.shape[0] // STEP // 2, normed.shape[0] // STEP, norm, 0)
    save(3, normed_out)
    straight(1)
    corner(0)
    local[0].wait()
    gathered(0)
    for i in (1, 2, 0):
        pltpu.make_async_copy(qkvo_out.at[i], weights.at[i], load_sem.at[i]).start()
    project(1, None)
    keys = exchange(1, kx_out)
    save(1, k_out)
    turn(1)
    project(2, 3)
    values = exchange(2, vx_out)
    save(2, v_out)
    corner(1)
    project(0, 2)
    save(0, q_out)
    gathered(1)
    for k in range(1, shards):
        remote(
            down_out.at[shard], down_out.at[lax.rem(shard + k, shards)],
            z_send.at[EARLY + 1, k - 1], z_recv.at[EARLY + 1, k - 1], z_peers[k - 1],
        ).wait_recv()
    keys.wait()
    values.wait()
    for copy in sent:
        copy.wait_send()
    for copy in local[1:]:
        copy.wait()


STEP = 256
EARLY = 2
ROOM = 67_000_000
WIDE = 512


def gather_weights(shards, squares, up, down, vec, x, segment):
    rows = squares[0].shape[0] // 2
    model = squares[0].shape[1]
    micro, length = segment.shape
    hidden = up.shape[1]
    any_space = pl.BlockSpec(memory_space=pl.ANY)
    vmem_space = pl.BlockSpec(memory_space=pltpu.VMEM)
    dma = pltpu.SemaphoreType.DMA
    low = jnp.bfloat16
    token = jax.ShapeDtypeStruct(x.shape, low)
    return pl.pallas_call(
        functools.partial(gather_body, shards, rows),
        name="gather_weights",
        out_shape=(
            jax.ShapeDtypeStruct((4, model, model), low),
            jax.ShapeDtypeStruct((model, hidden), low),
            jax.ShapeDtypeStruct((shards, rows, model), low),
            jax.ShapeDtypeStruct(vec.shape, jnp.float32),
            jax.ShapeDtypeStruct((micro, length, 128), low),
            jax.ShapeDtypeStruct((micro, length // 2, 128), jnp.float32),
        )
        + (token,) * 6,
        in_specs=[any_space] * 6 + [vmem_space] * 3,
        out_specs=(any_space,) * 3 + (vmem_space,) * 3 + (any_space,) * 6,
        scratch_shapes=[
            pltpu.VMEM((4, 2 * rows, model), low), pltpu.VMEM(up.shape, low),
            pltpu.VMEM((shards - 1,) + vec.shape, low),
            pltpu.VMEM((3, model, model), low),
            pltpu.VMEM(x.shape, low),
            pltpu.VMEM((3,) + x.shape, low),
            pltpu.VMEM((length, 128), jnp.int32),
            dma((5,)), dma((2,)),
            dma((EARLY + 2, shards - 1)), dma((EARLY + 2, shards - 1)),
        ]
        + [dma((EARLY, shards - 1))] * 4
        + [dma((EARLY, shards - 1, 2))] * 2
        + [dma((EARLY, shards - 1, 4))] * 2
        + [dma((3,)), dma((4,)), dma((2,)), dma((2,))],
        compiler_params=pltpu.CompilerParams(
            collective_id=0, has_side_effects=True, vmem_limit_bytes=ROOM
        ),
    )(*squares, up, down, vec, x, segment)


def add_into(out_ref, refs):
    total = refs[0][...].astype(jnp.float32)
    for ref in refs[1:]:
        total = total + ref[...].astype(jnp.float32)
    out_ref[...] = total.astype(out_ref.dtype)


def normal_parts(values):
    phi = 0.5 + 0.5 * lax.erf(values * 0.7071067811865476)
    return phi, values * (jnp.exp(-0.5 * values * values) * 0.3989422804014327)


def middle_body(
    shards, rows,
    mixed_in, x_in, grad_in, qkvo_in, up_w_in, down_w_in, down_z_in, vec_in,
    result_out, attn_out, mixed_out, d_out_out, up_out, down_out, sums_out,
    mixed, x, grad, out_w, up_w, down_w, middle, normed, turned, hidden, slope,
    up_grad, down_grad, up_mate, down_mate, up_first, down_first, down_second,
    load_sem, save_sem, uc_send, uc_recv, dc_send, dc_recv, f_send, f_recv, s_send, s_recv,
    x_send, x_recv, y_send, y_recv, d_send, d_recv, g_send, g_recv,
):
    rep, shard, side, quad, (dx, dy) = place()
    partner = (rep, shard, 1 - side)
    low, wide = jnp.bfloat16, jnp.float32
    steps = x.shape[0] // WIDE
    model = x.shape[1]
    width = 8 * rows
    loads = [
        pltpu.make_async_copy(src, dst, load_sem.at[i])
        for i, (src, dst) in enumerate(((mixed_in, mixed), (x_in, x), (qkvo_in.at[3], out_w), (grad_in, grad)))
    ]
    for f in range(shards):
        at = pl.ds(f * width, width)
        loads.append(pltpu.make_async_copy(up_w_in.at[:, at], up_w.at[f], load_sem.at[4 + f]))
    loads.append(pltpu.make_async_copy(down_w_in, down_w.at[shard], load_sem.at[4 + shards]))
    for k in range(1, shards):
        f = lax.rem(shard + k, shards)
        at = pl.ds(pl.multiple_of((quad * 2 + side) * rows, 16), rows)
        loads.append(pltpu.make_async_copy(down_z_in.at[f], down_w.at[f, at, :], load_sem.at[4 + shards + k]))
    for load in loads:
        load.start()
    x_peer, y_peer = (rep + dx, shard, side), (rep + dy, shard, side)
    x_quad, y_quad, d_quad = quad + dx, quad + dy, quad + dx + dy
    greet([x_peer, y_peer, partner])

    def piece(f, member, core, half=None):
        at = pl.ds(pl.multiple_of((member * 2 + core) * rows, 16), rows)
        if half is None:
            return down_w.at[f, at, :]
        return down_w.at[f, at, pl.ds(half * (model // 2), model // 2)]

    def hop(k, member, core, send, recv, peer, half=None):
        ref = piece(lax.rem(shard + k, shards), member, core, half)
        return remote(ref, ref, send, recv, peer)

    def own_piece(k, send, recv, peer):
        f = lax.rem(shard + k, shards)
        return remote(down_z_in.at[f], piece(f, quad, side), send, recv, peer)

    def straight(k):
        return (
            own_piece(k, x_send.at[k - 1], x_recv.at[k - 1], x_peer),
            own_piece(k, y_send.at[k - 1], y_recv.at[k - 1], y_peer),
            own_piece(k, g_send.at[k - 1, 0], g_recv.at[k - 1, 0], partner),
        )

    def turn():
        for k in range(1, shards):
            hop(k, x_quad, side, x_send.at[k - 1], x_recv.at[k - 1], x_peer).wait_recv()
            hop(k, x_quad, side, d_send.at[k - 1, 1], d_recv.at[k - 1, 1], y_peer, 1).start()
            hop(k, x_quad, side, g_send.at[k - 1, 1], g_recv.at[k - 1, 1], partner).start()
            hop(k, y_quad, side, y_send.at[k - 1], y_recv.at[k - 1], y_peer).wait_recv()
            hop(k, y_quad, side, d_send.at[k - 1, 0], d_recv.at[k - 1, 0], x_peer, 0).start()
            hop(k, y_quad, side, g_send.at[k - 1, 2], g_recv.at[k - 1, 2], partner).start()

    def corner():
        for k in range(1, shards):
            hop(k, d_quad, side, d_send.at[k - 1, 0], d_recv.at[k - 1, 0], x_peer, 0).wait_recv()
            hop(k, d_quad, side, d_send.at[k - 1, 1], d_recv.at[k - 1, 1], y_peer, 1).wait_recv()
            hop(k, d_quad, side, g_send.at[k - 1, 3], g_recv.at[k - 1, 3], partner).start()

    def gathered():
        for k in range(1, shards):
            for i, member in enumerate((quad, x_quad, y_quad, d_quad)):
                hop(k, member, 1 - side, g_send.at[k - 1, i], g_recv.at[k - 1, i], partner).wait_recv()

    def flushed():
        for k in range(1, shards):
            for copy in straight(k):
                copy.wait_send()
            hop(k, y_quad, side, d_send.at[k - 1, 0], d_recv.at[k - 1, 0], x_peer, 0).wait_send()
            hop(k, x_quad, side, d_send.at[k - 1, 1], d_recv.at[k - 1, 1], y_peer, 1).wait_send()
            for i in range(1, 4):
                hop(k, quad, side, g_send.at[k - 1, i], g_recv.at[k - 1, i], partner).wait_send()

    for k in range(1, shards):
        for copy in straight(k):
            copy.start()
    firsts = (up_first, down_first)

    def row(i):
        return vec_in[i:i + 1, :]

    def block(j):
        return pl.ds(pl.multiple_of(j * WIDE, WIDE), WIDE)

    def part(g, f, m):
        return up_grad.at[m, f, side] if g == 0 else down_grad.at[f, side, m]

    def mate(g, f, m):
        return up_mate.at[m, f] if g == 0 else down_mate.at[f, m]

    def flip_way(f, second):
        odd = lax.rem(f + second, 2)
        return dx + odd * (dy - dx)

    def up_cross(m):
        return remote(up_grad.at[m, :, 1 - side], up_mate.at[m], uc_send.at[m], uc_recv.at[m], partner)

    def down_cross(f):
        return remote(down_grad.at[f, 1 - side], down_mate.at[f], dc_send.at[f], dc_recv.at[f], partner)

    def f_copy(g, f, slot):
        way = flip_way(f, 0)
        member = quad + way if slot == 0 else quad + dx + dy
        return remote(part(g, f, member), firsts[g].at[f, slot], f_send.at[g, f, slot], f_recv.at[g, f, slot], (rep + way, shard, side))

    def s_copy(f):
        way = flip_way(f, 1)
        return remote(part(1, f, quad + way), down_second.at[f], s_send.at[f], s_recv.at[f], (rep + way, shard, side))

    def first_go(g, f, m):
        @pl.when(m == quad + dx + dy)
        def _():
            f_copy(g, f, 1).start()

        @pl.when(m == quad + flip_way(f, 0))
        def _():
            f_copy(g, f, 0).start()

    def down_merge(f):
        down_cross(f).wait_recv()
        for m in range(4):
            add_into(part(1, f, m), (part(1, f, m), mate(1, f, m)))
            first_go(1, f, m)

    def up_merge(m):
        up_cross(m).wait_recv()

        def step(f, carry):
            add_into(part(0, f, m), (part(0, f, m), mate(0, f, m)))
            first_go(0, f, m)
            return carry
        lax.fori_loop(0, shards, step, 0)

    def each(body):
        def step(f, carry):
            body(f)
            return carry
        lax.fori_loop(0, shards, step, 0)

    def down_fold(f):
        for slot in range(2):
            f_copy(1, f, slot).wait()
            member = quad if slot == 0 else quad + flip_way(f, 1)
            add_into(part(1, f, member), (part(1, f, member), down_first.at[f, slot]))
        s_copy(f).start()

    def down_settle(f):
        s_copy(f).wait()
        add_into(down_out.at[f], (part(1, f, quad), down_second.at[f]))

    def up_fold(f):
        for slot in range(2):
            f_copy(0, f, slot).wait()
            member = quad if slot == 0 else quad + flip_way(f, 1)
            add_into(up_out.at[slot, f], (part(0, f, member), up_first.at[f, slot]))

    saves = []

    def save(src, dst):
        copy = pltpu.make_async_copy(src, dst, save_sem.at[len(saves)])
        copy.start()
        saves.append(copy)

    for load in loads[:3]:
        load.wait()

    def attend_out(j, carry):
        at = block(j)
        values = x[at, :].astype(wide) + nn(mixed[at, :], out_w[...]) + row(4)
        middle[at, :] = values
        centre = values - jnp.mean(values, axis=-1, keepdims=True)
        scale = lax.rsqrt(jnp.mean(centre * centre, axis=-1, keepdims=True) + norm_eps)
        out = centre * scale * row(5) + row(6)
        normed[at, :] = out.astype(low)
        turned[:, at] = out.T.astype(low)
        return carry
    lax.fori_loop(0, steps, attend_out, 0)
    for load in loads[3:]:
        load.wait()

    def bias_at(f):
        first = f * width
        return pl.ds(8 + first // model, 1), pl.ds(pl.multiple_of(lax.rem(first, model), 128), width)

    def expand(f):
        bias = vec_in[bias_at(f)]

        def step(j, carry):
            at = block(j)
            inner = nn(normed[at, :], up_w[f]) + bias
            phi, bump = normal_parts(inner)
            hidden[f, at, :] = (inner * phi).astype(low)
            slope[f, at, :] = (phi + bump).astype(low)
            return carry
        lax.fori_loop(0, steps, step, 0)
        down_grad[f] = tn(hidden[f], grad[...]).astype(low).reshape(2, 4, rows, model)
        down_cross(f).start()

        @pl.when(f > 0)
        def _():
            down_merge(f - 1)

        @pl.when(f == 0)
        def _():
            turn()

        @pl.when(f == 1)
        def _():
            corner()
    each(expand)
    gathered()

    def contract(m):
        for h in range(model // width):
            f = m * (model // width) + h

            def step(j, total, f=f):
                at = block(j)
                value = (nt(grad[at, :], down_w[f]) * slope[f, at, :].astype(wide)).astype(low)
                slope[f, at, :] = value
                return total + jnp.sum(value.astype(wide), axis=0, keepdims=True)
            sums_out[bias_at(f)] = lax.fori_loop(0, steps, step, jnp.zeros((1, width), wide))
            product = nn(turned[...], slope[f]).astype(low)
            up_grad[m, :, :, :, pl.ds(h * width, width)] = product.reshape(shards, 2, rows, width)
        up_cross(m).start()

        @pl.when(m == 0)
        def _():
            down_merge(shards - 1)

        @pl.when(m > 0)
        def _():
            up_merge(m - 1)

    def contract_step(m, carry):
        contract(m)
        return carry
    lax.fori_loop(0, 4, contract_step, 0)
    up_merge(3)
    each(down_fold)

    def finish(j, carry):
        at = block(j)
        total = middle[at, :] + row(7)
        for f in range(shards):
            total = total + nn(hidden[f, at, :], down_w[f])
        x[at, :] = total.astype(low)
        return carry
    lax.fori_loop(0, steps, finish, 0)
    save(x, result_out)

    def back(j, carry):
        gain_sum, bias_sum, attn_sum, grad_sum = carry
        at = block(j)
        error = nt(slope[0, at, :], up_w[0])
        for f in range(1, shards):
            error = error + nt(slope[f, at, :], up_w[f])
        values = middle[at, :]
        centre = values - jnp.mean(values, axis=-1, keepdims=True)
        scale = lax.rsqrt(jnp.mean(centre * centre, axis=-1, keepdims=True) + norm_eps)
        unit = centre * scale
        scaled = error * row(5)
        mean_one = jnp.mean(scaled, axis=-1, keepdims=True)
        mean_two = jnp.mean(scaled * unit, axis=-1, keepdims=True)
        upstream = grad[at, :].astype(wide)
        attn = (upstream + scale * (scaled - mean_one - unit * mean_two)).astype(low)
        grad[at, :] = attn
        normed[at, :] = nt(attn, out_w[...]).astype(low)
        column = lambda array: jnp.sum(array, axis=0, keepdims=True)
        return (
            gain_sum + column(error * unit), bias_sum + column(error),
            attn_sum + column(attn.astype(wide)), grad_sum + column(upstream),
        )
    zero = jnp.zeros((1, model), wide)
    sums = lax.fori_loop(0, steps, back, (zero,) * 4)
    save(normed, mixed_out)
    save(grad, attn_out)
    for i, value in enumerate(sums):
        sums_out[i:i + 1, :] = value
    sums_out[4:8, :] = jnp.zeros((4, model), wide)
    sums_out[12:16, :] = jnp.zeros((4, model), wide)
    each(down_settle)
    out_w[...] = tn(mixed[...], grad[...]).astype(low)
    save(out_w, d_out_out)
    each(up_fold)
    for m in range(4):
        up_cross(m).wait_send()
    each(lambda f: down_cross(f).wait_send())
    flushed()
    for copy in saves:
        copy.wait()


def middle_layer(shards, mixed, x, grad, qkvo, up_w, down_w, down_z, vec):
    tokens, model = x.shape
    hidden = up_w.shape[1]
    rows = model // shards // 2
    width = 8 * rows
    any_space = pl.BlockSpec(memory_space=pl.ANY)
    vmem_space = pl.BlockSpec(memory_space=pltpu.VMEM)
    dma = pltpu.SemaphoreType.DMA
    low, wide = jnp.bfloat16, jnp.float32
    token = jax.ShapeDtypeStruct((tokens, model), low)
    flat = pltpu.VMEM((tokens, model), low)
    return pl.pallas_call(
        functools.partial(middle_body, shards, rows),
        name="middle_layer",
        out_shape=(
            token, token, token,
            jax.ShapeDtypeStruct((model, model), low),
            jax.ShapeDtypeStruct((2, shards, rows, model), low),
            jax.ShapeDtypeStruct((shards, rows, model), low),
            jax.ShapeDtypeStruct((16, model), wide),
        ),
        in_specs=[any_space] * 7 + [vmem_space],
        out_specs=(any_space,) * 4 + (vmem_space,) * 3,
        scratch_shapes=[
            flat, flat, flat,
            pltpu.VMEM((model, model), low),
            pltpu.VMEM((shards, model, width), low),
            pltpu.VMEM((shards, width, model), low),
            pltpu.VMEM((tokens, model), wide),
            flat,
            pltpu.VMEM((model, tokens), low),
            pltpu.VMEM((shards, tokens, width), low),
            pltpu.VMEM((shards, tokens, width), low),
            pltpu.VMEM((4, shards, 2, rows, model), low),
            pltpu.VMEM((shards, 2, 4, rows, model), low),
            pltpu.VMEM((4, shards, rows, model), low),
            pltpu.VMEM((shards, 4, rows, model), low),
            pltpu.VMEM((shards, 2, rows, model), low),
            pltpu.VMEM((shards, 2, rows, model), low),
            pltpu.VMEM((shards, rows, model), low),
            dma((4 + 2 * shards,)), dma((4,)),
            dma((4,)), dma((4,)), dma((shards,)), dma((shards,)),
            dma((2, shards, 2)), dma((2, shards, 2)), dma((shards,)), dma((shards,)),
        ]
        + [dma((shards - 1,))] * 4
        + [dma((shards - 1, 2))] * 2
        + [dma((shards - 1, 4))] * 2,
        compiler_params=pltpu.CompilerParams(
            collective_id=2, has_side_effects=True, vmem_limit_bytes=ROOM
        ),
    )(mixed, x, grad, qkvo, up_w, down_w, down_z, vec)


def final_body(
    shards, quads, rows,
    dq_in, dk_in, dv_in, dkx_in, dvx_in, normed_in, x_in, attn_in, w_in, d_out_in, up_in, down_in, vec_in, small_in,
    qkvo_out, up_out, down_out, vec_out, input_out,
    dq, dk, dv, dkx, dvx, normed, turned, x, attn, weights, grads, mate, first, second, up_sum, up_second,
    last, last_up, last_down, ring, ring_up, ring_down, full, full_up, full_down, vec_sum, vec_mate, vec_ring,
    load_sem, save_sem, w_send, w_recv, c_send, c_recv, f_send, f_recv, s_send, s_recv, z_send, z_recv, q_send, q_recv, u_send, u_recv,
    x_send, x_recv, y_send, y_recv, d_send, d_recv, g_send, g_recv, out_sem, v_send, v_recv,
):
    rep, shard, side, quad, (dx, dy) = place()
    low, wide = jnp.bfloat16, jnp.float32
    steps = x.shape[0] // STEP
    model = x.shape[1]
    x_peer, y_peer, partner = (rep + dx, shard, side), (rep + dy, shard, side), (rep, shard, 1 - side)
    x_quad, y_quad, d_quad = quad + dx, quad + dy, quad + dx + dy
    z_peers = [(rep, lax.rem(shard + k, shards), side) for k in range(1, shards)]
    q_peers = [(lax.rem(rep + 4 * k, 4 * quads), shard, side) for k in range(1, quads)]
    loads = [
        pltpu.make_async_copy(src, dst, load_sem.at[i])
        for i, (src, dst) in enumerate((
            (normed_in, normed), (dq_in, dq), (d_out_in, grads.at[3]), (dk_in, dk), (dv_in, dv),
            (w_in.at[0], weights.at[0]), (w_in.at[1], weights.at[1]), (w_in.at[2], weights.at[2]),
            (x_in, x), (attn_in, attn),
        ))
    ]
    for load in loads:
        load.start()
    greet(z_peers + q_peers + [x_peer, y_peer, partner])
    swaps = [
        remote(src, dst, w_send.at[i], w_recv.at[i], partner)
        for i, (src, dst) in enumerate(((dkx_in, dkx), (dvx_in, dvx)))
    ]
    for swap in swaps:
        swap.start()
    fulls, lasts, rings = (full, full_up, full_down), (last, last_up, last_down), (ring, ring_up, ring_down)

    def block(j):
        return pl.ds(pl.multiple_of(j * STEP, STEP), STEP)

    def part(f, m):
        return grads.at[m, f, side]

    def source(g, f):
        return (part(f, quad), up_sum.at[f], down_in.at[f])[g]

    def flip_way(f, after):
        odd = lax.rem(f + after, 2)
        return dx + odd * (dy - dx)

    def cross(m):
        return remote(grads.at[m, :, 1 - side], mate.at[m], c_send.at[m], c_recv.at[m], partner)

    def f_copy(f, slot):
        way = flip_way(f, 0)
        member = quad + way if slot == 0 else d_quad
        return remote(part(f, member), first.at[f, slot], f_send.at[f, slot], f_recv.at[f, slot], (rep + way, shard, side))

    def s_copy(f):
        way = flip_way(f, 1)
        return remote(part(f, quad + way), second.at[f], s_send.at[f], s_recv.at[f], (rep + way, shard, side))

    def z_copy(g, k):
        return remote(
            source(g, lax.rem(shard + k, shards)), lasts[g].at[shards - k - 1],
            z_send.at[g, k - 1], z_recv.at[g, shards - k - 1], z_peers[k - 1],
        )

    def z_wait(g, k):
        remote(source(g, shard), lasts[g].at[k - 1], z_send.at[g, k - 1], z_recv.at[g, k - 1], z_peers[k - 1]).wait_recv()

    def vec_copy(src, i, peer, slot=None):
        return remote(src, vec_mate.at[i if slot is None else slot], v_send.at[i], v_recv.at[i if slot is None else slot], peer)

    def spread(g, member, send, recv, peer, half=None, core=None):
        core = side if core is None else core
        ref = fulls[g].at[core, member]
        if half is not None:
            width = ref.shape[-1] // 2
            ref = fulls[g].at[core, member, :, pl.ds(half * width, width)]
        return remote(ref, ref, send, recv, peer)

    def swirl(g):
        mine = fulls[g].at[side, quad]
        for k in range(1, shards):
            z_wait(g, k)
        add_into(mine, [source(g, shard)] + [lasts[g].at[k] for k in range(shards - 1)])
        for k in range(1, quads):
            remote(mine, rings[g].at[quads - k - 1], q_send.at[g, k - 1], q_recv.at[g, quads - k - 1], q_peers[k - 1]).start()
        for k in range(1, quads):
            remote(mine, rings[g].at[k - 1], q_send.at[g, k - 1], q_recv.at[g, k - 1], q_peers[k - 1]).wait()
        if quads > 1:
            add_into(mine, [mine] + [rings[g].at[k] for k in range(quads - 1)])
        spread(g, quad, x_send.at[g], x_recv.at[g], x_peer).start()
        spread(g, quad, y_send.at[g], y_recv.at[g], y_peer).start()
        spread(g, quad, g_send.at[g, 0], g_recv.at[g, 0], partner).start()

    def turn(g):
        spread(g, x_quad, x_send.at[g], x_recv.at[g], x_peer).wait_recv()
        spread(g, x_quad, d_send.at[g, 1], d_recv.at[g, 1], y_peer, 1).start()
        spread(g, x_quad, g_send.at[g, 1], g_recv.at[g, 1], partner).start()
        spread(g, y_quad, y_send.at[g], y_recv.at[g], y_peer).wait_recv()
        spread(g, y_quad, d_send.at[g, 0], d_recv.at[g, 0], x_peer, 0).start()
        spread(g, y_quad, g_send.at[g, 2], g_recv.at[g, 2], partner).start()

    def corner(g):
        spread(g, d_quad, d_send.at[g, 0], d_recv.at[g, 0], x_peer, 0).wait_recv()
        spread(g, d_quad, d_send.at[g, 1], d_recv.at[g, 1], y_peer, 1).wait_recv()
        spread(g, d_quad, g_send.at[g, 3], g_recv.at[g, 3], partner).start()

    def target(g, m, core):
        if g == 0:
            return qkvo_out.at[m, pl.ds(core * rows, rows), :]
        if g == 1:
            return up_out.at[pl.ds(core * rows, rows), pl.ds(m * model, model)]
        return down_out.at[pl.ds((core * 4 + m) * rows, rows), :]

    def put(g, m, core):
        return pltpu.make_async_copy(fulls[g].at[core, m], target(g, m, core), out_sem.at[g, m, core])

    def finish(g):
        for i, member in enumerate((quad, x_quad, y_quad, d_quad)):
            spread(g, member, g_send.at[g, i], g_recv.at[g, i], partner, core=1 - side).wait_recv()
        for m in range(4):
            for core in range(2):
                put(g, m, core).start()

    def each(body):
        def step(f, carry):
            body(f)
            return carry
        lax.fori_loop(0, shards, step, 0)

    def column(array):
        return jnp.sum(array.astype(wide), axis=0, keepdims=True)

    def weight_grad(m, errors):
        grads[m] = nn(turned[...], errors[...]).astype(low).reshape(shards, 2, rows, model)
        cross(m).start()

    def merge(m):
        cross(m).wait_recv()

        def step(f, carry):
            add_into(part(f, m), (part(f, m), mate.at[m, f]))

            @pl.when(m == d_quad)
            def _():
                f_copy(f, 1).start()

            @pl.when(m == quad + flip_way(f, 0))
            def _():
                f_copy(f, 0).start()
            return carry
        lax.fori_loop(0, shards, step, 0)

    def u_copy(f):
        return remote(up_in.at[1, f], up_second.at[f], u_send.at[f], u_recv.at[f], (rep + flip_way(f, 1), shard, side))
    each(lambda f: u_copy(f).start())
    for k in range(1, shards):
        z_copy(2, k).start()
    loads[2].wait()
    cross(3).start()
    loads[0].wait()

    def flip(j, carry):
        turned[:, block(j)] = normed[block(j), :].astype(wide).T.astype(low)
        return carry
    lax.fori_loop(0, steps, flip, 0)
    loads[1].wait()
    weight_grad(0, dq)
    merge(3)
    for i, (mine, theirs) in enumerate(((dk, dkx), (dv, dvx))):
        loads[3 + i].wait()
        swaps[i].wait_recv()

        def join(j, carry, mine=mine, theirs=theirs):
            mine[block(j), :] = (mine[block(j), :].astype(wide) + theirs[block(j), :].astype(wide)).astype(low)
            return carry
        lax.fori_loop(0, steps, join, 0)
        weight_grad(1 + i, mine)
        merge(i)
    merge(2)

    def up_settle(f):
        u_copy(f).wait()
        add_into(up_sum.at[f], (up_in.at[0, f], up_second.at[f]))
    each(up_settle)
    for k in range(1, shards):
        z_copy(1, k).start()
    for load in loads[5:]:
        load.wait()

    def back(j, carry):
        at = block(j)
        error = nt(dq[at, :], weights[0]) + nt(dk[at, :], weights[1]) + nt(dv[at, :], weights[2])
        values = x[at, :].astype(wide)
        centre = values - jnp.mean(values, axis=-1, keepdims=True)
        scale = lax.rsqrt(jnp.mean(centre * centre, axis=-1, keepdims=True) + norm_eps)
        unit = centre * scale
        scaled = error * vec_in[0:1, :]
        mean_one = jnp.mean(scaled, axis=-1, keepdims=True)
        mean_two = jnp.mean(scaled * unit, axis=-1, keepdims=True)
        x[at, :] = (attn[at, :].astype(wide) + scale * (scaled - mean_one - unit * mean_two)).astype(low)
        gain, bias, query, value = carry
        return gain + column(error * unit), bias + column(error), query + column(dq[at, :]), value + column(dv[at, :])
    zero = jnp.zeros((1, model), wide)
    sums = lax.fori_loop(0, steps // 2, back, (zero,) * 4)

    def fold(f):
        for slot in range(2):
            f_copy(f, slot).wait()
            member = quad if slot == 0 else quad + flip_way(f, 1)
            add_into(part(f, member), (part(f, member), first.at[f, slot]))
        s_copy(f).start()
    each(fold)
    sums = lax.fori_loop(steps // 2, steps, back, sums)
    save = pltpu.make_async_copy(x, input_out, save_sem.at[0])
    save.start()
    vec_sum[...] = small_in[...]
    for i, value in enumerate(sums):
        vec_sum[4 + i:5 + i, :] = value
    vec_copy(vec_sum, 0, partner).start()

    def settle(f):
        s_copy(f).wait()
        add_into(part(f, quad), (part(f, quad), second.at[f]))
    each(settle)
    for k in range(1, shards):
        z_copy(0, k).start()
    vec_copy(vec_sum, 0, partner).wait()
    vec_sum[...] = vec_sum[...] + vec_mate[0]
    vec_copy(vec_sum, 1, x_peer).start()
    swirl(2)
    swirl(1)
    vec_copy(vec_sum, 1, x_peer).wait()
    vec_sum[...] = vec_sum[...] + vec_mate[1]
    vec_copy(vec_sum, 2, y_peer).start()
    turn(2)
    turn(1)
    vec_copy(vec_sum, 2, y_peer).wait()
    vec_sum[...] = vec_sum[...] + vec_mate[2]
    for k in range(1, shards):
        vec_copy(vec_sum, 2 + k, z_peers[k - 1], 2 + shards - k).start()
    corner(2)
    corner(1)
    swirl(0)
    finish(2)
    finish(1)
    total = vec_sum[...]
    for k in range(1, shards):
        vec_copy(vec_sum, 2 + k, z_peers[k - 1]).wait()
        total = total + vec_mate[2 + k]
    vec_ring[0] = total
    base = 2 + shards
    for k in range(1, quads):
        remote(vec_ring.at[0], vec_ring.at[quads - k], v_send.at[base + k], v_recv.at[base + quads - k], q_peers[k - 1]).start()
    for k in range(1, quads):
        remote(vec_ring.at[0], vec_ring.at[k], v_send.at[base + k], v_recv.at[base + k], q_peers[k - 1]).wait()
        total = total + vec_ring[k]
    vec_out[...] = total
    turn(0)
    corner(0)
    finish(0)
    for g in range(GROUPS):
        for m in range(4):
            for core in range(2):
                put(g, m, core).wait()
        for k in range(1, shards):
            z_copy(g, k).wait_send()
        spread(g, quad, x_send.at[g], x_recv.at[g], x_peer).wait_send()
        spread(g, quad, y_send.at[g], y_recv.at[g], y_peer).wait_send()
        spread(g, y_quad, d_send.at[g, 0], d_recv.at[g, 0], x_peer, 0).wait_send()
        spread(g, x_quad, d_send.at[g, 1], d_recv.at[g, 1], y_peer, 1).wait_send()
        for i in range(4):
            spread(g, quad, g_send.at[g, i], g_recv.at[g, i], partner).wait_send()
    for m in range(4):
        cross(m).wait_send()
    for swap in swaps:
        swap.wait_send()
    save.wait()


def final_layer(shards, quads, dq, dk, dv, dkx, dvx, normed, x, attn, w_qkvo, d_out, up, down, vec, small):
    tokens, model = x.shape
    rows = model // shards // 2
    any_space = pl.BlockSpec(memory_space=pl.ANY)
    vmem_space = pl.BlockSpec(memory_space=pltpu.VMEM)
    dma = pltpu.SemaphoreType.DMA
    low, wide = jnp.bfloat16, jnp.float32
    piece = (rows, model)
    spare = max(quads - 1, 1)
    flat = pltpu.VMEM((tokens, model), low)
    return pl.pallas_call(
        functools.partial(final_body, shards, quads, rows),
        name="final_layer",
        out_shape=(
            jax.ShapeDtypeStruct((4, 2 * rows, model), low),
            jax.ShapeDtypeStruct((2 * rows, 4 * model), low),
            jax.ShapeDtypeStruct((8 * rows, model), low),
            jax.ShapeDtypeStruct(small.shape, wide),
            jax.ShapeDtypeStruct((tokens, model), low),
        ),
        in_specs=[any_space] * 10 + [vmem_space] * 4,
        out_specs=(any_space,) * 3 + (vmem_space, any_space),
        scratch_shapes=[flat] * 6
        + [pltpu.VMEM((model, tokens), low), flat, flat, pltpu.VMEM((3, model, model), low)]
        + [
            pltpu.VMEM((4, shards, 2) + piece, low),
            pltpu.VMEM((4, shards) + piece, low),
            pltpu.VMEM((shards, 2) + piece, low),
            pltpu.VMEM((shards,) + piece, low),
            pltpu.VMEM((shards,) + piece, low),
            pltpu.VMEM((shards,) + piece, low),
        ]
        + [pltpu.VMEM((shards - 1,) + piece, low)] * 3
        + [pltpu.VMEM((spare,) + piece, low)] * 3
        + [pltpu.VMEM((2, 4) + piece, low)] * 3
        + [
            pltpu.VMEM(small.shape, wide),
            pltpu.VMEM((2 + shards,) + small.shape, wide),
            pltpu.VMEM((quads,) + small.shape, wide),
            dma((10,)), dma((1,)), dma((2,)), dma((2,)),
            dma((4,)), dma((4,)),
            dma((shards, 2)), dma((shards, 2)),
            dma((shards,)), dma((shards,)),
            dma((GROUPS, shards - 1)), dma((GROUPS, shards - 1)),
            dma((GROUPS, spare)), dma((GROUPS, spare)), dma((shards,)), dma((shards,)),
            dma((GROUPS,)), dma((GROUPS,)), dma((GROUPS,)), dma((GROUPS,)),
            dma((GROUPS, 2)), dma((GROUPS, 2)),
            dma((GROUPS, 4)), dma((GROUPS, 4)),
            dma((GROUPS, 4, 2)),
            dma((3 + shards + quads,)), dma((3 + shards + quads,)),
        ],
        compiler_params=pltpu.CompilerParams(
            collective_id=1, has_side_effects=True, vmem_limit_bytes=ROOM
        ),
    )(dq, dk, dv, dkx, dvx, normed, x, attn, w_qkvo, d_out, up, down, vec, small)


def on_device(
    shards, quads,
    layer_input, segment, rand_blocks, first_gain, first_bias, query_weight, query_bias,
    key_weight, value_weight, value_bias, out_weight, out_bias, second_gain, second_bias,
    up_weight, up_bias, down_weight, down_bias, cotangent,
):
    micro, _, half, model = layer_input.shape
    side = lax.axis_index("seq")
    rows = micro * half
    part = model // shards
    low, wide = jnp.bfloat16, jnp.float32
    shard = lax.axis_index("fsdp")
    rank = lax.broadcasted_iota(jnp.int32, (16, 1), 0)
    vec = jnp.zeros((16, part), low)
    for i, bias in enumerate((first_gain, first_bias, query_bias, value_bias, out_bias, second_gain, second_bias, down_bias)):
        vec = jnp.where(rank == i, bias[None, :], vec)
    vec = lax.dynamic_update_slice(jnp.zeros((16, model), low), vec, (0, shard * part))
    inside = lax.rem(shard * 4 * part, model)
    line = 8 + shard * 4 * part // model
    if 4 * part == model:
        vec = jnp.where(rank == line, up_bias[None, :], vec)
    else:
        vec = lax.dynamic_update_slice(vec, up_bias.reshape(1, 4 * part), (line, inside))
    w_qkvo, w_up, down_z, vec, aug, doc_bias, normed, queries, keys, values, keys_other, values_other = gather_weights(
        shards, (query_weight, key_weight, value_weight, out_weight), up_weight, down_weight, vec,
        layer_input.reshape(rows, model), segment[:, 0],
    )
    span, block_bias = tables(segment[:, 0], rand_blocks[:, 0], side, half)

    cut = lambda array: array.reshape(micro, half, model)
    attended = (span, cut(queries), cut(keys), cut(values), cut(keys_other), cut(values_other),
                aug, block_bias, doc_bias)
    mixed, lse = attend_forward(*attended)
    mixed_rows = mixed.reshape(rows, model)
    tokens = layer_input.reshape(rows, model)
    result, grad_attn, grad_mixed, d_out, d_up, d_down, small = middle_layer(
        shards, mixed_rows, tokens, cotangent.reshape(rows, model), w_qkvo, w_up, down_weight, down_z, vec
    )
    grads = [array.reshape(rows, model) for array in attend_backward(*attended, mixed, cut(grad_mixed), lse)]
    g_qkvo, g_up, g_down, small, input_grad = final_layer(
        shards, quads, *grads, normed, tokens, grad_attn, w_qkvo,
        d_out.reshape(shards, 2, part // 2, model), d_up, d_down, vec, small,
    )
    g_qkvo, g_up, g_down = g_qkvo.astype(wide), g_up.astype(wide), g_down.astype(wide)
    flat = lax.dynamic_slice(small, (0, shard * part), (8, part))
    d_b_up = lax.dynamic_slice(small, (line, inside), (1, 4 * part)).reshape(4 * part)
    shape = layer_input.shape
    return (
        result.reshape(shape), input_grad.reshape(shape), flat[4], flat[5], g_qkvo[0], flat[6],
        g_qkvo[1], g_qkvo[2], flat[7], g_qkvo[3], flat[2], flat[0], flat[1], g_up, d_b_up, g_down, flat[3],
    )


def solution(mesh):
    row = P(None, ("rep", "fsdp"), "seq", None)
    flat, wide = P("fsdp"), P("fsdp", None)
    shards, quads = mesh.shape["fsdp"], mesh.shape["rep"] // 4
    assert mesh.shape["seq"] == 2 and mesh.shape["rep"] % 4 == 0
    return jax.shard_map(
        functools.partial(on_device, shards, quads),
        mesh=mesh,
        in_specs=(
            row, P(None, ("rep", "fsdp"), None), P(None, ("rep", "fsdp"), None, None, None),
            flat, flat, wide, flat, wide, wide, flat, wide, flat, flat, flat, wide, flat, wide, flat, row,
        ),
        out_specs=(row, row, flat, flat, wide, flat, wide, wide, flat, wide, flat, flat, flat, wide, flat, wide, flat),
        check_vma=False,
    )
```

```python
import functools
import jax
import jax.numpy as jnp
from jax import lax
from jax.experimental import pallas as pl
from jax.experimental.pallas import tpu as pltpu
from jax.sharding import PartitionSpec as P

norm_eps = 1e-05

HEADS = 12
HDIM = 64
BLOCK = 64
TQ = 256
TK = 256
NEG = -1e30


def nt(a, b):
    return lax.dot_general(a, b, (((1,), (1,)), ((), ())), preferred_element_type=jnp.float32)


def tn(a, b):
    return lax.dot_general(a, b, (((0,), (0,)), ((), ())), preferred_element_type=jnp.float32)


def nn(a, b):
    return jnp.dot(a, b, preferred_element_type=jnp.float32)


def head_lanes(head):
    lane = lax.broadcasted_iota(jnp.int32, (1, 128), 1)
    return (lane < HDIM) if head == 0 else (lane >= HDIM)


def bias_rows(block_ref, doc_ref, head):
    rows = [
        jnp.broadcast_to(block_ref[0, 0, head, pl.ds(b, 1), :], (BLOCK, 128)) for b in range(TQ // BLOCK)
    ]
    return (jnp.concatenate(rows, axis=0) + doc_ref[0]).astype(jnp.bfloat16)


def unite(whole, own_ref, other_ref, side):
    half = own_ref.shape[1]
    whole[pl.ds(pl.multiple_of(side * half, TK), half), :] = own_ref[0]
    whole[pl.ds(pl.multiple_of((1 - side) * half, TK), half), :] = other_ref[0]


def forward_body(
    span_ref, q_ref, ko_ref, vo_ref, kx_ref, vx_ref, aug_ref, block_ref, doc_ref,
    out_ref, lse_ref, acc_ref, qa_ref, k_all, v_all,
):
    micro, tile = pl.program_id(0), pl.program_id(1)

    @pl.when(tile == 0)
    def _():
        unite(k_all, ko_ref, kx_ref, span_ref[micro, tile, 2])
        unite(v_all, vo_ref, vx_ref, span_ref[micro, tile, 2])

    group = q_ref.shape[2] // HDIM
    for head in range(group):
        cols = pl.ds(head // 2 * 128, 128)
        q_rows = q_ref[0, :, cols].astype(jnp.float32) * 0.125
        masked = jnp.where(head_lanes(head % 2), q_rows, 0.0).astype(jnp.bfloat16)
        qa_ref[head, :, 0:128] = masked
        qa_ref[head, :, 128:256] = bias_rows(block_ref, doc_ref, head)
    acc_ref[...] = jnp.zeros_like(acc_ref)

    def step(j, carry):
        at = pl.ds(pl.multiple_of(j * TK, TK), TK)
        aug = aug_ref[0, at, :]
        scores = []
        for head in range(group):
            cols = pl.ds(head // 2 * 128, 128)
            scores.append(nt(jnp.concatenate([k_all[at, cols], aug], axis=1), qa_ref[head]))
        fresh = []
        probs = []
        for head in range(group):
            top_new = jnp.maximum(carry[head], jnp.max(scores[head], axis=0, keepdims=True))
            probs.append(jnp.exp(scores[head] - top_new).astype(jnp.bfloat16))
            fresh.append(top_new)
        for head in range(group):
            cols = pl.ds(head // 2 * 128, 128)
            v_rows = jnp.where(head_lanes(head % 2), v_all[at, cols], jnp.bfloat16(1.0))
            part = tn(v_rows, probs[head])
            acc_ref[head] = acc_ref[head] * jnp.exp(carry[head] - fresh[head]) + part
        return tuple(fresh)

    state = tuple(jnp.full((1, TQ), -3e38, jnp.float32) for _ in range(group))
    state = lax.fori_loop(span_ref[micro, tile, 0], span_ref[micro, tile, 1], step, state)
    for pair in range(group // 2):
        done = []
        for head in range(2):
            at = pair * 2 + head
            mass = acc_ref[at, pl.ds((1 - head) * HDIM, 1), :]
            done.append(acc_ref[at, pl.ds(head * HDIM, HDIM), :] / mass)
            lse_ref[0, pair, pl.ds(head, 1), :] = state[at] + jnp.log(mass)
        out_ref[0, :, pl.ds(pair * 128, 128)] = jnp.concatenate(done, axis=0).T.astype(out_ref.dtype)


def backward_body(
    span_ref, q_ref, ko_ref, vo_ref, kx_ref, vx_ref, aug_ref, block_ref, doc_ref,
    mixed_ref, grad_ref, lse_ref,
    dq_ref, dko_ref, dvo_ref, dkx_ref, dvx_ref,
    dqt_ref, qa_ref, gm_ref, k_acc, v_acc, k_all, v_all,
):
    micro, tile = pl.program_id(0), pl.program_id(1)
    side = span_ref[micro, tile, 2]

    @pl.when(tile == 0)
    def _():
        unite(k_all, ko_ref, kx_ref, side)
        unite(v_all, vo_ref, vx_ref, side)
        k_acc[...] = jnp.zeros_like(k_acc)
        v_acc[...] = jnp.zeros_like(v_acc)

    group = q_ref.shape[2] // HDIM
    inner = []
    for pair in range(group // 2):
        cols = pl.ds(pair * 128, 128)
        q_rows = q_ref[0, :, cols].astype(jnp.float32) * 0.125
        grad_rows = grad_ref[0, :, cols].astype(jnp.float32)
        both = (mixed_ref[0, :, cols].astype(jnp.float32) * grad_rows).T
        for half in range(2):
            head = pair * 2 + half
            qa_ref[head, :, 0:128] = jnp.where(head_lanes(half), q_rows, 0.0).astype(jnp.bfloat16)
            qa_ref[head, :, 128:256] = bias_rows(block_ref, doc_ref, head)
            gm_ref[head] = jnp.where(head_lanes(half), grad_rows, 0.0).astype(jnp.bfloat16)
            inner.append(jnp.sum(both[half * HDIM:(half + 1) * HDIM, :], axis=0, keepdims=True))
    dqt_ref[...] = jnp.zeros_like(dqt_ref)

    def step(j, carry):
        at = pl.ds(pl.multiple_of(j * TK, TK), TK)
        aug = aug_ref[0, at, :]
        for chunk in range(0, group, CHUNK):
            heads = range(chunk, min(chunk + CHUNK, group))
            scores, grads, probs, souls = {}, {}, {}, {}
            for head in heads:
                cols = pl.ds(head // 2 * 128, 128)
                scores[head] = nt(jnp.concatenate([k_all[at, cols], aug], axis=1), qa_ref[head])
                grads[head] = nt(v_all[at, cols], gm_ref[head])
            for head in heads:
                weight = jnp.exp(scores[head] - lse_ref[0, head // 2, pl.ds(head % 2, 1), :])
                souls[head] = (weight * (grads[head] - carry[head])).astype(jnp.bfloat16)
                probs[head] = weight.astype(jnp.bfloat16)
            for head in heads:
                cols = pl.ds(head // 2 * 128, 128)
                dv = nn(probs[head], gm_ref[head])
                dk = nn(souls[head], qa_ref[head, :, 0:128])
                dqt = tn(k_all[at, cols], souls[head])
                lanes = pl.ds(head * HDIM, HDIM)
                half = head % 2
                dqt_ref[lanes, :] += dqt[half * HDIM:(half + 1) * HDIM, :]
                if half == 0:
                    dv_low, dk_low = dv, dk
                else:
                    k_acc[at, cols] += dk + dk_low
                    v_acc[at, cols] += dv + dv_low
        return carry

    lax.fori_loop(span_ref[micro, tile, 0], span_ref[micro, tile, 1], step, tuple(inner))
    for pair in range(group // 2):
        cols = pl.ds(pair * 128, 128)
        dq_ref[0, :, cols] = (dqt_ref[cols, :] * 0.125).T.astype(dq_ref.dtype)

    @pl.when(tile == pl.num_programs(1) - 1)
    def _():
        size = dko_ref.shape[1]
        mine = pl.ds(pl.multiple_of(side * size, TK), size)
        theirs = pl.ds(pl.multiple_of((1 - side) * size, TK), size)
        dko_ref[0] = k_acc[mine, :].astype(dko_ref.dtype)
        dvo_ref[0] = v_acc[mine, :].astype(dvo_ref.dtype)
        dkx_ref[0] = k_acc[theirs, :].astype(dkx_ref.dtype)
        dvx_ref[0] = v_acc[theirs, :].astype(dvx_ref.dtype)


CHUNK = 4


def specs(half, length, width, at):
    rows = pl.BlockSpec((1, TQ, width), lambda *i: at(*i) + (0,))
    side = pl.BlockSpec((1, half, width), lambda *i: (at(*i)[0], 0, 0))
    aug = pl.BlockSpec((1, length, 128), lambda *i: (at(*i)[0], 0, 0))
    block = pl.BlockSpec((1, 1, HEADS, TQ // BLOCK, 128), lambda *i: at(*i) + (0, 0, 0))
    doc = pl.BlockSpec((1, TQ, 128), lambda *i: at(*i) + (0,))
    lse = pl.BlockSpec((1, HEADS // 2, 2, TQ), lambda *i: (at(*i)[0], 0, 0, at(*i)[1]))
    return rows, side, aug, block, doc, lse


def attend_forward(span, q, ko, vo, kx, vx, aug, block, doc):
    micro, half, width = q.shape
    length = aug.shape[1]
    rows, side, aug_spec, blk, doc_spec, lse = specs(half, length, width, lambda m, t, s: (m, t))
    return pl.pallas_call(
        forward_body,
        name="attend_forward",
        out_shape=(
            jax.ShapeDtypeStruct((micro, half, width), jnp.bfloat16),
            jax.ShapeDtypeStruct((micro, HEADS // 2, 2, half), jnp.float32),
        ),
        grid_spec=pltpu.PrefetchScalarGridSpec(
            num_scalar_prefetch=1,
            grid=(micro, half // TQ),
            in_specs=[rows] + [side] * 4 + [aug_spec, blk, doc_spec],
            out_specs=(rows, lse),
            scratch_shapes=[
                pltpu.VMEM((HEADS, 128, TQ), jnp.float32),
                pltpu.VMEM((HEADS, TQ, 256), jnp.bfloat16),
                pltpu.VMEM((length, width), jnp.bfloat16),
                pltpu.VMEM((length, width), jnp.bfloat16),
            ],
        ),
        cost_estimate=pl.CostEstimate(flops=20_000_000_000, bytes_accessed=20_000_000, transcendentals=0),
    )(span, q, ko, vo, kx, vx, aug, block, doc)


def attend_backward(span, q, ko, vo, kx, vx, aug, block, doc, mixed, grad, lse):
    micro, half, width = q.shape
    length = aug.shape[1]
    rows, side, aug_spec, blk, doc_spec, lse_spec = specs(half, length, width, lambda m, t, s: (m, t))
    shape = jax.ShapeDtypeStruct((micro, half, width), jnp.bfloat16)
    return pl.pallas_call(
        backward_body,
        name="attend_backward",
        out_shape=(shape,) * 5,
        grid_spec=pltpu.PrefetchScalarGridSpec(
            num_scalar_prefetch=1,
            grid=(micro, half // TQ),
            in_specs=[rows] + [side] * 4 + [aug_spec, blk, doc_spec, rows, rows, lse_spec],
            out_specs=(rows,) + (side,) * 4,
            scratch_shapes=[
                pltpu.VMEM((width, TQ), jnp.float32),
                pltpu.VMEM((HEADS, TQ, 256), jnp.bfloat16),
                pltpu.VMEM((HEADS, TQ, 128), jnp.bfloat16),
                pltpu.VMEM((length, width), jnp.float32),
                pltpu.VMEM((length, width), jnp.float32),
                pltpu.VMEM((length, width), jnp.bfloat16),
                pltpu.VMEM((length, width), jnp.bfloat16),
            ],
        ),
        cost_estimate=pl.CostEstimate(flops=20_000_000_000, bytes_accessed=20_000_000, transcendentals=0),
    )(span, q, ko, vo, kx, vx, aug, block, doc, mixed, grad, lse)


def tables(segment, rand_blocks, side, half):
    micro, length = segment.shape
    blocks = length // BLOCK
    mine = half // BLOCK
    tiles = half // TQ
    own = lax.dynamic_slice_in_dim(segment, side * half, half, axis=1)
    q_block = side * mine + lax.broadcasted_iota(jnp.int32, (1, 1, mine, 1), 2)
    k_block = lax.broadcasted_iota(jnp.int32, (1, 1, 1, 128), 3)
    chosen = lax.dynamic_slice_in_dim(rand_blocks, side * mine, mine, axis=2)
    allowed = (jnp.abs(q_block - k_block) <= 1) | (k_block == 0) | (k_block == blocks - 1)
    allowed = allowed | (q_block == 0) | (q_block == blocks - 1) | (k_block >= blocks)
    for pick in range(rand_blocks.shape[3]):
        allowed = allowed | (chosen[:, :, :, pick:pick + 1] == k_block)
    block = jnp.where(allowed, 0.0, NEG).astype(jnp.float32)
    block = jnp.moveaxis(block.reshape(micro, HEADS, tiles, mine // tiles, 128), 2, 1)
    edges = own.reshape(micro, tiles, TQ)
    first, last = edges[:, :, :1], edges[:, :, TQ - 1:]
    begin = jnp.sum((segment[:, None, :] < first).astype(jnp.int32), axis=-1)
    end = jnp.sum((segment[:, None, :] <= last).astype(jnp.int32), axis=-1)
    span = jnp.stack([begin // TK, (end + TK - 1) // TK, jnp.full_like(begin, side)], axis=-1)
    return span, block


MESH = pl.DeviceIdType.MESH
GROUPS = 3


def place():
    rep, shard, side = lax.axis_index("rep"), lax.axis_index("fsdp"), lax.axis_index("seq")
    quad = lax.rem(rep, 4)
    across, along = lax.rem(quad, 2), quad // 2
    near = (1 - 2 * across, 2 - 4 * along)
    return rep, shard, side, quad, near


def chunk(refs, group, shard, quad, side, rows, half=None):
    width = 768 if half is None else 384
    offset = 0 if half is None else half * 384
    low = side * rows
    if group == 0:
        return refs[0].at[quad, pl.ds(pl.multiple_of(shard * (2 * rows) + low, 16), rows), pl.ds(offset, width)]
    at = pl.multiple_of(shard * (2 * rows) + low, 16)
    return refs[1].at[pl.ds(at, rows), pl.ds(pl.multiple_of(quad * 768 + offset, 128), width)]


def greet(peers):
    barrier = pltpu.get_barrier_semaphore()
    for peer in peers:
        pl.semaphore_signal(barrier, inc=1, device_id=peer, device_id_type=MESH)
    pl.semaphore_wait(barrier, len(peers))


def remote(src, dst, send, recv, peer):
    return pltpu.make_async_remote_copy(
        src_ref=src, dst_ref=dst, send_sem=send, recv_sem=recv, device_id=peer, device_id_type=MESH
    )


def gather_body(
    shards, rows, q_in, k_in, v_in, o_in, up_in, down_in, vec_in, x_in, segment_in,
    qkvo_out, up_out, down_out, vec_out, aug_out, doc_out, normed_out, q_out, k_out, v_out, kx_out, vx_out,
    qkvo_stage, up_stage, vec_all, weights, normed, results, columns,
    in_sem, out_sem, z_send, z_recv, x_send, x_recv, y_send, y_recv, d_send, d_recv, c_send, c_recv,
    load_sem, save_sem, swap_send, swap_recv,
):
    rep, shard, side, quad, (dx, dy) = place()
    squares, outs = (q_in, k_in, v_in, o_in), (qkvo_out, up_out)
    x_peer, y_peer, partner = (rep + dx, shard, side), (rep + dy, shard, side), (rep, shard, 1 - side)
    z_peers = [(rep, lax.rem(shard + k, shards), side) for k in range(1, shards)]
    staged = [pltpu.make_async_copy(src, qkvo_stage.at[i], in_sem.at[i]) for i, src in enumerate(squares)]
    staged.append(pltpu.make_async_copy(up_in, up_stage, in_sem.at[4]))
    for copy in staged:
        copy.start()
    greet(z_peers + [x_peer, y_peer, partner])
    sent = []

    def go(copy):
        copy.start()
        sent.append(copy)

    def mine(g, k, src):
        return remote(
            src, chunk(outs, g, shard, quad, side, rows),
            z_send.at[g, k - 1], z_recv.at[g, shards - k - 1], z_peers[k - 1],
        )

    own_rows = pl.ds(pl.multiple_of(side * rows, 16), rows)
    for g in range(EARLY):
        for k in range(1, shards):
            if g == 1:
                go(mine(g, k, up_in.at[own_rows, pl.ds(pl.multiple_of(quad * 768, 128), 768)]))
                continue
            for member, square in enumerate(squares):
                copy = mine(g, k, square.at[own_rows, :])
                pl.when(quad == member)(copy.start)
            sent.append(copy)
        if g == 0:
            for k in range(1, shards):
                go(remote(
                    vec_in, vec_all.at[k - 1],
                    z_send.at[EARLY, k - 1], z_recv.at[EARLY, k - 1], z_peers[k - 1],
                ))
    for k in range(1, shards):
        go(remote(
            down_in.at[pl.ds(pl.multiple_of((quad * 2 + side) * rows, 16), rows), :], down_out.at[shard],
            z_send.at[EARLY + 1, k - 1], z_recv.at[EARLY + 1, shards - k - 1], z_peers[k - 1],
        ))
    owned = (
        qkvo_out.at[:, pl.ds(pl.multiple_of(shard * 2 * rows, 16), 2 * rows), :],
        up_out.at[pl.ds(pl.multiple_of(shard * 2 * rows, 16), 2 * rows), :],
    )
    local = []
    for i, stage in enumerate((qkvo_stage, up_stage)):
        for copy in (staged[:4], staged[4:])[i]:
            copy.wait()
        copy = pltpu.make_async_copy(stage, owned[i], out_sem.at[i])
        copy.start()
        local.append(copy)
    length = segment_in.shape[1]
    half = doc_out.shape[1]
    blocks = length // BLOCK
    lane = lax.broadcasted_iota(jnp.int32, (1, 128), 1)
    place_of = lax.broadcasted_iota(jnp.int32, (length, 1), 0) // BLOCK
    for m in range(segment_in.shape[0]):
        numbers = jnp.broadcast_to(segment_in[m:m + 1, :].astype(jnp.float32), (128, length))
        columns[...] = numbers.T.astype(jnp.int32)
        hit = (lane == place_of) | (lane == columns[...] + blocks)
        aug_out[m] = jnp.where(hit, 1.0, 0.0).astype(aug_out.dtype)
        own = columns[pl.ds(pl.multiple_of(side * half, TQ), half), :]
        other = (lane >= blocks) & (lane < blocks + 4) & (lane != own + blocks)
        doc_out[m] = jnp.where(other, NEG, 0.0)

    def piece(g, k, member, core, half=None):
        return chunk(outs, g, lax.rem(shard + k, shards), member, core, rows, half)

    def hop(g, k, member, core, send, recv, peer, half=None):
        ref = piece(g, k, member, core, half)
        return remote(ref, ref, send, recv, peer)

    x_quad, y_quad, d_quad = quad + dx, quad + dy, quad + dx + dy

    def straight(g):
        for k in range(1, shards):
            hop(g, k, quad, side, z_send.at[g, k - 1], z_recv.at[g, k - 1], z_peers[k - 1]).wait_recv()
            go(hop(g, k, quad, side, x_send.at[g, k - 1], x_recv.at[g, k - 1], x_peer))
            go(hop(g, k, quad, side, y_send.at[g, k - 1], y_recv.at[g, k - 1], y_peer))
            go(hop(g, k, quad, side, c_send.at[g, k - 1, 0], c_recv.at[g, k - 1, 0], partner))

    def turn(g):
        for k in range(1, shards):
            hop(g, k, x_quad, side, x_send.at[g, k - 1], x_recv.at[g, k - 1], x_peer).wait_recv()
            go(hop(g, k, x_quad, side, d_send.at[g, k - 1, 1], d_recv.at[g, k - 1, 1], y_peer, 1))
            go(hop(g, k, x_quad, side, c_send.at[g, k - 1, 1], c_recv.at[g, k - 1, 1], partner))
            hop(g, k, y_quad, side, y_send.at[g, k - 1], y_recv.at[g, k - 1], y_peer).wait_recv()
            go(hop(g, k, y_quad, side, d_send.at[g, k - 1, 0], d_recv.at[g, k - 1, 0], x_peer, 0))
            go(hop(g, k, y_quad, side, c_send.at[g, k - 1, 2], c_recv.at[g, k - 1, 2], partner))

    def corner(g):
        for k in range(1, shards):
            hop(g, k, d_quad, side, d_send.at[g, k - 1, 0], d_recv.at[g, k - 1, 0], x_peer, 0).wait_recv()
            hop(g, k, d_quad, side, d_send.at[g, k - 1, 1], d_recv.at[g, k - 1, 1], y_peer, 1).wait_recv()
            go(hop(g, k, d_quad, side, c_send.at[g, k - 1, 3], c_recv.at[g, k - 1, 3], partner))

    def gathered(g):
        for k in range(1, shards):
            for i, member in enumerate((quad, x_quad, y_quad, d_quad)):
                hop(g, k, member, 1 - side, c_send.at[g, k - 1, i], c_recv.at[g, k - 1, i], partner).wait_recv()

    def save(i, target):
        copy = pltpu.make_async_copy(normed if i == 3 else results.at[i], target, save_sem.at[i])
        copy.start()
        local.append(copy)

    def norm(step, carry):
        at = pl.ds(pl.multiple_of(step * STEP, STEP), STEP)
        values = x_in[at, :].astype(jnp.float32)
        centre = values - jnp.mean(values, axis=-1, keepdims=True)
        scale = lax.rsqrt(jnp.mean(centre * centre, axis=-1, keepdims=True) + norm_eps)
        normed[at, :] = (centre * scale * vec_out[0:1, :] + vec_out[1:2, :]).astype(normed.dtype)
        return carry

    def project(i, row):
        pltpu.make_async_copy(qkvo_out.at[i], weights.at[i], load_sem.at[i]).wait()

        def step(j, carry):
            at = pl.ds(pl.multiple_of(j * STEP, STEP), STEP)
            product = nn(normed[at, :], weights[i])
            if row is not None:
                product = product + vec_out[row:row + 1, :]
            results[i, at, :] = product.astype(results.dtype)
            return carry
        lax.fori_loop(0, normed.shape[0] // STEP, step, 0)

    def exchange(i, target):
        copy = remote(results.at[i], target, swap_send.at[i - 1], swap_recv.at[i - 1], partner)
        copy.start()
        return copy

    straight(0)
    for k in range(1, shards):
        remote(
            vec_in, vec_all.at[k - 1], z_send.at[EARLY, k - 1], z_recv.at[EARLY, k - 1], z_peers[k - 1]
        ).wait_recv()
    total = vec_in[...].astype(jnp.float32)
    for k in range(1, shards):
        total = total + vec_all[k - 1].astype(jnp.float32)
    vec_out[...] = total
    lax.fori_loop(0, normed.shape[0] // STEP // 2, norm, 0)
    turn(0)
    lax.fori_loop(normed.shape[0] // STEP // 2, normed.shape[0] // STEP, norm, 0)
    save(3, normed_out)
    straight(1)
    corner(0)
    local[0].wait()
    gathered(0)
    for i in (1, 2, 0):
        pltpu.make_async_copy(qkvo_out.at[i], weights.at[i], load_sem.at[i]).start()
    project(1, None)
    keys = exchange(1, kx_out)
    save(1, k_out)
    turn(1)
    project(2, 3)
    values = exchange(2, vx_out)
    save(2, v_out)
    corner(1)
    project(0, 2)
    save(0, q_out)
    gathered(1)
    for k in range(1, shards):
        remote(
            down_out.at[shard], down_out.at[lax.rem(shard + k, shards)],
            z_send.at[EARLY + 1, k - 1], z_recv.at[EARLY + 1, k - 1], z_peers[k - 1],
        ).wait_recv()
    keys.wait()
    values.wait()
    for copy in sent:
        copy.wait_send()
    for copy in local[1:]:
        copy.wait()


STEP = 256
EARLY = 2
ROOM = 67_000_000
WIDE = 512


def gather_weights(shards, squares, up, down, vec, x, segment):
    rows = squares[0].shape[0] // 2
    model = squares[0].shape[1]
    micro, length = segment.shape
    hidden = up.shape[1]
    any_space = pl.BlockSpec(memory_space=pl.ANY)
    vmem_space = pl.BlockSpec(memory_space=pltpu.VMEM)
    dma = pltpu.SemaphoreType.DMA
    low = jnp.bfloat16
    token = jax.ShapeDtypeStruct(x.shape, low)
    return pl.pallas_call(
        functools.partial(gather_body, shards, rows),
        name="gather_weights",
        out_shape=(
            jax.ShapeDtypeStruct((4, model, model), low),
            jax.ShapeDtypeStruct((model, hidden), low),
            jax.ShapeDtypeStruct((shards, rows, model), low),
            jax.ShapeDtypeStruct(vec.shape, jnp.float32),
            jax.ShapeDtypeStruct((micro, length, 128), low),
            jax.ShapeDtypeStruct((micro, length // 2, 128), jnp.float32),
        )
        + (token,) * 6,
        in_specs=[any_space] * 6 + [vmem_space] * 3,
        out_specs=(any_space,) * 3 + (vmem_space,) * 3 + (any_space,) * 6,
        scratch_shapes=[
            pltpu.VMEM((4, 2 * rows, model), low), pltpu.VMEM(up.shape, low),
            pltpu.VMEM((shards - 1,) + vec.shape, low),
            pltpu.VMEM((3, model, model), low),
            pltpu.VMEM(x.shape, low),
            pltpu.VMEM((3,) + x.shape, low),
            pltpu.VMEM((length, 128), jnp.int32),
            dma((5,)), dma((2,)),
            dma((EARLY + 2, shards - 1)), dma((EARLY + 2, shards - 1)),
        ]
        + [dma((EARLY, shards - 1))] * 4
        + [dma((EARLY, shards - 1, 2))] * 2
        + [dma((EARLY, shards - 1, 4))] * 2
        + [dma((3,)), dma((4,)), dma((2,)), dma((2,))],
        compiler_params=pltpu.CompilerParams(
            collective_id=0, has_side_effects=True, vmem_limit_bytes=ROOM
        ),
    )(*squares, up, down, vec, x, segment)


def add_into(out_ref, refs):
    total = refs[0][...].astype(jnp.float32)
    for ref in refs[1:]:
        total = total + ref[...].astype(jnp.float32)
    out_ref[...] = total.astype(out_ref.dtype)


def normal_parts(values):
    phi = 0.5 + 0.5 * lax.erf(values * 0.7071067811865476)
    return phi, values * (jnp.exp(-0.5 * values * values) * 0.3989422804014327)


def middle_body(
    shards, rows,
    mixed_in, x_in, grad_in, qkvo_in, up_w_in, down_w_in, down_z_in, vec_in,
    result_out, attn_out, mixed_out, d_out_out, up_out, down_out, sums_out,
    mixed, x, grad, out_w, up_w, down_w, middle, normed, turned, hidden, slope,
    up_grad, down_grad, up_mate, down_mate, up_first, down_first, down_second,
    load_sem, save_sem, uc_send, uc_recv, dc_send, dc_recv, f_send, f_recv, s_send, s_recv,
    x_send, x_recv, y_send, y_recv, d_send, d_recv, g_send, g_recv,
):
    rep, shard, side, quad, (dx, dy) = place()
    partner = (rep, shard, 1 - side)
    low, wide = jnp.bfloat16, jnp.float32
    steps = x.shape[0] // WIDE
    model = x.shape[1]
    width = 8 * rows
    loads = [
        pltpu.make_async_copy(src, dst, load_sem.at[i])
        for i, (src, dst) in enumerate(((mixed_in, mixed), (x_in, x), (qkvo_in.at[3], out_w), (grad_in, grad)))
    ]
    for f in range(shards):
        at = pl.ds(f * width, width)
        loads.append(pltpu.make_async_copy(up_w_in.at[:, at], up_w.at[f], load_sem.at[4 + f]))
    loads.append(pltpu.make_async_copy(down_w_in, down_w.at[shard], load_sem.at[4 + shards]))
    for k in range(1, shards):
        f = lax.rem(shard + k, shards)
        at = pl.ds(pl.multiple_of((quad * 2 + side) * rows, 16), rows)
        loads.append(pltpu.make_async_copy(down_z_in.at[f], down_w.at[f, at, :], load_sem.at[4 + shards + k]))
    for load in loads:
        load.start()
    x_peer, y_peer = (rep + dx, shard, side), (rep + dy, shard, side)
    x_quad, y_quad, d_quad = quad + dx, quad + dy, quad + dx + dy
    greet([x_peer, y_peer, partner])

    def piece(f, member, core, half=None):
        at = pl.ds(pl.multiple_of((member * 2 + core) * rows, 16), rows)
        if half is None:
            return down_w.at[f, at, :]
        return down_w.at[f, at, pl.ds(half * (model // 2), model // 2)]

    def hop(k, member, core, send, recv, peer, half=None):
        ref = piece(lax.rem(shard + k, shards), member, core, half)
        return remote(ref, ref, send, recv, peer)

    def own_piece(k, send, recv, peer):
        f = lax.rem(shard + k, shards)
        return remote(down_z_in.at[f], piece(f, quad, side), send, recv, peer)

    def straight(k):
        return (
            own_piece(k, x_send.at[k - 1], x_recv.at[k - 1], x_peer),
            own_piece(k, y_send.at[k - 1], y_recv.at[k - 1], y_peer),
            own_piece(k, g_send.at[k - 1, 0], g_recv.at[k - 1, 0], partner),
        )

    def turn():
        for k in range(1, shards):
            hop(k, x_quad, side, x_send.at[k - 1], x_recv.at[k - 1], x_peer).wait_recv()
            hop(k, x_quad, side, d_send.at[k - 1, 1], d_recv.at[k - 1, 1], y_peer, 1).start()
            hop(k, x_quad, side, g_send.at[k - 1, 1], g_recv.at[k - 1, 1], partner).start()
            hop(k, y_quad, side, y_send.at[k - 1], y_recv.at[k - 1], y_peer).wait_recv()
            hop(k, y_quad, side, d_send.at[k - 1, 0], d_recv.at[k - 1, 0], x_peer, 0).start()
            hop(k, y_quad, side, g_send.at[k - 1, 2], g_recv.at[k - 1, 2], partner).start()

    def corner():
        for k in range(1, shards):
            hop(k, d_quad, side, d_send.at[k - 1, 0], d_recv.at[k - 1, 0], x_peer, 0).wait_recv()
            hop(k, d_quad, side, d_send.at[k - 1, 1], d_recv.at[k - 1, 1], y_peer, 1).wait_recv()
            hop(k, d_quad, side, g_send.at[k - 1, 3], g_recv.at[k - 1, 3], partner).start()

    def gathered():
        for k in range(1, shards):
            for i, member in enumerate((quad, x_quad, y_quad, d_quad)):
                hop(k, member, 1 - side, g_send.at[k - 1, i], g_recv.at[k - 1, i], partner).wait_recv()

    def flushed():
        for k in range(1, shards):
            for copy in straight(k):
                copy.wait_send()
            hop(k, y_quad, side, d_send.at[k - 1, 0], d_recv.at[k - 1, 0], x_peer, 0).wait_send()
            hop(k, x_quad, side, d_send.at[k - 1, 1], d_recv.at[k - 1, 1], y_peer, 1).wait_send()
            for i in range(1, 4):
                hop(k, quad, side, g_send.at[k - 1, i], g_recv.at[k - 1, i], partner).wait_send()

    for k in range(1, shards):
        for copy in straight(k):
            copy.start()
    firsts = (up_first, down_first)

    def row(i):
        return vec_in[i:i + 1, :]

    def block(j):
        return pl.ds(pl.multiple_of(j * WIDE, WIDE), WIDE)

    def part(g, f, m):
        return up_grad.at[m, f, side] if g == 0 else down_grad.at[f, side, m]

    def mate(g, f, m):
        return up_mate.at[m, f] if g == 0 else down_mate.at[f, m]

    def flip_way(f, second):
        odd = lax.rem(f + second, 2)
        return dx + odd * (dy - dx)

    def up_cross(m):
        return remote(up_grad.at[m, :, 1 - side], up_mate.at[m], uc_send.at[m], uc_recv.at[m], partner)

    def down_cross(f):
        return remote(down_grad.at[f, 1 - side], down_mate.at[f], dc_send.at[f], dc_recv.at[f], partner)

    def f_copy(g, f, slot):
        way = flip_way(f, 0)
        member = quad + way if slot == 0 else quad + dx + dy
        return remote(part(g, f, member), firsts[g].at[f, slot], f_send.at[g, f, slot], f_recv.at[g, f, slot], (rep + way, shard, side))

    def s_copy(f):
        way = flip_way(f, 1)
        return remote(part(1, f, quad + way), down_second.at[f], s_send.at[f], s_recv.at[f], (rep + way, shard, side))

    def first_go(g, f, m):
        @pl.when(m == quad + dx + dy)
        def _():
            f_copy(g, f, 1).start()

        @pl.when(m == quad + flip_way(f, 0))
        def _():
            f_copy(g, f, 0).start()

    def down_merge(f):
        down_cross(f).wait_recv()
        for m in range(4):
            add_into(part(1, f, m), (part(1, f, m), mate(1, f, m)))
            first_go(1, f, m)

    def up_merge(m):
        up_cross(m).wait_recv()

        def step(f, carry):
            add_into(part(0, f, m), (part(0, f, m), mate(0, f, m)))
            first_go(0, f, m)
            return carry
        lax.fori_loop(0, shards, step, 0)

    def each(body):
        def step(f, carry):
            body(f)
            return carry
        lax.fori_loop(0, shards, step, 0)

    def down_fold(f):
        for slot in range(2):
            f_copy(1, f, slot).wait()
            member = quad if slot == 0 else quad + flip_way(f, 1)
            add_into(part(1, f, member), (part(1, f, member), down_first.at[f, slot]))
        s_copy(f).start()

    def down_settle(f):
        s_copy(f).wait()
        add_into(down_out.at[f], (part(1, f, quad), down_second.at[f]))

    def up_fold(f):
        for slot in range(2):
            f_copy(0, f, slot).wait()
            member = quad if slot == 0 else quad + flip_way(f, 1)
            add_into(up_out.at[slot, f], (part(0, f, member), up_first.at[f, slot]))

    saves = []

    def save(src, dst):
        copy = pltpu.make_async_copy(src, dst, save_sem.at[len(saves)])
        copy.start()
        saves.append(copy)

    for load in loads[:3]:
        load.wait()

    def attend_out(j, carry):
        at = block(j)
        values = x[at, :].astype(wide) + nn(mixed[at, :], out_w[...]) + row(4)
        middle[at, :] = values
        centre = values - jnp.mean(values, axis=-1, keepdims=True)
        scale = lax.rsqrt(jnp.mean(centre * centre, axis=-1, keepdims=True) + norm_eps)
        out = centre * scale * row(5) + row(6)
        normed[at, :] = out.astype(low)
        turned[:, at] = out.T.astype(low)
        return carry
    lax.fori_loop(0, steps, attend_out, 0)
    for load in loads[3:]:
        load.wait()

    def bias_at(f):
        first = f * width
        return pl.ds(8 + first // model, 1), pl.ds(pl.multiple_of(lax.rem(first, model), 128), width)

    def expand(f):
        bias = vec_in[bias_at(f)]

        def step(j, carry):
            at = block(j)
            inner = nn(normed[at, :], up_w[f]) + bias
            phi, bump = normal_parts(inner)
            hidden[f, at, :] = (inner * phi).astype(low)
            slope[f, at, :] = (phi + bump).astype(low)
            return carry
        lax.fori_loop(0, steps, step, 0)
        down_grad[f] = tn(hidden[f], grad[...]).astype(low).reshape(2, 4, rows, model)
        down_cross(f).start()

        @pl.when(f > 0)
        def _():
            down_merge(f - 1)

        @pl.when(f == 0)
        def _():
            turn()

        @pl.when(f == 1)
        def _():
            corner()
    each(expand)
    gathered()

    def contract(m):
        for h in range(model // width):
            f = m * (model // width) + h

            def step(j, total, f=f):
                at = block(j)
                value = (nt(grad[at, :], down_w[f]) * slope[f, at, :].astype(wide)).astype(low)
                slope[f, at, :] = value
                return total + jnp.sum(value.astype(wide), axis=0, keepdims=True)
            sums_out[bias_at(f)] = lax.fori_loop(0, steps, step, jnp.zeros((1, width), wide))
            product = nn(turned[...], slope[f]).astype(low)
            up_grad[m, :, :, :, pl.ds(h * width, width)] = product.reshape(shards, 2, rows, width)
        up_cross(m).start()

        @pl.when(m == 0)
        def _():
            down_merge(shards - 1)

        @pl.when(m > 0)
        def _():
            up_merge(m - 1)

    def contract_step(m, carry):
        contract(m)
        return carry
    lax.fori_loop(0, 4, contract_step, 0)
    up_merge(3)
    each(down_fold)

    def finish(j, carry):
        at = block(j)
        total = middle[at, :] + row(7)
        for f in range(shards):
            total = total + nn(hidden[f, at, :], down_w[f])
        x[at, :] = total.astype(low)
        return carry
    lax.fori_loop(0, steps, finish, 0)
    save(x, result_out)

    def back(j, carry):
        gain_sum, bias_sum, attn_sum, grad_sum = carry
        at = block(j)
        error = nt(slope[0, at, :], up_w[0])
        for f in range(1, shards):
            error = error + nt(slope[f, at, :], up_w[f])
        values = middle[at, :]
        centre = values - jnp.mean(values, axis=-1, keepdims=True)
        scale = lax.rsqrt(jnp.mean(centre * centre, axis=-1, keepdims=True) + norm_eps)
        unit = centre * scale
        scaled = error * row(5)
        mean_one = jnp.mean(scaled, axis=-1, keepdims=True)
        mean_two = jnp.mean(scaled * unit, axis=-1, keepdims=True)
        upstream = grad[at, :].astype(wide)
        attn = (upstream + scale * (scaled - mean_one - unit * mean_two)).astype(low)
        grad[at, :] = attn
        normed[at, :] = nt(attn, out_w[...]).astype(low)
        column = lambda array: jnp.sum(array, axis=0, keepdims=True)
        return (
            gain_sum + column(error * unit), bias_sum + column(error),
            attn_sum + column(attn.astype(wide)), grad_sum + column(upstream),
        )
    zero = jnp.zeros((1, model), wide)
    sums = lax.fori_loop(0, steps, back, (zero,) * 4)
    save(normed, mixed_out)
    save(grad, attn_out)
    for i, value in enumerate(sums):
        sums_out[i:i + 1, :] = value
    sums_out[4:8, :] = jnp.zeros((4, model), wide)
    sums_out[12:16, :] = jnp.zeros((4, model), wide)
    each(down_settle)
    out_w[...] = tn(mixed[...], grad[...]).astype(low)
    save(out_w, d_out_out)
    each(up_fold)
    for m in range(4):
        up_cross(m).wait_send()
    each(lambda f: down_cross(f).wait_send())
    flushed()
    for copy in saves:
        copy.wait()


def middle_layer(shards, mixed, x, grad, qkvo, up_w, down_w, down_z, vec):
    tokens, model = x.shape
    hidden = up_w.shape[1]
    rows = model // shards // 2
    width = 8 * rows
    any_space = pl.BlockSpec(memory_space=pl.ANY)
    vmem_space = pl.BlockSpec(memory_space=pltpu.VMEM)
    dma = pltpu.SemaphoreType.DMA
    low, wide = jnp.bfloat16, jnp.float32
    token = jax.ShapeDtypeStruct((tokens, model), low)
    flat = pltpu.VMEM((tokens, model), low)
    return pl.pallas_call(
        functools.partial(middle_body, shards, rows),
        name="middle_layer",
        out_shape=(
            token, token, token,
            jax.ShapeDtypeStruct((model, model), low),
            jax.ShapeDtypeStruct((2, shards, rows, model), low),
            jax.ShapeDtypeStruct((shards, rows, model), low),
            jax.ShapeDtypeStruct((16, model), wide),
        ),
        in_specs=[any_space] * 7 + [vmem_space],
        out_specs=(any_space,) * 4 + (vmem_space,) * 3,
        scratch_shapes=[
            flat, flat, flat,
            pltpu.VMEM((model, model), low),
            pltpu.VMEM((shards, model, width), low),
            pltpu.VMEM((shards, width, model), low),
            pltpu.VMEM((tokens, model), wide),
            flat,
            pltpu.VMEM((model, tokens), low),
            pltpu.VMEM((shards, tokens, width), low),
            pltpu.VMEM((shards, tokens, width), low),
            pltpu.VMEM((4, shards, 2, rows, model), low),
            pltpu.VMEM((shards, 2, 4, rows, model), low),
            pltpu.VMEM((4, shards, rows, model), low),
            pltpu.VMEM((shards, 4, rows, model), low),
            pltpu.VMEM((shards, 2, rows, model), low),
            pltpu.VMEM((shards, 2, rows, model), low),
            pltpu.VMEM((shards, rows, model), low),
            dma((4 + 2 * shards,)), dma((4,)),
            dma((4,)), dma((4,)), dma((shards,)), dma((shards,)),
            dma((2, shards, 2)), dma((2, shards, 2)), dma((shards,)), dma((shards,)),
        ]
        + [dma((shards - 1,))] * 4
        + [dma((shards - 1, 2))] * 2
        + [dma((shards - 1, 4))] * 2,
        compiler_params=pltpu.CompilerParams(
            collective_id=2, has_side_effects=True, vmem_limit_bytes=ROOM
        ),
    )(mixed, x, grad, qkvo, up_w, down_w, down_z, vec)


def final_body(
    shards, quads, rows,
    dq_in, dk_in, dv_in, dkx_in, dvx_in, normed_in, x_in, attn_in, w_in, d_out_in, up_in, down_in, vec_in, small_in,
    qkvo_out, up_out, down_out, vec_out, input_out,
    dq, dk, dv, dkx, dvx, normed, turned, x, attn, weights, grads, mate, first, second, up_sum, up_second,
    last, last_up, last_down, ring, ring_up, ring_down, full, full_up, full_down, vec_sum, vec_mate, vec_ring,
    load_sem, save_sem, w_send, w_recv, c_send, c_recv, f_send, f_recv, s_send, s_recv, z_send, z_recv, q_send, q_recv, u_send, u_recv,
    x_send, x_recv, y_send, y_recv, d_send, d_recv, g_send, g_recv, out_sem, v_send, v_recv,
):
    rep, shard, side, quad, (dx, dy) = place()
    low, wide = jnp.bfloat16, jnp.float32
    steps = x.shape[0] // STEP
    model = x.shape[1]
    x_peer, y_peer, partner = (rep + dx, shard, side), (rep + dy, shard, side), (rep, shard, 1 - side)
    x_quad, y_quad, d_quad = quad + dx, quad + dy, quad + dx + dy
    z_peers = [(rep, lax.rem(shard + k, shards), side) for k in range(1, shards)]
    q_peers = [(lax.rem(rep + 4 * k, 4 * quads), shard, side) for k in range(1, quads)]
    loads = [
        pltpu.make_async_copy(src, dst, load_sem.at[i])
        for i, (src, dst) in enumerate((
            (normed_in, normed), (dq_in, dq), (d_out_in, grads.at[3]), (dk_in, dk), (dv_in, dv),
            (w_in.at[0], weights.at[0]), (w_in.at[1], weights.at[1]), (w_in.at[2], weights.at[2]),
            (x_in, x), (attn_in, attn),
        ))
    ]
    for load in loads:
        load.start()
    greet(z_peers + q_peers + [x_peer, y_peer, partner])
    swaps = [
        remote(src, dst, w_send.at[i], w_recv.at[i], partner)
        for i, (src, dst) in enumerate(((dkx_in, dkx), (dvx_in, dvx)))
    ]
    for swap in swaps:
        swap.start()
    fulls, lasts, rings = (full, full_up, full_down), (last, last_up, last_down), (ring, ring_up, ring_down)

    def block(j):
        return pl.ds(pl.multiple_of(j * STEP, STEP), STEP)

    def part(f, m):
        return grads.at[m, f, side]

    def source(g, f):
        return (part(f, quad), up_sum.at[f], down_in.at[f])[g]

    def flip_way(f, after):
        odd = lax.rem(f + after, 2)
        return dx + odd * (dy - dx)

    def cross(m):
        return remote(grads.at[m, :, 1 - side], mate.at[m], c_send.at[m], c_recv.at[m], partner)

    def f_copy(f, slot):
        way = flip_way(f, 0)
        member = quad + way if slot == 0 else d_quad
        return remote(part(f, member), first.at[f, slot], f_send.at[f, slot], f_recv.at[f, slot], (rep + way, shard, side))

    def s_copy(f):
        way = flip_way(f, 1)
        return remote(part(f, quad + way), second.at[f], s_send.at[f], s_recv.at[f], (rep + way, shard, side))

    def z_copy(g, k):
        return remote(
            source(g, lax.rem(shard + k, shards)), lasts[g].at[shards - k - 1],
            z_send.at[g, k - 1], z_recv.at[g, shards - k - 1], z_peers[k - 1],
        )

    def z_wait(g, k):
        remote(source(g, shard), lasts[g].at[k - 1], z_send.at[g, k - 1], z_recv.at[g, k - 1], z_peers[k - 1]).wait_recv()

    def vec_copy(src, i, peer, slot=None):
        return remote(src, vec_mate.at[i if slot is None else slot], v_send.at[i], v_recv.at[i if slot is None else slot], peer)

    def spread(g, member, send, recv, peer, half=None, core=None):
        core = side if core is None else core
        ref = fulls[g].at[core, member]
        if half is not None:
            width = ref.shape[-1] // 2
            ref = fulls[g].at[core, member, :, pl.ds(half * width, width)]
        return remote(ref, ref, send, recv, peer)

    def swirl(g):
        mine = fulls[g].at[side, quad]
        for k in range(1, shards):
            z_wait(g, k)
        add_into(mine, [source(g, shard)] + [lasts[g].at[k] for k in range(shards - 1)])
        for k in range(1, quads):
            remote(mine, rings[g].at[quads - k - 1], q_send.at[g, k - 1], q_recv.at[g, quads - k - 1], q_peers[k - 1]).start()
        for k in range(1, quads):
            remote(mine, rings[g].at[k - 1], q_send.at[g, k - 1], q_recv.at[g, k - 1], q_peers[k - 1]).wait()
        if quads > 1:
            add_into(mine, [mine] + [rings[g].at[k] for k in range(quads - 1)])
        spread(g, quad, x_send.at[g], x_recv.at[g], x_peer).start()
        spread(g, quad, y_send.at[g], y_recv.at[g], y_peer).start()
        spread(g, quad, g_send.at[g, 0], g_recv.at[g, 0], partner).start()

    def turn(g):
        spread(g, x_quad, x_send.at[g], x_recv.at[g], x_peer).wait_recv()
        spread(g, x_quad, d_send.at[g, 1], d_recv.at[g, 1], y_peer, 1).start()
        spread(g, x_quad, g_send.at[g, 1], g_recv.at[g, 1], partner).start()
        spread(g, y_quad, y_send.at[g], y_recv.at[g], y_peer).wait_recv()
        spread(g, y_quad, d_send.at[g, 0], d_recv.at[g, 0], x_peer, 0).start()
        spread(g, y_quad, g_send.at[g, 2], g_recv.at[g, 2], partner).start()

    def corner(g):
        spread(g, d_quad, d_send.at[g, 0], d_recv.at[g, 0], x_peer, 0).wait_recv()
        spread(g, d_quad, d_send.at[g, 1], d_recv.at[g, 1], y_peer, 1).wait_recv()
        spread(g, d_quad, g_send.at[g, 3], g_recv.at[g, 3], partner).start()

    def target(g, m, core):
        if g == 0:
            return qkvo_out.at[m, pl.ds(core * rows, rows), :]
        if g == 1:
            return up_out.at[pl.ds(core * rows, rows), pl.ds(m * model, model)]
        return down_out.at[pl.ds((core * 4 + m) * rows, rows), :]

    def put(g, m, core):
        return pltpu.make_async_copy(fulls[g].at[core, m], target(g, m, core), out_sem.at[g, m, core])

    def finish(g):
        for i, member in enumerate((quad, x_quad, y_quad, d_quad)):
            spread(g, member, g_send.at[g, i], g_recv.at[g, i], partner, core=1 - side).wait_recv()
        for m in range(4):
            for core in range(2):
                put(g, m, core).start()

    def each(body):
        def step(f, carry):
            body(f)
            return carry
        lax.fori_loop(0, shards, step, 0)

    def column(array):
        return jnp.sum(array.astype(wide), axis=0, keepdims=True)

    def weight_grad(m, errors):
        grads[m] = nn(turned[...], errors[...]).astype(low).reshape(shards, 2, rows, model)
        cross(m).start()

    def merge(m):
        cross(m).wait_recv()

        def step(f, carry):
            add_into(part(f, m), (part(f, m), mate.at[m, f]))

            @pl.when(m == d_quad)
            def _():
                f_copy(f, 1).start()

            @pl.when(m == quad + flip_way(f, 0))
            def _():
                f_copy(f, 0).start()
            return carry
        lax.fori_loop(0, shards, step, 0)

    def u_copy(f):
        return remote(up_in.at[1, f], up_second.at[f], u_send.at[f], u_recv.at[f], (rep + flip_way(f, 1), shard, side))
    each(lambda f: u_copy(f).start())
    for k in range(1, shards):
        z_copy(2, k).start()
    loads[2].wait()
    cross(3).start()
    loads[0].wait()

    def flip(j, carry):
        turned[:, block(j)] = normed[block(j), :].astype(wide).T.astype(low)
        return carry
    lax.fori_loop(0, steps, flip, 0)
    loads[1].wait()
    weight_grad(0, dq)
    merge(3)
    for i, (mine, theirs) in enumerate(((dk, dkx), (dv, dvx))):
        loads[3 + i].wait()
        swaps[i].wait_recv()

        def join(j, carry, mine=mine, theirs=theirs):
            mine[block(j), :] = (mine[block(j), :].astype(wide) + theirs[block(j), :].astype(wide)).astype(low)
            return carry
        lax.fori_loop(0, steps, join, 0)
        weight_grad(1 + i, mine)
        merge(i)
    merge(2)

    def up_settle(f):
        u_copy(f).wait()
        add_into(up_sum.at[f], (up_in.at[0, f], up_second.at[f]))
    each(up_settle)
    for k in range(1, shards):
        z_copy(1, k).start()
    for load in loads[5:]:
        load.wait()

    def back(j, carry):
        at = block(j)
        error = nt(dq[at, :], weights[0]) + nt(dk[at, :], weights[1]) + nt(dv[at, :], weights[2])
        values = x[at, :].astype(wide)
        centre = values - jnp.mean(values, axis=-1, keepdims=True)
        scale = lax.rsqrt(jnp.mean(centre * centre, axis=-1, keepdims=True) + norm_eps)
        unit = centre * scale
        scaled = error * vec_in[0:1, :]
        mean_one = jnp.mean(scaled, axis=-1, keepdims=True)
        mean_two = jnp.mean(scaled * unit, axis=-1, keepdims=True)
        x[at, :] = (attn[at, :].astype(wide) + scale * (scaled - mean_one - unit * mean_two)).astype(low)
        gain, bias, query, value = carry
        return gain + column(error * unit), bias + column(error), query + column(dq[at, :]), value + column(dv[at, :])
    zero = jnp.zeros((1, model), wide)
    sums = lax.fori_loop(0, steps // 2, back, (zero,) * 4)

    def fold(f):
        for slot in range(2):
            f_copy(f, slot).wait()
            member = quad if slot == 0 else quad + flip_way(f, 1)
            add_into(part(f, member), (part(f, member), first.at[f, slot]))
        s_copy(f).start()
    each(fold)
    swirl(2)
    sums = lax.fori_loop(steps // 2, steps, back, sums)
    save = pltpu.make_async_copy(x, input_out, save_sem.at[0])
    save.start()
    vec_sum[...] = small_in[...]
    for i, value in enumerate(sums):
        vec_sum[4 + i:5 + i, :] = value
    vec_copy(vec_sum, 0, partner).start()

    def settle(f):
        s_copy(f).wait()
        add_into(part(f, quad), (part(f, quad), second.at[f]))
    each(settle)
    for k in range(1, shards):
        z_copy(0, k).start()
    vec_copy(vec_sum, 0, partner).wait()
    vec_sum[...] = vec_sum[...] + vec_mate[0]
    vec_copy(vec_sum, 1, x_peer).start()
    swirl(1)
    vec_copy(vec_sum, 1, x_peer).wait()
    vec_sum[...] = vec_sum[...] + vec_mate[1]
    vec_copy(vec_sum, 2, y_peer).start()
    turn(2)
    turn(1)
    vec_copy(vec_sum, 2, y_peer).wait()
    vec_sum[...] = vec_sum[...] + vec_mate[2]
    for k in range(1, shards):
        vec_copy(vec_sum, 2 + k, z_peers[k - 1], 2 + shards - k).start()
    corner(2)
    corner(1)
    swirl(0)
    finish(2)
    finish(1)
    total = vec_sum[...]
    for k in range(1, shards):
        vec_copy(vec_sum, 2 + k, z_peers[k - 1]).wait()
        total = total + vec_mate[2 + k]
    vec_ring[0] = total
    base = 2 + shards
    for k in range(1, quads):
        remote(vec_ring.at[0], vec_ring.at[quads - k], v_send.at[base + k], v_recv.at[base + quads - k], q_peers[k - 1]).start()
    for k in range(1, quads):
        remote(vec_ring.at[0], vec_ring.at[k], v_send.at[base + k], v_recv.at[base + k], q_peers[k - 1]).wait()
        total = total + vec_ring[k]
    vec_out[...] = total
    turn(0)
    corner(0)
    finish(0)
    for g in range(GROUPS):
        for m in range(4):
            for core in range(2):
                put(g, m, core).wait()
        for k in range(1, shards):
            z_copy(g, k).wait_send()
        spread(g, quad, x_send.at[g], x_recv.at[g], x_peer).wait_send()
        spread(g, quad, y_send.at[g], y_recv.at[g], y_peer).wait_send()
        spread(g, y_quad, d_send.at[g, 0], d_recv.at[g, 0], x_peer, 0).wait_send()
        spread(g, x_quad, d_send.at[g, 1], d_recv.at[g, 1], y_peer, 1).wait_send()
        for i in range(4):
            spread(g, quad, g_send.at[g, i], g_recv.at[g, i], partner).wait_send()
    for m in range(4):
        cross(m).wait_send()
    for swap in swaps:
        swap.wait_send()
    save.wait()


def final_layer(shards, quads, dq, dk, dv, dkx, dvx, normed, x, attn, w_qkvo, d_out, up, down, vec, small):
    tokens, model = x.shape
    rows = model // shards // 2
    any_space = pl.BlockSpec(memory_space=pl.ANY)
    vmem_space = pl.BlockSpec(memory_space=pltpu.VMEM)
    dma = pltpu.SemaphoreType.DMA
    low, wide = jnp.bfloat16, jnp.float32
    piece = (rows, model)
    spare = max(quads - 1, 1)
    flat = pltpu.VMEM((tokens, model), low)
    return pl.pallas_call(
        functools.partial(final_body, shards, quads, rows),
        name="final_layer",
        out_shape=(
            jax.ShapeDtypeStruct((4, 2 * rows, model), low),
            jax.ShapeDtypeStruct((2 * rows, 4 * model), low),
            jax.ShapeDtypeStruct((8 * rows, model), low),
            jax.ShapeDtypeStruct(small.shape, wide),
            jax.ShapeDtypeStruct((tokens, model), low),
        ),
        in_specs=[any_space] * 10 + [vmem_space] * 4,
        out_specs=(any_space,) * 3 + (vmem_space, any_space),
        scratch_shapes=[flat] * 6
        + [pltpu.VMEM((model, tokens), low), flat, flat, pltpu.VMEM((3, model, model), low)]
        + [
            pltpu.VMEM((4, shards, 2) + piece, low),
            pltpu.VMEM((4, shards) + piece, low),
            pltpu.VMEM((shards, 2) + piece, low),
            pltpu.VMEM((shards,) + piece, low),
            pltpu.VMEM((shards,) + piece, low),
            pltpu.VMEM((shards,) + piece, low),
        ]
        + [pltpu.VMEM((shards - 1,) + piece, low)] * 3
        + [pltpu.VMEM((spare,) + piece, low)] * 3
        + [pltpu.VMEM((2, 4) + piece, low)] * 3
        + [
            pltpu.VMEM(small.shape, wide),
            pltpu.VMEM((2 + shards,) + small.shape, wide),
            pltpu.VMEM((quads,) + small.shape, wide),
            dma((10,)), dma((1,)), dma((2,)), dma((2,)),
            dma((4,)), dma((4,)),
            dma((shards, 2)), dma((shards, 2)),
            dma((shards,)), dma((shards,)),
            dma((GROUPS, shards - 1)), dma((GROUPS, shards - 1)),
            dma((GROUPS, spare)), dma((GROUPS, spare)), dma((shards,)), dma((shards,)),
            dma((GROUPS,)), dma((GROUPS,)), dma((GROUPS,)), dma((GROUPS,)),
            dma((GROUPS, 2)), dma((GROUPS, 2)),
            dma((GROUPS, 4)), dma((GROUPS, 4)),
            dma((GROUPS, 4, 2)),
            dma((3 + shards + quads,)), dma((3 + shards + quads,)),
        ],
        compiler_params=pltpu.CompilerParams(
            collective_id=1, has_side_effects=True, vmem_limit_bytes=ROOM
        ),
    )(dq, dk, dv, dkx, dvx, normed, x, attn, w_qkvo, d_out, up, down, vec, small)


def on_device(
    shards, quads,
    layer_input, segment, rand_blocks, first_gain, first_bias, query_weight, query_bias,
    key_weight, value_weight, value_bias, out_weight, out_bias, second_gain, second_bias,
    up_weight, up_bias, down_weight, down_bias, cotangent,
):
    micro, _, half, model = layer_input.shape
    side = lax.axis_index("seq")
    rows = micro * half
    part = model // shards
    low, wide = jnp.bfloat16, jnp.float32
    shard = lax.axis_index("fsdp")
    rank = lax.broadcasted_iota(jnp.int32, (16, 1), 0)
    vec = jnp.zeros((16, part), low)
    for i, bias in enumerate((first_gain, first_bias, query_bias, value_bias, out_bias, second_gain, second_bias, down_bias)):
        vec = jnp.where(rank == i, bias[None, :], vec)
    vec = lax.dynamic_update_slice(jnp.zeros((16, model), low), vec, (0, shard * part))
    inside = lax.rem(shard * 4 * part, model)
    line = 8 + shard * 4 * part // model
    if 4 * part == model:
        vec = jnp.where(rank == line, up_bias[None, :], vec)
    else:
        vec = lax.dynamic_update_slice(vec, up_bias.reshape(1, 4 * part), (line, inside))
    w_qkvo, w_up, down_z, vec, aug, doc_bias, normed, queries, keys, values, keys_other, values_other = gather_weights(
        shards, (query_weight, key_weight, value_weight, out_weight), up_weight, down_weight, vec,
        layer_input.reshape(rows, model), segment[:, 0],
    )
    span, block_bias = tables(segment[:, 0], rand_blocks[:, 0], side, half)

    cut = lambda array: array.reshape(micro, half, model)
    attended = (span, cut(queries), cut(keys), cut(values), cut(keys_other), cut(values_other),
                aug, block_bias, doc_bias)
    mixed, lse = attend_forward(*attended)
    mixed_rows = mixed.reshape(rows, model)
    tokens = layer_input.reshape(rows, model)
    result, grad_attn, grad_mixed, d_out, d_up, d_down, small = middle_layer(
        shards, mixed_rows, tokens, cotangent.reshape(rows, model), w_qkvo, w_up, down_weight, down_z, vec
    )
    grads = [array.reshape(rows, model) for array in attend_backward(*attended, mixed, cut(grad_mixed), lse)]
    g_qkvo, g_up, g_down, small, input_grad = final_layer(
        shards, quads, *grads, normed, tokens, grad_attn, w_qkvo,
        d_out.reshape(shards, 2, part // 2, model), d_up, d_down, vec, small,
    )
    g_qkvo, g_up, g_down = g_qkvo.astype(wide), g_up.astype(wide), g_down.astype(wide)
    flat = lax.dynamic_slice(small, (0, shard * part), (8, part))
    d_b_up = lax.dynamic_slice(small, (line, inside), (1, 4 * part)).reshape(4 * part)
    shape = layer_input.shape
    return (
        result.reshape(shape), input_grad.reshape(shape), flat[4], flat[5], g_qkvo[0], flat[6],
        g_qkvo[1], g_qkvo[2], flat[7], g_qkvo[3], flat[2], flat[0], flat[1], g_up, d_b_up, g_down, flat[3],
    )


def solution(mesh):
    row = P(None, ("rep", "fsdp"), "seq", None)
    flat, wide = P("fsdp"), P("fsdp", None)
    shards, quads = mesh.shape["fsdp"], mesh.shape["rep"] // 4
    assert mesh.shape["seq"] == 2 and mesh.shape["rep"] % 4 == 0
    return jax.shard_map(
        functools.partial(on_device, shards, quads),
        mesh=mesh,
        in_specs=(
            row, P(None, ("rep", "fsdp"), None), P(None, ("rep", "fsdp"), None, None, None),
            flat, flat, wide, flat, wide, wide, flat, wide, flat, flat, flat, wide, flat, wide, flat, row,
        ),
        out_specs=(row, row, flat, flat, wide, flat, wide, wide, flat, wide, flat, flat, flat, wide, flat, wide, flat),
        check_vma=False,
    )
```
